32 devices in a mesh: dp: 2 (over x), context: 4 (over z), experts: 4 (over y, core).
Axes of the slice: x: 2, y: 2, z: 4, core: 2. Of those that a mesh axis runs over, the one named last changes fastest.
Arguments:
- tokens: bfloat16 [2, 1024, 2048], P('dp', 'context'), may hold values from -6 to 6
- positions: int32 [2, 1024], P('dp', 'context'), may hold values from 0 to 1023
- routes: int32 [2, 1024, 4], P('dp', 'context'), may hold values from 0 to 7, all different within a row; in each aligned block of 64 rows (0 to 63, 64 to 127, ..., all dimensions but the last counted through in order) at most 48 rows name the same one
- out_grad: bfloat16 [2, 1024, 2048], P('dp', 'context'), may hold values from -6 to 6
- norm1_gain: bfloat16 [2048], replicated, may hold values from 0.25 to 1.75
- qkv_weight: bfloat16 [2048, 3, 2048], P(('dp', 'context'), None, 'experts'), may hold values from -0.125 to 0.125
- qkv_bias: bfloat16 [3, 2048], P(None, 'experts'), may hold values from -0.59765625 to 0.59765625
- out_weight: bfloat16 [2048, 2048], P('experts', ('dp', 'context')), may hold values from -0.5 to 0.5
- norm2_gain: bfloat16 [2048], replicated, may hold values from 0.25 to 1.75
- router_weight: bfloat16 [2048, 8], replicated, may hold values from -0.25 to 0.25
- expert_gate: bfloat16 [8, 2048, 1408], P('experts', ('dp', 'context')), may hold values from -0.125 to 0.125
- expert_up: bfloat16 [8, 2048, 1408], P('experts', ('dp', 'context')), may hold values from -0.125 to 0.125
- expert_down: bfloat16 [8, 1408, 2048], P('experts', None, ('dp', 'context')), may hold values from -0.3125 to 0.3125
- shared_gate: bfloat16 [2048], replicated, may hold values from -0.125 to 0.125
- shared_w_gate: bfloat16 [2048, 5632], P(('dp', 'context'), 'experts'), may hold values from -0.125 to 0.125
- shared_w_up: bfloat16 [2048, 5632], P(('dp', 'context'), 'experts'), may hold values from -0.125 to 0.125
- shared_w_down: bfloat16 [5632, 2048], P('experts', ('dp', 'context')), may hold values from -0.15625 to 0.15625
Outputs:
- block_out: bfloat16 [2, 1024, 2048], P('dp', 'context')
- tokens_grad: float32 [2, 1024, 2048], P('dp', 'context')
- norm1_gain_grad: float32 [2048], replicated
- qkv_weight_grad: float32 [2048, 3, 2048], P(('dp', 'context'), None, 'experts')
- qkv_bias_grad: float32 [3, 2048], P(None, 'experts')
- out_weight_grad: float32 [2048, 2048], P('experts', ('dp', 'context'))
- norm2_gain_grad: float32 [2048], replicated
- router_weight_grad: float32 [2048, 8], replicated
- expert_gate_grad: float32 [8, 2048, 1408], P('experts', ('dp', 'context'))
- expert_up_grad: float32 [8, 2048, 1408], P('experts', ('dp', 'context'))
- expert_down_grad: float32 [8, 1408, 2048], P('experts', None, ('dp', 'context'))
- shared_gate_grad: float32 [2048], replicated
- shared_w_gate_grad: float32 [2048, 5632], P(('dp', 'context'), 'experts')
- shared_w_up_grad: float32 [2048, 5632], P(('dp', 'context'), 'experts')
- shared_w_down_grad: float32 [5632, 2048], P('experts', ('dp', 'context'))
The draws below stay inside these ranges and needn't reach their ends.
Inputs may be any that keep to these rules, and one draw needn't show every extreme that they name: `routes`: in each aligned block of 64 rows of the flattened sequences and positions, no expert is named by more than 48 rows, a bound that some block reaches.
All inputs are finite; a program needn't handle non-finite values.
Results may differ from the reference program's by a relative error of at most 0.025.
Values may be sent and summed in bfloat16 or wider, within the bound.
A program may use at most 320 MiB of HBM per device.

```python
import math
import jax
import jax.numpy as jnp
import numpy as np
from jax import lax

D = 2048
HEADS = 16
HEAD_DIM = 128
FFE = 1408
SFF = 5632
TOP = 4
NUM_EXP = 8
SEQ = 1024
BATCH = 2
QROWS = 64
CAP = 48


def set_ends(values, key, low, high):
    longest = values.shape.index(max(values.shape))
    spots = []
    for shift in (0, 1):
        where = [jax.random.randint(jax.random.fold_in(key, axis), (), 0, length) for axis, length in enumerate(values.shape)]
        where[longest] = (where[longest] + shift) % values.shape[longest]
        spots.append(tuple(where))
    return values.at[spots[0]].set(low).at[spots[1]].set(high)


def steps_of(stream_key, extent, cuts, least, largest):
    def one(axis_at, blocks):
        heights = jax.random.uniform(jax.random.fold_in(jax.random.fold_in(stream_key, 6), axis_at), (blocks,), jnp.float32, least / len(cuts), largest / len(cuts))
        return jnp.repeat(jnp.exp(heights), extent[axis_at] // blocks).reshape((-1,) + (1,) * (len(extent) - axis_at - 1))

    level = one(*cuts[0])
    for cut in cuts[1:]:
        level = level * one(*cut)
    return level


def routed_block(stream_key, own, number, rows, count, top, most, slope):
    ranking = jax.random.permutation(stream_key, count)
    packed, ordinary = shares(count, rows * top, most, slope, True), shares(count, rows * top, most, slope, False)
    places = jnp.arange(count)

    def named(sizes, turn):
        used = int((sizes > 0).sum())
        fixed = max(1, used // 4)
        passed = fixed + (places - fixed + turn * (used - fixed)) % max(1, count - fixed)
        return jnp.zeros((count,), jnp.int32).at[ranking[jnp.where(places < fixed, places, passed)]].set(jnp.asarray(sizes, jnp.int32))

    sizes = jnp.where(number % 4 == 0, named(packed, number // 4), named(ordinary, number - number // 4 - 1))
    mixed = jax.random.permutation(jax.random.fold_in(own, 3), count)
    source_of, receiver = mixed[0:count // 2 * 2:2], mixed[1:count // 2 * 2:2]
    slack = jnp.minimum(sizes[source_of] - 1, most - sizes[receiver]) // 2
    slack = jnp.where((source_of == ranking[0]) | (receiver == ranking[0]) | (sizes[receiver] == 0), 0, jnp.maximum(slack, 0))
    passed = jax.random.randint(jax.random.fold_in(own, 4), (count // 2,), 0, 1 << 20) % (slack + 1)
    sizes = sizes.at[source_of].add(-passed).at[receiver].add(passed)
    items = jnp.searchsorted(jnp.cumsum(sizes), jnp.arange(rows * top), side="right").astype(jnp.int32)
    grid = items.reshape(top, rows).T
    grid = grid[jax.random.permutation(jax.random.fold_in(own, 1), rows)]
    turn = jax.random.randint(jax.random.fold_in(own, 2), (rows, 1), 0, top)
    return jnp.take_along_axis(grid, (jnp.arange(top)[None, :] + turn) % top, axis=1)


def shares(number_of, total, limit, skew, full):
    portions = [(1 << 20) // math.isqrt(grade ** skew) + 1 for grade in range(1, number_of + 1)]
    largest = limit if full else min(limit, max(-(-total // number_of), total * portions[0] // sum(portions)))
    least = 1 if total - largest >= number_of - 1 else 0
    holding, surplus = [largest] + [least] * (number_of - 1), total - largest - least * (number_of - 1)
    while surplus > 0:
        candidates = [i for i in range(1, number_of) if holding[i] < largest] or [i for i in range(1, number_of) if holding[i] < limit]
        mass, budget = sum([portions[i] for i in candidates]), surplus
        for i in candidates:
            more = min(limit - holding[i], max(1, budget * portions[i] // mass), surplus)
            holding[i] = holding[i] + more
            surplus = surplus - more
    return np.array(holding)


def centred(rng, extent, deviation, bound, shards=(), kind=jnp.bfloat16):
    drawn = jax.random.normal(rng, extent, jnp.float32) * deviation
    if len(shards) > 0:
        drawn = steps_of(rng, extent, shards, -0.22, 0.18) * drawn
    return jnp.clip(drawn, min=-bound, max=bound).astype(kind)


def setup_inputs(seed: int = 0) -> dict:
    keys = jax.random.split(jax.random.key(seed), 18)
    tokens = centred(keys[0], (BATCH, SEQ, D), 1.0, 6.0, ((0, 2), (1, 4)))
    positions = set_ends(jax.random.randint(keys[1], (BATCH, SEQ), 0, SEQ), jax.random.fold_in(keys[1], 1), 0, SEQ - 1).astype(jnp.int32)
    routes_keys = jax.random.split(jax.random.fold_in(keys[2], 1), BATCH * SEQ // QROWS)
    routes_turns = jax.random.permutation(jax.random.fold_in(keys[2], 3), BATCH * SEQ // QROWS)
    routes = jax.vmap(lambda own, number: routed_block(jax.random.fold_in(keys[2], 2), own, number, QROWS, NUM_EXP, TOP, CAP, 1))(routes_keys, routes_turns).reshape((BATCH, SEQ, TOP))
    out_grad = centred(keys[3], (BATCH, SEQ, D), 1.0, 6.0, ((0, 2), (1, 4)))
    norm1_gain = jnp.clip(1.0 + 0.15 * jax.random.normal(keys[4], (D,), jnp.float32), 0.25, 1.75).astype(jnp.bfloat16)
    qkv_weight = centred(keys[5], (D, 3, HEADS * HEAD_DIM), D ** -0.5, 0.125, ((0, 8), (2, 4)))
    qkv_bias = jnp.clip(jax.random.uniform(keys[6], (3, HEADS * HEAD_DIM), jnp.float32, -0.59765625, 0.59765625) * steps_of(keys[6], (3, HEADS * HEAD_DIM), ((1, 4),), -0.4, 0.0), -0.59765625, 0.59765625).astype(jnp.bfloat16)
    out_weight = centred(keys[7], (HEADS * HEAD_DIM, D), (HEADS * HEAD_DIM // 16) ** -0.5, 0.5, ((0, 4), (1, 8)))
    norm2_gain = jnp.clip(1.0 + 0.15 * jax.random.normal(keys[8], (D,), jnp.float32), 0.25, 1.75).astype(jnp.bfloat16)
    router_weight = centred(keys[9], (D, NUM_EXP), (D // 4) ** -0.5, 0.25)
    expert_gate = centred(keys[10], (NUM_EXP, D, FFE), D ** -0.5, 0.125, ((0, 4), (1, 8)))
    expert_up = centred(keys[11], (NUM_EXP, D, FFE), D ** -0.5, 0.125, ((0, 4), (1, 8)))
    expert_down = centred(keys[12], (NUM_EXP, FFE, D), (FFE // 4) ** -0.5, 0.3125, ((0, 4), (2, 8)))
    shared_gate = centred(keys[13], (D,), D ** -0.5, 0.125)
    shared_w_gate = centred(keys[14], (D, SFF), D ** -0.5, 0.125, ((0, 8), (1, 4)))
    shared_w_up = centred(keys[15], (D, SFF), D ** -0.5, 0.125, ((0, 8), (1, 4)))
    shared_w_down = centred(keys[16], (SFF, D), (SFF // 4) ** -0.5, 0.15625, ((0, 4), (1, 8)))
    return {"tokens": tokens, "positions": positions, "routes": routes, "out_grad": out_grad, "norm1_gain": norm1_gain, "qkv_weight": qkv_weight, "qkv_bias": qkv_bias, "out_weight": out_weight, "norm2_gain": norm2_gain, "router_weight": router_weight, "expert_gate": expert_gate, "expert_up": expert_up, "expert_down": expert_down, "shared_gate": shared_gate, "shared_w_gate": shared_w_gate, "shared_w_up": shared_w_up, "shared_w_down": shared_w_down}


EPSILON = 1e-06
ROPE_BASE = 1000000.0
MASKED = -1e+30
PRECISE = lax.Precision.HIGHEST

def rounded(value):
    return lax.optimization_barrier(value.astype(jnp.bfloat16)).astype(jnp.float32)

def rope_tables(position_ids):
    half_dim = HEAD_DIM // 2
    inverse = ROPE_BASE ** (-2.0 * jnp.arange(half_dim, dtype=jnp.float32) / HEAD_DIM)
    angles = position_ids.astype(jnp.float32)[:, None] * inverse[None, :]
    cosine = jnp.cos(angles)
    sine_part = jnp.sin(angles)
    return (jnp.concatenate([cosine, cosine], -1)[:, None, :], jnp.concatenate([sine_part, sine_part], -1)[:, None, :])

def rotate(value):
    half_dim = value.shape[-1] // 2
    return jnp.concatenate([-value[..., half_dim:], value[..., :half_dim]], -1)

def rotate_back(value):
    half_dim = value.shape[-1] // 2
    return jnp.concatenate([value[..., half_dim:], -value[..., :half_dim]], -1)

def silu_grad(gate_vals):
    sigmoid_vals = jax.nn.sigmoid(gate_vals)
    return sigmoid_vals * (1.0 + gate_vals * (1.0 - sigmoid_vals))

def block_rank(route_rows, expert_count):
    hits = (route_rows[:, :, None] == jnp.arange(expert_count, dtype=jnp.int32)[None, None, :]).astype(jnp.int32)
    flat_hits = hits.reshape(-1, expert_count)
    earlier = jnp.cumsum(flat_hits, axis=0) - flat_hits
    return lax.optimization_barrier(jnp.sum(earlier * flat_hits, -1)).reshape(route_rows.shape).astype(jnp.int32)

def attention_forward(query, key_rows, value_rows):
    scale = HEAD_DIM ** (-0.5)
    block_width = min(512, SEQ)
    key_index = jnp.arange(SEQ, dtype=jnp.int32)
    key_float = key_rows.astype(jnp.float32)
    value_float = value_rows.astype(jnp.float32)

    def one_block(carry, block_id):
        query_block = lax.dynamic_slice_in_dim(query, block_id * block_width, block_width, 0).astype(jnp.float32)
        scores = jnp.einsum('qhd,khd->hqk', query_block, key_float) * scale
        query_index = block_id * block_width + jnp.arange(block_width, dtype=jnp.int32)
        allowed = key_index[None, None, :] <= query_index[None, :, None]
        row_max = lax.optimization_barrier(jnp.max(jnp.where(allowed, scores, MASKED), -1))
        weights = jnp.where(allowed, jnp.exp(scores - row_max[..., None]), 0.0)
        row_sum = lax.optimization_barrier(jnp.sum(weights, -1))
        mixed = jnp.einsum('hqk,khd->qhd', rounded(weights), value_float)
        attended = (mixed / jnp.transpose(row_sum)[:, :, None]).astype(jnp.bfloat16)
        return (carry, (attended, jnp.transpose(row_max + jnp.log(row_sum))))
    _, (attended, log_sums) = lax.scan(one_block, 0, jnp.arange(SEQ // block_width, dtype=jnp.int32))
    return (attended.reshape(SEQ, HEADS, HEAD_DIM), log_sums.reshape(SEQ, HEADS))

def attention_backward(query, key_rows, value_rows, log_sums, delta, dattended):
    scale = HEAD_DIM ** (-0.5)
    block_width = min(512, SEQ)
    key_index = jnp.arange(SEQ, dtype=jnp.int32)
    key_float = key_rows.astype(jnp.float32)
    value_float = value_rows.astype(jnp.float32)

    def one_block(carry, block_id):
        dkey_sum, dvalue_sum = carry
        start_row = block_id * block_width
        query_block = lax.dynamic_slice_in_dim(query, start_row, block_width, 0).astype(jnp.float32)
        dout_block = lax.dynamic_slice_in_dim(dattended, start_row, block_width, 0).astype(jnp.float32)
        lse_block = lax.dynamic_slice_in_dim(log_sums, start_row, block_width, 0)
        delta_block = lax.dynamic_slice_in_dim(delta, start_row, block_width, 0)
        scores = jnp.einsum('qhd,khd->hqk', query_block, key_float) * scale
        query_index = start_row + jnp.arange(block_width, dtype=jnp.int32)
        allowed = key_index[None, None, :] <= query_index[None, :, None]
        prob_att = jnp.where(allowed, jnp.exp(scores - jnp.transpose(lse_block)[:, :, None]), 0.0)
        dvalue_sum = dvalue_sum + jnp.einsum('hqk,qhd->khd', rounded(prob_att), dout_block)
        dprob = jnp.einsum('qhd,khd->hqk', dout_block, value_float)
        dscore = rounded(prob_att * (dprob - jnp.transpose(delta_block)[:, :, None]))
        dquery_block = jnp.einsum('hqk,khd->qhd', dscore, key_float) * scale
        dkey_sum = dkey_sum + jnp.einsum('hqk,qhd->khd', dscore, query_block) * scale
        return ((dkey_sum, dvalue_sum), dquery_block)
    zeros_kv = jnp.zeros((SEQ, HEADS, HEAD_DIM), jnp.float32)
    (dkey_sum, dvalue_sum), dquery_blocks = lax.scan(one_block, (zeros_kv, zeros_kv), jnp.arange(SEQ // block_width, dtype=jnp.int32))
    return (dquery_blocks.reshape(SEQ, HEADS, HEAD_DIM), dkey_sum, dvalue_sum)

def sequence_pass(token_rows, position_ids, route_rows, grad_rows, norm1_gain, qkv_weight, qkv_bias, out_weight, norm2_gain, router_weight, expert_gate, expert_up, expert_down, shared_gate, shared_w_gate, shared_w_up, shared_w_down):
    head_span = HEADS * HEAD_DIM
    token_float = token_rows.astype(jnp.float32)
    inverse1 = lax.rsqrt(lax.optimization_barrier(jnp.mean(token_float * token_float, -1, keepdims=True)) + EPSILON)
    normed1 = token_float * inverse1
    gain1 = norm1_gain.astype(jnp.float32)
    normed1_b = (normed1 * gain1).astype(jnp.bfloat16)
    qkv_flat = qkv_weight.reshape(D, 3 * head_span)
    qkv = jnp.dot(normed1_b, qkv_flat, preferred_element_type=jnp.float32).reshape(SEQ, 3, head_span) + qkv_bias.astype(jnp.float32)[None]
    cosine, sine_part = rope_tables(position_ids)
    query_raw = qkv[:, 0].reshape(SEQ, HEADS, HEAD_DIM)
    key_raw = qkv[:, 1].reshape(SEQ, HEADS, HEAD_DIM)
    query = (query_raw * cosine + rotate(query_raw) * sine_part).astype(jnp.bfloat16)
    key_rows = (key_raw * cosine + rotate(key_raw) * sine_part).astype(jnp.bfloat16)
    value_rows = qkv[:, 2].reshape(SEQ, HEADS, HEAD_DIM).astype(jnp.bfloat16)
    attended, log_sums = attention_forward(query, key_rows, value_rows)
    attended_flat = attended.reshape(SEQ, head_span)
    hidden = token_float + jnp.dot(attended_flat, out_weight, preferred_element_type=jnp.float32)
    inverse2 = lax.rsqrt(lax.optimization_barrier(jnp.mean(hidden * hidden, -1, keepdims=True)) + EPSILON)
    normed2 = hidden * inverse2
    gain2 = norm2_gain.astype(jnp.float32)
    normed2_b = (normed2 * gain2).astype(jnp.bfloat16)
    normed2_f = normed2_b.astype(jnp.float32)
    logits = jnp.dot(normed2_b, router_weight, preferred_element_type=jnp.float32)
    prob = jax.nn.softmax(logits, -1)
    gate_k = jnp.take_along_axis(prob, route_rows, 1)
    block_count = SEQ // QROWS
    rank = jax.vmap(lambda part_rows: block_rank(part_rows, NUM_EXP))(route_rows.reshape(block_count, QROWS, TOP)).reshape(SEQ, TOP)
    slot_pos = (jnp.arange(SEQ, dtype=jnp.int32) // QROWS)[:, None] * CAP + rank
    expert_ids = route_rows.reshape(-1)
    slot_ids = slot_pos.reshape(-1)
    sources = jnp.broadcast_to(normed2_b[:, None, :], (SEQ, TOP, D)).reshape(-1, D)
    expert_in = jnp.zeros((NUM_EXP, block_count * CAP, D), jnp.bfloat16).at[expert_ids, slot_ids].set(sources)

    def expert_forward(item):
        in_rows, gate_w, up_w, down_w = item
        gate_vals = jnp.dot(in_rows, gate_w, preferred_element_type=jnp.float32)
        up_vals = jnp.dot(in_rows, up_w, preferred_element_type=jnp.float32)
        act_vals = (jax.nn.silu(gate_vals) * up_vals).astype(jnp.bfloat16)
        return jnp.dot(act_vals, down_w, preferred_element_type=jnp.float32).astype(jnp.bfloat16)
    expert_out = lax.map(expert_forward, (expert_in, expert_gate, expert_up, expert_down))
    picked = expert_out[expert_ids, slot_ids].reshape(SEQ, TOP, D).astype(jnp.float32)
    routed = lax.optimization_barrier(jnp.sum(gate_k[:, :, None] * picked, 1))
    shared_sig = jax.nn.sigmoid(jnp.dot(normed2_b, shared_gate[:, None], preferred_element_type=jnp.float32)[:, 0])
    shared_gvals = jnp.dot(normed2_b, shared_w_gate, preferred_element_type=jnp.float32)
    shared_uvals = jnp.dot(normed2_b, shared_w_up, preferred_element_type=jnp.float32)
    shared_act = (jax.nn.silu(shared_gvals) * shared_uvals).astype(jnp.bfloat16)
    shared_out = jnp.dot(shared_act, shared_w_down, preferred_element_type=jnp.float32)
    block_out = (hidden + routed + shared_sig[:, None] * shared_out).astype(jnp.bfloat16)
    grad_float = grad_rows.astype(jnp.float32)
    shared_dout = (shared_sig[:, None] * grad_float).astype(jnp.bfloat16)
    shared_dact = jnp.dot(shared_dout, shared_w_down.T, preferred_element_type=jnp.float32)
    shared_w_down_grad = jnp.dot(shared_act.T, shared_dout, preferred_element_type=jnp.float32)
    shared_dgate = (shared_dact * shared_uvals * silu_grad(shared_gvals)).astype(jnp.bfloat16)
    shared_dup = (shared_dact * jax.nn.silu(shared_gvals)).astype(jnp.bfloat16)
    shared_w_gate_grad = jnp.dot(normed2_b.T, shared_dgate, preferred_element_type=jnp.float32)
    shared_w_up_grad = jnp.dot(normed2_b.T, shared_dup, preferred_element_type=jnp.float32)
    coef = shared_sig * (1.0 - shared_sig) * lax.optimization_barrier(jnp.sum(grad_float * shared_out, -1))
    shared_gate_grad = jnp.dot(coef, normed2_f, precision=PRECISE)
    dnormed2 = jnp.dot(shared_dgate, shared_w_gate.T, preferred_element_type=jnp.float32) + jnp.dot(shared_dup, shared_w_up.T, preferred_element_type=jnp.float32)
    dnormed2 = dnormed2 + coef[:, None] * shared_gate.astype(jnp.float32)[None, :]
    dgate_k = lax.optimization_barrier(jnp.sum(grad_float[:, None, :] * picked, -1))
    dsources = (gate_k[:, :, None] * grad_float[:, None, :]).astype(jnp.bfloat16).reshape(-1, D)
    expert_dout = jnp.zeros((NUM_EXP, block_count * CAP, D), jnp.bfloat16).at[expert_ids, slot_ids].set(dsources)

    def expert_backward(item):
        in_rows, dout_rows, gate_w, up_w, down_w = item
        gate_vals = jnp.dot(in_rows, gate_w, preferred_element_type=jnp.float32)
        up_vals = jnp.dot(in_rows, up_w, preferred_element_type=jnp.float32)
        act_vals = (jax.nn.silu(gate_vals) * up_vals).astype(jnp.bfloat16)
        dact_vals = jnp.dot(dout_rows, down_w.T, preferred_element_type=jnp.float32)
        down_grad = jnp.dot(act_vals.T, dout_rows, preferred_element_type=jnp.float32)
        dgate_vals = (dact_vals * up_vals * silu_grad(gate_vals)).astype(jnp.bfloat16)
        dup_vals = (dact_vals * jax.nn.silu(gate_vals)).astype(jnp.bfloat16)
        gate_grad = jnp.dot(in_rows.T, dgate_vals, preferred_element_type=jnp.float32)
        up_grad = jnp.dot(in_rows.T, dup_vals, preferred_element_type=jnp.float32)
        din_rows = (jnp.dot(dgate_vals, gate_w.T, preferred_element_type=jnp.float32) + jnp.dot(dup_vals, up_w.T, preferred_element_type=jnp.float32)).astype(jnp.bfloat16)
        return (gate_grad, up_grad, down_grad, din_rows)
    expert_gate_grad, expert_up_grad, expert_down_grad, expert_din = lax.map(expert_backward, (expert_in, expert_dout, expert_gate, expert_up, expert_down))
    dnormed2 = dnormed2 + lax.optimization_barrier(jnp.sum(expert_din[expert_ids, slot_ids].reshape(SEQ, TOP, D).astype(jnp.float32), 1))
    route_hits = (route_rows[:, :, None] == jnp.arange(NUM_EXP, dtype=jnp.int32)[None, None, :]).astype(jnp.float32)
    dprob = lax.optimization_barrier(jnp.sum(route_hits * dgate_k[:, :, None], 1))
    dlogit = prob * (dprob - lax.optimization_barrier(jnp.sum(prob * dprob, -1, keepdims=True)))
    router_weight_grad = jnp.dot(normed2_f.T, dlogit, precision=PRECISE)
    dnormed2 = dnormed2 + jnp.dot(dlogit, router_weight.astype(jnp.float32).T, precision=PRECISE)
    norm2_gain_grad = lax.optimization_barrier(jnp.sum(dnormed2 * normed2, 0))
    dscaled2 = dnormed2 * gain2
    dhidden = grad_float + inverse2 * (dscaled2 - normed2 * lax.optimization_barrier(jnp.mean(dscaled2 * normed2, -1, keepdims=True)))
    dhidden_b = dhidden.astype(jnp.bfloat16)
    out_weight_grad = jnp.dot(attended_flat.T, dhidden_b, preferred_element_type=jnp.float32)
    dattended = jnp.dot(dhidden_b, out_weight.T, preferred_element_type=jnp.float32).astype(jnp.bfloat16).reshape(SEQ, HEADS, HEAD_DIM)
    delta = lax.optimization_barrier(jnp.sum(dattended.astype(jnp.float32) * attended.astype(jnp.float32), -1))
    dquery, dkey, dvalue = attention_backward(query, key_rows, value_rows, log_sums, delta, dattended)
    dquery_raw = dquery * cosine + rotate_back(dquery * sine_part)
    dkey_raw = dkey * cosine + rotate_back(dkey * sine_part)
    dqkv = jnp.stack([dquery_raw.reshape(SEQ, head_span), dkey_raw.reshape(SEQ, head_span), dvalue.reshape(SEQ, head_span)], 1)
    qkv_bias_grad = lax.optimization_barrier(jnp.sum(dqkv, 0))
    dqkv_b = dqkv.astype(jnp.bfloat16).reshape(SEQ, 3 * head_span)
    qkv_weight_grad = jnp.dot(normed1_b.T, dqkv_b, preferred_element_type=jnp.float32).reshape(D, 3, head_span)
    dnormed1 = jnp.dot(dqkv_b, qkv_flat.T, preferred_element_type=jnp.float32)
    norm1_gain_grad = lax.optimization_barrier(jnp.sum(dnormed1 * normed1, 0))
    dscaled1 = dnormed1 * gain1
    tokens_grad = dhidden + inverse1 * (dscaled1 - normed1 * lax.optimization_barrier(jnp.mean(dscaled1 * normed1, -1, keepdims=True)))
    grads = (norm1_gain_grad, qkv_weight_grad, qkv_bias_grad, out_weight_grad, norm2_gain_grad, router_weight_grad, expert_gate_grad, expert_up_grad, expert_down_grad, shared_gate_grad, shared_w_gate_grad, shared_w_up_grad, shared_w_down_grad)
    return (block_out, tokens_grad, grads)

def reference(tokens, positions, routes, out_grad, norm1_gain, qkv_weight, qkv_bias, out_weight, norm2_gain, router_weight, expert_gate, expert_up, expert_down, shared_gate, shared_w_gate, shared_w_up, shared_w_down):
    outputs = []
    input_grads = []
    totals = None
    for seq_id in range(BATCH):
        block_out, tokens_grad, grads = sequence_pass(tokens[seq_id], positions[seq_id], routes[seq_id], out_grad[seq_id], norm1_gain, qkv_weight, qkv_bias, out_weight, norm2_gain, router_weight, expert_gate, expert_up, expert_down, shared_gate, shared_w_gate, shared_w_up, shared_w_down)
        outputs.append(block_out)
        input_grads.append(tokens_grad)
        if totals is None:
            totals = grads
        else:
            totals = tuple((first + second for first, second in zip(totals, grads)))
    return (jnp.stack(outputs), jnp.stack(input_grads), totals[0], totals[1], totals[2], totals[3], totals[4], totals[5], totals[6], totals[7], totals[8], totals[9], totals[10], totals[11], totals[12])
```

```python
import jax
import jax.numpy as jnp
from jax import lax
from jax.sharding import PartitionSpec as P

HEAD_DIM = 128


EPSILON = 1e-06
ROPE_BASE = 1000000.0
MASKED = -1e30
PRECISE = lax.Precision.HIGHEST


def rope_tables(position_ids):
    half_dim = HEAD_DIM // 2
    inverse = ROPE_BASE ** (-2.0 * jnp.arange(half_dim, dtype=jnp.float32) / HEAD_DIM)
    angles = position_ids.astype(jnp.float32)[:, None] * inverse[None, :]
    cosine = jnp.cos(angles)
    sine_part = jnp.sin(angles)
    return (
        jnp.concatenate([cosine, cosine], -1)[:, None, :],
        jnp.concatenate([sine_part, sine_part], -1)[:, None, :],
    )


def rotate(value):
    half_dim = value.shape[-1] // 2
    return jnp.concatenate([-value[..., half_dim:], value[..., :half_dim]], -1)


def rotate_back(value):
    half_dim = value.shape[-1] // 2
    return jnp.concatenate([value[..., half_dim:], -value[..., :half_dim]], -1)


def silu_grad(gate_vals):
    sigmoid_vals = jax.nn.sigmoid(gate_vals)
    return sigmoid_vals * (1.0 + gate_vals * (1.0 - sigmoid_vals))


def block_rank(route_rows, expert_count):
    hits = (
        route_rows[:, :, None] == jnp.arange(expert_count, dtype=jnp.int32)[None, None, :]
    ).astype(jnp.int32)
    flat_hits = hits.reshape(-1, expert_count)
    earlier = jnp.cumsum(flat_hits, axis=0) - flat_hits
    return jnp.sum(earlier * flat_hits, -1).reshape(route_rows.shape)


def block_width_of():
    return 512


def gather_weights(shard_set):
    return (
        lax.all_gather(shard_set[0], ("dp", "context"), axis=0, tiled=True),
        lax.all_gather(shard_set[1], ("dp", "context"), axis=1, tiled=True),
        lax.all_gather(shard_set[2], ("dp", "context"), axis=1, tiled=True),
        lax.all_gather(shard_set[3], ("dp", "context"), axis=1, tiled=True),
        lax.all_gather(shard_set[4], ("dp", "context"), axis=2, tiled=True),
        lax.all_gather(shard_set[5], ("dp", "context"), axis=0, tiled=True),
        lax.all_gather(shard_set[6], ("dp", "context"), axis=0, tiled=True),
        lax.all_gather(shard_set[7], ("dp", "context"), axis=1, tiled=True),
    )


def forward_fold(query, query_first, scale, carry, piece):
    row_count, head_count, head_size = query.shape
    query_index = query_first + jnp.arange(row_count, dtype=jnp.int32)
    query_last = query_first + row_count - 1
    key_part, value_part = piece
    piece_rows = key_part.shape[0]
    block_width = block_width_of()
    block_count = piece_rows // block_width
    key_blocks = key_part.reshape(block_count, block_width, head_count, head_size)
    value_blocks = value_part.reshape(block_count, block_width, head_count, head_size)
    offsets = block_width * jnp.arange(block_count, dtype=jnp.int32)

    def forward_visit(state, item):
        key_block, value_block, first_key = item

        def forward_compute(current):
            run_max, run_sum, accum = current
            scores = (
                jnp.einsum("qhd,khd->hqk", query, key_block, preferred_element_type=jnp.float32)
                * scale
            )
            key_index = first_key + jnp.arange(block_width, dtype=jnp.int32)
            allowed = key_index[None, None, :] <= query_index[None, :, None]
            new_max = jnp.maximum(run_max, jnp.max(jnp.where(allowed, scores, MASKED), -1))
            weights = jnp.where(allowed, jnp.exp(scores - new_max[..., None]), 0.0)
            factor = jnp.exp(run_max - new_max)
            new_sum = run_sum * factor + jnp.sum(weights, -1)
            new_accum = accum * factor[..., None] + jnp.einsum(
                "hqk,khd->hqd",
                weights.astype(jnp.bfloat16),
                value_block,
                preferred_element_type=jnp.float32,
            )
            return (new_max, new_sum, new_accum)

        return (
            lax.cond(first_key > query_last, lambda current: current, forward_compute, state),
            None,
        )

    carry, _ = lax.scan(forward_visit, carry, (key_blocks, value_blocks, offsets))
    return carry


def key_grad_fold(key_rows, value_rows, key_first, scale, carry, piece):
    row_count, head_count, head_size = key_rows.shape
    key_index = key_first + jnp.arange(row_count, dtype=jnp.int32)
    query_part, dout_part, lse_part, delta_part = piece
    piece_rows = query_part.shape[0]
    block_width = block_width_of()
    block_count = piece_rows // block_width
    query_blocks = query_part.reshape(block_count, block_width, head_count, head_size)
    dout_blocks = dout_part.reshape(block_count, block_width, head_count, head_size)
    lse_blocks = lse_part.reshape(block_count, block_width, head_count)
    delta_blocks = delta_part.reshape(block_count, block_width, head_count)
    offsets = block_width * jnp.arange(block_count, dtype=jnp.int32)

    def key_visit(state, item):
        query_block, dout_block, lse_block, delta_block, first_query = item

        def key_compute(current):
            dkey_sum, dvalue_sum = current
            query_b = query_block.astype(jnp.bfloat16)
            dout_b = dout_block.astype(jnp.bfloat16)
            scores = (
                jnp.einsum("qhd,khd->hqk", query_b, key_rows, preferred_element_type=jnp.float32)
                * scale
            )
            query_index = first_query + jnp.arange(block_width, dtype=jnp.int32)
            allowed = key_index[None, None, :] <= query_index[None, :, None]
            prob_att = jnp.where(
                allowed, jnp.exp(scores - jnp.transpose(lse_block)[:, :, None]), 0.0
            )
            dvalue_sum = dvalue_sum + jnp.einsum(
                "hqk,qhd->hkd",
                prob_att.astype(jnp.bfloat16),
                dout_b,
                preferred_element_type=jnp.float32,
            )
            dprob = jnp.einsum(
                "qhd,khd->hqk", dout_b, value_rows, preferred_element_type=jnp.float32
            )
            dscore = (prob_att * (dprob - jnp.transpose(delta_block)[:, :, None])).astype(
                jnp.bfloat16
            )
            dkey_sum = (
                dkey_sum
                + jnp.einsum("hqk,qhd->hkd", dscore, query_b, preferred_element_type=jnp.float32)
                * scale
            )
            return (dkey_sum, dvalue_sum)

        return (
            lax.cond(
                first_query + block_width - 1 < key_first,
                lambda current: current,
                key_compute,
                state,
            ),
            None,
        )

    carry, _ = lax.scan(
        key_visit, carry, (query_blocks, dout_blocks, lse_blocks, delta_blocks, offsets)
    )
    return carry


def query_grad_fold(query, dattended, lse_heads, delta_heads, query_first, scale, carry, piece):
    row_count, head_count, head_size = query.shape
    query_index = query_first + jnp.arange(row_count, dtype=jnp.int32)
    query_last = query_first + row_count - 1
    key_part, value_part = piece
    piece_rows = key_part.shape[0]
    block_width = block_width_of()
    block_count = piece_rows // block_width
    key_blocks = key_part.reshape(block_count, block_width, head_count, head_size)
    value_blocks = value_part.reshape(block_count, block_width, head_count, head_size)
    offsets = block_width * jnp.arange(block_count, dtype=jnp.int32)

    def query_visit(state, item):
        key_block, value_block, first_key = item

        def query_compute(current):
            scores = (
                jnp.einsum("qhd,khd->hqk", query, key_block, preferred_element_type=jnp.float32)
                * scale
            )
            key_index = first_key + jnp.arange(block_width, dtype=jnp.int32)
            allowed = key_index[None, None, :] <= query_index[None, :, None]
            prob_att = jnp.where(allowed, jnp.exp(scores - lse_heads[:, :, None]), 0.0)
            dprob = jnp.einsum(
                "qhd,khd->hqk", dattended, value_block, preferred_element_type=jnp.float32
            )
            dscore = (prob_att * (dprob - delta_heads[:, :, None])).astype(jnp.bfloat16)
            return (
                current
                + jnp.einsum("hqk,khd->hqd", dscore, key_block, preferred_element_type=jnp.float32)
                * scale
            )

        return (
            lax.cond(first_key > query_last, lambda current: current, query_compute, state),
            None,
        )

    carry, _ = lax.scan(query_visit, carry, (key_blocks, value_blocks, offsets))
    return carry


def general_body(
    tokens,
    positions,
    routes,
    out_grad,
    norm1_gain,
    qkv_weight,
    qkv_bias,
    out_weight,
    norm2_gain,
    router_weight,
    expert_gate,
    expert_up,
    expert_down,
    shared_gate,
    shared_w_gate,
    shared_w_up,
    shared_w_down,
):
    row_count = tokens.shape[1]
    model_width = tokens.shape[2]
    head_span = qkv_bias.shape[1]
    heads_here = head_span // HEAD_DIM
    local_experts = expert_gate.shape[0]
    group_size = lax.axis_size("experts")
    quarter = row_count // group_size
    capacity = 3 * quarter // 4
    expert_count = local_experts * group_size
    group_index = lax.axis_index("experts")
    scale = HEAD_DIM ** (-0.5)
    shard_set = (
        qkv_weight,
        out_weight,
        expert_gate,
        expert_up,
        expert_down,
        shared_w_gate,
        shared_w_up,
        shared_w_down,
    )
    qkv_full, out_full, gate_full, up_full, down_full, sgate_full, sup_full, sdown_full = (
        gather_weights(shard_set)
    )
    token_float = tokens[0].astype(jnp.float32)
    inverse1 = lax.rsqrt(jnp.mean(token_float * token_float, -1, keepdims=True) + EPSILON)
    normed1 = token_float * inverse1
    gain1 = norm1_gain.astype(jnp.float32)
    normed1_b = (normed1 * gain1).astype(jnp.bfloat16)
    qkv_flat = qkv_full.reshape(model_width, 3 * head_span)
    qkv = (
        jnp.dot(normed1_b, qkv_flat, preferred_element_type=jnp.float32).reshape(
            row_count, 3, head_span
        )
        + qkv_bias.astype(jnp.float32)[None]
    )
    cosine, sine_part = rope_tables(positions[0])
    query_raw = qkv[:, 0].reshape(row_count, heads_here, HEAD_DIM)
    key_raw = qkv[:, 1].reshape(row_count, heads_here, HEAD_DIM)
    query = (query_raw * cosine + rotate(query_raw) * sine_part).astype(jnp.bfloat16)
    key_rows = (key_raw * cosine + rotate(key_raw) * sine_part).astype(jnp.bfloat16)
    value_flat = qkv[:, 2].astype(jnp.bfloat16)
    key_flat = key_rows.reshape(row_count, head_span)
    value_rows = value_flat.reshape(row_count, heads_here, HEAD_DIM)
    query_first = lax.axis_index("context") * row_count
    start_state = (
        jnp.full((heads_here, row_count), MASKED, jnp.float32),
        jnp.zeros((heads_here, row_count), jnp.float32),
        jnp.zeros((heads_here, row_count, HEAD_DIM), jnp.float32),
    )
    run_max, run_sum, accum = forward_fold(
        query,
        query_first,
        scale,
        start_state,
        (
            lax.all_gather(key_flat, "context", axis=0, tiled=True),
            lax.all_gather(value_flat, "context", axis=0, tiled=True),
        ),
    )
    attended = jnp.transpose(accum / run_sum[..., None], (1, 0, 2)).astype(jnp.bfloat16)
    lse_heads = run_max + jnp.log(run_sum)
    attended_flat = attended.reshape(row_count, head_span)
    head_part = jnp.dot(attended_flat, out_full, preferred_element_type=jnp.float32)
    hidden = token_float + lax.psum(head_part, "experts")
    inverse2 = lax.rsqrt(jnp.mean(hidden * hidden, -1, keepdims=True) + EPSILON)
    normed2 = hidden * inverse2
    gain2 = norm2_gain.astype(jnp.float32)
    normed2_b = (normed2 * gain2).astype(jnp.bfloat16)
    first_row = group_index * quarter
    normed2_q = lax.dynamic_slice_in_dim(normed2_b, first_row, quarter, 0)
    route_q = lax.dynamic_slice_in_dim(routes[0], first_row, quarter, 0)
    logits = jnp.dot(normed2_q, router_weight, preferred_element_type=jnp.float32)
    prob = jax.nn.softmax(logits, -1)
    gate_k = jnp.take_along_axis(prob, route_q, 1)
    slot_ids = route_q * capacity + block_rank(route_q, expert_count)
    slot_hits = (
        slot_ids[:, :, None] == jnp.arange(expert_count * capacity, dtype=jnp.int32)[None, None, :]
    )
    placer = jnp.sum(slot_hits.astype(jnp.bfloat16), 1)
    send_rows = (
        jnp.dot(placer.T, normed2_q, preferred_element_type=jnp.float32)
        .astype(jnp.bfloat16)
        .reshape(group_size, local_experts, capacity, model_width)
    )
    arrived = lax.all_to_all(send_rows, "experts", split_axis=0, concat_axis=0, tiled=True)
    expert_gvals = jnp.einsum(
        "secd,edf->secf", arrived, gate_full, preferred_element_type=jnp.float32
    )
    expert_uvals = jnp.einsum(
        "secd,edf->secf", arrived, up_full, preferred_element_type=jnp.float32
    )
    expert_act = (jax.nn.silu(expert_gvals) * expert_uvals).astype(jnp.bfloat16)
    expert_out = jnp.einsum(
        "secf,efd->secd", expert_act, down_full, preferred_element_type=jnp.float32
    ).astype(jnp.bfloat16)
    returned = lax.all_to_all(
        expert_out, "experts", split_axis=0, concat_axis=0, tiled=True
    ).reshape(expert_count * capacity, model_width)
    picked = returned[slot_ids].astype(jnp.float32)
    routed = jnp.sum(gate_k[:, :, None] * picked, 1)
    shared_sig = jax.nn.sigmoid(
        jnp.dot(normed2_b, shared_gate[:, None], preferred_element_type=jnp.float32)[:, 0]
    )
    shared_gvals = jnp.dot(normed2_b, sgate_full, preferred_element_type=jnp.float32)
    shared_uvals = jnp.dot(normed2_b, sup_full, preferred_element_type=jnp.float32)
    shared_act = (jax.nn.silu(shared_gvals) * shared_uvals).astype(jnp.bfloat16)
    shared_part = jnp.dot(shared_act, sdown_full, preferred_element_type=jnp.float32)
    routed_pad = lax.dynamic_update_slice_in_dim(
        jnp.zeros((row_count, model_width), jnp.float32), routed, first_row, 0
    )
    branch_total = lax.psum(
        (shared_sig[:, None] * shared_part + routed_pad).astype(jnp.bfloat16), "experts"
    ).astype(jnp.float32)
    block_out = (hidden + branch_total).astype(jnp.bfloat16)
    held = lax.optimization_barrier((shard_set, block_out))
    qkv_full, out_full, gate_full, up_full, down_full, sgate_full, sup_full, sdown_full = (
        gather_weights(held[0])
    )
    qkv_flat = qkv_full.reshape(model_width, 3 * head_span)
    grad_float = out_grad[0].astype(jnp.float32)
    grad_q = lax.dynamic_slice_in_dim(grad_float, first_row, quarter, 0)
    dgate_k = jnp.sum(grad_q[:, None, :] * picked, -1)
    weighted = jnp.sum(slot_hits.astype(jnp.float32) * gate_k[:, :, None], 1)
    dsend = (
        jnp.dot(weighted.T, grad_q, precision=PRECISE)
        .astype(jnp.bfloat16)
        .reshape(group_size, local_experts, capacity, model_width)
    )
    darrived = lax.all_to_all(dsend, "experts", split_axis=0, concat_axis=0, tiled=True)
    expert_dact = jnp.einsum(
        "secd,efd->secf", darrived, down_full, preferred_element_type=jnp.float32
    )
    down_grad = jnp.einsum(
        "secf,secd->efd", expert_act, darrived, preferred_element_type=jnp.float32
    )
    expert_dgate = (expert_dact * expert_uvals * silu_grad(expert_gvals)).astype(jnp.bfloat16)
    expert_dup = (expert_dact * jax.nn.silu(expert_gvals)).astype(jnp.bfloat16)
    gate_grad = jnp.einsum(
        "secd,secf->edf", arrived, expert_dgate, preferred_element_type=jnp.float32
    )
    up_grad = jnp.einsum("secd,secf->edf", arrived, expert_dup, preferred_element_type=jnp.float32)
    expert_din = (
        jnp.einsum("secf,edf->secd", expert_dgate, gate_full, preferred_element_type=jnp.float32)
        + jnp.einsum("secf,edf->secd", expert_dup, up_full, preferred_element_type=jnp.float32)
    ).astype(jnp.bfloat16)
    dreturned = lax.all_to_all(
        expert_din, "experts", split_axis=0, concat_axis=0, tiled=True
    ).reshape(expert_count * capacity, model_width)
    dnormed2_q = jnp.dot(placer, dreturned, preferred_element_type=jnp.float32)
    route_hits = (
        route_q[:, :, None] == jnp.arange(expert_count, dtype=jnp.int32)[None, None, :]
    ).astype(jnp.float32)
    dprob = jnp.sum(route_hits * dgate_k[:, :, None], 1)
    dlogit = prob * (dprob - jnp.sum(prob * dprob, -1, keepdims=True))
    router_part = jnp.dot(normed2_q.astype(jnp.float32).T, dlogit, precision=PRECISE)
    dnormed2_q = dnormed2_q + jnp.dot(
        dlogit, router_weight.astype(jnp.float32).T, precision=PRECISE
    )
    shared_dout = (shared_sig[:, None] * grad_float).astype(jnp.bfloat16)
    shared_dact = jnp.dot(shared_dout, sdown_full.T, preferred_element_type=jnp.float32)
    sdown_grad = jnp.dot(shared_act.T, shared_dout, preferred_element_type=jnp.float32)
    shared_dgate = (shared_dact * shared_uvals * silu_grad(shared_gvals)).astype(jnp.bfloat16)
    shared_dup = (shared_dact * jax.nn.silu(shared_gvals)).astype(jnp.bfloat16)
    sgate_grad = jnp.dot(normed2_b.T, shared_dgate, preferred_element_type=jnp.float32)
    sup_grad = jnp.dot(normed2_b.T, shared_dup, preferred_element_type=jnp.float32)
    row_dots = jnp.sum(grad_float * shared_part, -1)
    dnormed2_part = jnp.dot(
        shared_dgate, sgate_full.T, preferred_element_type=jnp.float32
    ) + jnp.dot(shared_dup, sup_full.T, preferred_element_type=jnp.float32)
    dnormed2_part = dnormed2_part + lax.dynamic_update_slice_in_dim(
        jnp.zeros((row_count, model_width), jnp.float32), dnormed2_q, first_row, 0
    )
    dnormed2, row_dots, router_grad = lax.psum((dnormed2_part, row_dots, router_part), "experts")
    coef = shared_sig * (1.0 - shared_sig) * row_dots
    dnormed2 = dnormed2 + coef[:, None] * shared_gate.astype(jnp.float32)[None, :]
    shared_gate_grad = jnp.dot(coef, normed2_b.astype(jnp.float32), precision=PRECISE)
    norm2_grad = jnp.sum(dnormed2 * normed2, 0)
    dscaled2 = dnormed2 * gain2
    dhidden = grad_float + inverse2 * (
        dscaled2 - normed2 * jnp.mean(dscaled2 * normed2, -1, keepdims=True)
    )
    dhidden_b = dhidden.astype(jnp.bfloat16)
    out_grad_part = jnp.dot(attended_flat.T, dhidden_b, preferred_element_type=jnp.float32)
    dattended = jnp.dot(dhidden_b, out_full.T, preferred_element_type=jnp.float32).astype(
        jnp.bfloat16
    )
    dattended3 = dattended.reshape(row_count, heads_here, HEAD_DIM)
    delta = jnp.sum(dattended3.astype(jnp.float32) * attended.astype(jnp.float32), -1)
    zero_state = jnp.zeros((heads_here, row_count, HEAD_DIM), jnp.float32)
    dkey_sum, dvalue_sum = key_grad_fold(
        key_rows,
        value_rows,
        query_first,
        scale,
        (zero_state, zero_state),
        (
            lax.all_gather(
                query.reshape(row_count, head_span).astype(jnp.float32),
                "context",
                axis=0,
                tiled=True,
            ),
            lax.all_gather(dattended.astype(jnp.float32), "context", axis=0, tiled=True),
            lax.all_gather(jnp.transpose(lse_heads), "context", axis=0, tiled=True),
            lax.all_gather(delta, "context", axis=0, tiled=True),
        ),
    )
    dquery_sum = query_grad_fold(
        query,
        dattended3,
        lse_heads,
        jnp.transpose(delta),
        query_first,
        scale,
        zero_state,
        (
            lax.all_gather(key_flat, "context", axis=0, tiled=True),
            lax.all_gather(value_flat, "context", axis=0, tiled=True),
        ),
    )
    dquery = jnp.transpose(dquery_sum, (1, 0, 2))
    dkey = jnp.transpose(dkey_sum, (1, 0, 2))
    dvalue = jnp.transpose(dvalue_sum, (1, 0, 2))
    dquery_raw = dquery * cosine + rotate_back(dquery * sine_part)
    dkey_raw = dkey * cosine + rotate_back(dkey * sine_part)
    dqkv = jnp.stack(
        [
            dquery_raw.reshape(row_count, head_span),
            dkey_raw.reshape(row_count, head_span),
            dvalue.reshape(row_count, head_span),
        ],
        1,
    )
    bias_grad = jnp.sum(dqkv, 0)
    dqkv_b = dqkv.astype(jnp.bfloat16).reshape(row_count, 3 * head_span)
    qkv_grad = jnp.dot(normed1_b.T, dqkv_b, preferred_element_type=jnp.float32).reshape(
        model_width, 3, head_span
    )
    dnormed1 = lax.psum(
        jnp.dot(dqkv_b, qkv_flat.T, preferred_element_type=jnp.float32).astype(jnp.bfloat16),
        "experts",
    ).astype(jnp.float32)
    norm1_grad = jnp.sum(dnormed1 * normed1, 0)
    dscaled1 = dnormed1 * gain1
    tokens_grad = dhidden + inverse1 * (
        dscaled1 - normed1 * jnp.mean(dscaled1 * normed1, -1, keepdims=True)
    )
    small_sums = (
        lax.psum(norm1_grad.astype(jnp.bfloat16), ("dp", "context")).astype(jnp.float32),
        lax.psum(norm2_grad.astype(jnp.bfloat16), ("dp", "context")).astype(jnp.float32),
        lax.psum(router_grad.astype(jnp.bfloat16), ("dp", "context")).astype(jnp.float32),
        lax.psum(shared_gate_grad.astype(jnp.bfloat16), ("dp", "context")).astype(jnp.float32),
        lax.psum(bias_grad.astype(jnp.bfloat16), ("dp", "context")).astype(jnp.float32),
    )
    large_sums = (
        lax.psum_scatter(
            qkv_grad.astype(jnp.bfloat16), ("dp", "context"), scatter_dimension=0, tiled=True
        ).astype(jnp.float32),
        lax.psum_scatter(
            out_grad_part.astype(jnp.bfloat16), ("dp", "context"), scatter_dimension=1, tiled=True
        ).astype(jnp.float32),
        lax.psum_scatter(
            gate_grad.astype(jnp.bfloat16), ("dp", "context"), scatter_dimension=1, tiled=True
        ).astype(jnp.float32),
        lax.psum_scatter(
            up_grad.astype(jnp.bfloat16), ("dp", "context"), scatter_dimension=1, tiled=True
        ).astype(jnp.float32),
        lax.psum_scatter(
            down_grad.astype(jnp.bfloat16), ("dp", "context"), scatter_dimension=2, tiled=True
        ).astype(jnp.float32),
        lax.psum_scatter(
            sgate_grad.astype(jnp.bfloat16), ("dp", "context"), scatter_dimension=0, tiled=True
        ).astype(jnp.float32),
        lax.psum_scatter(
            sup_grad.astype(jnp.bfloat16), ("dp", "context"), scatter_dimension=0, tiled=True
        ).astype(jnp.float32),
        lax.psum_scatter(
            sdown_grad.astype(jnp.bfloat16), ("dp", "context"), scatter_dimension=1, tiled=True
        ).astype(jnp.float32),
    )
    return (
        block_out[None],
        tokens_grad[None],
        small_sums[0],
        large_sums[0],
        small_sums[4],
        large_sums[1],
        small_sums[1],
        small_sums[2],
        large_sums[2],
        large_sums[3],
        large_sums[4],
        small_sums[3],
        large_sums[5],
        large_sums[6],
        large_sums[7],
    )


def swap_halves(value):
    return lax.ppermute(value, "dp", [(0, 1), (1, 0)])


def own_half_first(value):
    half = value.shape[-1] // 2
    turned = jnp.concatenate([value[..., half:], value[..., :half]], -1)
    return jnp.where(lax.axis_index("dp") == 0, value, turned)


def exchange(value):
    return lax.all_to_all(value, "context", split_axis=0, concat_axis=0, tiled=True)


def sum_rows(value):
    return lax.psum_scatter(value, ("context", "experts"), scatter_dimension=0, tiled=True)


def share_rows(value):
    return lax.all_gather(value, ("context", "experts"), axis=0, tiled=True)


def dot_nn(left, right):
    return jnp.dot(left, right, preferred_element_type=jnp.float32)


def dot_nt(left, right):
    return lax.dot_general(
        left, right, (((1,), (1,)), ((), ())), preferred_element_type=jnp.float32
    )


def dot_tn(left, right):
    return lax.dot_general(
        left, right, (((0,), (0,)), ((), ())), preferred_element_type=jnp.float32
    )


def split_body(
    tokens,
    positions,
    routes,
    out_grad,
    norm1_gain,
    qkv_weight,
    qkv_bias,
    out_weight,
    norm2_gain,
    router_weight,
    expert_gate,
    expert_up,
    expert_down,
    shared_gate,
    shared_w_gate,
    shared_w_up,
    shared_w_down,
):
    rows, width = tokens.shape[1], tokens.shape[2]
    parts = lax.axis_size("context")
    group_size = lax.axis_size("experts")
    place, group = lax.axis_index("context"), lax.axis_index("experts")
    local_experts = expert_gate.shape[0]
    expert_count = local_experts * group_size
    own_rows = rows // group_size
    length = rows * parts
    half = width // 2
    block = width // (2 * parts)
    hidden_here = shared_w_gate.shape[1] // parts
    stacks = local_experts + 1
    span = stacks * hidden_here
    scale = HEAD_DIM ** (-0.5)
    bf16 = jnp.bfloat16

    qkv_in = jnp.transpose(
        qkv_weight.reshape(block, 3, parts, HEAD_DIM), (2, 0, 1, 3)
    ).reshape(parts, block, 3 * HEAD_DIM)
    qkv_m = exchange(qkv_in).reshape(half, 3 * HEAD_DIM)
    qkv_o = swap_halves(qkv_m)
    out_m = jnp.transpose(exchange(out_weight.reshape(parts, HEAD_DIM, block)), (1, 0, 2)).reshape(
        HEAD_DIM, half
    )
    out_o = swap_halves(out_m)
    down_in = jnp.concatenate([shared_w_down[None], expert_down], 0)
    down_in = jnp.transpose(
        down_in.reshape(stacks, parts, hidden_here, block), (1, 0, 2, 3)
    ).reshape(parts, span, block)
    down_m = jnp.transpose(exchange(down_in), (1, 0, 2)).reshape(span, half)
    down_o = swap_halves(down_m)
    up_in = jnp.concatenate(
        [shared_w_gate[None], expert_gate, shared_w_up[None], expert_up], 0
    ).reshape(2 * stacks, block, parts, hidden_here)
    up_in = jnp.transpose(up_in, (2, 1, 0, 3)).reshape(parts, block, 2 * span)
    up_m = exchange(up_in).reshape(half, 2 * span)
    up_o = swap_halves(up_m)

    grad_all = lax.all_gather(own_half_first(out_grad[0]), "context", axis=0, tiled=True)
    position_all = lax.all_gather(positions[0], "context", axis=0, tiled=True)
    route_all = lax.all_gather(routes[0], "context", axis=0, tiled=True)

    gain1 = own_half_first(norm1_gain).astype(jnp.float32)
    gain2 = own_half_first(norm2_gain).astype(jnp.float32)
    token_rows = own_half_first(tokens[0]).astype(jnp.float32)
    inverse_rows = lax.rsqrt(jnp.mean(token_rows * token_rows, -1, keepdims=True) + EPSILON)
    xn1 = lax.all_gather(
        (token_rows * inverse_rows * gain1).astype(bf16), "context", axis=0, tiled=True
    )
    first = group * own_rows
    token_own = lax.dynamic_slice_in_dim(token_rows, first, own_rows, 0)
    inverse1 = lax.dynamic_slice_in_dim(inverse_rows, first, own_rows, 0)
    normed1 = token_own * inverse1
    grad_own = lax.dynamic_slice_in_dim(
        own_half_first(out_grad[0]).astype(jnp.float32), first, own_rows, 0
    )

    bias_here = lax.dynamic_slice_in_dim(
        qkv_bias.reshape(3, parts, HEAD_DIM), place, 1, 1
    ).reshape(1, 3 * HEAD_DIM)
    qkv = (
        dot_nn(xn1[:, :half], qkv_m)
        + dot_nn(xn1[:, half:], qkv_o)
        + bias_here.astype(jnp.float32)
    )
    cosine, sine_part = rope_tables(position_all)
    cosine, sine_part = cosine[:, 0], sine_part[:, 0]
    q_raw, k_raw, v_raw = jnp.split(qkv, 3, 1)
    query = (q_raw * cosine + rotate(q_raw) * sine_part).astype(bf16)
    key = (k_raw * cosine + rotate(k_raw) * sine_part).astype(bf16)
    value = v_raw.astype(bf16)
    index = jnp.arange(length, dtype=jnp.int32)
    allowed = index[None, :] <= index[:, None]
    scores = dot_nt(query, key) * scale
    row_max = jnp.max(jnp.where(allowed, scores, MASKED), -1, keepdims=True)
    weights = jnp.where(allowed, jnp.exp(scores - row_max), 0.0)
    row_sum = jnp.sum(weights, -1, keepdims=True)
    attended = (dot_nn(weights.astype(bf16), value) / row_sum).astype(bf16)
    lse = row_max + jnp.log(row_sum)

    head_part = jnp.concatenate([dot_nn(attended, out_m), dot_nn(attended, out_o)], 1)
    hidden = token_own + sum_rows(head_part.astype(bf16)).astype(jnp.float32)
    inverse2 = lax.rsqrt(jnp.mean(hidden * hidden, -1, keepdims=True) + EPSILON)
    normed2 = hidden * inverse2
    xn2_own = (normed2 * gain2).astype(bf16)
    xn2 = share_rows(xn2_own)

    router_here = own_half_first(router_weight.T).T
    gate_here = own_half_first(shared_gate)
    heads_w = jnp.concatenate([router_here, gate_here[:, None]], 1)
    logits_all = dot_nn(xn2, heads_w)
    prob_all = jax.nn.softmax(logits_all[:, :expert_count], -1)
    sig_all = jax.nn.sigmoid(logits_all[:, expert_count])
    named_all = jnp.sum(
        (
            route_all[:, :, None] == jnp.arange(expert_count, dtype=jnp.int32)[None, None, :]
        ).astype(jnp.float32),
        1,
    )
    gates_all = prob_all * named_all
    gates_here = lax.dynamic_slice_in_dim(gates_all, group * local_experts, local_experts, 1)
    coefs = jnp.concatenate([sig_all[:, None], gates_here], 1)

    up_vals = dot_nn(xn2[:, :half], up_m) + dot_nn(xn2[:, half:], up_o)
    g_vals, u_vals = up_vals[:, :span], up_vals[:, span:]
    sig_g = jax.nn.sigmoid(g_vals)
    silu_g = g_vals * sig_g
    act = silu_g * u_vals
    coef_wide = jnp.repeat(coefs, hidden_here, axis=1, total_repeat_length=span)
    act_c = (act * coef_wide).astype(bf16)
    raw = dot_nt(grad_all[:, :half], down_m) + dot_nt(grad_all[:, half:], down_o)
    dots = jnp.sum((raw * act).reshape(length, stacks, hidden_here), -1)
    dact = raw * coef_wide
    dg = (dact * u_vals * (sig_g * (1.0 + g_vals * (1.0 - sig_g)))).astype(bf16)
    du = (dact * silu_g).astype(bf16)
    dup = jnp.concatenate([dg, du], 1)
    branch_part = jnp.concatenate([dot_nn(act_c, down_m), dot_nn(act_c, down_o)], 1)
    dxn2_part = jnp.concatenate([dot_nt(dup, up_m), dot_nt(dup, up_o)], 1)
    dots_wide = jnp.concatenate(
        [
            lax.dynamic_update_slice_in_dim(
                jnp.zeros((length, expert_count), jnp.float32),
                dots[:, 1:],
                group * local_experts,
                1,
            ),
            dots[:, :1],
        ],
        1,
    )
    dxn2_sum = sum_rows(dxn2_part.astype(bf16)).astype(jnp.float32)
    dots_own = sum_rows(dots_wide)
    branch = sum_rows(branch_part.astype(bf16)).astype(jnp.float32)
    block_own = own_half_first((hidden + branch).astype(bf16))
    block_out = lax.all_gather(block_own, "experts", axis=0, tiled=True)

    row_first = place * rows + first
    prob = lax.dynamic_slice_in_dim(prob_all, row_first, own_rows, 0)
    named = lax.dynamic_slice_in_dim(named_all, row_first, own_rows, 0)
    sig_own = lax.dynamic_slice_in_dim(sig_all, row_first, own_rows, 0)
    dprob = dots_own[:, :expert_count] * named
    dlogit = prob * (dprob - jnp.sum(prob * dprob, -1, keepdims=True))
    coef = sig_own * (1.0 - sig_own) * dots_own[:, expert_count]
    xn2_float = xn2_own.astype(jnp.float32)
    router_grad = jnp.dot(xn2_float.T, dlogit, precision=PRECISE)
    shared_gate_grad = jnp.dot(coef, xn2_float, precision=PRECISE)
    dxn2 = (
        dxn2_sum
        + jnp.dot(dlogit, router_here.astype(jnp.float32).T, precision=PRECISE)
        + coef[:, None] * gate_here.astype(jnp.float32)[None, :]
    )
    norm2_grad = jnp.sum(dxn2 * normed2, 0)
    dscaled2 = dxn2 * gain2
    dhidden = grad_own + inverse2 * (
        dscaled2 - normed2 * jnp.mean(dscaled2 * normed2, -1, keepdims=True)
    )
    dhidden_all = share_rows(dhidden.astype(bf16))

    out_grad_part = dot_tn(attended, dhidden_all)
    dattended = (
        dot_nt(dhidden_all[:, :half], out_m) + dot_nt(dhidden_all[:, half:], out_o)
    ).astype(bf16)
    delta = jnp.sum(
        dattended.astype(jnp.float32) * attended.astype(jnp.float32), -1, keepdims=True
    )
    scores = dot_nt(query, key) * scale
    prob_att = jnp.where(allowed, jnp.exp(scores - lse), 0.0)
    dvalue = dot_tn(prob_att.astype(bf16), dattended)
    dscore = (prob_att * (dot_nt(dattended, value) - delta)).astype(bf16)
    dquery = dot_nn(dscore, key) * scale
    dkey = dot_tn(dscore, query) * scale
    dqkv = jnp.concatenate(
        [
            dquery * cosine + rotate_back(dquery * sine_part),
            dkey * cosine + rotate_back(dkey * sine_part),
            dvalue,
        ],
        1,
    )
    bias_part = jnp.sum(dqkv, 0)
    dqkv_b = dqkv.astype(bf16)
    qkv_grad = dot_tn(xn1, dqkv_b)
    dxn1_part = jnp.concatenate([dot_nt(dqkv_b, qkv_m), dot_nt(dqkv_b, qkv_o)], 1)
    dxn1 = sum_rows(dxn1_part.astype(bf16)).astype(jnp.float32)
    norm1_grad = jnp.sum(dxn1 * normed1, 0)
    dscaled1 = dxn1 * gain1
    tokens_grad_own = dhidden + inverse1 * (
        dscaled1 - normed1 * jnp.mean(dscaled1 * normed1, -1, keepdims=True)
    )
    tokens_grad = lax.all_gather(
        own_half_first(tokens_grad_own), "experts", axis=0, tiled=True
    )

    bias_wide = jnp.zeros((group_size, parts, 3 * HEAD_DIM), jnp.float32)
    bias_wide = lax.dynamic_update_slice(bias_wide, bias_part[None, None], (group, place, 0))
    small = jnp.concatenate(
        [
            own_half_first(norm1_grad),
            own_half_first(norm2_grad),
            own_half_first(shared_gate_grad),
            own_half_first(router_grad.T).T.reshape(-1),
            bias_wide.reshape(-1),
        ]
    )
    small = lax.psum(small, ("dp", "context", "experts"))
    router_size = width * expert_count
    bias_sum = small[3 * width + router_size :].reshape(group_size, parts, 3, HEAD_DIM)
    bias_grad = jnp.transpose(
        lax.dynamic_slice_in_dim(bias_sum, group, 1, 0)[0], (1, 0, 2)
    ).reshape(3, parts * HEAD_DIM)

    def halves(first_half, second_half):
        return (first_half + swap_halves(second_half.astype(bf16)).astype(jnp.float32)).astype(bf16)

    down_grad = halves(
        dot_tn(act_c, grad_all[:, :half]), dot_tn(act_c, grad_all[:, half:])
    )
    down_grad = exchange(jnp.transpose(down_grad.reshape(span, parts, block), (1, 0, 2)))
    down_grad = jnp.transpose(
        down_grad.reshape(parts, stacks, hidden_here, block), (1, 0, 2, 3)
    ).reshape(stacks, parts * hidden_here, block).astype(jnp.float32)
    up_grad = halves(dot_tn(xn2[:, :half], dup), dot_tn(xn2[:, half:], dup))
    up_grad = exchange(up_grad.reshape(parts, block, 2 * span))
    up_grad = jnp.transpose(
        up_grad.reshape(parts, block, 2 * stacks, hidden_here), (2, 1, 0, 3)
    ).reshape(2 * stacks, block, parts * hidden_here).astype(jnp.float32)
    out_w_grad = halves(out_grad_part[:, :half], out_grad_part[:, half:])
    out_w_grad = exchange(
        jnp.transpose(out_w_grad.reshape(HEAD_DIM, parts, block), (1, 0, 2))
    ).reshape(parts * HEAD_DIM, block).astype(jnp.float32)
    qkv_grad = halves(qkv_grad[:half], qkv_grad[half:])
    qkv_grad = exchange(qkv_grad.reshape(parts, block, 3 * HEAD_DIM))
    qkv_grad = jnp.transpose(
        qkv_grad.reshape(parts, block, 3, HEAD_DIM), (1, 2, 0, 3)
    ).reshape(block, 3, parts * HEAD_DIM).astype(jnp.float32)

    return (
        block_out[None],
        tokens_grad[None],
        small[:width],
        qkv_grad,
        bias_grad,
        out_w_grad,
        small[width : 2 * width],
        small[3 * width : 3 * width + router_size].reshape(width, expert_count),
        up_grad[1:stacks],
        up_grad[stacks + 1 :],
        down_grad[1:],
        small[2 * width : 3 * width],
        up_grad[0],
        up_grad[stacks],
        down_grad[0],
    )


def plan_of(mesh):
    one_head_each = mesh.shape["context"] * mesh.shape["experts"] == 16
    return split_body if one_head_each and mesh.shape["dp"] == 2 else general_body


def solution(mesh):
    return jax.shard_map(
        plan_of(mesh),
        mesh=mesh,
        in_specs=(
            P("dp", "context", None),
            P("dp", "context"),
            P("dp", "context", None),
            P("dp", "context", None),
            P(),
            P(("dp", "context"), None, "experts"),
            P(None, "experts"),
            P("experts", ("dp", "context")),
            P(),
            P(),
            P("experts", ("dp", "context"), None),
            P("experts", ("dp", "context"), None),
            P("experts", None, ("dp", "context")),
            P(),
            P(("dp", "context"), "experts"),
            P(("dp", "context"), "experts"),
            P("experts", ("dp", "context")),
        ),
        out_specs=(
            P("dp", "context", None),
            P("dp", "context", None),
            P(),
            P(("dp", "context"), None, "experts"),
            P(None, "experts"),
            P("experts", ("dp", "context")),
            P(),
            P(),
            P("experts", ("dp", "context"), None),
            P("experts", ("dp", "context"), None),
            P("experts", None, ("dp", "context")),
            P(),
            P(("dp", "context"), "experts"),
            P(("dp", "context"), "experts"),
            P("experts", ("dp", "context")),
        ),
        check_vma=False,
    )
```

```python
import functools

import jax
import jax.numpy as jnp
from jax import lax
from jax.experimental import pallas as pl
from jax.experimental.pallas import tpu as pltpu
from jax.sharding import PartitionSpec as P

HEAD_DIM = 128


EPSILON = 1e-06
ROPE_BASE = 1000000.0
MASKED = -1e30
PRECISE = lax.Precision.HIGHEST


def rope_tables(position_ids):
    half_dim = HEAD_DIM // 2
    inverse = ROPE_BASE ** (-2.0 * jnp.arange(half_dim, dtype=jnp.float32) / HEAD_DIM)
    angles = position_ids.astype(jnp.float32)[:, None] * inverse[None, :]
    cosine = jnp.cos(angles)
    sine_part = jnp.sin(angles)
    return (
        jnp.concatenate([cosine, cosine], -1)[:, None, :],
        jnp.concatenate([sine_part, sine_part], -1)[:, None, :],
    )


def rotate(value):
    half_dim = value.shape[-1] // 2
    return jnp.concatenate([-value[..., half_dim:], value[..., :half_dim]], -1)


def rotate_back(value):
    half_dim = value.shape[-1] // 2
    return jnp.concatenate([value[..., half_dim:], -value[..., :half_dim]], -1)


def silu_grad(gate_vals):
    sigmoid_vals = jax.nn.sigmoid(gate_vals)
    return sigmoid_vals * (1.0 + gate_vals * (1.0 - sigmoid_vals))


def block_rank(route_rows, expert_count):
    hits = (
        route_rows[:, :, None] == jnp.arange(expert_count, dtype=jnp.int32)[None, None, :]
    ).astype(jnp.int32)
    flat_hits = hits.reshape(-1, expert_count)
    earlier = jnp.cumsum(flat_hits, axis=0) - flat_hits
    return jnp.sum(earlier * flat_hits, -1).reshape(route_rows.shape)


def block_width_of():
    return 512


def gather_weights(shard_set):
    return (
        lax.all_gather(shard_set[0], ("dp", "context"), axis=0, tiled=True),
        lax.all_gather(shard_set[1], ("dp", "context"), axis=1, tiled=True),
        lax.all_gather(shard_set[2], ("dp", "context"), axis=1, tiled=True),
        lax.all_gather(shard_set[3], ("dp", "context"), axis=1, tiled=True),
        lax.all_gather(shard_set[4], ("dp", "context"), axis=2, tiled=True),
        lax.all_gather(shard_set[5], ("dp", "context"), axis=0, tiled=True),
        lax.all_gather(shard_set[6], ("dp", "context"), axis=0, tiled=True),
        lax.all_gather(shard_set[7], ("dp", "context"), axis=1, tiled=True),
    )


def forward_fold(query, query_first, scale, carry, piece):
    row_count, head_count, head_size = query.shape
    query_index = query_first + jnp.arange(row_count, dtype=jnp.int32)
    query_last = query_first + row_count - 1
    key_part, value_part = piece
    piece_rows = key_part.shape[0]
    block_width = block_width_of()
    block_count = piece_rows // block_width
    key_blocks = key_part.reshape(block_count, block_width, head_count, head_size)
    value_blocks = value_part.reshape(block_count, block_width, head_count, head_size)
    offsets = block_width * jnp.arange(block_count, dtype=jnp.int32)

    def forward_visit(state, item):
        key_block, value_block, first_key = item

        def forward_compute(current):
            run_max, run_sum, accum = current
            scores = (
                jnp.einsum("qhd,khd->hqk", query, key_block, preferred_element_type=jnp.float32)
                * scale
            )
            key_index = first_key + jnp.arange(block_width, dtype=jnp.int32)
            allowed = key_index[None, None, :] <= query_index[None, :, None]
            new_max = jnp.maximum(run_max, jnp.max(jnp.where(allowed, scores, MASKED), -1))
            weights = jnp.where(allowed, jnp.exp(scores - new_max[..., None]), 0.0)
            factor = jnp.exp(run_max - new_max)
            new_sum = run_sum * factor + jnp.sum(weights, -1)
            new_accum = accum * factor[..., None] + jnp.einsum(
                "hqk,khd->hqd",
                weights.astype(jnp.bfloat16),
                value_block,
                preferred_element_type=jnp.float32,
            )
            return (new_max, new_sum, new_accum)

        return (
            lax.cond(first_key > query_last, lambda current: current, forward_compute, state),
            None,
        )

    carry, _ = lax.scan(forward_visit, carry, (key_blocks, value_blocks, offsets))
    return carry


def key_grad_fold(key_rows, value_rows, key_first, scale, carry, piece):
    row_count, head_count, head_size = key_rows.shape
    key_index = key_first + jnp.arange(row_count, dtype=jnp.int32)
    query_part, dout_part, lse_part, delta_part = piece
    piece_rows = query_part.shape[0]
    block_width = block_width_of()
    block_count = piece_rows // block_width
    query_blocks = query_part.reshape(block_count, block_width, head_count, head_size)
    dout_blocks = dout_part.reshape(block_count, block_width, head_count, head_size)
    lse_blocks = lse_part.reshape(block_count, block_width, head_count)
    delta_blocks = delta_part.reshape(block_count, block_width, head_count)
    offsets = block_width * jnp.arange(block_count, dtype=jnp.int32)

    def key_visit(state, item):
        query_block, dout_block, lse_block, delta_block, first_query = item

        def key_compute(current):
            dkey_sum, dvalue_sum = current
            query_b = query_block.astype(jnp.bfloat16)
            dout_b = dout_block.astype(jnp.bfloat16)
            scores = (
                jnp.einsum("qhd,khd->hqk", query_b, key_rows, preferred_element_type=jnp.float32)
                * scale
            )
            query_index = first_query + jnp.arange(block_width, dtype=jnp.int32)
            allowed = key_index[None, None, :] <= query_index[None, :, None]
            prob_att = jnp.where(
                allowed, jnp.exp(scores - jnp.transpose(lse_block)[:, :, None]), 0.0
            )
            dvalue_sum = dvalue_sum + jnp.einsum(
                "hqk,qhd->hkd",
                prob_att.astype(jnp.bfloat16),
                dout_b,
                preferred_element_type=jnp.float32,
            )
            dprob = jnp.einsum(
                "qhd,khd->hqk", dout_b, value_rows, preferred_element_type=jnp.float32
            )
            dscore = (prob_att * (dprob - jnp.transpose(delta_block)[:, :, None])).astype(
                jnp.bfloat16
            )
            dkey_sum = (
                dkey_sum
                + jnp.einsum("hqk,qhd->hkd", dscore, query_b, preferred_element_type=jnp.float32)
                * scale
            )
            return (dkey_sum, dvalue_sum)

        return (
            lax.cond(
                first_query + block_width - 1 < key_first,
                lambda current: current,
                key_compute,
                state,
            ),
            None,
        )

    carry, _ = lax.scan(
        key_visit, carry, (query_blocks, dout_blocks, lse_blocks, delta_blocks, offsets)
    )
    return carry


def query_grad_fold(query, dattended, lse_heads, delta_heads, query_first, scale, carry, piece):
    row_count, head_count, head_size = query.shape
    query_index = query_first + jnp.arange(row_count, dtype=jnp.int32)
    query_last = query_first + row_count - 1
    key_part, value_part = piece
    piece_rows = key_part.shape[0]
    block_width = block_width_of()
    block_count = piece_rows // block_width
    key_blocks = key_part.reshape(block_count, block_width, head_count, head_size)
    value_blocks = value_part.reshape(block_count, block_width, head_count, head_size)
    offsets = block_width * jnp.arange(block_count, dtype=jnp.int32)

    def query_visit(state, item):
        key_block, value_block, first_key = item

        def query_compute(current):
            scores = (
                jnp.einsum("qhd,khd->hqk", query, key_block, preferred_element_type=jnp.float32)
                * scale
            )
            key_index = first_key + jnp.arange(block_width, dtype=jnp.int32)
            allowed = key_index[None, None, :] <= query_index[None, :, None]
            prob_att = jnp.where(allowed, jnp.exp(scores - lse_heads[:, :, None]), 0.0)
            dprob = jnp.einsum(
                "qhd,khd->hqk", dattended, value_block, preferred_element_type=jnp.float32
            )
            dscore = (prob_att * (dprob - delta_heads[:, :, None])).astype(jnp.bfloat16)
            return (
                current
                + jnp.einsum("hqk,khd->hqd", dscore, key_block, preferred_element_type=jnp.float32)
                * scale
            )

        return (
            lax.cond(first_key > query_last, lambda current: current, query_compute, state),
            None,
        )

    carry, _ = lax.scan(query_visit, carry, (key_blocks, value_blocks, offsets))
    return carry


def general_body(
    tokens,
    positions,
    routes,
    out_grad,
    norm1_gain,
    qkv_weight,
    qkv_bias,
    out_weight,
    norm2_gain,
    router_weight,
    expert_gate,
    expert_up,
    expert_down,
    shared_gate,
    shared_w_gate,
    shared_w_up,
    shared_w_down,
):
    row_count = tokens.shape[1]
    model_width = tokens.shape[2]
    head_span = qkv_bias.shape[1]
    heads_here = head_span // HEAD_DIM
    local_experts = expert_gate.shape[0]
    group_size = lax.axis_size("experts")
    quarter = row_count // group_size
    capacity = 3 * quarter // 4
    expert_count = local_experts * group_size
    group_index = lax.axis_index("experts")
    scale = HEAD_DIM ** (-0.5)
    shard_set = (
        qkv_weight,
        out_weight,
        expert_gate,
        expert_up,
        expert_down,
        shared_w_gate,
        shared_w_up,
        shared_w_down,
    )
    qkv_full, out_full, gate_full, up_full, down_full, sgate_full, sup_full, sdown_full = (
        gather_weights(shard_set)
    )
    token_float = tokens[0].astype(jnp.float32)
    inverse1 = lax.rsqrt(jnp.mean(token_float * token_float, -1, keepdims=True) + EPSILON)
    normed1 = token_float * inverse1
    gain1 = norm1_gain.astype(jnp.float32)
    normed1_b = (normed1 * gain1).astype(jnp.bfloat16)
    qkv_flat = qkv_full.reshape(model_width, 3 * head_span)
    qkv = (
        jnp.dot(normed1_b, qkv_flat, preferred_element_type=jnp.float32).reshape(
            row_count, 3, head_span
        )
        + qkv_bias.astype(jnp.float32)[None]
    )
    cosine, sine_part = rope_tables(positions[0])
    query_raw = qkv[:, 0].reshape(row_count, heads_here, HEAD_DIM)
    key_raw = qkv[:, 1].reshape(row_count, heads_here, HEAD_DIM)
    query = (query_raw * cosine + rotate(query_raw) * sine_part).astype(jnp.bfloat16)
    key_rows = (key_raw * cosine + rotate(key_raw) * sine_part).astype(jnp.bfloat16)
    value_flat = qkv[:, 2].astype(jnp.bfloat16)
    key_flat = key_rows.reshape(row_count, head_span)
    value_rows = value_flat.reshape(row_count, heads_here, HEAD_DIM)
    query_first = lax.axis_index("context") * row_count
    start_state = (
        jnp.full((heads_here, row_count), MASKED, jnp.float32),
        jnp.zeros((heads_here, row_count), jnp.float32),
        jnp.zeros((heads_here, row_count, HEAD_DIM), jnp.float32),
    )
    run_max, run_sum, accum = forward_fold(
        query,
        query_first,
        scale,
        start_state,
        (
            lax.all_gather(key_flat, "context", axis=0, tiled=True),
            lax.all_gather(value_flat, "context", axis=0, tiled=True),
        ),
    )
    attended = jnp.transpose(accum / run_sum[..., None], (1, 0, 2)).astype(jnp.bfloat16)
    lse_heads = run_max + jnp.log(run_sum)
    attended_flat = attended.reshape(row_count, head_span)
    head_part = jnp.dot(attended_flat, out_full, preferred_element_type=jnp.float32)
    hidden = token_float + lax.psum(head_part, "experts")
    inverse2 = lax.rsqrt(jnp.mean(hidden * hidden, -1, keepdims=True) + EPSILON)
    normed2 = hidden * inverse2
    gain2 = norm2_gain.astype(jnp.float32)
    normed2_b = (normed2 * gain2).astype(jnp.bfloat16)
    first_row = group_index * quarter
    normed2_q = lax.dynamic_slice_in_dim(normed2_b, first_row, quarter, 0)
    route_q = lax.dynamic_slice_in_dim(routes[0], first_row, quarter, 0)
    logits = jnp.dot(normed2_q, router_weight, preferred_element_type=jnp.float32)
    prob = jax.nn.softmax(logits, -1)
    gate_k = jnp.take_along_axis(prob, route_q, 1)
    slot_ids = route_q * capacity + block_rank(route_q, expert_count)
    slot_hits = (
        slot_ids[:, :, None] == jnp.arange(expert_count * capacity, dtype=jnp.int32)[None, None, :]
    )
    placer = jnp.sum(slot_hits.astype(jnp.bfloat16), 1)
    send_rows = (
        jnp.dot(placer.T, normed2_q, preferred_element_type=jnp.float32)
        .astype(jnp.bfloat16)
        .reshape(group_size, local_experts, capacity, model_width)
    )
    arrived = lax.all_to_all(send_rows, "experts", split_axis=0, concat_axis=0, tiled=True)
    expert_gvals = jnp.einsum(
        "secd,edf->secf", arrived, gate_full, preferred_element_type=jnp.float32
    )
    expert_uvals = jnp.einsum(
        "secd,edf->secf", arrived, up_full, preferred_element_type=jnp.float32
    )
    expert_act = (jax.nn.silu(expert_gvals) * expert_uvals).astype(jnp.bfloat16)
    expert_out = jnp.einsum(
        "secf,efd->secd", expert_act, down_full, preferred_element_type=jnp.float32
    ).astype(jnp.bfloat16)
    returned = lax.all_to_all(
        expert_out, "experts", split_axis=0, concat_axis=0, tiled=True
    ).reshape(expert_count * capacity, model_width)
    picked = returned[slot_ids].astype(jnp.float32)
    routed = jnp.sum(gate_k[:, :, None] * picked, 1)
    shared_sig = jax.nn.sigmoid(
        jnp.dot(normed2_b, shared_gate[:, None], preferred_element_type=jnp.float32)[:, 0]
    )
    shared_gvals = jnp.dot(normed2_b, sgate_full, preferred_element_type=jnp.float32)
    shared_uvals = jnp.dot(normed2_b, sup_full, preferred_element_type=jnp.float32)
    shared_act = (jax.nn.silu(shared_gvals) * shared_uvals).astype(jnp.bfloat16)
    shared_part = jnp.dot(shared_act, sdown_full, preferred_element_type=jnp.float32)
    routed_pad = lax.dynamic_update_slice_in_dim(
        jnp.zeros((row_count, model_width), jnp.float32), routed, first_row, 0
    )
    branch_total = lax.psum(
        (shared_sig[:, None] * shared_part + routed_pad).astype(jnp.bfloat16), "experts"
    ).astype(jnp.float32)
    block_out = (hidden + branch_total).astype(jnp.bfloat16)
    held = lax.optimization_barrier((shard_set, block_out))
    qkv_full, out_full, gate_full, up_full, down_full, sgate_full, sup_full, sdown_full = (
        gather_weights(held[0])
    )
    qkv_flat = qkv_full.reshape(model_width, 3 * head_span)
    grad_float = out_grad[0].astype(jnp.float32)
    grad_q = lax.dynamic_slice_in_dim(grad_float, first_row, quarter, 0)
    dgate_k = jnp.sum(grad_q[:, None, :] * picked, -1)
    weighted = jnp.sum(slot_hits.astype(jnp.float32) * gate_k[:, :, None], 1)
    dsend = (
        jnp.dot(weighted.T, grad_q, precision=PRECISE)
        .astype(jnp.bfloat16)
        .reshape(group_size, local_experts, capacity, model_width)
    )
    darrived = lax.all_to_all(dsend, "experts", split_axis=0, concat_axis=0, tiled=True)
    expert_dact = jnp.einsum(
        "secd,efd->secf", darrived, down_full, preferred_element_type=jnp.float32
    )
    down_grad = jnp.einsum(
        "secf,secd->efd", expert_act, darrived, preferred_element_type=jnp.float32
    )
    expert_dgate = (expert_dact * expert_uvals * silu_grad(expert_gvals)).astype(jnp.bfloat16)
    expert_dup = (expert_dact * jax.nn.silu(expert_gvals)).astype(jnp.bfloat16)
    gate_grad = jnp.einsum(
        "secd,secf->edf", arrived, expert_dgate, preferred_element_type=jnp.float32
    )
    up_grad = jnp.einsum("secd,secf->edf", arrived, expert_dup, preferred_element_type=jnp.float32)
    expert_din = (
        jnp.einsum("secf,edf->secd", expert_dgate, gate_full, preferred_element_type=jnp.float32)
        + jnp.einsum("secf,edf->secd", expert_dup, up_full, preferred_element_type=jnp.float32)
    ).astype(jnp.bfloat16)
    dreturned = lax.all_to_all(
        expert_din, "experts", split_axis=0, concat_axis=0, tiled=True
    ).reshape(expert_count * capacity, model_width)
    dnormed2_q = jnp.dot(placer, dreturned, preferred_element_type=jnp.float32)
    route_hits = (
        route_q[:, :, None] == jnp.arange(expert_count, dtype=jnp.int32)[None, None, :]
    ).astype(jnp.float32)
    dprob = jnp.sum(route_hits * dgate_k[:, :, None], 1)
    dlogit = prob * (dprob - jnp.sum(prob * dprob, -1, keepdims=True))
    router_part = jnp.dot(normed2_q.astype(jnp.float32).T, dlogit, precision=PRECISE)
    dnormed2_q = dnormed2_q + jnp.dot(
        dlogit, router_weight.astype(jnp.float32).T, precision=PRECISE
    )
    shared_dout = (shared_sig[:, None] * grad_float).astype(jnp.bfloat16)
    shared_dact = jnp.dot(shared_dout, sdown_full.T, preferred_element_type=jnp.float32)
    sdown_grad = jnp.dot(shared_act.T, shared_dout, preferred_element_type=jnp.float32)
    shared_dgate = (shared_dact * shared_uvals * silu_grad(shared_gvals)).astype(jnp.bfloat16)
    shared_dup = (shared_dact * jax.nn.silu(shared_gvals)).astype(jnp.bfloat16)
    sgate_grad = jnp.dot(normed2_b.T, shared_dgate, preferred_element_type=jnp.float32)
    sup_grad = jnp.dot(normed2_b.T, shared_dup, preferred_element_type=jnp.float32)
    row_dots = jnp.sum(grad_float * shared_part, -1)
    dnormed2_part = jnp.dot(
        shared_dgate, sgate_full.T, preferred_element_type=jnp.float32
    ) + jnp.dot(shared_dup, sup_full.T, preferred_element_type=jnp.float32)
    dnormed2_part = dnormed2_part + lax.dynamic_update_slice_in_dim(
        jnp.zeros((row_count, model_width), jnp.float32), dnormed2_q, first_row, 0
    )
    dnormed2, row_dots, router_grad = lax.psum((dnormed2_part, row_dots, router_part), "experts")
    coef = shared_sig * (1.0 - shared_sig) * row_dots
    dnormed2 = dnormed2 + coef[:, None] * shared_gate.astype(jnp.float32)[None, :]
    shared_gate_grad = jnp.dot(coef, normed2_b.astype(jnp.float32), precision=PRECISE)
    norm2_grad = jnp.sum(dnormed2 * normed2, 0)
    dscaled2 = dnormed2 * gain2
    dhidden = grad_float + inverse2 * (
        dscaled2 - normed2 * jnp.mean(dscaled2 * normed2, -1, keepdims=True)
    )
    dhidden_b = dhidden.astype(jnp.bfloat16)
    out_grad_part = jnp.dot(attended_flat.T, dhidden_b, preferred_element_type=jnp.float32)
    dattended = jnp.dot(dhidden_b, out_full.T, preferred_element_type=jnp.float32).astype(
        jnp.bfloat16
    )
    dattended3 = dattended.reshape(row_count, heads_here, HEAD_DIM)
    delta = jnp.sum(dattended3.astype(jnp.float32) * attended.astype(jnp.float32), -1)
    zero_state = jnp.zeros((heads_here, row_count, HEAD_DIM), jnp.float32)
    dkey_sum, dvalue_sum = key_grad_fold(
        key_rows,
        value_rows,
        query_first,
        scale,
        (zero_state, zero_state),
        (
            lax.all_gather(
                query.reshape(row_count, head_span).astype(jnp.float32),
                "context",
                axis=0,
                tiled=True,
            ),
            lax.all_gather(dattended.astype(jnp.float32), "context", axis=0, tiled=True),
            lax.all_gather(jnp.transpose(lse_heads), "context", axis=0, tiled=True),
            lax.all_gather(delta, "context", axis=0, tiled=True),
        ),
    )
    dquery_sum = query_grad_fold(
        query,
        dattended3,
        lse_heads,
        jnp.transpose(delta),
        query_first,
        scale,
        zero_state,
        (
            lax.all_gather(key_flat, "context", axis=0, tiled=True),
            lax.all_gather(value_flat, "context", axis=0, tiled=True),
        ),
    )
    dquery = jnp.transpose(dquery_sum, (1, 0, 2))
    dkey = jnp.transpose(dkey_sum, (1, 0, 2))
    dvalue = jnp.transpose(dvalue_sum, (1, 0, 2))
    dquery_raw = dquery * cosine + rotate_back(dquery * sine_part)
    dkey_raw = dkey * cosine + rotate_back(dkey * sine_part)
    dqkv = jnp.stack(
        [
            dquery_raw.reshape(row_count, head_span),
            dkey_raw.reshape(row_count, head_span),
            dvalue.reshape(row_count, head_span),
        ],
        1,
    )
    bias_grad = jnp.sum(dqkv, 0)
    dqkv_b = dqkv.astype(jnp.bfloat16).reshape(row_count, 3 * head_span)
    qkv_grad = jnp.dot(normed1_b.T, dqkv_b, preferred_element_type=jnp.float32).reshape(
        model_width, 3, head_span
    )
    dnormed1 = lax.psum(
        jnp.dot(dqkv_b, qkv_flat.T, preferred_element_type=jnp.float32).astype(jnp.bfloat16),
        "experts",
    ).astype(jnp.float32)
    norm1_grad = jnp.sum(dnormed1 * normed1, 0)
    dscaled1 = dnormed1 * gain1
    tokens_grad = dhidden + inverse1 * (
        dscaled1 - normed1 * jnp.mean(dscaled1 * normed1, -1, keepdims=True)
    )
    small_sums = (
        lax.psum(norm1_grad.astype(jnp.bfloat16), ("dp", "context")).astype(jnp.float32),
        lax.psum(norm2_grad.astype(jnp.bfloat16), ("dp", "context")).astype(jnp.float32),
        lax.psum(router_grad.astype(jnp.bfloat16), ("dp", "context")).astype(jnp.float32),
        lax.psum(shared_gate_grad.astype(jnp.bfloat16), ("dp", "context")).astype(jnp.float32),
        lax.psum(bias_grad.astype(jnp.bfloat16), ("dp", "context")).astype(jnp.float32),
    )
    large_sums = (
        lax.psum_scatter(
            qkv_grad.astype(jnp.bfloat16), ("dp", "context"), scatter_dimension=0, tiled=True
        ).astype(jnp.float32),
        lax.psum_scatter(
            out_grad_part.astype(jnp.bfloat16), ("dp", "context"), scatter_dimension=1, tiled=True
        ).astype(jnp.float32),
        lax.psum_scatter(
            gate_grad.astype(jnp.bfloat16), ("dp", "context"), scatter_dimension=1, tiled=True
        ).astype(jnp.float32),
        lax.psum_scatter(
            up_grad.astype(jnp.bfloat16), ("dp", "context"), scatter_dimension=1, tiled=True
        ).astype(jnp.float32),
        lax.psum_scatter(
            down_grad.astype(jnp.bfloat16), ("dp", "context"), scatter_dimension=2, tiled=True
        ).astype(jnp.float32),
        lax.psum_scatter(
            sgate_grad.astype(jnp.bfloat16), ("dp", "context"), scatter_dimension=0, tiled=True
        ).astype(jnp.float32),
        lax.psum_scatter(
            sup_grad.astype(jnp.bfloat16), ("dp", "context"), scatter_dimension=0, tiled=True
        ).astype(jnp.float32),
        lax.psum_scatter(
            sdown_grad.astype(jnp.bfloat16), ("dp", "context"), scatter_dimension=1, tiled=True
        ).astype(jnp.float32),
    )
    return (
        block_out[None],
        tokens_grad[None],
        small_sums[0],
        large_sums[0],
        small_sums[4],
        large_sums[1],
        small_sums[1],
        small_sums[2],
        large_sums[2],
        large_sums[3],
        large_sums[4],
        small_sums[3],
        large_sums[5],
        large_sums[6],
        large_sums[7],
    )


def own_half_first(value):
    half = value.shape[-1] // 2
    turned = jnp.concatenate([value[..., half:], value[..., :half]], -1)
    return jnp.where(lax.axis_index("dp") == 0, value, turned)


def dot_nn(left, right):
    return jnp.dot(left, right, preferred_element_type=jnp.float32)


def dot_nt(left, right):
    return lax.dot_general(
        left, right, (((1,), (1,)), ((), ())), preferred_element_type=jnp.float32
    )


def dot_tn(left, right):
    return lax.dot_general(
        left, right, (((0,), (0,)), ((), ())), preferred_element_type=jnp.float32
    )


MESH = pl.DeviceIdType.MESH
DMA = pltpu.SemaphoreType.DMA


def remote(source, target, send_sem, recv_sem, device):
    return pltpu.make_async_remote_copy(
        src_ref=source,
        dst_ref=target,
        send_sem=send_sem,
        recv_sem=recv_sem,
        device_id=device,
        device_id_type=MESH,
    )


def rows_at(ref, start, size):
    return ref.at[pl.ds(pl.multiple_of(start, 16), size), :]


def lanes_at(ref, start, size):
    return ref.at[:, pl.ds(pl.multiple_of(start, 128), size)]


class Spot:
    def __init__(self):
        self.parts = lax.axis_size("context")
        self.place, self.group = lax.axis_index("context"), lax.axis_index("experts")
        self.twin = {"dp": 1 - lax.axis_index("dp")}
        self.across = lax.rem(self.group + 2, 4)
        self.beside = self.group + 1 - 2 * lax.rem(self.group, 2)
        self.corner = lax.rem(self.beside + 2, 4)
        self.has_left, self.has_right = self.place > 0, self.place < self.parts - 1

    def greet(self, whole_line, twins):
        barrier = pltpu.get_barrier_semaphore()
        devices = [{"experts": self.across}, {"experts": self.beside}]
        if twins:
            devices.append(self.twin)
        for device in devices:
            pl.semaphore_signal(barrier, inc=1, device_id=device, device_id_type=MESH)
        count = len(devices)
        if whole_line:
            for gap in range(1, self.parts):
                device = {"context": lax.rem(self.place + gap, self.parts)}
                pl.semaphore_signal(barrier, inc=1, device_id=device, device_id_type=MESH)
            pl.semaphore_wait(barrier, count + self.parts - 1)
        else:
            for step, there in ((-1, self.has_left), (1, self.has_right)):

                @pl.when(there)
                def _():
                    device = {"context": self.place + step}
                    pl.semaphore_signal(barrier, inc=1, device_id=device, device_id_type=MESH)

            ends = jnp.where(self.has_left & self.has_right, 0, 1)
            pl.semaphore_wait(barrier, count + 2 - ends)

    def far_first(self):
        upper = self.place // (self.parts // 2)
        return [3 * (1 - upper), 2 - upper, 1 + 4 * upper - self.place, self.place]

    def others(self, gap, body):
        @pl.when(self.place >= gap)
        def _():
            body(self.place - gap)

        @pl.when(self.place + gap < self.parts)
        def _():
            body(self.place + gap)


class Share:
    def __init__(self, spot, own, out, sems):
        self.spot, self.own, self.out = spot, own, out
        self.local_sem, self.right_s, self.left_s, self.line_r, self.across_s, self.across_r, self.beside_s, self.beside_r = sems

    @staticmethod
    def sems(parts):
        return [DMA, DMA((parts,)), DMA((parts,)), DMA((parts,)), DMA((parts,)), DMA((parts,)), DMA((2 * parts,)), DMA((2 * parts,))]

    def block(self, part, column):
        rows = self.own.shape[0]
        return rows_at(self.out, (part * 4 + column) * rows, rows)

    def to_right(self, part, source):
        s = self.spot
        return remote(source, self.block(part, s.group), self.right_s.at[part], self.line_r.at[part], {"context": s.place + 1})

    def to_left(self, part, source):
        s = self.spot
        return remote(source, self.block(part, s.group), self.left_s.at[part], self.line_r.at[part], {"context": s.place - 1})

    def to_across(self, part, source):
        s = self.spot
        return remote(source, self.block(part, s.group), self.across_s.at[part], self.across_r.at[part], {"experts": s.across})

    def to_beside(self, part, column, slot, source):
        s = self.spot
        return remote(source, self.block(part, column), self.beside_s.at[slot], self.beside_r.at[slot], {"experts": s.beside})

    def begin(self):
        s = self.spot

        @pl.when(s.has_right)
        def _():
            self.to_right(s.place, self.own).start()

        @pl.when(s.has_left)
        def _():
            self.to_left(s.place, self.own).start()

        self.to_across(s.place, self.own).start()
        self.to_beside(s.place, s.group, s.place, self.own).start()
        self.local().start()

    def local(self):
        return pltpu.make_async_copy(self.own, self.block(self.spot.place, self.spot.group), self.local_sem)

    def pass_on(self, part):
        s = self.spot
        self.to_across(part, self.block(part, s.group)).wait_recv()
        self.to_beside(part, s.across, s.parts + part, self.block(part, s.across)).start()

    def arrival(self, part, onward, there):
        s = self.spot
        mine = self.block(part, s.group)
        self.to_right(part, mine).wait_recv()

        @pl.when(there)
        def _():
            onward(part, mine).start()

        self.to_across(part, mine).start()
        self.to_beside(part, s.group, part, mine).start()

    def step(self, gap):
        s = self.spot

        @pl.when(s.place >= gap)
        def _():
            self.arrival(s.place - gap, self.to_right, s.has_right)

        @pl.when(s.place + gap < s.parts)
        def _():
            self.arrival(s.place + gap, self.to_left, s.has_left)

        if gap == 1:
            self.pass_on(s.place)
        else:
            s.others(gap - 1, self.pass_on)

    def end(self):
        s = self.spot
        s.others(s.parts - 1, self.pass_on)
        self.local().wait()
        for part in range(s.parts):
            self.to_beside(part, s.beside, part, self.own).wait_recv()
            self.to_beside(part, s.beside, s.parts + part, self.own).wait_recv()
            self.to_across(part, self.own).wait_send()
            self.to_beside(part, s.group, part, self.own).wait_send()
            self.to_beside(part, s.group, s.parts + part, self.own).wait_send()

            @pl.when(s.has_right & (part <= s.place))
            def _():
                self.to_right(part, self.own).wait_send()

            @pl.when(s.has_left & (part >= s.place))
            def _():
                self.to_left(part, self.own).wait_send()


class Sum:
    def __init__(self, spot, part_ref, out, scratch):
        self.spot, self.part_ref, self.out = spot, part_ref, out
        (self.beside_buf, self.across_out, self.across_buf, self.line_out, self.left_buf, self.right_buf,
         self.beside_s, self.beside_r, self.across_s, self.across_r, self.right_s, self.left_s, self.from_left, self.from_right) = scratch
        self.order = spot.far_first()

    @staticmethod
    def scratch(parts, rows, width):
        one = pltpu.VMEM((parts, rows, width), jnp.bfloat16)
        two = pltpu.VMEM((2 * parts, rows, width), jnp.bfloat16)
        return [two, one, one, one, one, one, DMA((2 * parts,)), DMA((2 * parts,))] + [DMA((parts,))] * 6

    def base(self, part, column):
        rows = self.out.shape[0]
        return pl.multiple_of((part * 4 + column) * rows, rows)

    def to_beside(self, part, column, slot):
        source = self.part_ref.at[pl.ds(self.base(part, column), self.out.shape[0]), :]
        return remote(source, self.beside_buf.at[slot], self.beside_s.at[slot], self.beside_r.at[slot], {"experts": self.spot.beside})

    def to_across(self, part):
        return remote(self.across_out.at[part], self.across_buf.at[part], self.across_s.at[part], self.across_r.at[part], {"experts": self.spot.across})

    def to_right(self, part):
        return remote(self.line_out.at[part], self.left_buf.at[part], self.right_s.at[part], self.from_left.at[part], {"context": self.spot.place + 1})

    def to_left(self, part):
        return remote(self.line_out.at[part], self.right_buf.at[part], self.left_s.at[part], self.from_right.at[part], {"context": self.spot.place - 1})

    def chunks(self, body):
        step = 16

        def one(index, carry):
            start = pl.multiple_of(index * step, step)
            body(pl.ds(start, step), start, step)
            return carry

        lax.fori_loop(0, self.out.shape[0] // step, one, 0)

    def mine(self, base, start, step):
        return self.part_ref[pl.ds(pl.multiple_of(base + start, step), step), :].astype(jnp.float32)

    def begin(self):
        s = self.spot
        for part in self.order:
            self.to_beside(part, s.corner, s.parts + part).start()
        for part in self.order:
            self.to_beside(part, s.beside, part).start()

    def cross(self, index):
        s, part = self.spot, self.order[index]
        self.to_beside(part, s.corner, s.parts + part).wait_recv()
        base = self.base(part, s.across)

        def add(at, start, step):
            total = self.mine(base, start, step) + self.beside_buf[s.parts + part, at, :].astype(jnp.float32)
            self.across_out[part, at, :] = total.astype(jnp.bfloat16)

        self.chunks(add)
        self.to_across(part).start()

    def line(self, index):
        s, part = self.spot, self.order[index]
        self.to_beside(part, s.beside, part).wait_recv()
        self.to_across(part).wait_recv()
        base = self.base(part, s.group)
        f32 = jnp.float32

        def total(at, start, step):
            return self.mine(base, start, step) + self.beside_buf[part, at, :].astype(f32) + self.across_buf[part, at, :].astype(f32)

        def send(buf):
            def add(at, start, step):
                value = total(at, start, step)
                if buf is not None:
                    value = value + buf[part, at, :].astype(f32)
                self.line_out[part, at, :] = value.astype(jnp.bfloat16)

            self.chunks(add)

        if index < s.parts - 1:
            goes_right = part > s.place
            goes_left = jnp.logical_not(goes_right)

            @pl.when(goes_right & s.has_left)
            def _():
                self.to_right(part).wait_recv()
                send(self.left_buf)

            @pl.when(goes_left & s.has_right)
            def _():
                self.to_left(part).wait_recv()
                send(self.right_buf)

            @pl.when((goes_right & jnp.logical_not(s.has_left)) | (goes_left & jnp.logical_not(s.has_right)))
            def _():
                send(None)

            @pl.when(goes_right)
            def _():
                self.to_right(part).start()

            @pl.when(goes_left)
            def _():
                self.to_left(part).start()
        else:

            def keep(at, start, step):
                self.out[at, :] = total(at, start, step)

            self.chunks(keep)
            for there, copy, buf in ((s.has_left, self.to_right, self.left_buf), (s.has_right, self.to_left, self.right_buf)):

                @pl.when(there)
                def _():
                    copy(part).wait_recv()

                    def add(at, start, step):
                        self.out[at, :] = self.out[at, :] + buf[part, at, :].astype(f32)

                    self.chunks(add)

    def end(self):
        s = self.spot
        for part in range(s.parts):
            self.to_beside(part, s.corner, s.parts + part).wait_send()
            self.to_beside(part, s.beside, part).wait_send()
            self.to_across(part).wait_send()

            @pl.when(part > s.place)
            def _():
                self.to_right(part).wait_send()

            @pl.when(part < s.place)
            def _():
                self.to_left(part).wait_send()


class Move:
    def __init__(self, spot, items, sems):
        self.spot, self.items = spot, items
        self.line_s, self.line_r, self.twin_s, self.twin_r, self.local_sem = sems

    @staticmethod
    def sems(count, parts):
        return [DMA((count * parts,))] * 4 + [DMA((count,))]

    def to(self, number, target, source):
        s, (src, dst) = self.spot, self.items[number]
        return remote(src(target), dst(0, source), self.line_s.at[number * s.parts + target], self.line_r.at[number * s.parts + source], {"context": target})

    def on(self, number, source, view):
        s, (_, dst) = self.spot, self.items[number]
        slot = number * s.parts + source
        return remote(view, dst(1, source), self.twin_s.at[slot], self.twin_r.at[slot], s.twin)

    def local(self, number):
        s, (src, dst) = self.spot, self.items[number]
        return pltpu.make_async_copy(src(s.place), dst(0, s.place), self.local_sem.at[number])

    def own(self, number):
        s, (src, _) = self.spot, self.items[number]
        self.on(number, s.place, src(s.place)).start()
        self.local(number).start()

    def send(self, number):
        s = self.spot
        for gap in range(s.parts - 1, 0, -1):
            s.others(gap, lambda target: self.to(number, target, s.place).start())

    def forward(self, number, gap):
        s, (_, dst) = self.spot, self.items[number]

        def one(source):
            self.to(number, s.place, source).wait_recv()
            self.on(number, source, dst(0, source)).start()

        s.others(gap, one)

    def end(self):
        s = self.spot
        for number, (src, dst) in enumerate(self.items):
            self.local(number).wait()
            for part in range(s.parts):
                self.on(number, part, dst(0, part)).wait()

                @pl.when(part != s.place)
                def _():
                    self.to(number, part, s.place).wait_send()


class Return:
    def __init__(self, spot, items, got, mine, sems):
        self.spot, self.items, self.got, self.mine_buf = spot, items, got, mine
        self.twin_s, self.twin_r, self.load, self.line_s, self.line_r, self.local_sem = sems
        self.order = spot.far_first()
        self.bases = []
        for item in items:
            self.bases.append(self.bases[-1][1] if self.bases else 0)
            self.bases[-1] = (self.bases[-1], self.bases[-1] + len(item["pieces"]) * spot.parts)

    @staticmethod
    def scratch(shapes, pieces, parts):
        count = len(shapes)
        buf = [pltpu.VMEM((parts,) + shape, jnp.bfloat16) for shape in shapes]
        sems = [DMA((count * parts,))] * 3 + [DMA((sum(pieces) * parts,))] * 2 + [DMA((sum(pieces),))]
        return buf + buf + sems

    def swap(self, number, part):
        item, slot = self.items[number], number * self.spot.parts + part
        return remote(item["block"](1, part), self.got[number].at[part], self.twin_s.at[slot], self.twin_r.at[slot], self.spot.twin)

    def fetch(self, number, part):
        item, slot = self.items[number], number * self.spot.parts + part
        return pltpu.make_async_copy(item["block"](0, part), self.mine_buf[number].at[part], self.load.at[slot])

    def start(self, number):
        for part in self.order:
            self.swap(number, part).start()
            self.fetch(number, part).start()

    def piece(self, number, which, target, source, short):
        s = self.spot
        cut, out = self.items[number]["pieces"][which]
        slot = self.bases[number][0] + which * s.parts
        return remote(cut(self.mine_buf[number].at[target], short), out(source, short), self.line_s.at[slot + target], self.line_r.at[slot + source], {"context": target})

    def keep(self, number, which, short):
        s = self.spot
        cut, out = self.items[number]["pieces"][which]
        slot = self.bases[number][0] // s.parts + which
        return pltpu.make_async_copy(cut(self.mine_buf[number].at[s.place], short), out(s.place, short), self.local_sem.at[slot])

    def by_width(self, source, body):
        last = source == self.spot.parts - 1
        if not isinstance(source, int):

            @pl.when(last)
            def _():
                body(True)

            @pl.when(jnp.logical_not(last))
            def _():
                body(False)
        else:
            body(last)

    def reduce(self, number, index):
        s, part = self.spot, self.order[index]
        item = self.items[number]
        self.swap(number, part).wait_recv()
        self.fetch(number, part).wait()
        mine, got = self.mine_buf[number], self.got[number]
        rows, step = mine.shape[1], 32

        def one(at, carry):
            span = pl.ds(pl.multiple_of(at * step, step), step)
            total = mine[part, span, :].astype(jnp.float32) + got[part, span, :].astype(jnp.float32)
            mine[part, span, :] = total.astype(jnp.bfloat16)
            return carry

        lax.fori_loop(0, rows // step, one, 0)
        for which in range(len(item["pieces"])):
            if index < s.parts - 1:
                self.by_width(s.place, lambda short: self.piece(number, which, part, s.place, short).start())
            else:
                self.by_width(s.place, lambda short: self.keep(number, which, short).start())

    def end(self):
        s = self.spot
        for number, item in enumerate(self.items):
            for part in range(s.parts):
                self.swap(number, part).wait_send()
                for which in range(len(item["pieces"])):

                    @pl.when(part != s.place)
                    def _():
                        self.by_width(s.place, lambda short: self.piece(number, which, part, s.place, short).wait_send())
                        self.by_width(part, lambda short: self.piece(number, which, s.place, part, short).wait_recv())

            for which in range(len(item["pieces"])):
                self.by_width(s.place, lambda short: self.keep(number, which, short).wait())


def comm_call(kernel, number, name, out_shape, out_specs, in_specs, scratch, bytes_moved):
    return pl.pallas_call(
        kernel,
        out_shape=out_shape,
        in_specs=in_specs,
        out_specs=out_specs,
        scratch_shapes=scratch,
        compiler_params=pltpu.CompilerParams(collective_id=number, has_side_effects=True),
        cost_estimate=pl.CostEstimate(flops=0, bytes_accessed=bytes_moved, transcendentals=0),
        name=name,
    )


IN_VMEM = pl.BlockSpec(memory_space=pltpu.VMEM)
IN_PLACE = pl.BlockSpec(memory_space=pl.ANY)
WINDOW = 384


def window_of(index, length):
    return jnp.minimum(index * WINDOW, length - WINDOW)


def share_first(value, qkv_in, out_weight, number):
    parts = lax.axis_size("context")
    rows, width = value.shape
    block, span = qkv_in.shape[0] // parts, qkv_in.shape[1]
    head, lanes = out_weight.shape[0] // parts, out_weight.shape[1]
    share_sems, move_sems = Share.sems(parts), Move.sems(2, parts)

    def kernel(own_ref, qkv_ref, outw_ref, all_ref, wqkv_ref, wout_ref, *sems):
        spot = Spot()
        share = Share(spot, own_ref, all_ref, sems[: len(share_sems)])
        items = [
            (
                lambda target: rows_at(qkv_ref, target * block, block),
                lambda side, source: rows_at(wqkv_ref, (side * parts + source) * block, block),
            ),
            (
                lambda target: rows_at(outw_ref, target * head, head),
                lambda side, source: lanes_at(wout_ref, (side * parts + source) * lanes, lanes),
            ),
        ]
        move = Move(spot, items, sems[len(share_sems) :])
        spot.greet(True, True)
        share.begin()
        for item in range(2):
            move.own(item)
        move.send(0)
        share.step(1)
        move.send(1)
        move.forward(0, 1)
        share.step(2)
        move.forward(0, 2)
        share.step(3)
        move.forward(0, 3)
        for gap in (1, 2, 3):
            move.forward(1, gap)
        share.end()
        move.end()

    bf16 = jnp.bfloat16
    return comm_call(
        kernel,
        number,
        "share_first",
        [
            jax.ShapeDtypeStruct((rows * parts * 4, width), value.dtype),
            jax.ShapeDtypeStruct((2 * parts * block, span), bf16),
            jax.ShapeDtypeStruct((head, 2 * parts * lanes), bf16),
        ],
        [IN_PLACE] * 3,
        [IN_VMEM, IN_PLACE, IN_PLACE],
        share_sems + move_sems,
        180_000_000,
    )(value, qkv_in, out_weight)


def sum_and_move(value, shared_down, expert_down, number):
    parts = lax.axis_size("context")
    total, width = value.shape
    rows = total // (4 * parts)
    hidden, lanes = shared_down.shape
    count = 1 + expert_down.shape[0]
    sum_scratch, move_sems = Sum.scratch(parts, rows, width), Move.sems(count, parts)

    def kernel(part_ref, shared_ref, expert_ref, out_ref, wd_ref, *scratch):
        spot = Spot()
        summed = Sum(spot, part_ref, out_ref, scratch[: len(sum_scratch)])

        def item(k):
            ref = shared_ref if k == 0 else expert_ref.at[k - 1]
            return (
                lambda target: rows_at(ref, window_of(target, hidden), WINDOW),
                lambda side, source: wd_ref.at[
                    pl.ds(k * WINDOW, WINDOW),
                    pl.ds(pl.multiple_of((side * parts + source) * lanes, lanes), lanes),
                ],
            )

        move = Move(spot, [item(k) for k in range(count)], scratch[len(sum_scratch) :])
        spot.greet(True, True)
        summed.begin()
        for k in range(count):
            move.own(k)
        move.send(0)
        move.send(1)
        for index in range(parts):
            summed.cross(index)
        for gap in (1, 2, 3):
            move.forward(0, gap)
        for index in range(parts):
            summed.line(index)
        for k in range(2, count):
            move.send(k)
        for k in range(1, count):
            for gap in (1, 2, 3):
                move.forward(k, gap)
        summed.end()
        move.end()

    return comm_call(
        kernel,
        number,
        "sum_and_move",
        [
            jax.ShapeDtypeStruct((rows, width), jnp.float32),
            jax.ShapeDtypeStruct((count * WINDOW, 2 * parts * lanes), jnp.bfloat16),
        ],
        [IN_VMEM, IN_PLACE],
        [IN_VMEM, IN_PLACE, IN_PLACE],
        sum_scratch + move_sems,
        180_000_000,
    )(value, shared_down, expert_down)


def share_and_move(value, shared_gate, shared_up, expert_gate, expert_up, number):
    parts = lax.axis_size("context")
    rows, width = value.shape
    block, hidden = shared_gate.shape
    stacks = 1 + expert_gate.shape[0]
    count = 2 * stacks
    share_sems, move_sems = Share.sems(parts), Move.sems(count, parts)

    def kernel(own_ref, sg_ref, su_ref, eg_ref, eu_ref, all_ref, wgu_ref, *sems):
        spot = Spot()
        share = Share(spot, own_ref, all_ref, sems[: len(share_sems)])

        def item(number):
            k = number // 2
            shared, expert = (sg_ref, eg_ref) if number % 2 == 0 else (su_ref, eu_ref)
            ref = shared if k == 0 else expert.at[k - 1]
            return (
                lambda target: lanes_at(ref, window_of(target, hidden), WINDOW),
                lambda side, source: wgu_ref.at[
                    pl.ds(pl.multiple_of((side * parts + source) * block, block), block),
                    pl.ds(number * WINDOW, WINDOW),
                ],
            )

        move = Move(spot, [item(number) for number in range(count)], sems[len(share_sems) :])
        spot.greet(True, True)
        share.begin()
        for number in range(count):
            move.own(number)
        move.send(0)
        share.step(1)
        move.send(1)
        share.step(2)
        for gap in (1, 2, 3):
            move.forward(0, gap)
        share.step(3)
        for number in range(2, count):
            move.send(number)
        for number in range(1, count):
            for gap in (1, 2, 3):
                move.forward(number, gap)
        share.end()
        move.end()

    return comm_call(
        kernel,
        number,
        "share_and_move",
        [
            jax.ShapeDtypeStruct((rows * parts * 4, width), value.dtype),
            jax.ShapeDtypeStruct((2 * parts * block, count * WINDOW), jnp.bfloat16),
        ],
        [IN_PLACE] * 2,
        [IN_VMEM] + [IN_PLACE] * 4,
        share_sems + move_sems,
        300_000_000,
    )(value, shared_gate, shared_up, expert_gate, expert_up)


def up_item(grads_ref, k, gate_ref, up_ref, block, parts):
    hidden = gate_ref.shape[1]
    tail = hidden - (parts - 1) * WINDOW

    def cut(offset):
        return lambda buf, short: buf.at[:, pl.ds(offset + (WINDOW - tail if short else 0), tail if short else WINDOW)]

    def out(ref):
        return lambda source, short: ref.at[:, pl.ds(hidden - tail, tail)] if short else lanes_at(ref, source * WINDOW, WINDOW)

    return {
        "block": lambda side, part: grads_ref.at[
            pl.ds(pl.multiple_of((side * parts + part) * block, block), block), pl.ds(2 * k * WINDOW, 2 * WINDOW)
        ],
        "pieces": [(cut(0), out(gate_ref)), (cut(WINDOW), out(up_ref))],
        "shape": (block, 2 * WINDOW),
    }


def down_item(grads_ref, k, down_ref, parts):
    hidden, lanes = down_ref.shape
    tail = hidden - (parts - 1) * WINDOW
    return {
        "block": lambda side, part: grads_ref.at[
            pl.ds(k * WINDOW, WINDOW), pl.ds(pl.multiple_of((side * parts + part) * lanes, lanes), lanes)
        ],
        "pieces": [
            (
                lambda buf, short: buf.at[pl.ds(WINDOW - tail if short else 0, tail if short else WINDOW), :],
                lambda source, short: down_ref.at[pl.ds(hidden - tail, tail), :] if short else rows_at(down_ref, source * WINDOW, WINDOW),
            )
        ],
        "shape": (WINDOW, lanes),
    }


def sum_and_return(value, up_grads, k, number):
    parts = lax.axis_size("context")
    total, width = value.shape
    rows = total // (4 * parts)
    block = up_grads.shape[0] // (2 * parts)
    hidden = WINDOW * parts - 128
    sum_scratch = Sum.scratch(parts, rows, width)
    back_scratch = Return.scratch([(block, 2 * WINDOW)], [2], parts)

    def kernel(part_ref, grads_ref, out_ref, gate_ref, up_ref, *scratch):
        spot = Spot()
        summed = Sum(spot, part_ref, out_ref, scratch[: len(sum_scratch)])
        got, mine, *sems = scratch[len(sum_scratch) :]
        back = Return(spot, [up_item(grads_ref, k, gate_ref, up_ref, block, parts)], [got], [mine], sems)
        spot.greet(True, True)
        summed.begin()
        back.start(0)
        for index in range(parts):
            summed.cross(index)
        back.reduce(0, 0)
        back.reduce(0, 1)
        summed.line(0)
        summed.line(1)
        back.reduce(0, 2)
        back.reduce(0, 3)
        summed.line(2)
        summed.line(3)
        summed.end()
        back.end()

    piece = jax.ShapeDtypeStruct((block, hidden), jnp.bfloat16)
    return comm_call(
        kernel,
        number,
        "sum_and_return",
        [jax.ShapeDtypeStruct((rows, width), jnp.float32), piece, piece],
        [IN_VMEM, IN_PLACE, IN_PLACE],
        [IN_VMEM, IN_PLACE],
        sum_scratch + back_scratch,
        250_000_000,
    )(value, up_grads)


def share_and_return(value, down_grads, k, number):
    parts = lax.axis_size("context")
    rows, width = value.shape
    lanes = down_grads.shape[1] // (2 * parts)
    hidden = WINDOW * parts - 128
    share_sems = Share.sems(parts)
    back_scratch = Return.scratch([(WINDOW, lanes)], [1], parts)

    def kernel(own_ref, grads_ref, all_ref, down_ref, *scratch):
        spot = Spot()
        share = Share(spot, own_ref, all_ref, scratch[: len(share_sems)])
        got, mine, *sems = scratch[len(share_sems) :]
        back = Return(spot, [down_item(grads_ref, k, down_ref, parts)], [got], [mine], sems)
        spot.greet(True, True)
        share.begin()
        back.start(0)
        share.step(1)
        share.step(2)
        back.reduce(0, 0)
        share.step(3)
        for index in range(1, parts):
            back.reduce(0, index)
        share.end()
        back.end()

    return comm_call(
        kernel,
        number,
        "share_and_return",
        [
            jax.ShapeDtypeStruct((rows * parts * 4, width), value.dtype),
            jax.ShapeDtypeStruct((hidden, lanes), jnp.bfloat16),
        ],
        [IN_PLACE, IN_PLACE],
        [IN_VMEM, IN_PLACE],
        share_sems + back_scratch,
        180_000_000,
    )(value, down_grads)


class Group:
    def __init__(self, spot, own, out, sems):
        self.spot, self.own, self.out = spot, own, out
        self.local_sem, self.across_s, self.across_r, self.beside_s, self.beside_r = sems

    @staticmethod
    def sems():
        return [DMA, DMA, DMA, DMA((2,)), DMA((2,))]

    def block(self, column):
        rows = self.own.shape[0]
        return rows_at(self.out, column * rows, rows)

    def to_across(self):
        s = self.spot
        return remote(self.own, self.block(s.group), self.across_s, self.across_r, {"experts": s.across})

    def to_beside(self, slot):
        s = self.spot
        column = s.across if slot else s.group
        source = self.block(column) if slot else self.own
        return remote(source, self.block(column), self.beside_s.at[slot], self.beside_r.at[slot], {"experts": s.beside})

    def local(self):
        return pltpu.make_async_copy(self.own, self.block(self.spot.group), self.local_sem)

    def begin(self):
        self.to_across().start()
        self.to_beside(0).start()
        self.local().start()

    def end(self):
        self.to_across().wait_recv()
        self.to_beside(1).start()
        self.local().wait()
        self.to_across().wait_send()
        for slot in range(2):
            self.to_beside(slot).wait()


class Total:
    def __init__(self, spot, value, out, scratch):
        self.out = out
        self.sent, self.got, self.send_s, self.recv_s = scratch
        place = spot.place
        self.turns = [
            spot.twin,
            {"context": place + 1 - 2 * lax.rem(place, 2)},
            {"context": lax.rem(place + 2, spot.parts)},
            {"experts": spot.beside},
            {"experts": spot.across},
        ]
        self.value = value

    @staticmethod
    def scratch(shape):
        buf = pltpu.VMEM((5,) + shape, jnp.float32)
        return [buf, buf, DMA((5,)), DMA((5,))]

    def copy(self, index):
        return remote(self.sent.at[index], self.got.at[index], self.send_s.at[index], self.recv_s.at[index], self.turns[index])

    def begin(self):
        self.out[...] = self.value[...]
        self.send(0)

    def send(self, index):
        self.sent[index] = self.out[...]
        self.copy(index).start()

    def take(self, index):
        self.copy(index).wait()
        self.out[...] = self.out[...] + self.got[index]


def last_exchange(up_grads, down_grads, out_grads, qkv_grads, branch, hidden, tokens_grad, small, ups, downs, number):
    parts = lax.axis_size("context")
    block = up_grads.shape[0] // (2 * parts)
    lanes = down_grads.shape[1] // (2 * parts)
    units = WINDOW * parts - 128
    head, span = out_grads.shape[0], qkv_grads.shape[1]
    rows, width = hidden.shape
    shapes = [(head, lanes), (block, span)] + [(block, 2 * WINDOW)] * len(ups) + [(WINDOW, lanes)] * len(downs)
    pieces = [1, 1] + [2] * len(ups) + [1] * len(downs)
    count, bf16 = len(shapes), jnp.bfloat16
    groups = [
        Return.scratch(shapes, pieces, parts),
        Sum.scratch(parts, rows, width) + [pltpu.VMEM((rows, width), jnp.float32), pltpu.VMEM((rows, width), bf16)],
        Total.scratch(small.shape),
        Group.sems(),
        Group.sems(),
    ]
    piece, column = jax.ShapeDtypeStruct((block, units), bf16), jax.ShapeDtypeStruct((units, lanes), bf16)
    out_shape = [jax.ShapeDtypeStruct((parts * head, lanes), bf16), jax.ShapeDtypeStruct((parts * block, span), bf16)]
    out_shape += [piece] * (2 * len(ups)) + [column] * len(downs)
    out_shape += [
        jax.ShapeDtypeStruct((4 * rows, width), bf16),
        jax.ShapeDtypeStruct((4 * rows, width), jnp.float32),
        jax.ShapeDtypeStruct(small.shape, jnp.float32),
    ]

    def kernel(upg_ref, downg_ref, outg_ref, qkvg_ref, branch_ref, hidden_ref, tokens_ref, small_ref, *rest):
        outs, scratch = rest[: len(out_shape)], list(rest[len(out_shape) :])
        sets = []
        for one in groups:
            sets.append(scratch[: len(one)])
            scratch = scratch[len(one) :]
        grads, (block_all, tokens_all, small_out) = outs[:-3], outs[-3:]
        items = [
            {
                "block": lambda side, part: lanes_at(outg_ref, (side * parts + part) * lanes, lanes),
                "pieces": [(lambda buf, short: buf, lambda source, short: rows_at(grads[0], source * head, head))],
            },
            {
                "block": lambda side, part: rows_at(qkvg_ref, (side * parts + part) * block, block),
                "pieces": [(lambda buf, short: buf, lambda source, short: rows_at(grads[1], source * block, block))],
            },
        ]
        items += [up_item(upg_ref, k, grads[2 + 2 * i], grads[3 + 2 * i], block, parts) for i, k in enumerate(ups)]
        items += [down_item(downg_ref, k, grads[2 + 2 * len(ups) + i], parts) for i, k in enumerate(downs)]
        spot = Spot()
        back = Return(spot, items, sets[0][:count], sets[0][count : 2 * count], sets[0][2 * count :])
        total_branch, own_block = sets[1][-2:]
        summed = Sum(spot, branch_ref, total_branch, sets[1][:-2])
        total = Total(spot, small_ref, small_out, sets[2])
        tokens_group = Group(spot, tokens_ref, tokens_all, sets[3])
        block_group = Group(spot, own_block, block_all, sets[4])
        spot.greet(True, True)
        total.begin()
        summed.begin()
        back.start(0)
        back.start(1)
        total.take(0)
        total.send(1)
        for index in range(parts):
            summed.cross(index)
        total.take(1)
        total.send(2)
        for item in range(2, count):
            back.start(item)
        for index in range(parts):
            back.reduce(0, index)
        total.take(2)
        total.send(3)
        for index in range(parts):
            back.reduce(1, index)
        total.take(3)
        total.send(4)
        summed.line(0)
        summed.line(1)
        total.take(4)
        tokens_group.begin()
        back.reduce(2, 0)
        summed.line(2)
        back.reduce(2, 1)
        summed.line(3)
        half = width // 2

        def finish(at, start, step):
            value = (hidden_ref[at, :] + total_branch[at, :]).astype(bf16)
            turned = lax.axis_index("dp") == 0

            @pl.when(turned)
            def _():
                own_block[at, :] = value

            @pl.when(jnp.logical_not(turned))
            def _():
                own_block[at, :half] = value[:, half:]
                own_block[at, half:] = value[:, :half]

        summed.chunks(finish)
        block_group.begin()
        for index in range(2, parts):
            back.reduce(2, index)
        for item in range(3, count):
            for index in range(parts):
                back.reduce(item, index)
        summed.end()
        tokens_group.end()
        block_group.end()
        back.end()

    return comm_call(
        kernel,
        number,
        "last_exchange",
        out_shape,
        [IN_PLACE] * (len(out_shape) - 1) + [IN_VMEM],
        [IN_PLACE] * 4 + [IN_VMEM] * 4,
        [one for group in groups for one in group],
        300_000_000,
    )(up_grads, down_grads, out_grads, qkv_grads, branch, hidden, tokens_grad, small)


def hidden_kernel(parts, stacks, units, both_ref, wgu_ref, wd_ref, coef_ref, send_ref, branch_ref, dup_ref, act_ref, dx_acc, out_acc, dot_acc):
    width = branch_ref.shape[1]
    f32, bf16 = jnp.float32, jnp.bfloat16
    repeated = jnp.where(lax.axis_index("context") == parts - 1, WINDOW * parts - units, 0)
    lane = lax.broadcasted_iota(jnp.int32, (1, WINDOW), 1)
    fresh = jnp.where(lane >= repeated, 1.0, 0.0)
    group = lax.axis_index("experts")
    column = lax.broadcasted_iota(jnp.int32, (1, 128), 1)
    dot_acc[...] = jnp.zeros_like(dot_acc)
    for k in range(stacks):
        up = pl.ds(2 * k * WINDOW, 2 * WINDOW)
        down = pl.ds(k * WINDOW, WINDOW)
        vals = jnp.dot(both_ref[:, :width], wgu_ref[:, up], preferred_element_type=f32)
        raw = dot_nt(both_ref[:, width:], wd_ref[down, :]) * fresh
        g_vals, u_vals = vals[:, :WINDOW], vals[:, WINDOW:]
        sig_g = jax.nn.sigmoid(g_vals)
        silu_g = g_vals * sig_g
        act = silu_g * u_vals
        coef = coef_ref[:, k : k + 1]
        at = (stacks - 1) * 4 if k == 0 else group * (stacks - 1) + k - 1
        dots = jnp.sum(raw * act, -1, keepdims=True)
        dot_acc[...] += dots * jnp.where(column == at, 1.0, 0.0)
        act_ref[:, down] = (act * (coef * fresh)).astype(bf16)
        dact = raw * coef
        dup_ref[:, pl.ds(2 * k * WINDOW, WINDOW)] = (dact * u_vals * (sig_g * (1.0 + g_vals * (1.0 - sig_g)))).astype(bf16)
        dup_ref[:, pl.ds((2 * k + 1) * WINDOW, WINDOW)] = (dact * silu_g).astype(bf16)
        out_part = jnp.dot(act_ref[:, down], wd_ref[down, :], preferred_element_type=f32)
        dx_part = dot_nt(dup_ref[:, up], wgu_ref[:, up])
        if k == 0:
            out_acc[...] = out_part
            dx_acc[...] = dx_part
        elif k < stacks - 1:
            out_acc[...] += out_part
            dx_acc[...] += dx_part
        else:
            branch_ref[...] = (out_acc[...] + out_part).astype(bf16)
            send_ref[:, :width] = (dx_acc[...] + dx_part).astype(bf16)
    send_ref[:, width:] = dot_acc[...].astype(bf16)


def hidden_units(both, wgu, wd, coefs, units):
    length, width = both.shape[0], both.shape[1] // 2
    stacks = wd.shape[0] // WINDOW
    step = min(256, length)
    bf16 = jnp.bfloat16

    def rows_block(columns):
        return pl.BlockSpec((step, columns), lambda i: (i, 0))

    def whole(array):
        return pl.BlockSpec(array.shape, lambda i: (0, 0), pipeline_mode=pl.Buffered(1))

    return pl.pallas_call(
        functools.partial(hidden_kernel, lax.axis_size("context"), stacks, units),
        grid=(length // step,),
        in_specs=[rows_block(2 * width), whole(wgu), whole(wd), rows_block(coefs.shape[1])],
        out_specs=[rows_block(width + 128), rows_block(width), rows_block(wgu.shape[1]), rows_block(wd.shape[0])],
        out_shape=[
            jax.ShapeDtypeStruct((length, width + 128), bf16),
            jax.ShapeDtypeStruct((length, width), bf16),
            jax.ShapeDtypeStruct((length, wgu.shape[1]), bf16),
            jax.ShapeDtypeStruct((length, wd.shape[0]), bf16),
        ],
        scratch_shapes=[
            pltpu.VMEM((step, width), jnp.float32),
            pltpu.VMEM((step, width), jnp.float32),
            pltpu.VMEM((step, 128), jnp.float32),
        ],
        cost_estimate=pl.CostEstimate(
            flops=6 * length * width * wgu.shape[1], bytes_accessed=40_000_000, transcendentals=length * wd.shape[0]
        ),
        name="hidden_units",
    )(both, wgu, wd, coefs)


def split_body(
    tokens,
    positions,
    routes,
    out_grad,
    norm1_gain,
    qkv_weight,
    qkv_bias,
    out_weight,
    norm2_gain,
    router_weight,
    expert_gate,
    expert_up,
    expert_down,
    shared_gate,
    shared_w_gate,
    shared_w_up,
    shared_w_down,
):
    rows, width = tokens.shape[1], tokens.shape[2]
    parts = lax.axis_size("context")
    group_size = lax.axis_size("experts")
    place, group = lax.axis_index("context"), lax.axis_index("experts")
    local_experts = expert_gate.shape[0]
    expert_count = local_experts * group_size
    own_rows = rows // group_size
    length = rows * parts
    half = width // 2
    block = width // (2 * parts)
    hidden_here = shared_w_gate.shape[1] // parts
    stacks = local_experts + 1
    scale = HEAD_DIM ** (-0.5)
    bf16 = jnp.bfloat16

    first = group * own_rows

    def own_of(array):
        return lax.dynamic_slice_in_dim(array, first, own_rows, 0)

    grad_own_b = own_half_first(own_of(out_grad[0]))
    grad_own = grad_own_b.astype(jnp.float32)
    gain1 = own_half_first(norm1_gain).astype(jnp.float32)
    gain2 = own_half_first(norm2_gain).astype(jnp.float32)
    token_own = own_half_first(own_of(tokens[0])).astype(jnp.float32)
    inverse1 = lax.rsqrt(jnp.mean(token_own * token_own, -1, keepdims=True) + EPSILON)
    normed1 = token_own * inverse1
    places_own = own_of(positions[0])[:, None]
    facts = jnp.concatenate([places_own // 64, places_own % 64, own_of(routes[0])], 1)
    facts = jnp.pad(facts, ((0, 0), (0, 128 - facts.shape[1]))).astype(bf16)
    send1 = jnp.concatenate([(normed1 * gain1).astype(bf16), facts], 1)
    qkv_in = jnp.transpose(
        qkv_weight.reshape(block, 3, parts, HEAD_DIM), (2, 0, 1, 3)
    ).reshape(parts * block, 3 * HEAD_DIM)
    shared1, qkv_w, out_w = share_first(send1, qkv_in, out_weight, 1)
    xn1, facts = shared1[:, :width], shared1[:, width:].astype(jnp.int32)
    position_all = facts[:, 0] * 64 + facts[:, 1]
    route_all = facts[:, 2 : 2 + routes.shape[2]]

    bias_here = lax.dynamic_slice_in_dim(
        qkv_bias.reshape(3, parts, HEAD_DIM), place, 1, 1
    ).reshape(1, 3 * HEAD_DIM)
    qkv = (
        dot_nn(xn1, qkv_w)
        + bias_here.astype(jnp.float32)
    )
    cosine, sine_part = rope_tables(position_all)
    cosine, sine_part = cosine[:, 0], sine_part[:, 0]
    q_raw, k_raw, v_raw = jnp.split(qkv, 3, 1)
    query = (q_raw * cosine + rotate(q_raw) * sine_part).astype(bf16)
    key = (k_raw * cosine + rotate(k_raw) * sine_part).astype(bf16)
    value = v_raw.astype(bf16)
    index = jnp.arange(length, dtype=jnp.int32)
    allowed = index[None, :] <= index[:, None]
    scores = dot_nt(query, key) * scale
    row_max = jnp.max(jnp.where(allowed, scores, MASKED), -1, keepdims=True)
    weights = jnp.where(allowed, jnp.exp(scores - row_max), 0.0)
    row_sum = jnp.sum(weights, -1, keepdims=True)
    attended = (dot_nn(weights.astype(bf16), value) / row_sum).astype(bf16)
    lse = row_max + jnp.log(row_sum)

    head_part = dot_nn(attended, out_w).astype(bf16)
    head_sum, down_w = sum_and_move(head_part, shared_w_down, expert_down, 2)
    hidden = token_own + head_sum
    inverse2 = lax.rsqrt(jnp.mean(hidden * hidden, -1, keepdims=True) + EPSILON)
    normed2 = hidden * inverse2
    xn2_own = (normed2 * gain2).astype(bf16)
    both, up_w = share_and_move(
        jnp.concatenate([xn2_own, grad_own_b], 1), shared_w_gate, shared_w_up, expert_gate, expert_up, 3
    )
    xn2, grad_all = both[:, :width], both[:, width:]

    router_here = own_half_first(router_weight.T).T
    gate_here = own_half_first(shared_gate)
    heads_w = jnp.concatenate([router_here, gate_here[:, None]], 1)
    logits_all = dot_nn(xn2, heads_w)
    prob_all = jax.nn.softmax(logits_all[:, :expert_count], -1)
    sig_all = jax.nn.sigmoid(logits_all[:, expert_count])
    named_all = jnp.sum(
        (
            route_all[:, :, None] == jnp.arange(expert_count, dtype=jnp.int32)[None, None, :]
        ).astype(jnp.float32),
        1,
    )
    gates_all = prob_all * named_all
    gates_here = lax.dynamic_slice_in_dim(gates_all, group * local_experts, local_experts, 1)
    coefs = jnp.concatenate([sig_all[:, None], gates_here], 1)

    coefs = jnp.pad(coefs, ((0, 0), (0, 128 - stacks)))
    send4, branch_part, dup, act_c = hidden_units(both, up_w, down_w, coefs, shared_w_gate.shape[1])
    up_g = dot_tn(xn2, dup).astype(bf16)
    down_g = dot_tn(act_c, grad_all).astype(bf16)
    send4, up_g, down_g = lax.optimization_barrier((send4, up_g, down_g))
    up_grads, down_grads = [None] * (2 * stacks), [None] * stacks
    sums, up_grads[0], up_grads[1] = sum_and_return(send4, up_g, 0, 4)
    dxn2_sum, dots_own = sums[:, :width], sums[:, width:]

    row_first = place * rows + first
    prob = lax.dynamic_slice_in_dim(prob_all, row_first, own_rows, 0)
    named = lax.dynamic_slice_in_dim(named_all, row_first, own_rows, 0)
    sig_own = lax.dynamic_slice_in_dim(sig_all, row_first, own_rows, 0)
    dprob = dots_own[:, :expert_count] * named
    dlogit = prob * (dprob - jnp.sum(prob * dprob, -1, keepdims=True))
    coef = sig_own * (1.0 - sig_own) * dots_own[:, expert_count]
    xn2_float = xn2_own.astype(jnp.float32)
    router_grad = jnp.dot(xn2_float.T, dlogit, precision=PRECISE)
    shared_gate_grad = jnp.dot(coef, xn2_float, precision=PRECISE)
    dxn2 = (
        dxn2_sum
        + jnp.dot(dlogit, router_here.astype(jnp.float32).T, precision=PRECISE)
        + coef[:, None] * gate_here.astype(jnp.float32)[None, :]
    )
    norm2_grad = jnp.sum(dxn2 * normed2, 0)
    dscaled2 = dxn2 * gain2
    dhidden = grad_own + inverse2 * (
        dscaled2 - normed2 * jnp.mean(dscaled2 * normed2, -1, keepdims=True)
    )
    dhidden_all, down_grads[0] = share_and_return(dhidden.astype(bf16), down_g, 0, 5)

    out_g = dot_tn(attended, dhidden_all).astype(bf16)
    dattended = dot_nt(dhidden_all, out_w).astype(bf16)
    delta = jnp.sum(
        dattended.astype(jnp.float32) * attended.astype(jnp.float32), -1, keepdims=True
    )
    scores = dot_nt(query, key) * scale
    prob_att = jnp.where(allowed, jnp.exp(scores - lse), 0.0)
    dvalue = dot_tn(prob_att.astype(bf16), dattended)
    dscore = (prob_att * (dot_nt(dattended, value) - delta)).astype(bf16)
    dquery = dot_nn(dscore, key) * scale
    dkey = dot_tn(dscore, query) * scale
    dqkv = jnp.concatenate(
        [
            dquery * cosine + rotate_back(dquery * sine_part),
            dkey * cosine + rotate_back(dkey * sine_part),
            dvalue,
        ],
        1,
    )
    bias_part = jnp.sum(dqkv, 0)
    dqkv_b = dqkv.astype(bf16)
    qkv_g = dot_tn(xn1, dqkv_b).astype(bf16)
    dxn1_part = dot_nt(dqkv_b, qkv_w).astype(bf16)
    dxn1, up_grads[2], up_grads[3] = sum_and_return(dxn1_part, up_g, 1, 6)
    norm1_grad = jnp.sum(dxn1 * normed1, 0)
    dscaled1 = dxn1 * gain1
    tokens_grad_own = dhidden + inverse1 * (
        dscaled1 - normed1 * jnp.mean(dscaled1 * normed1, -1, keepdims=True)
    )

    bias_wide = jnp.zeros((group_size, parts, 3 * HEAD_DIM), jnp.float32)
    bias_wide = lax.dynamic_update_slice(bias_wide, bias_part[None, None], (group, place, 0))
    small = jnp.concatenate(
        [
            own_half_first(norm1_grad),
            own_half_first(norm2_grad),
            own_half_first(shared_gate_grad),
            own_half_first(router_grad.T).T.reshape(-1),
            bias_wide.reshape(-1),
        ]
    )
    out_w_grad, qkv_grad, *others, block_out, tokens_grad, small = last_exchange(
        up_g,
        down_g,
        out_g,
        qkv_g,
        branch_part,
        hidden,
        own_half_first(tokens_grad_own),
        small.reshape(-1, 128),
        list(range(2, stacks)),
        list(range(1, stacks)),
        7,
    )
    small = small.reshape(-1)
    up_grads[4:] = others[: 2 * (stacks - 2)]
    down_grads[1:] = others[2 * (stacks - 2) :]
    router_size = width * expert_count
    bias_sum = small[3 * width + router_size :].reshape(group_size, parts, 3, HEAD_DIM)
    bias_grad = jnp.transpose(
        lax.dynamic_slice_in_dim(bias_sum, group, 1, 0)[0], (1, 0, 2)
    ).reshape(3, parts * HEAD_DIM)

    qkv_grad = jnp.transpose(
        qkv_grad.reshape(parts, block, 3, HEAD_DIM), (1, 2, 0, 3)
    ).reshape(block, 3, parts * HEAD_DIM)

    def wide(array):
        return array.astype(jnp.float32)

    return (
        block_out[None],
        tokens_grad[None],
        small[:width],
        wide(qkv_grad),
        bias_grad,
        wide(out_w_grad),
        small[width : 2 * width],
        small[3 * width : 3 * width + router_size].reshape(width, expert_count),
        wide(jnp.stack(up_grads[2::2])),
        wide(jnp.stack(up_grads[3::2])),
        wide(jnp.stack(down_grads[1:])),
        small[2 * width : 3 * width],
        wide(up_grads[0]),
        wide(up_grads[1]),
        wide(down_grads[0]),
    )


def plan_of(mesh):
    sizes = mesh.shape
    return split_body if (sizes["dp"], sizes["context"], sizes["experts"]) == (2, 4, 4) else general_body


def solution(mesh):
    return jax.shard_map(
        plan_of(mesh),
        mesh=mesh,
        in_specs=(
            P("dp", "context", None),
            P("dp", "context"),
            P("dp", "context", None),
            P("dp", "context", None),
            P(),
            P(("dp", "context"), None, "experts"),
            P(None, "experts"),
            P("experts", ("dp", "context")),
            P(),
            P(),
            P("experts", ("dp", "context"), None),
            P("experts", ("dp", "context"), None),
            P("experts", None, ("dp", "context")),
            P(),
            P(("dp", "context"), "experts"),
            P(("dp", "context"), "experts"),
            P("experts", ("dp", "context")),
        ),
        out_specs=(
            P("dp", "context", None),
            P("dp", "context", None),
            P(),
            P(("dp", "context"), None, "experts"),
            P(None, "experts"),
            P("experts", ("dp", "context")),
            P(),
            P(),
            P("experts", ("dp", "context"), None),
            P("experts", ("dp", "context"), None),
            P("experts", None, ("dp", "context")),
            P(),
            P(("dp", "context"), "experts"),
            P(("dp", "context"), "experts"),
            P("experts", ("dp", "context")),
        ),
        check_vma=False,
    )
```

```python
import functools

import jax
import jax.numpy as jnp
from jax import lax
from jax.experimental import pallas as pl
from jax.experimental.pallas import tpu as pltpu
from jax.sharding import PartitionSpec as P

HEAD_DIM = 128


EPSILON = 1e-06
ROPE_BASE = 1000000.0
MASKED = -1e30
PRECISE = lax.Precision.HIGHEST


def rope_tables(position_ids):
    half_dim = HEAD_DIM // 2
    inverse = ROPE_BASE ** (-2.0 * jnp.arange(half_dim, dtype=jnp.float32) / HEAD_DIM)
    angles = position_ids.astype(jnp.float32)[:, None] * inverse[None, :]
    cosine = jnp.cos(angles)
    sine_part = jnp.sin(angles)
    return (
        jnp.concatenate([cosine, cosine], -1)[:, None, :],
        jnp.concatenate([sine_part, sine_part], -1)[:, None, :],
    )


def rotate(value):
    half_dim = value.shape[-1] // 2
    return jnp.concatenate([-value[..., half_dim:], value[..., :half_dim]], -1)


def rotate_back(value):
    half_dim = value.shape[-1] // 2
    return jnp.concatenate([value[..., half_dim:], -value[..., :half_dim]], -1)


def silu_grad(gate_vals):
    sigmoid_vals = jax.nn.sigmoid(gate_vals)
    return sigmoid_vals * (1.0 + gate_vals * (1.0 - sigmoid_vals))


def block_rank(route_rows, expert_count):
    hits = (
        route_rows[:, :, None] == jnp.arange(expert_count, dtype=jnp.int32)[None, None, :]
    ).astype(jnp.int32)
    flat_hits = hits.reshape(-1, expert_count)
    earlier = jnp.cumsum(flat_hits, axis=0) - flat_hits
    return jnp.sum(earlier * flat_hits, -1).reshape(route_rows.shape)


def block_width_of():
    return 512


def gather_weights(shard_set):
    return (
        lax.all_gather(shard_set[0], ("dp", "context"), axis=0, tiled=True),
        lax.all_gather(shard_set[1], ("dp", "context"), axis=1, tiled=True),
        lax.all_gather(shard_set[2], ("dp", "context"), axis=1, tiled=True),
        lax.all_gather(shard_set[3], ("dp", "context"), axis=1, tiled=True),
        lax.all_gather(shard_set[4], ("dp", "context"), axis=2, tiled=True),
        lax.all_gather(shard_set[5], ("dp", "context"), axis=0, tiled=True),
        lax.all_gather(shard_set[6], ("dp", "context"), axis=0, tiled=True),
        lax.all_gather(shard_set[7], ("dp", "context"), axis=1, tiled=True),
    )


def forward_fold(query, query_first, scale, carry, piece):
    row_count, head_count, head_size = query.shape
    query_index = query_first + jnp.arange(row_count, dtype=jnp.int32)
    query_last = query_first + row_count - 1
    key_part, value_part = piece
    piece_rows = key_part.shape[0]
    block_width = block_width_of()
    block_count = piece_rows // block_width
    key_blocks = key_part.reshape(block_count, block_width, head_count, head_size)
    value_blocks = value_part.reshape(block_count, block_width, head_count, head_size)
    offsets = block_width * jnp.arange(block_count, dtype=jnp.int32)

    def forward_visit(state, item):
        key_block, value_block, first_key = item

        def forward_compute(current):
            run_max, run_sum, accum = current
            scores = (
                jnp.einsum("qhd,khd->hqk", query, key_block, preferred_element_type=jnp.float32)
                * scale
            )
            key_index = first_key + jnp.arange(block_width, dtype=jnp.int32)
            allowed = key_index[None, None, :] <= query_index[None, :, None]
            new_max = jnp.maximum(run_max, jnp.max(jnp.where(allowed, scores, MASKED), -1))
            weights = jnp.where(allowed, jnp.exp(scores - new_max[..., None]), 0.0)
            factor = jnp.exp(run_max - new_max)
            new_sum = run_sum * factor + jnp.sum(weights, -1)
            new_accum = accum * factor[..., None] + jnp.einsum(
                "hqk,khd->hqd",
                weights.astype(jnp.bfloat16),
                value_block,
                preferred_element_type=jnp.float32,
            )
            return (new_max, new_sum, new_accum)

        return (
            lax.cond(first_key > query_last, lambda current: current, forward_compute, state),
            None,
        )

    carry, _ = lax.scan(forward_visit, carry, (key_blocks, value_blocks, offsets))
    return carry


def key_grad_fold(key_rows, value_rows, key_first, scale, carry, piece):
    row_count, head_count, head_size = key_rows.shape
    key_index = key_first + jnp.arange(row_count, dtype=jnp.int32)
    query_part, dout_part, lse_part, delta_part = piece
    piece_rows = query_part.shape[0]
    block_width = block_width_of()
    block_count = piece_rows // block_width
    query_blocks = query_part.reshape(block_count, block_width, head_count, head_size)
    dout_blocks = dout_part.reshape(block_count, block_width, head_count, head_size)
    lse_blocks = lse_part.reshape(block_count, block_width, head_count)
    delta_blocks = delta_part.reshape(block_count, block_width, head_count)
    offsets = block_width * jnp.arange(block_count, dtype=jnp.int32)

    def key_visit(state, item):
        query_block, dout_block, lse_block, delta_block, first_query = item

        def key_compute(current):
            dkey_sum, dvalue_sum = current
            query_b = query_block.astype(jnp.bfloat16)
            dout_b = dout_block.astype(jnp.bfloat16)
            scores = (
                jnp.einsum("qhd,khd->hqk", query_b, key_rows, preferred_element_type=jnp.float32)
                * scale
            )
            query_index = first_query + jnp.arange(block_width, dtype=jnp.int32)
            allowed = key_index[None, None, :] <= query_index[None, :, None]
            prob_att = jnp.where(
                allowed, jnp.exp(scores - jnp.transpose(lse_block)[:, :, None]), 0.0
            )
            dvalue_sum = dvalue_sum + jnp.einsum(
                "hqk,qhd->hkd",
                prob_att.astype(jnp.bfloat16),
                dout_b,
                preferred_element_type=jnp.float32,
            )
            dprob = jnp.einsum(
                "qhd,khd->hqk", dout_b, value_rows, preferred_element_type=jnp.float32
            )
            dscore = (prob_att * (dprob - jnp.transpose(delta_block)[:, :, None])).astype(
                jnp.bfloat16
            )
            dkey_sum = (
                dkey_sum
                + jnp.einsum("hqk,qhd->hkd", dscore, query_b, preferred_element_type=jnp.float32)
                * scale
            )
            return (dkey_sum, dvalue_sum)

        return (
            lax.cond(
                first_query + block_width - 1 < key_first,
                lambda current: current,
                key_compute,
                state,
            ),
            None,
        )

    carry, _ = lax.scan(
        key_visit, carry, (query_blocks, dout_blocks, lse_blocks, delta_blocks, offsets)
    )
    return carry


def query_grad_fold(query, dattended, lse_heads, delta_heads, query_first, scale, carry, piece):
    row_count, head_count, head_size = query.shape
    query_index = query_first + jnp.arange(row_count, dtype=jnp.int32)
    query_last = query_first + row_count - 1
    key_part, value_part = piece
    piece_rows = key_part.shape[0]
    block_width = block_width_of()
    block_count = piece_rows // block_width
    key_blocks = key_part.reshape(block_count, block_width, head_count, head_size)
    value_blocks = value_part.reshape(block_count, block_width, head_count, head_size)
    offsets = block_width * jnp.arange(block_count, dtype=jnp.int32)

    def query_visit(state, item):
        key_block, value_block, first_key = item

        def query_compute(current):
            scores = (
                jnp.einsum("qhd,khd->hqk", query, key_block, preferred_element_type=jnp.float32)
                * scale
            )
            key_index = first_key + jnp.arange(block_width, dtype=jnp.int32)
            allowed = key_index[None, None, :] <= query_index[None, :, None]
            prob_att = jnp.where(allowed, jnp.exp(scores - lse_heads[:, :, None]), 0.0)
            dprob = jnp.einsum(
                "qhd,khd->hqk", dattended, value_block, preferred_element_type=jnp.float32
            )
            dscore = (prob_att * (dprob - delta_heads[:, :, None])).astype(jnp.bfloat16)
            return (
                current
                + jnp.einsum("hqk,khd->hqd", dscore, key_block, preferred_element_type=jnp.float32)
                * scale
            )

        return (
            lax.cond(first_key > query_last, lambda current: current, query_compute, state),
            None,
        )

    carry, _ = lax.scan(query_visit, carry, (key_blocks, value_blocks, offsets))
    return carry


def general_body(
    tokens,
    positions,
    routes,
    out_grad,
    norm1_gain,
    qkv_weight,
    qkv_bias,
    out_weight,
    norm2_gain,
    router_weight,
    expert_gate,
    expert_up,
    expert_down,
    shared_gate,
    shared_w_gate,
    shared_w_up,
    shared_w_down,
):
    row_count = tokens.shape[1]
    model_width = tokens.shape[2]
    head_span = qkv_bias.shape[1]
    heads_here = head_span // HEAD_DIM
    local_experts = expert_gate.shape[0]
    group_size = lax.axis_size("experts")
    quarter = row_count // group_size
    capacity = 3 * quarter // 4
    expert_count = local_experts * group_size
    group_index = lax.axis_index("experts")
    scale = HEAD_DIM ** (-0.5)
    shard_set = (
        qkv_weight,
        out_weight,
        expert_gate,
        expert_up,
        expert_down,
        shared_w_gate,
        shared_w_up,
        shared_w_down,
    )
    qkv_full, out_full, gate_full, up_full, down_full, sgate_full, sup_full, sdown_full = (
        gather_weights(shard_set)
    )
    token_float = tokens[0].astype(jnp.float32)
    inverse1 = lax.rsqrt(jnp.mean(token_float * token_float, -1, keepdims=True) + EPSILON)
    normed1 = token_float * inverse1
    gain1 = norm1_gain.astype(jnp.float32)
    normed1_b = (normed1 * gain1).astype(jnp.bfloat16)
    qkv_flat = qkv_full.reshape(model_width, 3 * head_span)
    qkv = (
        jnp.dot(normed1_b, qkv_flat, preferred_element_type=jnp.float32).reshape(
            row_count, 3, head_span
        )
        + qkv_bias.astype(jnp.float32)[None]
    )
    cosine, sine_part = rope_tables(positions[0])
    query_raw = qkv[:, 0].reshape(row_count, heads_here, HEAD_DIM)
    key_raw = qkv[:, 1].reshape(row_count, heads_here, HEAD_DIM)
    query = (query_raw * cosine + rotate(query_raw) * sine_part).astype(jnp.bfloat16)
    key_rows = (key_raw * cosine + rotate(key_raw) * sine_part).astype(jnp.bfloat16)
    value_flat = qkv[:, 2].astype(jnp.bfloat16)
    key_flat = key_rows.reshape(row_count, head_span)
    value_rows = value_flat.reshape(row_count, heads_here, HEAD_DIM)
    query_first = lax.axis_index("context") * row_count
    start_state = (
        jnp.full((heads_here, row_count), MASKED, jnp.float32),
        jnp.zeros((heads_here, row_count), jnp.float32),
        jnp.zeros((heads_here, row_count, HEAD_DIM), jnp.float32),
    )
    run_max, run_sum, accum = forward_fold(
        query,
        query_first,
        scale,
        start_state,
        (
            lax.all_gather(key_flat, "context", axis=0, tiled=True),
            lax.all_gather(value_flat, "context", axis=0, tiled=True),
        ),
    )
    attended = jnp.transpose(accum / run_sum[..., None], (1, 0, 2)).astype(jnp.bfloat16)
    lse_heads = run_max + jnp.log(run_sum)
    attended_flat = attended.reshape(row_count, head_span)
    head_part = jnp.dot(attended_flat, out_full, preferred_element_type=jnp.float32)
    hidden = token_float + lax.psum(head_part, "experts")
    inverse2 = lax.rsqrt(jnp.mean(hidden * hidden, -1, keepdims=True) + EPSILON)
    normed2 = hidden * inverse2
    gain2 = norm2_gain.astype(jnp.float32)
    normed2_b = (normed2 * gain2).astype(jnp.bfloat16)
    first_row = group_index * quarter
    normed2_q = lax.dynamic_slice_in_dim(normed2_b, first_row, quarter, 0)
    route_q = lax.dynamic_slice_in_dim(routes[0], first_row, quarter, 0)
    logits = jnp.dot(normed2_q, router_weight, preferred_element_type=jnp.float32)
    prob = jax.nn.softmax(logits, -1)
    gate_k = jnp.take_along_axis(prob, route_q, 1)
    slot_ids = route_q * capacity + block_rank(route_q, expert_count)
    slot_hits = (
        slot_ids[:, :, None] == jnp.arange(expert_count * capacity, dtype=jnp.int32)[None, None, :]
    )
    placer = jnp.sum(slot_hits.astype(jnp.bfloat16), 1)
    send_rows = (
        jnp.dot(placer.T, normed2_q, preferred_element_type=jnp.float32)
        .astype(jnp.bfloat16)
        .reshape(group_size, local_experts, capacity, model_width)
    )
    arrived = lax.all_to_all(send_rows, "experts", split_axis=0, concat_axis=0, tiled=True)
    expert_gvals = jnp.einsum(
        "secd,edf->secf", arrived, gate_full, preferred_element_type=jnp.float32
    )
    expert_uvals = jnp.einsum(
        "secd,edf->secf", arrived, up_full, preferred_element_type=jnp.float32
    )
    expert_act = (jax.nn.silu(expert_gvals) * expert_uvals).astype(jnp.bfloat16)
    expert_out = jnp.einsum(
        "secf,efd->secd", expert_act, down_full, preferred_element_type=jnp.float32
    ).astype(jnp.bfloat16)
    returned = lax.all_to_all(
        expert_out, "experts", split_axis=0, concat_axis=0, tiled=True
    ).reshape(expert_count * capacity, model_width)
    picked = returned[slot_ids].astype(jnp.float32)
    routed = jnp.sum(gate_k[:, :, None] * picked, 1)
    shared_sig = jax.nn.sigmoid(
        jnp.dot(normed2_b, shared_gate[:, None], preferred_element_type=jnp.float32)[:, 0]
    )
    shared_gvals = jnp.dot(normed2_b, sgate_full, preferred_element_type=jnp.float32)
    shared_uvals = jnp.dot(normed2_b, sup_full, preferred_element_type=jnp.float32)
    shared_act = (jax.nn.silu(shared_gvals) * shared_uvals).astype(jnp.bfloat16)
    shared_part = jnp.dot(shared_act, sdown_full, preferred_element_type=jnp.float32)
    routed_pad = lax.dynamic_update_slice_in_dim(
        jnp.zeros((row_count, model_width), jnp.float32), routed, first_row, 0
    )
    branch_total = lax.psum(
        (shared_sig[:, None] * shared_part + routed_pad).astype(jnp.bfloat16), "experts"
    ).astype(jnp.float32)
    block_out = (hidden + branch_total).astype(jnp.bfloat16)
    held = lax.optimization_barrier((shard_set, block_out))
    qkv_full, out_full, gate_full, up_full, down_full, sgate_full, sup_full, sdown_full = (
        gather_weights(held[0])
    )
    qkv_flat = qkv_full.reshape(model_width, 3 * head_span)
    grad_float = out_grad[0].astype(jnp.float32)
    grad_q = lax.dynamic_slice_in_dim(grad_float, first_row, quarter, 0)
    dgate_k = jnp.sum(grad_q[:, None, :] * picked, -1)
    weighted = jnp.sum(slot_hits.astype(jnp.float32) * gate_k[:, :, None], 1)
    dsend = (
        jnp.dot(weighted.T, grad_q, precision=PRECISE)
        .astype(jnp.bfloat16)
        .reshape(group_size, local_experts, capacity, model_width)
    )
    darrived = lax.all_to_all(dsend, "experts", split_axis=0, concat_axis=0, tiled=True)
    expert_dact = jnp.einsum(
        "secd,efd->secf", darrived, down_full, preferred_element_type=jnp.float32
    )
    down_grad = jnp.einsum(
        "secf,secd->efd", expert_act, darrived, preferred_element_type=jnp.float32
    )
    expert_dgate = (expert_dact * expert_uvals * silu_grad(expert_gvals)).astype(jnp.bfloat16)
    expert_dup = (expert_dact * jax.nn.silu(expert_gvals)).astype(jnp.bfloat16)
    gate_grad = jnp.einsum(
        "secd,secf->edf", arrived, expert_dgate, preferred_element_type=jnp.float32
    )
    up_grad = jnp.einsum("secd,secf->edf", arrived, expert_dup, preferred_element_type=jnp.float32)
    expert_din = (
        jnp.einsum("secf,edf->secd", expert_dgate, gate_full, preferred_element_type=jnp.float32)
        + jnp.einsum("secf,edf->secd", expert_dup, up_full, preferred_element_type=jnp.float32)
    ).astype(jnp.bfloat16)
    dreturned = lax.all_to_all(
        expert_din, "experts", split_axis=0, concat_axis=0, tiled=True
    ).reshape(expert_count * capacity, model_width)
    dnormed2_q = jnp.dot(placer, dreturned, preferred_element_type=jnp.float32)
    route_hits = (
        route_q[:, :, None] == jnp.arange(expert_count, dtype=jnp.int32)[None, None, :]
    ).astype(jnp.float32)
    dprob = jnp.sum(route_hits * dgate_k[:, :, None], 1)
    dlogit = prob * (dprob - jnp.sum(prob * dprob, -1, keepdims=True))
    router_part = jnp.dot(normed2_q.astype(jnp.float32).T, dlogit, precision=PRECISE)
    dnormed2_q = dnormed2_q + jnp.dot(
        dlogit, router_weight.astype(jnp.float32).T, precision=PRECISE
    )
    shared_dout = (shared_sig[:, None] * grad_float).astype(jnp.bfloat16)
    shared_dact = jnp.dot(shared_dout, sdown_full.T, preferred_element_type=jnp.float32)
    sdown_grad = jnp.dot(shared_act.T, shared_dout, preferred_element_type=jnp.float32)
    shared_dgate = (shared_dact * shared_uvals * silu_grad(shared_gvals)).astype(jnp.bfloat16)
    shared_dup = (shared_dact * jax.nn.silu(shared_gvals)).astype(jnp.bfloat16)
    sgate_grad = jnp.dot(normed2_b.T, shared_dgate, preferred_element_type=jnp.float32)
    sup_grad = jnp.dot(normed2_b.T, shared_dup, preferred_element_type=jnp.float32)
    row_dots = jnp.sum(grad_float * shared_part, -1)
    dnormed2_part = jnp.dot(
        shared_dgate, sgate_full.T, preferred_element_type=jnp.float32
    ) + jnp.dot(shared_dup, sup_full.T, preferred_element_type=jnp.float32)
    dnormed2_part = dnormed2_part + lax.dynamic_update_slice_in_dim(
        jnp.zeros((row_count, model_width), jnp.float32), dnormed2_q, first_row, 0
    )
    dnormed2, row_dots, router_grad = lax.psum((dnormed2_part, row_dots, router_part), "experts")
    coef = shared_sig * (1.0 - shared_sig) * row_dots
    dnormed2 = dnormed2 + coef[:, None] * shared_gate.astype(jnp.float32)[None, :]
    shared_gate_grad = jnp.dot(coef, normed2_b.astype(jnp.float32), precision=PRECISE)
    norm2_grad = jnp.sum(dnormed2 * normed2, 0)
    dscaled2 = dnormed2 * gain2
    dhidden = grad_float + inverse2 * (
        dscaled2 - normed2 * jnp.mean(dscaled2 * normed2, -1, keepdims=True)
    )
    dhidden_b = dhidden.astype(jnp.bfloat16)
    out_grad_part = jnp.dot(attended_flat.T, dhidden_b, preferred_element_type=jnp.float32)
    dattended = jnp.dot(dhidden_b, out_full.T, preferred_element_type=jnp.float32).astype(
        jnp.bfloat16
    )
    dattended3 = dattended.reshape(row_count, heads_here, HEAD_DIM)
    delta = jnp.sum(dattended3.astype(jnp.float32) * attended.astype(jnp.float32), -1)
    zero_state = jnp.zeros((heads_here, row_count, HEAD_DIM), jnp.float32)
    dkey_sum, dvalue_sum = key_grad_fold(
        key_rows,
        value_rows,
        query_first,
        scale,
        (zero_state, zero_state),
        (
            lax.all_gather(
                query.reshape(row_count, head_span).astype(jnp.float32),
                "context",
                axis=0,
                tiled=True,
            ),
            lax.all_gather(dattended.astype(jnp.float32), "context", axis=0, tiled=True),
            lax.all_gather(jnp.transpose(lse_heads), "context", axis=0, tiled=True),
            lax.all_gather(delta, "context", axis=0, tiled=True),
        ),
    )
    dquery_sum = query_grad_fold(
        query,
        dattended3,
        lse_heads,
        jnp.transpose(delta),
        query_first,
        scale,
        zero_state,
        (
            lax.all_gather(key_flat, "context", axis=0, tiled=True),
            lax.all_gather(value_flat, "context", axis=0, tiled=True),
        ),
    )
    dquery = jnp.transpose(dquery_sum, (1, 0, 2))
    dkey = jnp.transpose(dkey_sum, (1, 0, 2))
    dvalue = jnp.transpose(dvalue_sum, (1, 0, 2))
    dquery_raw = dquery * cosine + rotate_back(dquery * sine_part)
    dkey_raw = dkey * cosine + rotate_back(dkey * sine_part)
    dqkv = jnp.stack(
        [
            dquery_raw.reshape(row_count, head_span),
            dkey_raw.reshape(row_count, head_span),
            dvalue.reshape(row_count, head_span),
        ],
        1,
    )
    bias_grad = jnp.sum(dqkv, 0)
    dqkv_b = dqkv.astype(jnp.bfloat16).reshape(row_count, 3 * head_span)
    qkv_grad = jnp.dot(normed1_b.T, dqkv_b, preferred_element_type=jnp.float32).reshape(
        model_width, 3, head_span
    )
    dnormed1 = lax.psum(
        jnp.dot(dqkv_b, qkv_flat.T, preferred_element_type=jnp.float32).astype(jnp.bfloat16),
        "experts",
    ).astype(jnp.float32)
    norm1_grad = jnp.sum(dnormed1 * normed1, 0)
    dscaled1 = dnormed1 * gain1
    tokens_grad = dhidden + inverse1 * (
        dscaled1 - normed1 * jnp.mean(dscaled1 * normed1, -1, keepdims=True)
    )
    small_sums = (
        lax.psum(norm1_grad.astype(jnp.bfloat16), ("dp", "context")).astype(jnp.float32),
        lax.psum(norm2_grad.astype(jnp.bfloat16), ("dp", "context")).astype(jnp.float32),
        lax.psum(router_grad.astype(jnp.bfloat16), ("dp", "context")).astype(jnp.float32),
        lax.psum(shared_gate_grad.astype(jnp.bfloat16), ("dp", "context")).astype(jnp.float32),
        lax.psum(bias_grad.astype(jnp.bfloat16), ("dp", "context")).astype(jnp.float32),
    )
    large_sums = (
        lax.psum_scatter(
            qkv_grad.astype(jnp.bfloat16), ("dp", "context"), scatter_dimension=0, tiled=True
        ).astype(jnp.float32),
        lax.psum_scatter(
            out_grad_part.astype(jnp.bfloat16), ("dp", "context"), scatter_dimension=1, tiled=True
        ).astype(jnp.float32),
        lax.psum_scatter(
            gate_grad.astype(jnp.bfloat16), ("dp", "context"), scatter_dimension=1, tiled=True
        ).astype(jnp.float32),
        lax.psum_scatter(
            up_grad.astype(jnp.bfloat16), ("dp", "context"), scatter_dimension=1, tiled=True
        ).astype(jnp.float32),
        lax.psum_scatter(
            down_grad.astype(jnp.bfloat16), ("dp", "context"), scatter_dimension=2, tiled=True
        ).astype(jnp.float32),
        lax.psum_scatter(
            sgate_grad.astype(jnp.bfloat16), ("dp", "context"), scatter_dimension=0, tiled=True
        ).astype(jnp.float32),
        lax.psum_scatter(
            sup_grad.astype(jnp.bfloat16), ("dp", "context"), scatter_dimension=0, tiled=True
        ).astype(jnp.float32),
        lax.psum_scatter(
            sdown_grad.astype(jnp.bfloat16), ("dp", "context"), scatter_dimension=1, tiled=True
        ).astype(jnp.float32),
    )
    return (
        block_out[None],
        tokens_grad[None],
        small_sums[0],
        large_sums[0],
        small_sums[4],
        large_sums[1],
        small_sums[1],
        small_sums[2],
        large_sums[2],
        large_sums[3],
        large_sums[4],
        small_sums[3],
        large_sums[5],
        large_sums[6],
        large_sums[7],
    )


def own_half_first(value):
    half = value.shape[-1] // 2
    turned = jnp.concatenate([value[..., half:], value[..., :half]], -1)
    return jnp.where(lax.axis_index("dp") == 0, value, turned)


def dot_nn(left, right):
    return jnp.dot(left, right, preferred_element_type=jnp.float32)


def dot_nt(left, right):
    return lax.dot_general(
        left, right, (((1,), (1,)), ((), ())), preferred_element_type=jnp.float32
    )


def dot_tn(left, right):
    return lax.dot_general(
        left, right, (((0,), (0,)), ((), ())), preferred_element_type=jnp.float32
    )


MESH = pl.DeviceIdType.MESH
DMA = pltpu.SemaphoreType.DMA


def remote(source, target, send_sem, recv_sem, device):
    return pltpu.make_async_remote_copy(
        src_ref=source,
        dst_ref=target,
        send_sem=send_sem,
        recv_sem=recv_sem,
        device_id=device,
        device_id_type=MESH,
    )


def rows_at(ref, start, size):
    return ref.at[pl.ds(pl.multiple_of(start, 16), size), :]


def lanes_at(ref, start, size):
    return ref.at[:, pl.ds(pl.multiple_of(start, 128), size)]


class Spot:
    def __init__(self):
        self.parts = lax.axis_size("context")
        self.place, self.group = lax.axis_index("context"), lax.axis_index("experts")
        self.twin = {"dp": 1 - lax.axis_index("dp")}
        self.across = lax.rem(self.group + 2, 4)
        self.beside = self.group + 1 - 2 * lax.rem(self.group, 2)
        self.corner = lax.rem(self.beside + 2, 4)
        self.has_left, self.has_right = self.place > 0, self.place < self.parts - 1

    def greet(self, whole_line, twins):
        barrier = pltpu.get_barrier_semaphore()
        devices = [{"experts": self.across}, {"experts": self.beside}]
        if twins:
            devices.append(self.twin)
        for device in devices:
            pl.semaphore_signal(barrier, inc=1, device_id=device, device_id_type=MESH)
        count = len(devices)
        if whole_line:
            for gap in range(1, self.parts):
                device = {"context": lax.rem(self.place + gap, self.parts)}
                pl.semaphore_signal(barrier, inc=1, device_id=device, device_id_type=MESH)
            pl.semaphore_wait(barrier, count + self.parts - 1)
        else:
            for step, there in ((-1, self.has_left), (1, self.has_right)):

                @pl.when(there)
                def _():
                    device = {"context": self.place + step}
                    pl.semaphore_signal(barrier, inc=1, device_id=device, device_id_type=MESH)

            ends = jnp.where(self.has_left & self.has_right, 0, 1)
            pl.semaphore_wait(barrier, count + 2 - ends)

    def far_first(self):
        upper = self.place // (self.parts // 2)
        return [3 * (1 - upper), 2 - upper, 1 + 4 * upper - self.place, self.place]

    def others(self, gap, body):
        @pl.when(self.place >= gap)
        def _():
            body(self.place - gap)

        @pl.when(self.place + gap < self.parts)
        def _():
            body(self.place + gap)


class Share:
    def __init__(self, spot, own, out, sems):
        self.spot, self.own, self.out = spot, own, out
        self.local_sem, self.right_s, self.left_s, self.line_r, self.across_s, self.across_r, self.beside_s, self.beside_r = sems

    @staticmethod
    def sems(parts):
        return [DMA, DMA((parts,)), DMA((parts,)), DMA((parts,)), DMA((parts,)), DMA((parts,)), DMA((2 * parts,)), DMA((2 * parts,))]

    def block(self, part, column):
        rows = self.own.shape[0]
        return rows_at(self.out, (part * 4 + column) * rows, rows)

    def to_right(self, part, source):
        s = self.spot
        return remote(source, self.block(part, s.group), self.right_s.at[part], self.line_r.at[part], {"context": s.place + 1})

    def to_left(self, part, source):
        s = self.spot
        return remote(source, self.block(part, s.group), self.left_s.at[part], self.line_r.at[part], {"context": s.place - 1})

    def to_across(self, part, source):
        s = self.spot
        return remote(source, self.block(part, s.group), self.across_s.at[part], self.across_r.at[part], {"experts": s.across})

    def to_beside(self, part, column, slot, source):
        s = self.spot
        return remote(source, self.block(part, column), self.beside_s.at[slot], self.beside_r.at[slot], {"experts": s.beside})

    def begin(self):
        s = self.spot

        @pl.when(s.has_right)
        def _():
            self.to_right(s.place, self.own).start()

        @pl.when(s.has_left)
        def _():
            self.to_left(s.place, self.own).start()

        self.to_across(s.place, self.own).start()
        self.to_beside(s.place, s.group, s.place, self.own).start()
        self.local().start()

    def local(self):
        return pltpu.make_async_copy(self.own, self.block(self.spot.place, self.spot.group), self.local_sem)

    def pass_on(self, part):
        s = self.spot
        self.to_across(part, self.block(part, s.group)).wait_recv()
        self.to_beside(part, s.across, s.parts + part, self.block(part, s.across)).start()

    def arrival(self, part, onward, there):
        s = self.spot
        mine = self.block(part, s.group)
        self.to_right(part, mine).wait_recv()

        @pl.when(there)
        def _():
            onward(part, mine).start()

        self.to_across(part, mine).start()
        self.to_beside(part, s.group, part, mine).start()

    def step(self, gap):
        s = self.spot

        @pl.when(s.place >= gap)
        def _():
            self.arrival(s.place - gap, self.to_right, s.has_right)

        @pl.when(s.place + gap < s.parts)
        def _():
            self.arrival(s.place + gap, self.to_left, s.has_left)

        if gap == 1:
            self.pass_on(s.place)
        else:
            s.others(gap - 1, self.pass_on)

    def end(self):
        s = self.spot
        s.others(s.parts - 1, self.pass_on)
        self.local().wait()
        for part in range(s.parts):
            self.to_beside(part, s.beside, part, self.own).wait_recv()
            self.to_beside(part, s.beside, s.parts + part, self.own).wait_recv()
            self.to_across(part, self.own).wait_send()
            self.to_beside(part, s.group, part, self.own).wait_send()
            self.to_beside(part, s.group, s.parts + part, self.own).wait_send()

            @pl.when(s.has_right & (part <= s.place))
            def _():
                self.to_right(part, self.own).wait_send()

            @pl.when(s.has_left & (part >= s.place))
            def _():
                self.to_left(part, self.own).wait_send()


class Sum:
    def __init__(self, spot, part_ref, out, scratch):
        self.spot, self.part_ref, self.out = spot, part_ref, out
        (self.beside_buf, self.across_out, self.across_buf, self.line_out, self.left_buf, self.right_buf,
         self.beside_s, self.beside_r, self.across_s, self.across_r, self.right_s, self.left_s, self.from_left, self.from_right) = scratch
        self.order = spot.far_first()

    @staticmethod
    def scratch(parts, rows, width):
        one = pltpu.VMEM((parts, rows, width), jnp.bfloat16)
        two = pltpu.VMEM((2 * parts, rows, width), jnp.bfloat16)
        return [two, one, one, one, one, one, DMA((2 * parts,)), DMA((2 * parts,))] + [DMA((parts,))] * 6

    def base(self, part, column):
        rows = self.out.shape[0]
        return pl.multiple_of((part * 4 + column) * rows, rows)

    def to_beside(self, part, column, slot):
        source = self.part_ref.at[pl.ds(self.base(part, column), self.out.shape[0]), :]
        return remote(source, self.beside_buf.at[slot], self.beside_s.at[slot], self.beside_r.at[slot], {"experts": self.spot.beside})

    def to_across(self, part):
        return remote(self.across_out.at[part], self.across_buf.at[part], self.across_s.at[part], self.across_r.at[part], {"experts": self.spot.across})

    def to_right(self, part):
        return remote(self.line_out.at[part], self.left_buf.at[part], self.right_s.at[part], self.from_left.at[part], {"context": self.spot.place + 1})

    def to_left(self, part):
        return remote(self.line_out.at[part], self.right_buf.at[part], self.left_s.at[part], self.from_right.at[part], {"context": self.spot.place - 1})

    def chunks(self, body):
        step = 16

        def one(index, carry):
            start = pl.multiple_of(index * step, step)
            body(pl.ds(start, step), start, step)
            return carry

        lax.fori_loop(0, self.out.shape[0] // step, one, 0)

    def mine(self, base, start, step):
        return self.part_ref[pl.ds(pl.multiple_of(base + start, step), step), :].astype(jnp.float32)

    def begin(self):
        s = self.spot
        for part in self.order:
            self.to_beside(part, s.corner, s.parts + part).start()
        for part in self.order:
            self.to_beside(part, s.beside, part).start()

    def cross(self, index):
        s, part = self.spot, self.order[index]
        self.to_beside(part, s.corner, s.parts + part).wait_recv()
        base = self.base(part, s.across)

        def add(at, start, step):
            total = self.mine(base, start, step) + self.beside_buf[s.parts + part, at, :].astype(jnp.float32)
            self.across_out[part, at, :] = total.astype(jnp.bfloat16)

        self.chunks(add)
        self.to_across(part).start()

    def line(self, index):
        s, part = self.spot, self.order[index]
        self.to_beside(part, s.beside, part).wait_recv()
        self.to_across(part).wait_recv()
        base = self.base(part, s.group)
        f32 = jnp.float32

        def total(at, start, step):
            return self.mine(base, start, step) + self.beside_buf[part, at, :].astype(f32) + self.across_buf[part, at, :].astype(f32)

        def send(buf):
            def add(at, start, step):
                value = total(at, start, step)
                if buf is not None:
                    value = value + buf[part, at, :].astype(f32)
                self.line_out[part, at, :] = value.astype(jnp.bfloat16)

            self.chunks(add)

        if index < s.parts - 1:
            goes_right = part > s.place
            goes_left = jnp.logical_not(goes_right)

            @pl.when(goes_right & s.has_left)
            def _():
                self.to_right(part).wait_recv()
                send(self.left_buf)

            @pl.when(goes_left & s.has_right)
            def _():
                self.to_left(part).wait_recv()
                send(self.right_buf)

            @pl.when((goes_right & jnp.logical_not(s.has_left)) | (goes_left & jnp.logical_not(s.has_right)))
            def _():
                send(None)

            @pl.when(goes_right)
            def _():
                self.to_right(part).start()

            @pl.when(goes_left)
            def _():
                self.to_left(part).start()
        else:

            def keep(at, start, step):
                self.out[at, :] = total(at, start, step)

            self.chunks(keep)
            for there, copy, buf in ((s.has_left, self.to_right, self.left_buf), (s.has_right, self.to_left, self.right_buf)):

                @pl.when(there)
                def _():
                    copy(part).wait_recv()

                    def add(at, start, step):
                        self.out[at, :] = self.out[at, :] + buf[part, at, :].astype(f32)

                    self.chunks(add)

    def end(self):
        s = self.spot
        for part in range(s.parts):
            self.to_beside(part, s.corner, s.parts + part).wait_send()
            self.to_beside(part, s.beside, part).wait_send()
            self.to_across(part).wait_send()

            @pl.when(part > s.place)
            def _():
                self.to_right(part).wait_send()

            @pl.when(part < s.place)
            def _():
                self.to_left(part).wait_send()


class Move:
    def __init__(self, spot, items, sems):
        self.spot, self.items = spot, items
        self.line_s, self.line_r, self.twin_s, self.twin_r, self.local_sem = sems

    @staticmethod
    def sems(count, parts):
        return [DMA((count * parts,))] * 4 + [DMA((count,))]

    def to(self, number, target, source):
        s, (src, dst) = self.spot, self.items[number]
        return remote(src(target), dst(0, source), self.line_s.at[number * s.parts + target], self.line_r.at[number * s.parts + source], {"context": target})

    def on(self, number, source, view):
        s, (_, dst) = self.spot, self.items[number]
        slot = number * s.parts + source
        return remote(view, dst(1, source), self.twin_s.at[slot], self.twin_r.at[slot], s.twin)

    def local(self, number):
        s, (src, dst) = self.spot, self.items[number]
        return pltpu.make_async_copy(src(s.place), dst(0, s.place), self.local_sem.at[number])

    def own(self, number):
        s, (src, _) = self.spot, self.items[number]
        self.on(number, s.place, src(s.place)).start()
        self.local(number).start()

    def send_gap(self, number, gap):
        s = self.spot
        s.others(gap, lambda target: self.to(number, target, s.place).start())

    def send(self, number):
        for gap in range(self.spot.parts - 1, 0, -1):
            self.send_gap(number, gap)

    def forward(self, number, gap):
        s, (_, dst) = self.spot, self.items[number]

        def one(source):
            self.to(number, s.place, source).wait_recv()
            self.on(number, source, dst(0, source)).start()

        s.others(gap, one)

    def ready(self, number):
        s, (_, dst) = self.spot, self.items[number]
        self.local(number).wait()
        for part in range(s.parts):
            self.on(number, part, dst(0, part)).wait_recv()

    def sent(self):
        s = self.spot
        for number, (_, dst) in enumerate(self.items):
            for part in range(s.parts):
                self.on(number, part, dst(0, part)).wait_send()

                @pl.when(part != s.place)
                def _():
                    self.to(number, part, s.place).wait_send()

    def end(self):
        for number in range(len(self.items)):
            self.ready(number)
        self.sent()


class Return:
    def __init__(self, spot, items, got, mine, sems):
        self.spot, self.items, self.got, self.mine_buf = spot, items, got, mine
        self.twin_s, self.twin_r, self.load, self.line_s, self.line_r, self.local_sem = sems
        self.order = spot.far_first()
        self.bases = []
        for item in items:
            self.bases.append(self.bases[-1][1] if self.bases else 0)
            self.bases[-1] = (self.bases[-1], self.bases[-1] + len(item["pieces"]) * spot.parts)

    @staticmethod
    def scratch(shapes, pieces, parts):
        count = len(shapes)
        buf = [pltpu.VMEM((parts,) + shape, jnp.bfloat16) for shape in shapes]
        sems = [DMA((count * parts,))] * 3 + [DMA((sum(pieces) * parts,))] * 2 + [DMA((sum(pieces),))]
        return buf + buf + sems

    def swap(self, number, part):
        item, slot = self.items[number], number * self.spot.parts + part
        return remote(item["block"](1, part), self.got[number].at[part], self.twin_s.at[slot], self.twin_r.at[slot], self.spot.twin)

    def fetch(self, number, part):
        item, slot = self.items[number], number * self.spot.parts + part
        return pltpu.make_async_copy(item["block"](0, part), self.mine_buf[number].at[part], self.load.at[slot])

    def start(self, number):
        for part in self.order:
            self.swap(number, part).start()
            self.fetch(number, part).start()

    def piece(self, number, which, target, source, short):
        s = self.spot
        cut, out = self.items[number]["pieces"][which]
        slot = self.bases[number][0] + which * s.parts
        return remote(cut(self.mine_buf[number].at[target], short), out(source, short), self.line_s.at[slot + target], self.line_r.at[slot + source], {"context": target})

    def keep(self, number, which, short):
        s = self.spot
        cut, out = self.items[number]["pieces"][which]
        slot = self.bases[number][0] // s.parts + which
        return pltpu.make_async_copy(cut(self.mine_buf[number].at[s.place], short), out(s.place, short), self.local_sem.at[slot])

    def by_width(self, source, body):
        last = source == self.spot.parts - 1
        if not isinstance(source, int):

            @pl.when(last)
            def _():
                body(True)

            @pl.when(jnp.logical_not(last))
            def _():
                body(False)
        else:
            body(last)

    def reduce(self, number, index):
        s, part = self.spot, self.order[index]
        item = self.items[number]
        self.swap(number, part).wait_recv()
        self.fetch(number, part).wait()
        mine, got = self.mine_buf[number], self.got[number]
        rows, step = mine.shape[1], 32

        def one(at, carry):
            span = pl.ds(pl.multiple_of(at * step, step), step)
            total = mine[part, span, :].astype(jnp.float32) + got[part, span, :].astype(jnp.float32)
            mine[part, span, :] = total.astype(jnp.bfloat16)
            return carry

        lax.fori_loop(0, rows // step, one, 0)
        for which in range(len(item["pieces"])):
            if index < s.parts - 1:
                self.by_width(s.place, lambda short: self.piece(number, which, part, s.place, short).start())
            else:
                self.by_width(s.place, lambda short: self.keep(number, which, short).start())

    def end(self):
        s = self.spot
        for number, item in enumerate(self.items):
            for part in range(s.parts):
                self.swap(number, part).wait_send()
                for which in range(len(item["pieces"])):

                    @pl.when(part != s.place)
                    def _():
                        self.by_width(s.place, lambda short: self.piece(number, which, part, s.place, short).wait_send())
                        self.by_width(part, lambda short: self.piece(number, which, s.place, part, short).wait_recv())

            for which in range(len(item["pieces"])):
                self.by_width(s.place, lambda short: self.keep(number, which, short).wait())


def comm_call(kernel, number, name, out_shape, out_specs, in_specs, scratch, bytes_moved):
    return pl.pallas_call(
        kernel,
        out_shape=out_shape,
        in_specs=in_specs,
        out_specs=out_specs,
        scratch_shapes=scratch,
        compiler_params=pltpu.CompilerParams(collective_id=number, has_side_effects=True),
        cost_estimate=pl.CostEstimate(flops=0, bytes_accessed=bytes_moved, transcendentals=0),
        name=name,
    )


IN_VMEM = pl.BlockSpec(memory_space=pltpu.VMEM)
IN_PLACE = pl.BlockSpec(memory_space=pl.ANY)
WINDOW = 384


def window_of(index, length):
    return jnp.minimum(index * WINDOW, length - WINDOW)


def turn(value, cosine, sine_part):
    return value * cosine + pltpu.roll(value, HEAD_DIM // 2, 1) * sine_part


def turn_tables(facts):
    both = facts[:, :HEAD_DIM].astype(jnp.float32) + facts[:, HEAD_DIM:].astype(jnp.float32)
    swapped = pltpu.roll(both, HEAD_DIM // 2, 1)
    low = lax.broadcasted_iota(jnp.int32, (1, HEAD_DIM), 1) < HEAD_DIM // 2
    return jnp.where(low, both, swapped), jnp.where(low, -swapped, both)


def attention_first(value, qkv_in, out_weight, bias, shared_down, expert_down, number):
    parts = lax.axis_size("context")
    rows, wide = value.shape
    block, span = qkv_in.shape[0] // parts, qkv_in.shape[1]
    head, lanes = out_weight.shape[0] // parts, out_weight.shape[1]
    width, length = 2 * parts * lanes, rows * parts * 4
    units = shared_down.shape[0]
    count = 1 + expert_down.shape[0]
    step = 256
    scale = HEAD_DIM ** (-0.5)
    f32, bf16 = jnp.float32, jnp.bfloat16
    sets = [
        [
            pltpu.VMEM((length, wide), bf16),
            pltpu.VMEM((2 * parts * block, span), bf16),
            pltpu.VMEM((head, width), bf16),
            pltpu.VMEM((length, width), bf16),
            DMA((3,)),
        ],
        Share.sems(parts),
        Move.sems(2 + count, parts),
        Sum.scratch(parts, rows, width),
    ]

    def kernel(own_ref, qkv_ref, outw_ref, bias_ref, shared_ref, expert_ref,
               all_hbm, wqkv_hbm, wout_hbm, wd_ref, q_ref, k_ref, v_ref, att_ref, lse_ref, sum_ref, *scratch):
        scratch, split = list(scratch), []
        for one in sets:
            split.append(scratch[: len(one)])
            scratch = scratch[len(one) :]
        all_ref, wqkv_ref, wout_ref, part_ref, keep = split[0]
        spot = Spot()
        share = Share(spot, own_ref, all_ref, split[1])
        items = [
            (
                lambda target: rows_at(qkv_ref, target * block, block),
                lambda side, source: rows_at(wqkv_ref, (side * parts + source) * block, block),
            ),
            (
                lambda target: rows_at(outw_ref, target * head, head),
                lambda side, source: lanes_at(wout_ref, (side * parts + source) * lanes, lanes),
            ),
        ]

        def down(k):
            ref = shared_ref if k == 0 else expert_ref.at[k - 1]
            return (
                lambda target: rows_at(ref, window_of(target, units), WINDOW),
                lambda side, source: wd_ref.at[
                    pl.ds(k * WINDOW, WINDOW),
                    pl.ds(pl.multiple_of((side * parts + source) * lanes, lanes), lanes),
                ],
            )

        move = Move(spot, items + [down(k) for k in range(count)], split[2])
        summed = Sum(spot, part_ref, sum_ref, split[3])
        copies = [
            pltpu.make_async_copy(source, target, keep.at[index])
            for index, (source, target) in enumerate(((all_ref, all_hbm), (wqkv_ref, wqkv_hbm), (wout_ref, wout_hbm)))
        ]

        def project(index, carry):
            at = pl.ds(pl.multiple_of(index * step, step), step)
            qkv = jnp.dot(all_ref[at, :width], wqkv_ref[...], preferred_element_type=f32) + bias_ref[...]
            cosine, sine_part = turn_tables(all_ref[at, width:])
            q_ref[at, :] = turn(qkv[:, :HEAD_DIM], cosine, sine_part).astype(bf16)
            k_ref[at, :] = turn(qkv[:, HEAD_DIM : 2 * HEAD_DIM], cosine, sine_part).astype(bf16)
            v_ref[at, :] = qkv[:, 2 * HEAD_DIM :].astype(bf16)
            return carry

        def attend(index, carry):
            start = pl.multiple_of(index * step, step)
            at = pl.ds(start, step)
            scores = dot_nt(q_ref[at, :], k_ref[...]) * scale
            query_index = start + lax.broadcasted_iota(jnp.int32, scores.shape, 0)
            allowed = lax.broadcasted_iota(jnp.int32, scores.shape, 1) <= query_index
            row_max = jnp.max(jnp.where(allowed, scores, MASKED), -1, keepdims=True)
            weights = jnp.where(allowed, jnp.exp(scores - row_max), 0.0)
            row_sum = jnp.sum(weights, -1, keepdims=True)
            attended = (jnp.dot(weights.astype(bf16), v_ref[...], preferred_element_type=f32) / row_sum).astype(bf16)
            att_ref[at, :] = attended
            lse_ref[at, :] = jnp.broadcast_to(row_max + jnp.log(row_sum), (step, HEAD_DIM))
            part_ref[at, :] = jnp.dot(attended, wout_ref[...], preferred_element_type=f32).astype(bf16)
            return carry

        spot.greet(True, True)
        share.begin()
        for number in range(len(move.items)):
            move.own(number)
        move.send_gap(0, 3)
        share.step(1)
        move.send_gap(0, 2)
        share.step(2)
        move.send_gap(0, 1)
        share.step(3)
        move.send(1)
        move.send(2)
        for gap in (1, 2, 3):
            move.forward(0, gap)
        for gap in (1, 2, 3):
            move.forward(1, gap)
        share.end()
        copies[0].start()
        move.ready(0)
        copies[1].start()
        lax.fori_loop(0, length // step, project, 0)
        move.ready(1)
        copies[2].start()
        for number in range(3, len(move.items)):
            move.send(number)
        lax.fori_loop(0, length // step, attend, 0)
        summed.begin()
        for gap in (1, 2, 3):
            move.forward(2, gap)
        for index in range(parts):
            summed.cross(index)
        for number in range(3, len(move.items)):
            for gap in (1, 2, 3):
                move.forward(number, gap)
        for index in range(parts):
            summed.line(index)
        summed.end()
        for number in range(2, len(move.items)):
            move.ready(number)
        move.sent()
        for copy in copies:
            copy.wait()

    heads = jax.ShapeDtypeStruct((length, HEAD_DIM), bf16)
    return comm_call(
        kernel,
        number,
        "attention_first",
        [
            jax.ShapeDtypeStruct((length, wide), bf16),
            jax.ShapeDtypeStruct((2 * parts * block, span), bf16),
            jax.ShapeDtypeStruct((head, width), bf16),
            jax.ShapeDtypeStruct((count * WINDOW, width), bf16),
            heads,
            heads,
            heads,
            heads,
            jax.ShapeDtypeStruct((length, HEAD_DIM), f32),
            jax.ShapeDtypeStruct((rows, width), f32),
        ],
        [IN_PLACE] * 4 + [IN_VMEM] * 6,
        [IN_VMEM, IN_PLACE, IN_PLACE, IN_VMEM, IN_PLACE, IN_PLACE],
        [one for group in sets for one in group],
        250_000_000,
    )(value, qkv_in, out_weight, bias, shared_down, expert_down)


def share_move_compute(value, shared_gate, shared_up, expert_gate, expert_up, wd, number):
    parts = lax.axis_size("context")
    rows, wide = value.shape
    width = wd.shape[1]
    block, units = shared_gate.shape
    stacks = 1 + expert_gate.shape[0]
    count = 2 * stacks
    length = rows * parts * 4
    experts = (stacks - 1) * 4
    step = 256
    f32, bf16 = jnp.float32, jnp.bfloat16
    share_sems, move_sems = Share.sems(parts), Move.sems(count, parts)
    scratch = [
        pltpu.VMEM((length, wide), bf16),
        pltpu.VMEM((2 * parts * block, count * WINDOW), bf16),
        pltpu.VMEM(wd.shape, bf16),
        pltpu.VMEM((length, width), f32),
        pltpu.VMEM((length, width), f32),
        pltpu.VMEM((length, 128), f32),
        pltpu.VMEM((length, stacks * WINDOW), bf16),
        pltpu.VMEM((length, count * WINDOW), bf16),
        pltpu.VMEM((2, step, width + 128), bf16),
        pltpu.VMEM((2, step, width), bf16),
        DMA((2,)),
        DMA((stacks,)),
        DMA((stacks,)),
        DMA((length // step,)),
        DMA((length // step,)),
    ]

    def kernel(own_ref, sg_ref, su_ref, eg_ref, eu_ref, wd_hbm, both_hbm, send_hbm, branch_hbm, dup_hbm, act_hbm, *rest):
        both, wgu, wd_ref, dx_acc, out_acc, dot_acc, act_ref, dup_ref, send_buf, branch_buf, load, act_s, dup_s, send_s, branch_s = rest[: len(scratch)]
        sems = rest[len(scratch) :]
        spot = Spot()
        share = Share(spot, own_ref, both, sems[: len(share_sems)])

        def item(number):
            k = number // 2
            shared, expert = (sg_ref, eg_ref) if number % 2 == 0 else (su_ref, eu_ref)
            ref = shared if k == 0 else expert.at[k - 1]
            return (
                lambda target: lanes_at(ref, window_of(target, units), WINDOW),
                lambda side, source: wgu.at[
                    pl.ds(pl.multiple_of((side * parts + source) * block, block), block),
                    pl.ds(number * WINDOW, WINDOW),
                ],
            )

        move = Move(spot, [item(number) for number in range(count)], sems[len(share_sems) :])
        weights = pltpu.make_async_copy(wd_hbm, wd_ref, load.at[0])
        keep = pltpu.make_async_copy(both, both_hbm, load.at[1])
        repeated = jnp.where(spot.place == parts - 1, WINDOW * parts - units, 0)
        lane = lax.broadcasted_iota(jnp.int32, (1, WINDOW), 1)
        fresh = jnp.where(lane >= repeated, 1.0, 0.0)
        column = lax.broadcasted_iota(jnp.int32, (1, 128), 1)

        def send_out(index):
            at = pl.ds(pl.multiple_of(index * step, step), step)
            return pltpu.make_async_copy(send_buf.at[lax.rem(index, 2)], send_hbm.at[at, :], send_s.at[index])

        def branch_out(index):
            at = pl.ds(pl.multiple_of(index * step, step), step)
            return pltpu.make_async_copy(branch_buf.at[lax.rem(index, 2)], branch_hbm.at[at, :], branch_s.at[index])

        def act_out(k):
            at = pl.ds(k * WINDOW, WINDOW)
            return pltpu.make_async_copy(act_ref.at[:, at], act_hbm.at[:, at], act_s.at[k])

        def dup_out(k):
            at = pl.ds(2 * k * WINDOW, 2 * WINDOW)
            return pltpu.make_async_copy(dup_ref.at[:, at], dup_hbm.at[:, at], dup_s.at[k])

        def compute(k, first, last):
            up, down = pl.ds(2 * k * WINDOW, 2 * WINDOW), pl.ds(k * WINDOW, WINDOW)
            at = experts if k == 0 else spot.group * (stacks - 1) + k - 1
            here = jnp.where(column == at, 1.0, 0.0)
            both_parts = jnp.where((column == at) | (column == at + 64), 1.0, 0.0)

            def one(index, carry):
                rows_here = pl.ds(pl.multiple_of(index * step, step), step)
                vals = jnp.dot(both[rows_here, :width], wgu[:, up], preferred_element_type=f32)
                raw = dot_nt(both[rows_here, width : 2 * width], wd_ref[down, :]) * fresh
                coef = jnp.sum(both[rows_here, 2 * width :].astype(f32) * both_parts, -1, keepdims=True)
                g_vals, u_vals = vals[:, :WINDOW], vals[:, WINDOW:]
                sig_g = jax.nn.sigmoid(g_vals)
                silu_g = g_vals * sig_g
                act = silu_g * u_vals
                dots = jnp.sum(raw * act, -1, keepdims=True) * here
                act_ref[rows_here, down] = (act * (coef * fresh)).astype(bf16)
                dact = raw * coef
                dup_ref[rows_here, pl.ds(2 * k * WINDOW, WINDOW)] = (
                    dact * u_vals * (sig_g * (1.0 + g_vals * (1.0 - sig_g)))
                ).astype(bf16)
                dup_ref[rows_here, pl.ds((2 * k + 1) * WINDOW, WINDOW)] = (dact * silu_g).astype(bf16)
                out_part = jnp.dot(act_ref[rows_here, down], wd_ref[down, :], preferred_element_type=f32)
                dx_part = dot_nt(dup_ref[rows_here, up], wgu[:, up])
                if k == 0:
                    out_acc[rows_here, :] = out_part
                    dx_acc[rows_here, :] = dx_part
                    dot_acc[rows_here, :] = dots
                elif k < stacks - 1:
                    out_acc[rows_here, :] += out_part
                    dx_acc[rows_here, :] += dx_part
                    dot_acc[rows_here, :] += dots
                else:

                    @pl.when(index >= 2)
                    def _():
                        send_out(index - 2).wait()
                        branch_out(index - 2).wait()

                    slot = lax.rem(index, 2)
                    branch_buf[slot] = (out_acc[rows_here, :] + out_part).astype(bf16)
                    send_buf[slot, :, :width] = (dx_acc[rows_here, :] + dx_part).astype(bf16)
                    send_buf[slot, :, width:] = (dot_acc[rows_here, :] + dots).astype(bf16)
                    send_out(index).start()
                    branch_out(index).start()
                return carry

            lax.fori_loop(first, last, one, 0)

        def forward(number):
            for gap in (1, 2, 3):
                move.forward(number, gap)

        spot.greet(True, True)
        share.begin()
        weights.start()
        for number in range(count):
            move.own(number)
        move.send(0)
        share.step(1)
        move.send(1)
        share.step(2)
        forward(0)
        share.step(3)
        for number in range(2, count):
            move.send(number)
        share.end()
        keep.start()
        forward(1)
        weights.wait()
        pieces = length // step
        for k in range(stacks):
            if k < stacks - 1:
                forward(2 * k + 2)
            move.ready(2 * k)
            move.ready(2 * k + 1)
            compute(k, 0, pieces // 2)
            if k < stacks - 1:
                forward(2 * k + 3)
            compute(k, pieces // 2, pieces)
            act_out(k).start()
            dup_out(k).start()
        for index in (pieces - 2, pieces - 1):
            send_out(index).wait()
            branch_out(index).wait()
        for k in range(stacks):
            act_out(k).wait()
            dup_out(k).wait()
        keep.wait()
        move.sent()

    return comm_call(
        kernel,
        number,
        "share_move_compute",
        [
            jax.ShapeDtypeStruct((length, wide), bf16),
            jax.ShapeDtypeStruct((length, width + 128), bf16),
            jax.ShapeDtypeStruct((length, width), bf16),
            jax.ShapeDtypeStruct((length, count * WINDOW), bf16),
            jax.ShapeDtypeStruct((length, stacks * WINDOW), bf16),
        ],
        [IN_PLACE] * 5,
        [IN_VMEM] + [IN_PLACE] * 5,
        scratch + share_sems + move_sems,
        300_000_000,
    )(value, shared_gate, shared_up, expert_gate, expert_up, wd)


def up_item(grads_ref, k, gate_ref, up_ref, block, parts):
    hidden = gate_ref.shape[1]
    tail = hidden - (parts - 1) * WINDOW

    def cut(offset):
        return lambda buf, short: buf.at[:, pl.ds(offset + (WINDOW - tail if short else 0), tail if short else WINDOW)]

    def out(ref):
        return lambda source, short: ref.at[:, pl.ds(hidden - tail, tail)] if short else lanes_at(ref, source * WINDOW, WINDOW)

    return {
        "block": lambda side, part: grads_ref.at[
            pl.ds(pl.multiple_of((side * parts + part) * block, block), block), pl.ds(2 * k * WINDOW, 2 * WINDOW)
        ],
        "pieces": [(cut(0), out(gate_ref)), (cut(WINDOW), out(up_ref))],
        "shape": (block, 2 * WINDOW),
    }


def down_item(grads_ref, k, down_ref, parts):
    hidden, lanes = down_ref.shape
    tail = hidden - (parts - 1) * WINDOW
    return {
        "block": lambda side, part: grads_ref.at[
            pl.ds(k * WINDOW, WINDOW), pl.ds(pl.multiple_of((side * parts + part) * lanes, lanes), lanes)
        ],
        "pieces": [
            (
                lambda buf, short: buf.at[pl.ds(WINDOW - tail if short else 0, tail if short else WINDOW), :],
                lambda source, short: down_ref.at[pl.ds(hidden - tail, tail), :] if short else rows_at(down_ref, source * WINDOW, WINDOW),
            )
        ],
        "shape": (WINDOW, lanes),
    }


def attention_last(send4, up_grads, down_grads, hidden, grad, gain, chances, named, router, out_w, qkv_w, heads, lse, turns, number):
    parts = lax.axis_size("context")
    length, width = send4.shape[0], hidden.shape[1]
    rows, wide = hidden.shape[0], send4.shape[1]
    block = up_grads.shape[0] // (2 * parts)
    lanes = down_grads.shape[1] // (2 * parts)
    units = WINDOW * parts - 128
    step = 256
    experts = 8
    scale = HEAD_DIM ** (-0.5)
    f32, bf16 = jnp.float32, jnp.bfloat16
    shapes, pieces = [(block, 2 * WINDOW), (WINDOW, lanes)], [2, 1]
    sets = [
        [
            pltpu.VMEM((rows, wide), f32),
            pltpu.VMEM((rows, width), bf16),
            pltpu.VMEM((length, width), bf16),
            pltpu.VMEM((length, width), bf16),
            pltpu.VMEM((length, HEAD_DIM), bf16),
            pltpu.VMEM((length, HEAD_DIM), f32),
            pltpu.VMEM((length, HEAD_DIM), f32),
            pltpu.VMEM((length, HEAD_DIM), f32),
            DMA,
        ],
        Sum.scratch(parts, rows, wide),
        Share.sems(parts),
        Sum.scratch(parts, rows, width),
        Return.scratch(shapes, pieces, parts),
    ]

    def kernel(send_ref, upg_ref, downg_ref, hidden_ref, grad_ref, gain_ref, chance_ref, named_ref, router_ref, wout_ref, wqkv_ref,
               q_ref, k_ref, v_ref, att_ref, lse_ref, turn_ref,
               dh_hbm, gate_out, up_out, down_out, dots_ref, dxn2_ref, dhidden_ref, dqkv_ref, bias_ref, dxn1_ref, *scratch):
        scratch, split = list(scratch), []
        for one in sets:
            split.append(scratch[: len(one)])
            scratch = scratch[len(one) :]
        sums, dh_own, dh_all, part_ref, datt_ref, dq_acc, dk_acc, dv_acc, keep_sem = split[0]
        spot = Spot()
        first = Sum(spot, send_ref, sums, split[1])
        share = Share(spot, dh_own, dh_all, split[2])
        second = Sum(spot, part_ref, dxn1_ref, split[3])
        items = [up_item(upg_ref, 0, gate_out, up_out, block, parts), down_item(downg_ref, 0, down_out, parts)]
        back = Return(spot, items, split[4][:2], split[4][2:4], split[4][4:])
        keep = pltpu.make_async_copy(dh_all, dh_hbm, keep_sem)

        def owner():
            lane = lax.broadcasted_iota(jnp.int32, (rows, 128), 1)
            dots = sums[:, width:]
            dots_ref[...] = dots
            chance = chance_ref[...]
            dprob = dots * named_ref[...]
            prob = jnp.where(lane < experts, chance, 0.0)
            dlogit = prob * (dprob - jnp.sum(prob * dprob, -1, keepdims=True))
            mix = jnp.where(lane < experts, dlogit, jnp.where(lane == experts, chance * (1.0 - chance) * dots, 0.0))
            dxn2_ref[...] = jnp.dot(mix, router_ref[...], precision=PRECISE, preferred_element_type=f32)

            def one(index, carry):
                at = pl.ds(pl.multiple_of(index * 16, 16), 16)
                dxn2 = dxn2_ref[at, :] + sums[at, :width]
                dxn2_ref[at, :] = dxn2
                value = hidden_ref[at, :]
                inverse = lax.rsqrt(jnp.mean(value * value, -1, keepdims=True) + EPSILON)
                normed = value * inverse
                scaled = dxn2 * gain_ref[...]
                dhidden = grad_ref[at, :].astype(f32) + inverse * (scaled - normed * jnp.mean(scaled * normed, -1, keepdims=True))
                dhidden_ref[at, :] = dhidden
                dh_own[at, :] = dhidden.astype(bf16)
                return carry

            lax.fori_loop(0, rows // 16, one, 0)

        def attend(index, carry):
            start = pl.multiple_of(index * step, step)
            at = pl.ds(start, step)
            datt = dot_nt(dh_all[at, :], wout_ref[...]).astype(bf16)
            delta = jnp.sum(datt.astype(f32) * att_ref[at, :].astype(f32), -1, keepdims=True)
            scores = dot_nt(q_ref[at, :], k_ref[...]) * scale
            query_index = start + lax.broadcasted_iota(jnp.int32, scores.shape, 0)
            allowed = lax.broadcasted_iota(jnp.int32, scores.shape, 1) <= query_index
            prob = jnp.where(allowed, jnp.exp(scores - lse_ref[at, :1]), 0.0)
            dscore = (prob * (dot_nt(datt, v_ref[...]) - delta)).astype(bf16)
            dq_acc[at, :] = jnp.dot(dscore, k_ref[...], preferred_element_type=f32) * scale
            dk_acc[...] += dot_tn(dscore, q_ref[at, :])
            dv_acc[...] += dot_tn(prob.astype(bf16), datt)
            return carry

        def project(index, carry):
            at = pl.ds(pl.multiple_of(index * step, step), step)
            cosine, sine_part = turn_tables(turn_ref[at, :])
            dq, dk, dv = dq_acc[at, :], dk_acc[at, :] * scale, dv_acc[at, :]
            dq = dq * cosine - pltpu.roll(dq, HEAD_DIM // 2, 1) * sine_part
            dk = dk * cosine - pltpu.roll(dk, HEAD_DIM // 2, 1) * sine_part
            for which, value in enumerate((dq, dk, dv)):
                bias_ref[:, pl.ds(which * HEAD_DIM, HEAD_DIM)] += jnp.sum(value, 0, keepdims=True)
                dqkv_ref[at, pl.ds(which * HEAD_DIM, HEAD_DIM)] = value.astype(bf16)
            part_ref[at, :] = dot_nt(dqkv_ref[at, :], wqkv_ref[...]).astype(bf16)
            return carry

        spot.greet(True, True)
        first.begin()
        back.start(0)
        back.start(1)
        dk_acc[...] = jnp.zeros_like(dk_acc)
        dv_acc[...] = jnp.zeros_like(dv_acc)
        bias_ref[...] = jnp.zeros_like(bias_ref)
        for index in range(parts):
            first.cross(index)
        back.reduce(0, 0)
        back.reduce(0, 1)
        for index in range(parts):
            first.line(index)
        owner()
        share.begin()
        share.step(1)
        share.step(2)
        back.reduce(0, 2)
        share.step(3)
        back.reduce(0, 3)
        share.end()
        keep.start()
        back.reduce(1, 0)
        back.reduce(1, 1)
        lax.fori_loop(0, length // step, attend, 0)
        lax.fori_loop(0, length // step, project, 0)
        second.begin()
        back.reduce(1, 2)
        for index in range(parts):
            second.cross(index)
        back.reduce(1, 3)
        for index in range(parts):
            second.line(index)
        first.end()
        second.end()
        back.end()
        keep.wait()

    piece = jax.ShapeDtypeStruct((block, units), bf16)
    return comm_call(
        kernel,
        number,
        "attention_last",
        [
            jax.ShapeDtypeStruct((length, width), bf16),
            piece,
            piece,
            jax.ShapeDtypeStruct((units, lanes), bf16),
            jax.ShapeDtypeStruct((rows, 128), f32),
            jax.ShapeDtypeStruct((rows, width), f32),
            jax.ShapeDtypeStruct((rows, width), f32),
            jax.ShapeDtypeStruct((length, 3 * HEAD_DIM), bf16),
            jax.ShapeDtypeStruct((1, 3 * HEAD_DIM), f32),
            jax.ShapeDtypeStruct((rows, width), f32),
        ],
        [IN_PLACE] * 4 + [IN_VMEM] * 6,
        [IN_VMEM, IN_PLACE, IN_PLACE] + [IN_VMEM] * 14,
        [one for group in sets for one in group],
        250_000_000,
    )(send4, up_grads, down_grads, hidden, grad, gain, chances, named, router, out_w, qkv_w, *heads, lse, turns)


class Group:
    def __init__(self, spot, own, out, sems):
        self.spot, self.own, self.out = spot, own, out
        self.local_sem, self.across_s, self.across_r, self.beside_s, self.beside_r = sems

    @staticmethod
    def sems():
        return [DMA, DMA, DMA, DMA((2,)), DMA((2,))]

    def block(self, column):
        rows = self.own.shape[0]
        return rows_at(self.out, column * rows, rows)

    def to_across(self):
        s = self.spot
        return remote(self.own, self.block(s.group), self.across_s, self.across_r, {"experts": s.across})

    def to_beside(self, slot):
        s = self.spot
        column = s.across if slot else s.group
        source = self.block(column) if slot else self.own
        return remote(source, self.block(column), self.beside_s.at[slot], self.beside_r.at[slot], {"experts": s.beside})

    def local(self):
        return pltpu.make_async_copy(self.own, self.block(self.spot.group), self.local_sem)

    def begin(self):
        self.to_across().start()
        self.to_beside(0).start()
        self.local().start()

    def end(self):
        self.to_across().wait_recv()
        self.to_beside(1).start()
        self.local().wait()
        self.to_across().wait_send()
        for slot in range(2):
            self.to_beside(slot).wait()


class Total:
    def __init__(self, spot, value, out, scratch):
        self.out = out
        self.sent, self.got, self.send_s, self.recv_s = scratch
        place = spot.place
        self.turns = [
            spot.twin,
            {"context": place + 1 - 2 * lax.rem(place, 2)},
            {"context": lax.rem(place + 2, spot.parts)},
            {"experts": spot.beside},
            {"experts": spot.across},
        ]
        self.value = value

    @staticmethod
    def scratch(shape):
        buf = pltpu.VMEM((5,) + shape, jnp.float32)
        return [buf, buf, DMA((5,)), DMA((5,))]

    def copy(self, index):
        return remote(self.sent.at[index], self.got.at[index], self.send_s.at[index], self.recv_s.at[index], self.turns[index])

    def begin(self):
        self.out[...] = self.value[...]
        self.send(0)

    def send(self, index):
        self.sent[index] = self.out[...]
        self.copy(index).start()

    def take(self, index):
        self.copy(index).wait()
        self.out[...] = self.out[...] + self.got[index]


def last_exchange(up_grads, down_grads, out_grads, qkv_grads, branch, hidden, tokens_grad, small, ups, downs, number):
    parts = lax.axis_size("context")
    block = up_grads.shape[0] // (2 * parts)
    lanes = down_grads.shape[1] // (2 * parts)
    units = WINDOW * parts - 128
    head, span = out_grads.shape[0], qkv_grads.shape[1]
    rows, width = hidden.shape
    shapes = [(head, lanes), (block, span)] + [(block, 2 * WINDOW)] * len(ups) + [(WINDOW, lanes)] * len(downs)
    pieces = [1, 1] + [2] * len(ups) + [1] * len(downs)
    count, bf16 = len(shapes), jnp.bfloat16
    groups = [
        Return.scratch(shapes, pieces, parts),
        Sum.scratch(parts, rows, width) + [pltpu.VMEM((rows, width), jnp.float32), pltpu.VMEM((rows, width), bf16)],
        Total.scratch(small.shape),
        Group.sems(),
        Group.sems(),
    ]
    piece, column = jax.ShapeDtypeStruct((block, units), bf16), jax.ShapeDtypeStruct((units, lanes), bf16)
    out_shape = [jax.ShapeDtypeStruct((parts * head, lanes), bf16), jax.ShapeDtypeStruct((parts * block, span), bf16)]
    out_shape += [piece] * (2 * len(ups)) + [column] * len(downs)
    out_shape += [
        jax.ShapeDtypeStruct((4 * rows, width), bf16),
        jax.ShapeDtypeStruct((4 * rows, width), jnp.float32),
        jax.ShapeDtypeStruct(small.shape, jnp.float32),
    ]

    def kernel(upg_ref, downg_ref, outg_ref, qkvg_ref, branch_ref, hidden_ref, tokens_ref, small_ref, *rest):
        outs, scratch = rest[: len(out_shape)], list(rest[len(out_shape) :])
        sets = []
        for one in groups:
            sets.append(scratch[: len(one)])
            scratch = scratch[len(one) :]
        grads, (block_all, tokens_all, small_out) = outs[:-3], outs[-3:]
        items = [
            {
                "block": lambda side, part: lanes_at(outg_ref, (side * parts + part) * lanes, lanes),
                "pieces": [(lambda buf, short: buf, lambda source, short: rows_at(grads[0], source * head, head))],
            },
            {
                "block": lambda side, part: rows_at(qkvg_ref, (side * parts + part) * block, block),
                "pieces": [(lambda buf, short: buf, lambda source, short: rows_at(grads[1], source * block, block))],
            },
        ]
        items += [up_item(upg_ref, k, grads[2 + 2 * i], grads[3 + 2 * i], block, parts) for i, k in enumerate(ups)]
        items += [down_item(downg_ref, k, grads[2 + 2 * len(ups) + i], parts) for i, k in enumerate(downs)]
        spot = Spot()
        back = Return(spot, items, sets[0][:count], sets[0][count : 2 * count], sets[0][2 * count :])
        total_branch, own_block = sets[1][-2:]
        summed = Sum(spot, branch_ref, total_branch, sets[1][:-2])
        total = Total(spot, small_ref, small_out, sets[2])
        tokens_group = Group(spot, tokens_ref, tokens_all, sets[3])
        block_group = Group(spot, own_block, block_all, sets[4])
        spot.greet(True, True)
        total.begin()
        summed.begin()
        back.start(0)
        back.start(1)
        total.take(0)
        total.send(1)
        for index in range(parts):
            summed.cross(index)
        total.take(1)
        total.send(2)
        for item in range(2, count):
            back.start(item)
        for index in range(parts):
            back.reduce(0, index)
        total.take(2)
        total.send(3)
        for index in range(parts):
            back.reduce(1, index)
        total.take(3)
        total.send(4)
        summed.line(0)
        summed.line(1)
        total.take(4)
        tokens_group.begin()
        back.reduce(2, 0)
        summed.line(2)
        back.reduce(2, 1)
        summed.line(3)
        half = width // 2

        def finish(at, start, step):
            value = (hidden_ref[at, :] + total_branch[at, :]).astype(bf16)
            turned = lax.axis_index("dp") == 0

            @pl.when(turned)
            def _():
                own_block[at, :] = value

            @pl.when(jnp.logical_not(turned))
            def _():
                own_block[at, :half] = value[:, half:]
                own_block[at, half:] = value[:, :half]

        summed.chunks(finish)
        block_group.begin()
        for index in range(2, parts):
            back.reduce(2, index)
        for item in range(3, count):
            for index in range(parts):
                back.reduce(item, index)
        summed.end()
        tokens_group.end()
        block_group.end()
        back.end()

    return comm_call(
        kernel,
        number,
        "last_exchange",
        out_shape,
        [IN_PLACE] * (len(out_shape) - 1) + [IN_VMEM],
        [IN_PLACE] * 4 + [IN_VMEM] * 4,
        [one for group in groups for one in group],
        300_000_000,
    )(up_grads, down_grads, out_grads, qkv_grads, branch, hidden, tokens_grad, small)


def split_body(
    tokens,
    positions,
    routes,
    out_grad,
    norm1_gain,
    qkv_weight,
    qkv_bias,
    out_weight,
    norm2_gain,
    router_weight,
    expert_gate,
    expert_up,
    expert_down,
    shared_gate,
    shared_w_gate,
    shared_w_up,
    shared_w_down,
):
    rows, width = tokens.shape[1], tokens.shape[2]
    parts = lax.axis_size("context")
    group_size = lax.axis_size("experts")
    place, group = lax.axis_index("context"), lax.axis_index("experts")
    local_experts = expert_gate.shape[0]
    expert_count = local_experts * group_size
    own_rows = rows // group_size
    length = rows * parts
    half = width // 2
    block = width // (2 * parts)
    hidden_here = shared_w_gate.shape[1] // parts
    stacks = local_experts + 1
    scale = HEAD_DIM ** (-0.5)
    bf16 = jnp.bfloat16

    first = group * own_rows

    def own_of(array):
        return lax.dynamic_slice_in_dim(array, first, own_rows, 0)

    grad_own_b = own_half_first(own_of(out_grad[0]))
    grad_own = grad_own_b.astype(jnp.float32)
    gain1 = own_half_first(norm1_gain).astype(jnp.float32)
    gain2 = own_half_first(norm2_gain).astype(jnp.float32)
    token_own = own_half_first(own_of(tokens[0])).astype(jnp.float32)
    inverse1 = lax.rsqrt(jnp.mean(token_own * token_own, -1, keepdims=True) + EPSILON)
    normed1 = token_own * inverse1
    half_dim = HEAD_DIM // 2
    frequency = ROPE_BASE ** (-2.0 * jnp.arange(half_dim, dtype=jnp.float32) / HEAD_DIM)
    angles = own_of(positions[0]).astype(jnp.float32)[:, None] * frequency[None, :]
    turns = jnp.concatenate([jnp.cos(angles), jnp.sin(angles)], 1)
    turns_high = turns.astype(bf16)
    turns_low = (turns - turns_high.astype(jnp.float32)).astype(bf16)
    send1 = jnp.concatenate([(normed1 * gain1).astype(bf16), turns_high, turns_low], 1)
    qkv_in = jnp.transpose(
        qkv_weight.reshape(block, 3, parts, HEAD_DIM), (2, 0, 1, 3)
    ).reshape(parts * block, 3 * HEAD_DIM)
    bias_here = lax.dynamic_slice_in_dim(
        qkv_bias.reshape(3, parts, HEAD_DIM), place, 1, 1
    ).reshape(1, 3 * HEAD_DIM)
    shared1, qkv_w, out_w, down_w, query, key, value, attended, lse, head_sum = attention_first(
        send1, qkv_in, out_weight, bias_here.astype(jnp.float32), shared_w_down, expert_down, 1
    )
    xn1, turns = shared1[:, :width], shared1[:, width:]
    hidden = token_own + head_sum
    inverse2 = lax.rsqrt(jnp.mean(hidden * hidden, -1, keepdims=True) + EPSILON)
    normed2 = hidden * inverse2
    xn2_own = (normed2 * gain2).astype(bf16)
    router_here = own_half_first(router_weight.T).T
    gate_here = own_half_first(shared_gate)
    heads_w = jnp.concatenate([router_here, gate_here[:, None]], 1)
    logits = dot_nn(xn2_own, heads_w)
    prob = jax.nn.softmax(logits[:, :expert_count], -1)
    sig_own = jax.nn.sigmoid(logits[:, expert_count])
    named = jnp.sum(
        (
            own_of(routes[0])[:, :, None] == jnp.arange(expert_count, dtype=jnp.int32)[None, None, :]
        ).astype(jnp.float32),
        1,
    )
    gates = jnp.pad(
        jnp.concatenate([prob * named, sig_own[:, None]], 1), ((0, 0), (0, 63 - expert_count))
    )
    gates_high = gates.astype(bf16)
    gates_low = (gates - gates_high.astype(jnp.float32)).astype(bf16)
    send3 = jnp.concatenate([xn2_own, grad_own_b, gates_high, gates_low], 1)

    both, send4, branch_part, dup, act_c = share_move_compute(
        send3, shared_w_gate, shared_w_up, expert_gate, expert_up, down_w, 3
    )
    up_g = dot_tn(both[:, :width], dup).astype(bf16)
    down_g = dot_tn(act_c, both[:, width : 2 * width]).astype(bf16)
    send4, up_g, down_g = lax.optimization_barrier((send4, up_g, down_g))
    up_grads, down_grads = [None] * (2 * stacks), [None] * stacks
    side = 128 - expert_count - 1
    chances = jnp.pad(jnp.concatenate([prob, sig_own[:, None]], 1), ((0, 0), (0, side)))
    named_wide = jnp.pad(named, ((0, 0), (0, 128 - expert_count)))
    router_wide = jnp.pad(heads_w.T.astype(jnp.float32), ((0, side), (0, 0)))
    (
        dhidden_all,
        up_grads[0],
        up_grads[1],
        down_grads[0],
        dots_own,
        dxn2,
        dhidden,
        dqkv_b,
        bias_part,
        dxn1,
    ) = attention_last(
        send4,
        up_g,
        down_g,
        hidden,
        grad_own_b,
        gain2[None, :],
        chances,
        named_wide,
        router_wide,
        out_w,
        qkv_w,
        (query, key, value, attended),
        lse,
        turns,
        4,
    )
    out_g = dot_tn(attended, dhidden_all).astype(bf16)
    qkv_g = dot_tn(xn1, dqkv_b).astype(bf16)

    dprob = dots_own[:, :expert_count] * named
    dlogit = prob * (dprob - jnp.sum(prob * dprob, -1, keepdims=True))
    coef = sig_own * (1.0 - sig_own) * dots_own[:, expert_count]
    xn2_float = xn2_own.astype(jnp.float32)
    router_grad = jnp.dot(xn2_float.T, dlogit, precision=PRECISE)
    shared_gate_grad = jnp.dot(coef, xn2_float, precision=PRECISE)
    norm2_grad = jnp.sum(dxn2 * normed2, 0)
    norm1_grad = jnp.sum(dxn1 * normed1, 0)
    dscaled1 = dxn1 * gain1
    tokens_grad_own = dhidden + inverse1 * (
        dscaled1 - normed1 * jnp.mean(dscaled1 * normed1, -1, keepdims=True)
    )

    bias_wide = jnp.zeros((group_size, parts, 3 * HEAD_DIM), jnp.float32)
    bias_wide = lax.dynamic_update_slice(bias_wide, bias_part[None], (group, place, 0))
    small = jnp.concatenate(
        [
            own_half_first(norm1_grad),
            own_half_first(norm2_grad),
            own_half_first(shared_gate_grad),
            own_half_first(router_grad.T).T.reshape(-1),
            bias_wide.reshape(-1),
        ]
    )
    out_w_grad, qkv_grad, *others, block_out, tokens_grad, small = last_exchange(
        up_g,
        down_g,
        out_g,
        qkv_g,
        branch_part,
        hidden,
        own_half_first(tokens_grad_own),
        small.reshape(-1, 128),
        list(range(1, stacks)),
        list(range(1, stacks)),
        7,
    )
    small = small.reshape(-1)
    up_grads[2:] = others[: 2 * (stacks - 1)]
    down_grads[1:] = others[2 * (stacks - 1) :]
    router_size = width * expert_count
    bias_sum = small[3 * width + router_size :].reshape(group_size, parts, 3, HEAD_DIM)
    bias_grad = jnp.transpose(
        lax.dynamic_slice_in_dim(bias_sum, group, 1, 0)[0], (1, 0, 2)
    ).reshape(3, parts * HEAD_DIM)

    qkv_grad = jnp.transpose(
        qkv_grad.reshape(parts, block, 3, HEAD_DIM), (1, 2, 0, 3)
    ).reshape(block, 3, parts * HEAD_DIM)

    def wide(array):
        return array.astype(jnp.float32)

    return (
        block_out[None],
        tokens_grad[None],
        small[:width],
        wide(qkv_grad),
        bias_grad,
        wide(out_w_grad),
        small[width : 2 * width],
        small[3 * width : 3 * width + router_size].reshape(width, expert_count),
        wide(jnp.stack(up_grads[2::2])),
        wide(jnp.stack(up_grads[3::2])),
        wide(jnp.stack(down_grads[1:])),
        small[2 * width : 3 * width],
        wide(up_grads[0]),
        wide(up_grads[1]),
        wide(down_grads[0]),
    )


def plan_of(mesh):
    sizes = mesh.shape
    return split_body if (sizes["dp"], sizes["context"], sizes["experts"]) == (2, 4, 4) else general_body


def solution(mesh):
    return jax.shard_map(
        plan_of(mesh),
        mesh=mesh,
        in_specs=(
            P("dp", "context", None),
            P("dp", "context"),
            P("dp", "context", None),
            P("dp", "context", None),
            P(),
            P(("dp", "context"), None, "experts"),
            P(None, "experts"),
            P("experts", ("dp", "context")),
            P(),
            P(),
            P("experts", ("dp", "context"), None),
            P("experts", ("dp", "context"), None),
            P("experts", None, ("dp", "context")),
            P(),
            P(("dp", "context"), "experts"),
            P(("dp", "context"), "experts"),
            P("experts", ("dp", "context")),
        ),
        out_specs=(
            P("dp", "context", None),
            P("dp", "context", None),
            P(),
            P(("dp", "context"), None, "experts"),
            P(None, "experts"),
            P("experts", ("dp", "context")),
            P(),
            P(),
            P("experts", ("dp", "context"), None),
            P("experts", ("dp", "context"), None),
            P("experts", None, ("dp", "context")),
            P(),
            P(("dp", "context"), "experts"),
            P(("dp", "context"), "experts"),
            P("experts", ("dp", "context")),
        ),
        check_vma=False,
    )
```

```python
import functools

import jax
import jax.numpy as jnp
from jax import lax
from jax.experimental import pallas as pl
from jax.experimental.pallas import tpu as pltpu
from jax.sharding import PartitionSpec as P

HEAD_DIM = 128


EPSILON = 1e-06
ROPE_BASE = 1000000.0
MASKED = -1e30
PRECISE = lax.Precision.HIGHEST


def rope_tables(position_ids):
    half_dim = HEAD_DIM // 2
    inverse = ROPE_BASE ** (-2.0 * jnp.arange(half_dim, dtype=jnp.float32) / HEAD_DIM)
    angles = position_ids.astype(jnp.float32)[:, None] * inverse[None, :]
    cosine = jnp.cos(angles)
    sine_part = jnp.sin(angles)
    return (
        jnp.concatenate([cosine, cosine], -1)[:, None, :],
        jnp.concatenate([sine_part, sine_part], -1)[:, None, :],
    )


def rotate(value):
    half_dim = value.shape[-1] // 2
    return jnp.concatenate([-value[..., half_dim:], value[..., :half_dim]], -1)


def rotate_back(value):
    half_dim = value.shape[-1] // 2
    return jnp.concatenate([value[..., half_dim:], -value[..., :half_dim]], -1)


def silu_grad(gate_vals):
    sigmoid_vals = jax.nn.sigmoid(gate_vals)
    return sigmoid_vals * (1.0 + gate_vals * (1.0 - sigmoid_vals))


def block_rank(route_rows, expert_count):
    hits = (
        route_rows[:, :, None] == jnp.arange(expert_count, dtype=jnp.int32)[None, None, :]
    ).astype(jnp.int32)
    flat_hits = hits.reshape(-1, expert_count)
    earlier = jnp.cumsum(flat_hits, axis=0) - flat_hits
    return jnp.sum(earlier * flat_hits, -1).reshape(route_rows.shape)


def block_width_of():
    return 512


def gather_weights(shard_set):
    return (
        lax.all_gather(shard_set[0], ("dp", "context"), axis=0, tiled=True),
        lax.all_gather(shard_set[1], ("dp", "context"), axis=1, tiled=True),
        lax.all_gather(shard_set[2], ("dp", "context"), axis=1, tiled=True),
        lax.all_gather(shard_set[3], ("dp", "context"), axis=1, tiled=True),
        lax.all_gather(shard_set[4], ("dp", "context"), axis=2, tiled=True),
        lax.all_gather(shard_set[5], ("dp", "context"), axis=0, tiled=True),
        lax.all_gather(shard_set[6], ("dp", "context"), axis=0, tiled=True),
        lax.all_gather(shard_set[7], ("dp", "context"), axis=1, tiled=True),
    )


def forward_fold(query, query_first, scale, carry, piece):
    row_count, head_count, head_size = query.shape
    query_index = query_first + jnp.arange(row_count, dtype=jnp.int32)
    query_last = query_first + row_count - 1
    key_part, value_part = piece
    piece_rows = key_part.shape[0]
    block_width = block_width_of()
    block_count = piece_rows // block_width
    key_blocks = key_part.reshape(block_count, block_width, head_count, head_size)
    value_blocks = value_part.reshape(block_count, block_width, head_count, head_size)
    offsets = block_width * jnp.arange(block_count, dtype=jnp.int32)

    def forward_visit(state, item):
        key_block, value_block, first_key = item

        def forward_compute(current):
            run_max, run_sum, accum = current
            scores = (
                jnp.einsum("qhd,khd->hqk", query, key_block, preferred_element_type=jnp.float32)
                * scale
            )
            key_index = first_key + jnp.arange(block_width, dtype=jnp.int32)
            allowed = key_index[None, None, :] <= query_index[None, :, None]
            new_max = jnp.maximum(run_max, jnp.max(jnp.where(allowed, scores, MASKED), -1))
            weights = jnp.where(allowed, jnp.exp(scores - new_max[..., None]), 0.0)
            factor = jnp.exp(run_max - new_max)
            new_sum = run_sum * factor + jnp.sum(weights, -1)
            new_accum = accum * factor[..., None] + jnp.einsum(
                "hqk,khd->hqd",
                weights.astype(jnp.bfloat16),
                value_block,
                preferred_element_type=jnp.float32,
            )
            return (new_max, new_sum, new_accum)

        return (
            lax.cond(first_key > query_last, lambda current: current, forward_compute, state),
            None,
        )

    carry, _ = lax.scan(forward_visit, carry, (key_blocks, value_blocks, offsets))
    return carry


def key_grad_fold(key_rows, value_rows, key_first, scale, carry, piece):
    row_count, head_count, head_size = key_rows.shape
    key_index = key_first + jnp.arange(row_count, dtype=jnp.int32)
    query_part, dout_part, lse_part, delta_part = piece
    piece_rows = query_part.shape[0]
    block_width = block_width_of()
    block_count = piece_rows // block_width
    query_blocks = query_part.reshape(block_count, block_width, head_count, head_size)
    dout_blocks = dout_part.reshape(block_count, block_width, head_count, head_size)
    lse_blocks = lse_part.reshape(block_count, block_width, head_count)
    delta_blocks = delta_part.reshape(block_count, block_width, head_count)
    offsets = block_width * jnp.arange(block_count, dtype=jnp.int32)

    def key_visit(state, item):
        query_block, dout_block, lse_block, delta_block, first_query = item

        def key_compute(current):
            dkey_sum, dvalue_sum = current
            query_b = query_block.astype(jnp.bfloat16)
            dout_b = dout_block.astype(jnp.bfloat16)
            scores = (
                jnp.einsum("qhd,khd->hqk", query_b, key_rows, preferred_element_type=jnp.float32)
                * scale
            )
            query_index = first_query + jnp.arange(block_width, dtype=jnp.int32)
            allowed = key_index[None, None, :] <= query_index[None, :, None]
            prob_att = jnp.where(
                allowed, jnp.exp(scores - jnp.transpose(lse_block)[:, :, None]), 0.0
            )
            dvalue_sum = dvalue_sum + jnp.einsum(
                "hqk,qhd->hkd",
                prob_att.astype(jnp.bfloat16),
                dout_b,
                preferred_element_type=jnp.float32,
            )
            dprob = jnp.einsum(
                "qhd,khd->hqk", dout_b, value_rows, preferred_element_type=jnp.float32
            )
            dscore = (prob_att * (dprob - jnp.transpose(delta_block)[:, :, None])).astype(
                jnp.bfloat16
            )
            dkey_sum = (
                dkey_sum
                + jnp.einsum("hqk,qhd->hkd", dscore, query_b, preferred_element_type=jnp.float32)
                * scale
            )
            return (dkey_sum, dvalue_sum)

        return (
            lax.cond(
                first_query + block_width - 1 < key_first,
                lambda current: current,
                key_compute,
                state,
            ),
            None,
        )

    carry, _ = lax.scan(
        key_visit, carry, (query_blocks, dout_blocks, lse_blocks, delta_blocks, offsets)
    )
    return carry


def query_grad_fold(query, dattended, lse_heads, delta_heads, query_first, scale, carry, piece):
    row_count, head_count, head_size = query.shape
    query_index = query_first + jnp.arange(row_count, dtype=jnp.int32)
    query_last = query_first + row_count - 1
    key_part, value_part = piece
    piece_rows = key_part.shape[0]
    block_width = block_width_of()
    block_count = piece_rows // block_width
    key_blocks = key_part.reshape(block_count, block_width, head_count, head_size)
    value_blocks = value_part.reshape(block_count, block_width, head_count, head_size)
    offsets = block_width * jnp.arange(block_count, dtype=jnp.int32)

    def query_visit(state, item):
        key_block, value_block, first_key = item

        def query_compute(current):
            scores = (
                jnp.einsum("qhd,khd->hqk", query, key_block, preferred_element_type=jnp.float32)
                * scale
            )
            key_index = first_key + jnp.arange(block_width, dtype=jnp.int32)
            allowed = key_index[None, None, :] <= query_index[None, :, None]
            prob_att = jnp.where(allowed, jnp.exp(scores - lse_heads[:, :, None]), 0.0)
            dprob = jnp.einsum(
                "qhd,khd->hqk", dattended, value_block, preferred_element_type=jnp.float32
            )
            dscore = (prob_att * (dprob - delta_heads[:, :, None])).astype(jnp.bfloat16)
            return (
                current
                + jnp.einsum("hqk,khd->hqd", dscore, key_block, preferred_element_type=jnp.float32)
                * scale
            )

        return (
            lax.cond(first_key > query_last, lambda current: current, query_compute, state),
            None,
        )

    carry, _ = lax.scan(query_visit, carry, (key_blocks, value_blocks, offsets))
    return carry


def general_body(
    tokens,
    positions,
    routes,
    out_grad,
    norm1_gain,
    qkv_weight,
    qkv_bias,
    out_weight,
    norm2_gain,
    router_weight,
    expert_gate,
    expert_up,
    expert_down,
    shared_gate,
    shared_w_gate,
    shared_w_up,
    shared_w_down,
):
    row_count = tokens.shape[1]
    model_width = tokens.shape[2]
    head_span = qkv_bias.shape[1]
    heads_here = head_span // HEAD_DIM
    local_experts = expert_gate.shape[0]
    group_size = lax.axis_size("experts")
    quarter = row_count // group_size
    capacity = 3 * quarter // 4
    expert_count = local_experts * group_size
    group_index = lax.axis_index("experts")
    scale = HEAD_DIM ** (-0.5)
    shard_set = (
        qkv_weight,
        out_weight,
        expert_gate,
        expert_up,
        expert_down,
        shared_w_gate,
        shared_w_up,
        shared_w_down,
    )
    qkv_full, out_full, gate_full, up_full, down_full, sgate_full, sup_full, sdown_full = (
        gather_weights(shard_set)
    )
    token_float = tokens[0].astype(jnp.float32)
    inverse1 = lax.rsqrt(jnp.mean(token_float * token_float, -1, keepdims=True) + EPSILON)
    normed1 = token_float * inverse1
    gain1 = norm1_gain.astype(jnp.float32)
    normed1_b = (normed1 * gain1).astype(jnp.bfloat16)
    qkv_flat = qkv_full.reshape(model_width, 3 * head_span)
    qkv = (
        jnp.dot(normed1_b, qkv_flat, preferred_element_type=jnp.float32).reshape(
            row_count, 3, head_span
        )
        + qkv_bias.astype(jnp.float32)[None]
    )
    cosine, sine_part = rope_tables(positions[0])
    query_raw = qkv[:, 0].reshape(row_count, heads_here, HEAD_DIM)
    key_raw = qkv[:, 1].reshape(row_count, heads_here, HEAD_DIM)
    query = (query_raw * cosine + rotate(query_raw) * sine_part).astype(jnp.bfloat16)
    key_rows = (key_raw * cosine + rotate(key_raw) * sine_part).astype(jnp.bfloat16)
    value_flat = qkv[:, 2].astype(jnp.bfloat16)
    key_flat = key_rows.reshape(row_count, head_span)
    value_rows = value_flat.reshape(row_count, heads_here, HEAD_DIM)
    query_first = lax.axis_index("context") * row_count
    start_state = (
        jnp.full((heads_here, row_count), MASKED, jnp.float32),
        jnp.zeros((heads_here, row_count), jnp.float32),
        jnp.zeros((heads_here, row_count, HEAD_DIM), jnp.float32),
    )
    run_max, run_sum, accum = forward_fold(
        query,
        query_first,
        scale,
        start_state,
        (
            lax.all_gather(key_flat, "context", axis=0, tiled=True),
            lax.all_gather(value_flat, "context", axis=0, tiled=True),
        ),
    )
    attended = jnp.transpose(accum / run_sum[..., None], (1, 0, 2)).astype(jnp.bfloat16)
    lse_heads = run_max + jnp.log(run_sum)
    attended_flat = attended.reshape(row_count, head_span)
    head_part = jnp.dot(attended_flat, out_full, preferred_element_type=jnp.float32)
    hidden = token_float + lax.psum(head_part, "experts")
    inverse2 = lax.rsqrt(jnp.mean(hidden * hidden, -1, keepdims=True) + EPSILON)
    normed2 = hidden * inverse2
    gain2 = norm2_gain.astype(jnp.float32)
    normed2_b = (normed2 * gain2).astype(jnp.bfloat16)
    first_row = group_index * quarter
    normed2_q = lax.dynamic_slice_in_dim(normed2_b, first_row, quarter, 0)
    route_q = lax.dynamic_slice_in_dim(routes[0], first_row, quarter, 0)
    logits = jnp.dot(normed2_q, router_weight, preferred_element_type=jnp.float32)
    prob = jax.nn.softmax(logits, -1)
    gate_k = jnp.take_along_axis(prob, route_q, 1)
    slot_ids = route_q * capacity + block_rank(route_q, expert_count)
    slot_hits = (
        slot_ids[:, :, None] == jnp.arange(expert_count * capacity, dtype=jnp.int32)[None, None, :]
    )
    placer = jnp.sum(slot_hits.astype(jnp.bfloat16), 1)
    send_rows = (
        jnp.dot(placer.T, normed2_q, preferred_element_type=jnp.float32)
        .astype(jnp.bfloat16)
        .reshape(group_size, local_experts, capacity, model_width)
    )
    arrived = lax.all_to_all(send_rows, "experts", split_axis=0, concat_axis=0, tiled=True)
    expert_gvals = jnp.einsum(
        "secd,edf->secf", arrived, gate_full, preferred_element_type=jnp.float32
    )
    expert_uvals = jnp.einsum(
        "secd,edf->secf", arrived, up_full, preferred_element_type=jnp.float32
    )
    expert_act = (jax.nn.silu(expert_gvals) * expert_uvals).astype(jnp.bfloat16)
    expert_out = jnp.einsum(
        "secf,efd->secd", expert_act, down_full, preferred_element_type=jnp.float32
    ).astype(jnp.bfloat16)
    returned = lax.all_to_all(
        expert_out, "experts", split_axis=0, concat_axis=0, tiled=True
    ).reshape(expert_count * capacity, model_width)
    picked = returned[slot_ids].astype(jnp.float32)
    routed = jnp.sum(gate_k[:, :, None] * picked, 1)
    shared_sig = jax.nn.sigmoid(
        jnp.dot(normed2_b, shared_gate[:, None], preferred_element_type=jnp.float32)[:, 0]
    )
    shared_gvals = jnp.dot(normed2_b, sgate_full, preferred_element_type=jnp.float32)
    shared_uvals = jnp.dot(normed2_b, sup_full, preferred_element_type=jnp.float32)
    shared_act = (jax.nn.silu(shared_gvals) * shared_uvals).astype(jnp.bfloat16)
    shared_part = jnp.dot(shared_act, sdown_full, preferred_element_type=jnp.float32)
    routed_pad = lax.dynamic_update_slice_in_dim(
        jnp.zeros((row_count, model_width), jnp.float32), routed, first_row, 0
    )
    branch_total = lax.psum(
        (shared_sig[:, None] * shared_part + routed_pad).astype(jnp.bfloat16), "experts"
    ).astype(jnp.float32)
    block_out = (hidden + branch_total).astype(jnp.bfloat16)
    held = lax.optimization_barrier((shard_set, block_out))
    qkv_full, out_full, gate_full, up_full, down_full, sgate_full, sup_full, sdown_full = (
        gather_weights(held[0])
    )
    qkv_flat = qkv_full.reshape(model_width, 3 * head_span)
    grad_float = out_grad[0].astype(jnp.float32)
    grad_q = lax.dynamic_slice_in_dim(grad_float, first_row, quarter, 0)
    dgate_k = jnp.sum(grad_q[:, None, :] * picked, -1)
    weighted = jnp.sum(slot_hits.astype(jnp.float32) * gate_k[:, :, None], 1)
    dsend = (
        jnp.dot(weighted.T, grad_q, precision=PRECISE)
        .astype(jnp.bfloat16)
        .reshape(group_size, local_experts, capacity, model_width)
    )
    darrived = lax.all_to_all(dsend, "experts", split_axis=0, concat_axis=0, tiled=True)
    expert_dact = jnp.einsum(
        "secd,efd->secf", darrived, down_full, preferred_element_type=jnp.float32
    )
    down_grad = jnp.einsum(
        "secf,secd->efd", expert_act, darrived, preferred_element_type=jnp.float32
    )
    expert_dgate = (expert_dact * expert_uvals * silu_grad(expert_gvals)).astype(jnp.bfloat16)
    expert_dup = (expert_dact * jax.nn.silu(expert_gvals)).astype(jnp.bfloat16)
    gate_grad = jnp.einsum(
        "secd,secf->edf", arrived, expert_dgate, preferred_element_type=jnp.float32
    )
    up_grad = jnp.einsum("secd,secf->edf", arrived, expert_dup, preferred_element_type=jnp.float32)
    expert_din = (
        jnp.einsum("secf,edf->secd", expert_dgate, gate_full, preferred_element_type=jnp.float32)
        + jnp.einsum("secf,edf->secd", expert_dup, up_full, preferred_element_type=jnp.float32)
    ).astype(jnp.bfloat16)
    dreturned = lax.all_to_all(
        expert_din, "experts", split_axis=0, concat_axis=0, tiled=True
    ).reshape(expert_count * capacity, model_width)
    dnormed2_q = jnp.dot(placer, dreturned, preferred_element_type=jnp.float32)
    route_hits = (
        route_q[:, :, None] == jnp.arange(expert_count, dtype=jnp.int32)[None, None, :]
    ).astype(jnp.float32)
    dprob = jnp.sum(route_hits * dgate_k[:, :, None], 1)
    dlogit = prob * (dprob - jnp.sum(prob * dprob, -1, keepdims=True))
    router_part = jnp.dot(normed2_q.astype(jnp.float32).T, dlogit, precision=PRECISE)
    dnormed2_q = dnormed2_q + jnp.dot(
        dlogit, router_weight.astype(jnp.float32).T, precision=PRECISE
    )
    shared_dout = (shared_sig[:, None] * grad_float).astype(jnp.bfloat16)
    shared_dact = jnp.dot(shared_dout, sdown_full.T, preferred_element_type=jnp.float32)
    sdown_grad = jnp.dot(shared_act.T, shared_dout, preferred_element_type=jnp.float32)
    shared_dgate = (shared_dact * shared_uvals * silu_grad(shared_gvals)).astype(jnp.bfloat16)
    shared_dup = (shared_dact * jax.nn.silu(shared_gvals)).astype(jnp.bfloat16)
    sgate_grad = jnp.dot(normed2_b.T, shared_dgate, preferred_element_type=jnp.float32)
    sup_grad = jnp.dot(normed2_b.T, shared_dup, preferred_element_type=jnp.float32)
    row_dots = jnp.sum(grad_float * shared_part, -1)
    dnormed2_part = jnp.dot(
        shared_dgate, sgate_full.T, preferred_element_type=jnp.float32
    ) + jnp.dot(shared_dup, sup_full.T, preferred_element_type=jnp.float32)
    dnormed2_part = dnormed2_part + lax.dynamic_update_slice_in_dim(
        jnp.zeros((row_count, model_width), jnp.float32), dnormed2_q, first_row, 0
    )
    dnormed2, row_dots, router_grad = lax.psum((dnormed2_part, row_dots, router_part), "experts")
    coef = shared_sig * (1.0 - shared_sig) * row_dots
    dnormed2 = dnormed2 + coef[:, None] * shared_gate.astype(jnp.float32)[None, :]
    shared_gate_grad = jnp.dot(coef, normed2_b.astype(jnp.float32), precision=PRECISE)
    norm2_grad = jnp.sum(dnormed2 * normed2, 0)
    dscaled2 = dnormed2 * gain2
    dhidden = grad_float + inverse2 * (
        dscaled2 - normed2 * jnp.mean(dscaled2 * normed2, -1, keepdims=True)
    )
    dhidden_b = dhidden.astype(jnp.bfloat16)
    out_grad_part = jnp.dot(attended_flat.T, dhidden_b, preferred_element_type=jnp.float32)
    dattended = jnp.dot(dhidden_b, out_full.T, preferred_element_type=jnp.float32).astype(
        jnp.bfloat16
    )
    dattended3 = dattended.reshape(row_count, heads_here, HEAD_DIM)
    delta = jnp.sum(dattended3.astype(jnp.float32) * attended.astype(jnp.float32), -1)
    zero_state = jnp.zeros((heads_here, row_count, HEAD_DIM), jnp.float32)
    dkey_sum, dvalue_sum = key_grad_fold(
        key_rows,
        value_rows,
        query_first,
        scale,
        (zero_state, zero_state),
        (
            lax.all_gather(
                query.reshape(row_count, head_span).astype(jnp.float32),
                "context",
                axis=0,
                tiled=True,
            ),
            lax.all_gather(dattended.astype(jnp.float32), "context", axis=0, tiled=True),
            lax.all_gather(jnp.transpose(lse_heads), "context", axis=0, tiled=True),
            lax.all_gather(delta, "context", axis=0, tiled=True),
        ),
    )
    dquery_sum = query_grad_fold(
        query,
        dattended3,
        lse_heads,
        jnp.transpose(delta),
        query_first,
        scale,
        zero_state,
        (
            lax.all_gather(key_flat, "context", axis=0, tiled=True),
            lax.all_gather(value_flat, "context", axis=0, tiled=True),
        ),
    )
    dquery = jnp.transpose(dquery_sum, (1, 0, 2))
    dkey = jnp.transpose(dkey_sum, (1, 0, 2))
    dvalue = jnp.transpose(dvalue_sum, (1, 0, 2))
    dquery_raw = dquery * cosine + rotate_back(dquery * sine_part)
    dkey_raw = dkey * cosine + rotate_back(dkey * sine_part)
    dqkv = jnp.stack(
        [
            dquery_raw.reshape(row_count, head_span),
            dkey_raw.reshape(row_count, head_span),
            dvalue.reshape(row_count, head_span),
        ],
        1,
    )
    bias_grad = jnp.sum(dqkv, 0)
    dqkv_b = dqkv.astype(jnp.bfloat16).reshape(row_count, 3 * head_span)
    qkv_grad = jnp.dot(normed1_b.T, dqkv_b, preferred_element_type=jnp.float32).reshape(
        model_width, 3, head_span
    )
    dnormed1 = lax.psum(
        jnp.dot(dqkv_b, qkv_flat.T, preferred_element_type=jnp.float32).astype(jnp.bfloat16),
        "experts",
    ).astype(jnp.float32)
    norm1_grad = jnp.sum(dnormed1 * normed1, 0)
    dscaled1 = dnormed1 * gain1
    tokens_grad = dhidden + inverse1 * (
        dscaled1 - normed1 * jnp.mean(dscaled1 * normed1, -1, keepdims=True)
    )
    small_sums = (
        lax.psum(norm1_grad.astype(jnp.bfloat16), ("dp", "context")).astype(jnp.float32),
        lax.psum(norm2_grad.astype(jnp.bfloat16), ("dp", "context")).astype(jnp.float32),
        lax.psum(router_grad.astype(jnp.bfloat16), ("dp", "context")).astype(jnp.float32),
        lax.psum(shared_gate_grad.astype(jnp.bfloat16), ("dp", "context")).astype(jnp.float32),
        lax.psum(bias_grad.astype(jnp.bfloat16), ("dp", "context")).astype(jnp.float32),
    )
    large_sums = (
        lax.psum_scatter(
            qkv_grad.astype(jnp.bfloat16), ("dp", "context"), scatter_dimension=0, tiled=True
        ).astype(jnp.float32),
        lax.psum_scatter(
            out_grad_part.astype(jnp.bfloat16), ("dp", "context"), scatter_dimension=1, tiled=True
        ).astype(jnp.float32),
        lax.psum_scatter(
            gate_grad.astype(jnp.bfloat16), ("dp", "context"), scatter_dimension=1, tiled=True
        ).astype(jnp.float32),
        lax.psum_scatter(
            up_grad.astype(jnp.bfloat16), ("dp", "context"), scatter_dimension=1, tiled=True
        ).astype(jnp.float32),
        lax.psum_scatter(
            down_grad.astype(jnp.bfloat16), ("dp", "context"), scatter_dimension=2, tiled=True
        ).astype(jnp.float32),
        lax.psum_scatter(
            sgate_grad.astype(jnp.bfloat16), ("dp", "context"), scatter_dimension=0, tiled=True
        ).astype(jnp.float32),
        lax.psum_scatter(
            sup_grad.astype(jnp.bfloat16), ("dp", "context"), scatter_dimension=0, tiled=True
        ).astype(jnp.float32),
        lax.psum_scatter(
            sdown_grad.astype(jnp.bfloat16), ("dp", "context"), scatter_dimension=1, tiled=True
        ).astype(jnp.float32),
    )
    return (
        block_out[None],
        tokens_grad[None],
        small_sums[0],
        large_sums[0],
        small_sums[4],
        large_sums[1],
        small_sums[1],
        small_sums[2],
        large_sums[2],
        large_sums[3],
        large_sums[4],
        small_sums[3],
        large_sums[5],
        large_sums[6],
        large_sums[7],
    )


def own_half_first(value):
    half = value.shape[-1] // 2
    turned = jnp.concatenate([value[..., half:], value[..., :half]], -1)
    return jnp.where(lax.axis_index("dp") == 0, value, turned)


def dot_nn(left, right):
    return jnp.dot(left, right, preferred_element_type=jnp.float32)


def dot_nt(left, right):
    return lax.dot_general(
        left, right, (((1,), (1,)), ((), ())), preferred_element_type=jnp.float32
    )


def dot_tn(left, right):
    return lax.dot_general(
        left, right, (((0,), (0,)), ((), ())), preferred_element_type=jnp.float32
    )


MESH = pl.DeviceIdType.MESH
DMA = pltpu.SemaphoreType.DMA


def remote(source, target, send_sem, recv_sem, device):
    return pltpu.make_async_remote_copy(
        src_ref=source,
        dst_ref=target,
        send_sem=send_sem,
        recv_sem=recv_sem,
        device_id=device,
        device_id_type=MESH,
    )


def rows_at(ref, start, size):
    return ref.at[pl.ds(pl.multiple_of(start, 16), size), :]


def lanes_at(ref, start, size):
    return ref.at[:, pl.ds(pl.multiple_of(start, 128), size)]


def by_width(device, narrow, body):
    if narrow is None:
        body(False)
    elif isinstance(device, int):
        body(device == narrow)
    else:

        @pl.when(device == narrow)
        def _():
            body(True)

        @pl.when(device != narrow)
        def _():
            body(False)


class Spot:
    def __init__(self):
        self.parts = lax.axis_size("context")
        self.place, self.group = lax.axis_index("context"), lax.axis_index("experts")
        self.twin = {"dp": 1 - lax.axis_index("dp")}
        self.across = lax.rem(self.group + 2, 4)
        self.beside = self.group + 1 - 2 * lax.rem(self.group, 2)
        self.corner = lax.rem(self.beside + 2, 4)
        self.has_left, self.has_right = self.place > 0, self.place < self.parts - 1

    def greet(self, whole_line, twins):
        barrier = pltpu.get_barrier_semaphore()
        devices = [{"experts": self.across}, {"experts": self.beside}]
        if twins:
            devices.append(self.twin)
        for device in devices:
            pl.semaphore_signal(barrier, inc=1, device_id=device, device_id_type=MESH)
        count = len(devices)
        if whole_line:
            for gap in range(1, self.parts):
                device = {"context": lax.rem(self.place + gap, self.parts)}
                pl.semaphore_signal(barrier, inc=1, device_id=device, device_id_type=MESH)
            pl.semaphore_wait(barrier, count + self.parts - 1)
        else:
            for step, there in ((-1, self.has_left), (1, self.has_right)):

                @pl.when(there)
                def _():
                    device = {"context": self.place + step}
                    pl.semaphore_signal(barrier, inc=1, device_id=device, device_id_type=MESH)

            ends = jnp.where(self.has_left & self.has_right, 0, 1)
            pl.semaphore_wait(barrier, count + 2 - ends)

    def far_first(self):
        upper = self.place // (self.parts // 2)
        return [3 * (1 - upper), 2 - upper, 1 + 4 * upper - self.place, self.place]

    def others(self, gap, body):
        @pl.when(self.place >= gap)
        def _():
            body(self.place - gap)

        @pl.when(self.place + gap < self.parts)
        def _():
            body(self.place + gap)


class Share:
    def __init__(self, spot, own, out, sems):
        self.spot, self.own, self.out = spot, own, out
        self.local_sem, self.right_s, self.left_s, self.line_r, self.across_s, self.across_r, self.beside_s, self.beside_r = sems

    @staticmethod
    def sems(parts):
        return [DMA, DMA((parts,)), DMA((parts,)), DMA((parts,)), DMA((parts,)), DMA((parts,)), DMA((2 * parts,)), DMA((2 * parts,))]

    def block(self, part, column):
        rows = self.own.shape[0]
        return rows_at(self.out, (part * 4 + column) * rows, rows)

    def to_right(self, part, source):
        s = self.spot
        return remote(source, self.block(part, s.group), self.right_s.at[part], self.line_r.at[part], {"context": s.place + 1})

    def to_left(self, part, source):
        s = self.spot
        return remote(source, self.block(part, s.group), self.left_s.at[part], self.line_r.at[part], {"context": s.place - 1})

    def to_across(self, part, source):
        s = self.spot
        return remote(source, self.block(part, s.group), self.across_s.at[part], self.across_r.at[part], {"experts": s.across})

    def to_beside(self, part, column, slot, source):
        s = self.spot
        return remote(source, self.block(part, column), self.beside_s.at[slot], self.beside_r.at[slot], {"experts": s.beside})

    def begin(self):
        s = self.spot

        @pl.when(s.has_right)
        def _():
            self.to_right(s.place, self.own).start()

        @pl.when(s.has_left)
        def _():
            self.to_left(s.place, self.own).start()

        self.to_across(s.place, self.own).start()
        self.to_beside(s.place, s.group, s.place, self.own).start()
        self.local().start()

    def local(self):
        return pltpu.make_async_copy(self.own, self.block(self.spot.place, self.spot.group), self.local_sem)

    def pass_on(self, part):
        s = self.spot
        self.to_across(part, self.block(part, s.group)).wait_recv()
        self.to_beside(part, s.across, s.parts + part, self.block(part, s.across)).start()

    def arrival(self, part, onward, there):
        s = self.spot
        mine = self.block(part, s.group)
        self.to_right(part, mine).wait_recv()

        @pl.when(there)
        def _():
            onward(part, mine).start()

        self.to_across(part, mine).start()
        self.to_beside(part, s.group, part, mine).start()

    def step(self, gap):
        s = self.spot

        @pl.when(s.place >= gap)
        def _():
            self.arrival(s.place - gap, self.to_right, s.has_right)

        @pl.when(s.place + gap < s.parts)
        def _():
            self.arrival(s.place + gap, self.to_left, s.has_left)

        if gap == 1:
            self.pass_on(s.place)
        else:
            s.others(gap - 1, self.pass_on)

    def end(self):
        s = self.spot
        s.others(s.parts - 1, self.pass_on)
        self.local().wait()
        for part in range(s.parts):
            self.to_beside(part, s.beside, part, self.own).wait_recv()
            self.to_beside(part, s.beside, s.parts + part, self.own).wait_recv()
            self.to_across(part, self.own).wait_send()
            self.to_beside(part, s.group, part, self.own).wait_send()
            self.to_beside(part, s.group, s.parts + part, self.own).wait_send()

            @pl.when(s.has_right & (part <= s.place))
            def _():
                self.to_right(part, self.own).wait_send()

            @pl.when(s.has_left & (part >= s.place))
            def _():
                self.to_left(part, self.own).wait_send()


class Sum:
    def __init__(self, spot, part_ref, out, scratch):
        self.spot, self.part_ref, self.out = spot, part_ref, out
        (self.beside_buf, self.across_out, self.across_buf, self.line_out, self.left_buf, self.right_buf,
         self.beside_s, self.beside_r, self.across_s, self.across_r, self.right_s, self.left_s, self.from_left, self.from_right) = scratch
        self.order = spot.far_first()

    @staticmethod
    def scratch(parts, rows, width):
        one = pltpu.VMEM((parts, rows, width), jnp.bfloat16)
        two = pltpu.VMEM((2 * parts, rows, width), jnp.bfloat16)
        return [two, one, one, one, one, one, DMA((2 * parts,)), DMA((2 * parts,))] + [DMA((parts,))] * 6

    def base(self, part, column):
        rows = self.out.shape[0]
        return pl.multiple_of((part * 4 + column) * rows, rows)

    def to_beside(self, part, column, slot):
        source = self.part_ref.at[pl.ds(self.base(part, column), self.out.shape[0]), :]
        return remote(source, self.beside_buf.at[slot], self.beside_s.at[slot], self.beside_r.at[slot], {"experts": self.spot.beside})

    def to_across(self, part):
        return remote(self.across_out.at[part], self.across_buf.at[part], self.across_s.at[part], self.across_r.at[part], {"experts": self.spot.across})

    def to_right(self, part):
        return remote(self.line_out.at[part], self.left_buf.at[part], self.right_s.at[part], self.from_left.at[part], {"context": self.spot.place + 1})

    def to_left(self, part):
        return remote(self.line_out.at[part], self.right_buf.at[part], self.left_s.at[part], self.from_right.at[part], {"context": self.spot.place - 1})

    def chunks(self, body):
        step = 16

        def one(index, carry):
            start = pl.multiple_of(index * step, step)
            body(pl.ds(start, step), start, step)
            return carry

        lax.fori_loop(0, self.out.shape[0] // step, one, 0)

    def mine(self, base, start, step):
        return self.part_ref[pl.ds(pl.multiple_of(base + start, step), step), :].astype(jnp.float32)

    def begin(self):
        s = self.spot
        for part in self.order:
            self.to_beside(part, s.corner, s.parts + part).start()
        for part in self.order:
            self.to_beside(part, s.beside, part).start()

    def cross(self, index):
        s, part = self.spot, self.order[index]
        self.to_beside(part, s.corner, s.parts + part).wait_recv()
        base = self.base(part, s.across)

        def add(at, start, step):
            total = self.mine(base, start, step) + self.beside_buf[s.parts + part, at, :].astype(jnp.float32)
            self.across_out[part, at, :] = total.astype(jnp.bfloat16)

        self.chunks(add)
        self.to_across(part).start()

    def line(self, index):
        s, part = self.spot, self.order[index]
        self.to_beside(part, s.beside, part).wait_recv()
        self.to_across(part).wait_recv()
        base = self.base(part, s.group)
        f32 = jnp.float32

        def total(at, start, step):
            return self.mine(base, start, step) + self.beside_buf[part, at, :].astype(f32) + self.across_buf[part, at, :].astype(f32)

        def send(buf):
            def add(at, start, step):
                value = total(at, start, step)
                if buf is not None:
                    value = value + buf[part, at, :].astype(f32)
                self.line_out[part, at, :] = value.astype(jnp.bfloat16)

            self.chunks(add)

        if index < s.parts - 1:
            goes_right = part > s.place
            goes_left = jnp.logical_not(goes_right)

            @pl.when(goes_right & s.has_left)
            def _():
                self.to_right(part).wait_recv()
                send(self.left_buf)

            @pl.when(goes_left & s.has_right)
            def _():
                self.to_left(part).wait_recv()
                send(self.right_buf)

            @pl.when((goes_right & jnp.logical_not(s.has_left)) | (goes_left & jnp.logical_not(s.has_right)))
            def _():
                send(None)

            @pl.when(goes_right)
            def _():
                self.to_right(part).start()

            @pl.when(goes_left)
            def _():
                self.to_left(part).start()
        else:

            def keep(at, start, step):
                self.out[at, :] = total(at, start, step)

            self.chunks(keep)
            for there, copy, buf in ((s.has_left, self.to_right, self.left_buf), (s.has_right, self.to_left, self.right_buf)):

                @pl.when(there)
                def _():
                    copy(part).wait_recv()

                    def add(at, start, step):
                        self.out[at, :] = self.out[at, :] + buf[part, at, :].astype(f32)

                    self.chunks(add)

    def end(self):
        s = self.spot
        for part in range(s.parts):
            self.to_beside(part, s.corner, s.parts + part).wait_send()
            self.to_beside(part, s.beside, part).wait_send()
            self.to_across(part).wait_send()

            @pl.when(part > s.place)
            def _():
                self.to_right(part).wait_send()

            @pl.when(part < s.place)
            def _():
                self.to_left(part).wait_send()


class Move:
    def __init__(self, spot, items, sems):
        self.spot, self.items = spot, items
        self.line_s, self.line_r, self.twin_s, self.twin_r, self.local_sem = sems

    @staticmethod
    def sems(count, parts):
        return [DMA((count * parts,))] * 4 + [DMA((count,))]

    def fit(self, number, device, body):
        by_width(device, self.items[number]["short"], body)

    def to(self, number, target, source, short):
        s, item = self.spot, self.items[number]
        sems = self.line_s.at[number * s.parts + target], self.line_r.at[number * s.parts + source]
        return remote(item["src"](target, short), item["dst"](0, source, short), *sems, {"context": target})

    def on(self, number, source, short, view=None):
        s, item = self.spot, self.items[number]
        slot = number * s.parts + source
        view = item["dst"](0, source, short) if view is None else view
        return remote(view, item["dst"](1, source, short), self.twin_s.at[slot], self.twin_r.at[slot], s.twin)

    def local(self, number, short):
        s, item = self.spot, self.items[number]
        return pltpu.make_async_copy(item["src"](s.place, short), item["dst"](0, s.place, short), self.local_sem.at[number])

    def own(self, number):
        s, item = self.spot, self.items[number]

        def one(short):
            self.on(number, s.place, short, item["src"](s.place, short)).start()
            self.local(number, short).start()

        self.fit(number, s.place, one)

    def send_gap(self, number, gap):
        s = self.spot

        def one(target):
            self.fit(number, target, lambda short: self.to(number, target, s.place, short).start())

        s.others(gap, one)

    def send(self, number):
        for gap in range(self.spot.parts - 1, 0, -1):
            self.send_gap(number, gap)

    def forward(self, number, gap):
        s = self.spot

        def one(source):
            def step(short):
                self.to(number, s.place, source, short).wait_recv()
                self.on(number, source, short).start()

            self.fit(number, s.place, step)

        s.others(gap, one)

    def ready(self, number):
        s = self.spot

        def one(short):
            self.local(number, short).wait()
            for part in range(s.parts):
                self.on(number, part, short).wait_recv()

        self.fit(number, s.place, one)

    def sent(self):
        s = self.spot
        for number in range(len(self.items)):

            def one(short):
                for part in range(s.parts):
                    self.on(number, part, short).wait_send()

            self.fit(number, s.place, one)
            for part in range(s.parts):

                @pl.when(part != s.place)
                def _():
                    self.fit(number, part, lambda short: self.to(number, part, s.place, short).wait_send())

    def end(self):
        for number in range(len(self.items)):
            self.ready(number)
        self.sent()


class Return:
    def __init__(self, spot, items, got, mine, sems):
        self.spot, self.items, self.got, self.mine_buf = spot, items, got, mine
        self.twin_s, self.twin_r, self.load, self.line_s, self.line_r, self.local_sem = sems
        self.order = spot.far_first()
        self.bases = []
        for item in items:
            self.bases.append(self.bases[-1][1] if self.bases else 0)
            self.bases[-1] = (self.bases[-1], self.bases[-1] + len(item["pieces"]) * spot.parts)

    @staticmethod
    def scratch(shapes, pieces, parts):
        count = len(shapes)
        buf = [pltpu.VMEM((parts,) + shape, jnp.bfloat16) for shape in shapes]
        sems = [DMA((count * parts,))] * 3 + [DMA((sum(pieces) * parts,))] * 2 + [DMA((sum(pieces),))]
        return buf + buf + sems

    def swap(self, number, part):
        item, slot = self.items[number], number * self.spot.parts + part
        return remote(item["block"](1, part), self.got[number].at[part], self.twin_s.at[slot], self.twin_r.at[slot], self.spot.twin)

    def fetch(self, number, part):
        item, slot = self.items[number], number * self.spot.parts + part
        return pltpu.make_async_copy(item["block"](0, part), self.mine_buf[number].at[part], self.load.at[slot])

    def start(self, number):
        for part in self.order:
            self.swap(number, part).start()
            self.fetch(number, part).start()

    def piece(self, number, which, target, source, short):
        s = self.spot
        cut, out = self.items[number]["pieces"][which]
        slot = self.bases[number][0] + which * s.parts
        return remote(cut(self.mine_buf[number].at[target], short), out(source, short), self.line_s.at[slot + target], self.line_r.at[slot + source], {"context": target})

    def keep(self, number, which, short):
        s = self.spot
        cut, out = self.items[number]["pieces"][which]
        slot = self.bases[number][0] // s.parts + which
        return pltpu.make_async_copy(cut(self.mine_buf[number].at[s.place], short), out(s.place, short), self.local_sem.at[slot])

    def fit(self, number, source, body):
        by_width(source, self.items[number].get("short"), body)

    def reduce(self, number, index):
        s, part = self.spot, self.order[index]
        item = self.items[number]
        self.swap(number, part).wait_recv()
        self.fetch(number, part).wait()
        mine, got = self.mine_buf[number], self.got[number]
        rows, step = mine.shape[1], 32

        def one(at, carry):
            span = pl.ds(pl.multiple_of(at * step, step), step)
            total = mine[part, span, :].astype(jnp.float32) + got[part, span, :].astype(jnp.float32)
            mine[part, span, :] = total.astype(jnp.bfloat16)
            return carry

        lax.fori_loop(0, rows // step, one, 0)
        for which in range(len(item["pieces"])):
            if index < s.parts - 1:
                self.fit(number, s.place, lambda short: self.piece(number, which, part, s.place, short).start())
            else:
                self.fit(number, s.place, lambda short: self.keep(number, which, short).start())

    def end(self):
        s = self.spot
        for number, item in enumerate(self.items):
            for part in range(s.parts):
                self.swap(number, part).wait_send()
                for which in range(len(item["pieces"])):

                    @pl.when(part != s.place)
                    def _():
                        self.fit(number, s.place, lambda short: self.piece(number, which, part, s.place, short).wait_send())
                        self.fit(number, part, lambda short: self.piece(number, which, s.place, part, short).wait_recv())

            for which in range(len(item["pieces"])):
                self.fit(number, s.place, lambda short: self.keep(number, which, short).wait())


class Grads:
    def __init__(self, both, width, dup, act, up_out, down_out, up_buf, down_buf, up_s, down_s):
        self.both, self.width, self.dup, self.act = both, width, dup, act
        self.up_out, self.down_out, self.up_buf, self.down_buf = up_out, down_out, up_buf, down_buf
        self.up_s, self.down_s = up_s, down_s
        self.step = 256

    @staticmethod
    def scratch():
        up, down = pltpu.VMEM((2, 256, 2 * WINDOW), jnp.bfloat16), pltpu.VMEM((2, WINDOW, 256), jnp.bfloat16)
        return [up, down, DMA((2,)), DMA((2,))]

    def copies(self, index):
        at = pl.ds(pl.multiple_of(index * self.step, self.step), self.step)
        slot = lax.rem(index, 2)
        return (
            lambda: pltpu.make_async_copy(self.up_buf.at[slot], self.up_out.at[at, :], self.up_s.at[slot]),
            lambda: pltpu.make_async_copy(self.down_buf.at[slot], self.down_out.at[:, at], self.down_s.at[slot]),
        )

    def run(self):
        count = self.width // self.step

        def one(index, carry):
            up_copy, down_copy = self.copies(index)

            @pl.when(index >= 2)
            def _():
                up_copy().wait()
                down_copy().wait()

            slot = lax.rem(index, 2)
            at = pl.multiple_of(index * self.step, self.step)
            up = dot_tn(self.both[:, pl.ds(at, self.step)], self.dup[...])
            self.up_buf[slot] = up.astype(jnp.bfloat16)
            down = dot_tn(self.act[...], self.both[:, pl.ds(self.width + at, self.step)])
            self.down_buf[slot] = down.astype(jnp.bfloat16)
            up_copy().start()
            down_copy().start()
            return carry

        lax.fori_loop(0, count, one, 0)
        for index in (count - 2, count - 1):
            for copy in self.copies(index):
                copy().wait()


def comm_call(kernel, number, name, out_shape, out_specs, in_specs, scratch, bytes_moved):
    return pl.pallas_call(
        kernel,
        out_shape=out_shape,
        in_specs=in_specs,
        out_specs=out_specs,
        scratch_shapes=scratch,
        compiler_params=pltpu.CompilerParams(collective_id=number, has_side_effects=True),
        cost_estimate=pl.CostEstimate(flops=0, bytes_accessed=bytes_moved, transcendentals=0),
        name=name,
    )


IN_VMEM = pl.BlockSpec(memory_space=pltpu.VMEM)
IN_PLACE = pl.BlockSpec(memory_space=pl.ANY)
WINDOW = 384


SPARE = 128


def narrow_of(k):
    return 0 if k % 2 else 3


def window_of(k, index, narrow):
    if narrow_of(k) == 0:
        return (0, WINDOW - SPARE, 0) if narrow else (index * WINDOW - SPARE, WINDOW, 0)
    return (index * WINDOW, WINDOW - SPARE, SPARE) if narrow else (index * WINDOW, WINDOW, 0)


def first_unit(value):
    return value if isinstance(value, int) else pl.multiple_of(value, SPARE)


def units_at(ref, k, index, narrow, axis, base=0):
    start, size, inside = window_of(k, index, narrow)
    start = first_unit(start) if base is None else base + inside
    return ref.at[pl.ds(start, size), :] if axis == 0 else ref.at[:, pl.ds(start, size)]


def turn(value, cosine, sine_part):
    return value * cosine + pltpu.roll(value, HEAD_DIM // 2, 1) * sine_part


def turn_tables(facts):
    both = facts[:, :HEAD_DIM].astype(jnp.float32) + facts[:, HEAD_DIM:].astype(jnp.float32)
    swapped = pltpu.roll(both, HEAD_DIM // 2, 1)
    low = lax.broadcasted_iota(jnp.int32, (1, HEAD_DIM), 1) < HEAD_DIM // 2
    return jnp.where(low, both, swapped), jnp.where(low, -swapped, both)


def attention_first(value, qkv_in, out_weight, bias, shared_down, expert_down, number):
    parts = lax.axis_size("context")
    rows, wide = value.shape
    block, span = qkv_in.shape[0] // parts, qkv_in.shape[1]
    head, lanes = out_weight.shape[0] // parts, out_weight.shape[1]
    width, length = 2 * parts * lanes, rows * parts * 4
    count = 1 + expert_down.shape[0]
    step = 256
    scale = HEAD_DIM ** (-0.5)
    f32, bf16 = jnp.float32, jnp.bfloat16
    sets = [
        [
            pltpu.VMEM((length, wide), bf16),
            pltpu.VMEM((2 * parts * block, span), bf16),
            pltpu.VMEM((head, width), bf16),
            pltpu.VMEM((length, width), bf16),
            DMA((3,)),
        ],
        Share.sems(parts),
        Move.sems(2 + count, parts),
        Sum.scratch(parts, rows, width),
    ]

    def kernel(own_ref, qkv_ref, outw_ref, bias_ref, shared_ref, expert_ref,
               all_hbm, wqkv_hbm, wout_hbm, wd_ref, q_ref, k_ref, v_ref, att_ref, lse_ref, sum_ref, *scratch):
        scratch, split = list(scratch), []
        for one in sets:
            split.append(scratch[: len(one)])
            scratch = scratch[len(one) :]
        all_ref, wqkv_ref, wout_ref, part_ref, keep = split[0]
        spot = Spot()
        share = Share(spot, own_ref, all_ref, split[1])
        items = [
            {
                "src": lambda target, short: rows_at(qkv_ref, target * block, block),
                "dst": lambda side, source, short: rows_at(wqkv_ref, (side * parts + source) * block, block),
                "short": None,
            },
            {
                "src": lambda target, short: rows_at(outw_ref, target * head, head),
                "dst": lambda side, source, short: lanes_at(wout_ref, (side * parts + source) * lanes, lanes),
                "short": None,
            },
        ]

        def down(k):
            ref = shared_ref if k == 0 else expert_ref.at[k - 1]
            return {
                "src": lambda target, short: units_at(ref, k, target, short, 0, None),
                "dst": lambda side, source, short: lanes_at(
                    units_at(wd_ref, k, 0, short, 0, k * WINDOW), (side * parts + source) * lanes, lanes
                ),
                "short": narrow_of(k),
            }

        move = Move(spot, items + [down(k) for k in range(count)], split[2])
        summed = Sum(spot, part_ref, sum_ref, split[3])
        copies = [
            pltpu.make_async_copy(source, target, keep.at[index])
            for index, (source, target) in enumerate(((all_ref, all_hbm), (wqkv_ref, wqkv_hbm), (wout_ref, wout_hbm)))
        ]

        def project(index, carry):
            at = pl.ds(pl.multiple_of(index * step, step), step)
            qkv = jnp.dot(all_ref[at, :width], wqkv_ref[...], preferred_element_type=f32) + bias_ref[...]
            cosine, sine_part = turn_tables(all_ref[at, width:])
            q_ref[at, :] = turn(qkv[:, :HEAD_DIM], cosine, sine_part).astype(bf16)
            k_ref[at, :] = turn(qkv[:, HEAD_DIM : 2 * HEAD_DIM], cosine, sine_part).astype(bf16)
            v_ref[at, :] = qkv[:, 2 * HEAD_DIM :].astype(bf16)
            return carry

        def attend(index, carry):
            start = pl.multiple_of(index * step, step)
            at = pl.ds(start, step)
            scores = dot_nt(q_ref[at, :], k_ref[...]) * scale
            query_index = start + lax.broadcasted_iota(jnp.int32, scores.shape, 0)
            allowed = lax.broadcasted_iota(jnp.int32, scores.shape, 1) <= query_index
            row_max = jnp.max(jnp.where(allowed, scores, MASKED), -1, keepdims=True)
            weights = jnp.where(allowed, jnp.exp(scores - row_max), 0.0)
            row_sum = jnp.sum(weights, -1, keepdims=True)
            attended = (jnp.dot(weights.astype(bf16), v_ref[...], preferred_element_type=f32) / row_sum).astype(bf16)
            att_ref[at, :] = attended
            lse_ref[at, :] = jnp.broadcast_to(row_max + jnp.log(row_sum), (step, HEAD_DIM))
            part_ref[at, :] = jnp.dot(attended, wout_ref[...], preferred_element_type=f32).astype(bf16)
            return carry

        spot.greet(True, True)
        share.begin()
        for number in range(len(move.items)):
            move.own(number)
        move.send_gap(0, 3)
        share.step(1)
        move.send_gap(0, 2)
        share.step(2)
        move.send_gap(0, 1)
        share.step(3)
        move.send(1)
        move.send(2)
        for gap in (1, 2, 3):
            move.forward(0, gap)
        for gap in (1, 2, 3):
            move.forward(1, gap)
        share.end()
        copies[0].start()
        move.ready(0)
        copies[1].start()
        lax.fori_loop(0, length // step, project, 0)
        move.ready(1)
        copies[2].start()
        for number in range(3, len(move.items)):
            move.send(number)
        lax.fori_loop(0, length // step, attend, 0)
        summed.begin()
        for gap in (1, 2, 3):
            move.forward(2, gap)
        for index in range(parts):
            summed.cross(index)
        for number in range(3, len(move.items)):
            for gap in (1, 2, 3):
                move.forward(number, gap)
        for index in range(parts):
            summed.line(index)
        summed.end()
        for number in range(2, len(move.items)):
            move.ready(number)
        move.sent()
        for copy in copies:
            copy.wait()

    heads = jax.ShapeDtypeStruct((length, HEAD_DIM), bf16)
    return comm_call(
        kernel,
        number,
        "attention_first",
        [
            jax.ShapeDtypeStruct((length, wide), bf16),
            jax.ShapeDtypeStruct((2 * parts * block, span), bf16),
            jax.ShapeDtypeStruct((head, width), bf16),
            jax.ShapeDtypeStruct((count * WINDOW, width), bf16),
            heads,
            heads,
            heads,
            heads,
            jax.ShapeDtypeStruct((length, HEAD_DIM), f32),
            jax.ShapeDtypeStruct((rows, width), f32),
        ],
        [IN_PLACE] * 4 + [IN_VMEM] * 6,
        [IN_VMEM, IN_PLACE, IN_PLACE, IN_VMEM, IN_PLACE, IN_PLACE],
        [one for group in sets for one in group],
        250_000_000,
    )(value, qkv_in, out_weight, bias, shared_down, expert_down)


def share_move_compute(value, shared_gate, shared_up, expert_gate, expert_up, wd, number):
    parts = lax.axis_size("context")
    rows, wide = value.shape
    width = wd.shape[1]
    block = shared_gate.shape[0]
    stacks = 1 + expert_gate.shape[0]
    count = 2 * stacks
    length = rows * parts * 4
    experts = (stacks - 1) * 4
    step = 256
    f32, bf16 = jnp.float32, jnp.bfloat16
    share_sems, move_sems, grad_scratch = Share.sems(parts), Move.sems(count, parts), Grads.scratch()
    scratch = [
        pltpu.VMEM((length, wide), bf16),
        pltpu.VMEM((2 * parts * block, count * WINDOW), bf16),
        pltpu.VMEM(wd.shape, bf16),
        pltpu.VMEM((length, width), f32),
        pltpu.VMEM((length, width), f32),
        pltpu.VMEM((length, 128), f32),
        pltpu.VMEM((length, stacks * WINDOW), bf16),
        pltpu.VMEM((length, count * WINDOW), bf16),
        pltpu.VMEM((2, step, width + 128), bf16),
        pltpu.VMEM((2, step, width), bf16),
        DMA((2,)),
        DMA((stacks,)),
        DMA((stacks,)),
        DMA((length // step,)),
        DMA((length // step,)),
    ]

    def kernel(own_ref, sg_ref, su_ref, eg_ref, eu_ref, wd_hbm, both_hbm, send_hbm, branch_hbm, dup_hbm, act_hbm, upg_hbm, downg_hbm, *rest):
        both, wgu, wd_ref, dx_acc, out_acc, dot_acc, act_ref, dup_ref, send_buf, branch_buf, load, act_s, dup_s, send_s, branch_s = rest[: len(scratch)]
        grad_refs, sems = rest[len(scratch) : len(scratch) + 4], rest[len(scratch) + 4 :]
        spot = Spot()
        share = Share(spot, own_ref, both, sems[: len(share_sems)])

        def item(number):
            k = number // 2
            shared, expert = (sg_ref, eg_ref) if number % 2 == 0 else (su_ref, eu_ref)
            ref = shared if k == 0 else expert.at[k - 1]
            return {
                "src": lambda target, short: units_at(ref, k, target, short, 1, None),
                "dst": lambda side, source, short: rows_at(
                    units_at(wgu, k, 0, short, 1, number * WINDOW), (side * parts + source) * block, block
                ),
                "short": narrow_of(k),
            }

        move = Move(spot, [item(number) for number in range(count)], sems[len(share_sems) :])
        weights = pltpu.make_async_copy(wd_hbm, wd_ref, load.at[0])
        keep = pltpu.make_async_copy(both, both_hbm, load.at[1])
        column = lax.broadcasted_iota(jnp.int32, (1, 128), 1)

        def send_out(index):
            at = pl.ds(pl.multiple_of(index * step, step), step)
            return pltpu.make_async_copy(send_buf.at[lax.rem(index, 2)], send_hbm.at[at, :], send_s.at[index])

        def branch_out(index):
            at = pl.ds(pl.multiple_of(index * step, step), step)
            return pltpu.make_async_copy(branch_buf.at[lax.rem(index, 2)], branch_hbm.at[at, :], branch_s.at[index])

        def act_out():
            return pltpu.make_async_copy(act_ref.at[:, pl.ds((stacks - 1) * WINDOW, WINDOW)], act_hbm, act_s.at[0])

        def dup_out():
            return pltpu.make_async_copy(dup_ref.at[:, pl.ds(2 * (stacks - 1) * WINDOW, 2 * WINDOW)], dup_hbm, dup_s.at[0])

        def gradients(k):
            up, down = pl.ds(2 * k * WINDOW, 2 * WINDOW), pl.ds(k * WINDOW, WINDOW)
            Grads(both, width, dup_ref.at[:, up], act_ref.at[:, down], upg_hbm.at[:, up], downg_hbm.at[down, :], *grad_refs).run()

        def compute(k, first, last):
            up, down = pl.ds(2 * k * WINDOW, 2 * WINDOW), pl.ds(k * WINDOW, WINDOW)
            at = experts if k == 0 else spot.group * (stacks - 1) + k - 1
            here = jnp.where(column == at, 1.0, 0.0)
            both_parts = jnp.where((column == at) | (column == at + 64), 1.0, 0.0)

            def one(index, carry):
                rows_here = pl.ds(pl.multiple_of(index * step, step), step)
                vals = jnp.dot(both[rows_here, :width], wgu[:, up], preferred_element_type=f32)
                raw = dot_nt(both[rows_here, width : 2 * width], wd_ref[down, :])
                coef = jnp.sum(both[rows_here, 2 * width :].astype(f32) * both_parts, -1, keepdims=True)
                g_vals, u_vals = vals[:, :WINDOW], vals[:, WINDOW:]
                sig_g = jax.nn.sigmoid(g_vals)
                silu_g = g_vals * sig_g
                act = silu_g * u_vals
                dots = jnp.sum(raw * act, -1, keepdims=True) * here
                act_ref[rows_here, down] = (act * coef).astype(bf16)
                dact = raw * coef
                dup_ref[rows_here, pl.ds(2 * k * WINDOW, WINDOW)] = (
                    dact * u_vals * (sig_g * (1.0 + g_vals * (1.0 - sig_g)))
                ).astype(bf16)
                dup_ref[rows_here, pl.ds((2 * k + 1) * WINDOW, WINDOW)] = (dact * silu_g).astype(bf16)
                out_part = jnp.dot(act_ref[rows_here, down], wd_ref[down, :], preferred_element_type=f32)
                dx_part = dot_nt(dup_ref[rows_here, up], wgu[:, up])
                if k == 0:
                    out_acc[rows_here, :] = out_part
                    dx_acc[rows_here, :] = dx_part
                    dot_acc[rows_here, :] = dots
                elif k < stacks - 1:
                    out_acc[rows_here, :] += out_part
                    dx_acc[rows_here, :] += dx_part
                    dot_acc[rows_here, :] += dots
                else:

                    @pl.when(index >= 2)
                    def _():
                        send_out(index - 2).wait()
                        branch_out(index - 2).wait()

                    slot = lax.rem(index, 2)
                    branch_buf[slot] = (out_acc[rows_here, :] + out_part).astype(bf16)
                    send_buf[slot, :, :width] = (dx_acc[rows_here, :] + dx_part).astype(bf16)
                    send_buf[slot, :, width:] = (dot_acc[rows_here, :] + dots).astype(bf16)
                    send_out(index).start()
                    branch_out(index).start()
                return carry

            lax.fori_loop(first, last, one, 0)

        def forward(number):
            for gap in (1, 2, 3):
                move.forward(number, gap)

        spot.greet(True, True)
        share.begin()
        weights.start()
        for number in range(count):
            move.own(number)
        move.send(0)
        share.step(1)
        move.send(1)
        share.step(2)
        forward(0)
        share.step(3)
        for number in range(2, count):
            move.send(number)
        share.end()
        keep.start()
        forward(1)
        weights.wait()
        for k in range(stacks):

            @pl.when(spot.place == narrow_of(k))
            def _():
                spare = 0 if narrow_of(k) else WINDOW - SPARE
                wd_ref[pl.ds(k * WINDOW + spare, SPARE), :] = jnp.zeros((SPARE, width), bf16)
                for which in (2 * k, 2 * k + 1):
                    wgu[:, pl.ds(which * WINDOW + spare, SPARE)] = jnp.zeros((2 * parts * block, SPARE), bf16)

        pieces = length // step
        for k in range(stacks):
            if k < stacks - 1:
                forward(2 * k + 2)
            move.ready(2 * k)
            move.ready(2 * k + 1)
            compute(k, 0, pieces // 2)
            if k < stacks - 1:
                forward(2 * k + 3)
            compute(k, pieces // 2, pieces)
            if k < stacks - 1:
                gradients(k)
        act_out().start()
        dup_out().start()
        for index in (pieces - 2, pieces - 1):
            send_out(index).wait()
            branch_out(index).wait()
        act_out().wait()
        dup_out().wait()
        keep.wait()
        move.sent()

    return comm_call(
        kernel,
        number,
        "share_move_compute",
        [
            jax.ShapeDtypeStruct((length, wide), bf16),
            jax.ShapeDtypeStruct((length, width + 128), bf16),
            jax.ShapeDtypeStruct((length, width), bf16),
            jax.ShapeDtypeStruct((length, 2 * WINDOW), bf16),
            jax.ShapeDtypeStruct((length, WINDOW), bf16),
            jax.ShapeDtypeStruct((width, 2 * (stacks - 1) * WINDOW), bf16),
            jax.ShapeDtypeStruct(((stacks - 1) * WINDOW, width), bf16),
        ],
        [IN_PLACE] * 7,
        [IN_VMEM] + [IN_PLACE] * 5,
        scratch + grad_scratch + share_sems + move_sems,
        300_000_000,
    )(value, shared_gate, shared_up, expert_gate, expert_up, wd)


def up_item(grads_ref, at, k, gate_ref, up_ref, block, parts):
    def piece(offset, ref):
        return (
            lambda buf, short: units_at(buf, k, 0, short, 1, offset),
            lambda source, short: units_at(ref, k, source, short, 1, None),
        )

    return {
        "block": lambda side, part: grads_ref.at[
            pl.ds(pl.multiple_of((side * parts + part) * block, block), block), pl.ds(2 * at * WINDOW, 2 * WINDOW)
        ],
        "pieces": [piece(0, gate_ref), piece(WINDOW, up_ref)],
        "short": narrow_of(k),
    }


def down_item(grads_ref, at, k, down_ref, parts):
    lanes = down_ref.shape[1]
    return {
        "block": lambda side, part: grads_ref.at[
            pl.ds(at * WINDOW, WINDOW), pl.ds(pl.multiple_of((side * parts + part) * lanes, lanes), lanes)
        ],
        "pieces": [
            (
                lambda buf, short: units_at(buf, k, 0, short, 0),
                lambda source, short: units_at(down_ref, k, source, short, 0, None),
            )
        ],
        "short": narrow_of(k),
    }


def attention_last(send4, up_grads, down_grads, hidden, grad, gain, chances, named, router, out_w, qkv_w, heads, lse, shared, number):
    parts = lax.axis_size("context")
    length, width = send4.shape[0], hidden.shape[1]
    rows, wide = hidden.shape[0], send4.shape[1]
    block = up_grads.shape[0] // (2 * parts)
    lanes = down_grads.shape[1] // (2 * parts)
    units = WINDOW * parts - 128
    step = 256
    experts = 8
    scale = HEAD_DIM ** (-0.5)
    f32, bf16 = jnp.float32, jnp.bfloat16
    shapes, pieces = [(block, 2 * WINDOW), (WINDOW, lanes), (block, 2 * WINDOW)], [2, 1, 2]
    sets = [
        [
            pltpu.VMEM((rows, wide), f32),
            pltpu.VMEM((rows, width), bf16),
            pltpu.VMEM((length, width), bf16),
            pltpu.VMEM((length, width), bf16),
            pltpu.VMEM((length, 3 * HEAD_DIM), bf16),
            pltpu.VMEM((length, HEAD_DIM), f32),
            pltpu.VMEM((length, HEAD_DIM), f32),
            pltpu.VMEM((length, HEAD_DIM), f32),
            pltpu.VMEM(shared.shape, bf16),
            DMA((2,)),
        ],
        Sum.scratch(parts, rows, wide),
        Share.sems(parts),
        Sum.scratch(parts, rows, width),
        Return.scratch(shapes, pieces, parts),
    ]

    def kernel(send_ref, upg_ref, downg_ref, hidden_ref, grad_ref, gain_ref, chance_ref, named_ref, router_ref, wout_ref, wqkv_ref,
               q_ref, k_ref, v_ref, att_ref, lse_ref, shared_hbm,
               dh_hbm, gate_out, up_out, down_out, gate_out1, up_out1, dots_ref, dxn2_ref, dhidden_ref, outg_ref, qkvg_ref, bias_ref, dxn1_ref, *scratch):
        scratch, split = list(scratch), []
        for one in sets:
            split.append(scratch[: len(one)])
            scratch = scratch[len(one) :]
        sums, dh_own, dh_all, part_ref, dqkv_ref, dq_acc, dk_acc, dv_acc, shared_ref, keep_sem = split[0]
        spot = Spot()
        first = Sum(spot, send_ref, sums, split[1])
        share = Share(spot, dh_own, dh_all, split[2])
        second = Sum(spot, part_ref, dxn1_ref, split[3])
        items = [
            up_item(upg_ref, 0, 0, gate_out, up_out, block, parts),
            down_item(downg_ref, 0, 0, down_out, parts),
            up_item(upg_ref, 1, 1, gate_out1, up_out1, block, parts),
        ]
        back = Return(spot, items, split[4][:3], split[4][3:6], split[4][6:])
        keep = pltpu.make_async_copy(dh_all, dh_hbm, keep_sem.at[0])
        fetch = pltpu.make_async_copy(shared_hbm, shared_ref, keep_sem.at[1])

        def owner():
            lane = lax.broadcasted_iota(jnp.int32, (rows, 128), 1)
            dots = sums[:, width:]
            dots_ref[...] = dots
            chance = chance_ref[...]
            dprob = dots * named_ref[...]
            prob = jnp.where(lane < experts, chance, 0.0)
            dlogit = prob * (dprob - jnp.sum(prob * dprob, -1, keepdims=True))
            mix = jnp.where(lane < experts, dlogit, jnp.where(lane == experts, chance * (1.0 - chance) * dots, 0.0))
            dxn2_ref[...] = jnp.dot(mix, router_ref[...], precision=PRECISE, preferred_element_type=f32)

            def one(index, carry):
                at = pl.ds(pl.multiple_of(index * 16, 16), 16)
                dxn2 = dxn2_ref[at, :] + sums[at, :width]
                dxn2_ref[at, :] = dxn2
                value = hidden_ref[at, :]
                inverse = lax.rsqrt(jnp.mean(value * value, -1, keepdims=True) + EPSILON)
                normed = value * inverse
                scaled = dxn2 * gain_ref[...]
                dhidden = grad_ref[at, :].astype(f32) + inverse * (scaled - normed * jnp.mean(scaled * normed, -1, keepdims=True))
                dhidden_ref[at, :] = dhidden
                dh_own[at, :] = dhidden.astype(bf16)
                return carry

            lax.fori_loop(0, rows // 16, one, 0)

        def attend(index, carry):
            start = pl.multiple_of(index * step, step)
            at = pl.ds(start, step)
            datt = dot_nt(dh_all[at, :], wout_ref[...]).astype(bf16)
            delta = jnp.sum(datt.astype(f32) * att_ref[at, :].astype(f32), -1, keepdims=True)
            scores = dot_nt(q_ref[at, :], k_ref[...]) * scale
            query_index = start + lax.broadcasted_iota(jnp.int32, scores.shape, 0)
            allowed = lax.broadcasted_iota(jnp.int32, scores.shape, 1) <= query_index
            prob = jnp.where(allowed, jnp.exp(scores - lse_ref[at, :1]), 0.0)
            dscore = (prob * (dot_nt(datt, v_ref[...]) - delta)).astype(bf16)
            dq_acc[at, :] = jnp.dot(dscore, k_ref[...], preferred_element_type=f32) * scale
            dk_acc[...] += dot_tn(dscore, q_ref[at, :])
            dv_acc[...] += dot_tn(prob.astype(bf16), datt)
            return carry

        def project(index, carry):
            at = pl.ds(pl.multiple_of(index * step, step), step)
            cosine, sine_part = turn_tables(shared_ref[at, width:])
            dq, dk, dv = dq_acc[at, :], dk_acc[at, :] * scale, dv_acc[at, :]
            dq = dq * cosine - pltpu.roll(dq, HEAD_DIM // 2, 1) * sine_part
            dk = dk * cosine - pltpu.roll(dk, HEAD_DIM // 2, 1) * sine_part
            for which, value in enumerate((dq, dk, dv)):
                bias_ref[:, pl.ds(which * HEAD_DIM, HEAD_DIM)] += jnp.sum(value, 0, keepdims=True)
                dqkv_ref[at, pl.ds(which * HEAD_DIM, HEAD_DIM)] = value.astype(bf16)
            part_ref[at, :] = dot_nt(dqkv_ref[at, :], wqkv_ref[...]).astype(bf16)
            return carry

        def features(index, carry):
            at = pl.ds(pl.multiple_of(index * step, step), step)
            qkvg_ref[at, :] = dot_tn(shared_ref[:, at], dqkv_ref[...]).astype(bf16)
            outg_ref[:, at] = dot_tn(att_ref[...], dh_all[:, at]).astype(bf16)
            return carry

        spot.greet(True, True)
        first.begin()
        for number in range(3):
            back.start(number)
        fetch.start()
        dk_acc[...] = jnp.zeros_like(dk_acc)
        dv_acc[...] = jnp.zeros_like(dv_acc)
        bias_ref[...] = jnp.zeros_like(bias_ref)
        for index in range(parts):
            first.cross(index)
        back.reduce(0, 0)
        back.reduce(0, 1)
        for index in range(parts):
            first.line(index)
        owner()
        share.begin()
        share.step(1)
        share.step(2)
        back.reduce(0, 2)
        share.step(3)
        back.reduce(0, 3)
        share.end()
        keep.start()
        for index in range(parts):
            back.reduce(1, index)
        lax.fori_loop(0, length // step, attend, 0)
        fetch.wait()
        lax.fori_loop(0, length // step, project, 0)
        second.begin()
        back.reduce(2, 0)
        for index in range(parts):
            second.cross(index)
        back.reduce(2, 1)
        lax.fori_loop(0, width // step, features, 0)
        for index in range(parts):
            second.line(index)
        back.reduce(2, 2)
        back.reduce(2, 3)
        first.end()
        second.end()
        back.end()
        keep.wait()

    piece = jax.ShapeDtypeStruct((block, units), bf16)
    return comm_call(
        kernel,
        number,
        "attention_last",
        [
            jax.ShapeDtypeStruct((length, width), bf16),
            piece,
            piece,
            jax.ShapeDtypeStruct((units, lanes), bf16),
            piece,
            piece,
            jax.ShapeDtypeStruct((rows, 128), f32),
            jax.ShapeDtypeStruct((rows, width), f32),
            jax.ShapeDtypeStruct((rows, width), f32),
            jax.ShapeDtypeStruct((HEAD_DIM, width), bf16),
            jax.ShapeDtypeStruct((width, 3 * HEAD_DIM), bf16),
            jax.ShapeDtypeStruct((1, 3 * HEAD_DIM), f32),
            jax.ShapeDtypeStruct((rows, width), f32),
        ],
        [IN_PLACE] * 6 + [IN_VMEM] * 7,
        [IN_VMEM, IN_PLACE, IN_PLACE] + [IN_VMEM] * 13 + [IN_PLACE],
        [one for group in sets for one in group],
        250_000_000,
    )(send4, up_grads, down_grads, hidden, grad, gain, chances, named, router, out_w, qkv_w, *heads, lse, shared)


class Group:
    def __init__(self, spot, own, out, sems):
        self.spot, self.own, self.out = spot, own, out
        self.local_sem, self.across_s, self.across_r, self.beside_s, self.beside_r = sems

    @staticmethod
    def sems():
        return [DMA, DMA, DMA, DMA((2,)), DMA((2,))]

    def block(self, column):
        rows = self.own.shape[0]
        return rows_at(self.out, column * rows, rows)

    def to_across(self):
        s = self.spot
        return remote(self.own, self.block(s.group), self.across_s, self.across_r, {"experts": s.across})

    def to_beside(self, slot):
        s = self.spot
        column = s.across if slot else s.group
        source = self.block(column) if slot else self.own
        return remote(source, self.block(column), self.beside_s.at[slot], self.beside_r.at[slot], {"experts": s.beside})

    def local(self):
        return pltpu.make_async_copy(self.own, self.block(self.spot.group), self.local_sem)

    def begin(self):
        self.to_across().start()
        self.to_beside(0).start()
        self.local().start()

    def end(self):
        self.to_across().wait_recv()
        self.to_beside(1).start()
        self.local().wait()
        self.to_across().wait_send()
        for slot in range(2):
            self.to_beside(slot).wait()


class Total:
    def __init__(self, spot, value, out, scratch):
        self.out = out
        self.sent, self.got, self.send_s, self.recv_s = scratch
        place = spot.place
        self.turns = [
            spot.twin,
            {"context": place + 1 - 2 * lax.rem(place, 2)},
            {"context": lax.rem(place + 2, spot.parts)},
            {"experts": spot.beside},
            {"experts": spot.across},
        ]
        self.value = value

    @staticmethod
    def scratch(shape):
        buf = pltpu.VMEM((5,) + shape, jnp.float32)
        return [buf, buf, DMA((5,)), DMA((5,))]

    def copy(self, index):
        return remote(self.sent.at[index], self.got.at[index], self.send_s.at[index], self.recv_s.at[index], self.turns[index])

    def begin(self):
        self.out[...] = self.value[...]
        self.send(0)

    def send(self, index):
        self.sent[index] = self.out[...]
        self.copy(index).start()

    def take(self, index):
        self.copy(index).wait()
        self.out[...] = self.out[...] + self.got[index]


def last_exchange(down_grads, out_grads, qkv_grads, both, dup, act, branch, hidden, tokens_grad, small, number):
    parts = lax.axis_size("context")
    rows, width = hidden.shape
    block = lanes = width // (2 * parts)
    units = WINDOW * parts - 128
    head, span = out_grads.shape[0], qkv_grads.shape[1]
    shapes = [(head, lanes), (block, span), (WINDOW, lanes), (block, 2 * WINDOW), (WINDOW, lanes)]
    pieces = [1, 1, 1, 2, 1]
    count, bf16 = len(shapes), jnp.bfloat16
    groups = [
        Return.scratch(shapes, pieces, parts),
        Sum.scratch(parts, rows, width) + [pltpu.VMEM((rows, width), jnp.float32), pltpu.VMEM((rows, width), bf16)],
        Total.scratch(small.shape),
        Group.sems(),
        Group.sems(),
        Grads.scratch() + [pltpu.VMEM(both.shape, bf16), pltpu.VMEM(dup.shape, bf16), pltpu.VMEM(act.shape, bf16), DMA((3,))],
    ]
    piece, column = jax.ShapeDtypeStruct((block, units), bf16), jax.ShapeDtypeStruct((units, lanes), bf16)
    out_shape = [jax.ShapeDtypeStruct((parts * head, lanes), bf16), jax.ShapeDtypeStruct((parts * block, span), bf16)]
    out_shape += [column, piece, piece, column]
    out_shape += [
        jax.ShapeDtypeStruct((width, 2 * WINDOW), bf16),
        jax.ShapeDtypeStruct((WINDOW, width), bf16),
        jax.ShapeDtypeStruct((4 * rows, width), bf16),
        jax.ShapeDtypeStruct((4 * rows, width), jnp.float32),
        jax.ShapeDtypeStruct(small.shape, jnp.float32),
    ]

    def kernel(downg_ref, outg_ref, qkvg_ref, both_hbm, dup_hbm, act_hbm, branch_ref, hidden_ref, tokens_ref, small_ref, *rest):
        outs, scratch = rest[: len(out_shape)], list(rest[len(out_shape) :])
        sets = []
        for one in groups:
            sets.append(scratch[: len(one)])
            scratch = scratch[len(one) :]
        grads, (upg2_hbm, downg2_hbm, block_all, tokens_all, small_out) = outs[:-5], outs[-5:]
        *grad_refs, both_ref, dup_ref, act_ref, load = sets[5]
        loads = [
            pltpu.make_async_copy(source, target, load.at[index])
            for index, (source, target) in enumerate(((both_hbm, both_ref), (dup_hbm, dup_ref), (act_hbm, act_ref)))
        ]
        items = [
            {
                "block": lambda side, part: lanes_at(outg_ref, (side * parts + part) * lanes, lanes),
                "pieces": [(lambda buf, short: buf, lambda source, short: rows_at(grads[0], source * head, head))],
            },
            {
                "block": lambda side, part: rows_at(qkvg_ref, (side * parts + part) * block, block),
                "pieces": [(lambda buf, short: buf, lambda source, short: rows_at(grads[1], source * block, block))],
            },
        ]
        items += [
            down_item(downg_ref, 1, 1, grads[2], parts),
            up_item(upg2_hbm, 0, 2, grads[3], grads[4], block, parts),
            down_item(downg2_hbm, 0, 2, grads[5], parts),
        ]
        spot = Spot()
        back = Return(spot, items, sets[0][:count], sets[0][count : 2 * count], sets[0][2 * count :])
        total_branch, own_block = sets[1][-2:]
        summed = Sum(spot, branch_ref, total_branch, sets[1][:-2])
        total = Total(spot, small_ref, small_out, sets[2])
        tokens_group = Group(spot, tokens_ref, tokens_all, sets[3])
        block_group = Group(spot, own_block, block_all, sets[4])
        spot.greet(True, True)
        total.begin()
        summed.begin()
        for item in range(3):
            back.start(item)
        for copy in loads:
            copy.start()
        total.take(0)
        total.send(1)
        for index in range(parts):
            summed.cross(index)
        total.take(1)
        total.send(2)
        for index in range(parts):
            back.reduce(0, index)
        total.take(2)
        total.send(3)
        for index in range(parts):
            back.reduce(1, index)
        total.take(3)
        total.send(4)
        for copy in loads:
            copy.wait()
        Grads(both_ref, width, dup_ref, act_ref, upg2_hbm, downg2_hbm, *grad_refs).run()
        back.start(3)
        back.start(4)
        for index in range(parts):
            back.reduce(2, index)
        total.take(4)
        tokens_group.begin()
        for index in range(parts):
            summed.line(index)
        half = width // 2

        def finish(at, start, step):
            value = (hidden_ref[at, :] + total_branch[at, :]).astype(bf16)
            turned = lax.axis_index("dp") == 0

            @pl.when(turned)
            def _():
                own_block[at, :] = value

            @pl.when(jnp.logical_not(turned))
            def _():
                own_block[at, :half] = value[:, half:]
                own_block[at, half:] = value[:, :half]

        summed.chunks(finish)
        block_group.begin()
        for item in range(3, count):
            for index in range(parts):
                back.reduce(item, index)
        summed.end()
        tokens_group.end()
        block_group.end()
        back.end()

    return comm_call(
        kernel,
        number,
        "last_exchange",
        out_shape,
        [IN_PLACE] * (len(out_shape) - 1) + [IN_VMEM],
        [IN_PLACE] * 6 + [IN_VMEM] * 4,
        [one for group in groups for one in group],
        300_000_000,
    )(down_grads, out_grads, qkv_grads, both, dup, act, branch, hidden, tokens_grad, small)


def widen(singles, pairs):
    steps = 8

    def spec(shape):
        if len(shape) == 3:
            return pl.BlockSpec((shape[0], shape[1] // steps, shape[2]), lambda i: (0, i, 0))
        return pl.BlockSpec((shape[0] // steps, shape[1]), lambda i: (i, 0))

    kinds = [jnp.bfloat16 if keep else jnp.float32 for _, keep in singles]
    arrays = [array for array, _ in singles] + [one for pair in pairs for one in pair]
    out_shape = [jax.ShapeDtypeStruct(array.shape, kind) for (array, _), kind in zip(singles, kinds)]
    out_shape += [jax.ShapeDtypeStruct((2,) + pair[0].shape, jnp.float32) for pair in pairs]
    count = len(singles)

    def kernel(*refs):
        sources, targets = refs[: len(arrays)], refs[len(arrays) :]
        for source, target in zip(sources[:count], targets[:count]):
            target[...] = source[...].astype(target.dtype)
        for index, target in enumerate(targets[count:]):
            for which in range(2):
                target[which] = sources[count + 2 * index + which][...].astype(jnp.float32)

    return pl.pallas_call(
        kernel,
        grid=(steps,),
        in_specs=[spec(array.shape) for array in arrays],
        out_specs=[spec(one.shape) for one in out_shape],
        out_shape=out_shape,
        name="widen",
    )(*arrays)


def split_body(
    tokens,
    positions,
    routes,
    out_grad,
    norm1_gain,
    qkv_weight,
    qkv_bias,
    out_weight,
    norm2_gain,
    router_weight,
    expert_gate,
    expert_up,
    expert_down,
    shared_gate,
    shared_w_gate,
    shared_w_up,
    shared_w_down,
):
    rows, width = tokens.shape[1], tokens.shape[2]
    parts = lax.axis_size("context")
    group_size = lax.axis_size("experts")
    place, group = lax.axis_index("context"), lax.axis_index("experts")
    local_experts = expert_gate.shape[0]
    expert_count = local_experts * group_size
    own_rows = rows // group_size
    length = rows * parts
    half = width // 2
    block = width // (2 * parts)
    hidden_here = shared_w_gate.shape[1] // parts
    stacks = local_experts + 1
    scale = HEAD_DIM ** (-0.5)
    bf16 = jnp.bfloat16

    first = group * own_rows

    def own_of(array):
        return lax.dynamic_slice_in_dim(array, first, own_rows, 0)

    grad_own_b = own_half_first(own_of(out_grad[0]))
    grad_own = grad_own_b.astype(jnp.float32)
    gain1 = own_half_first(norm1_gain).astype(jnp.float32)
    gain2 = own_half_first(norm2_gain).astype(jnp.float32)
    token_own = own_half_first(own_of(tokens[0])).astype(jnp.float32)
    inverse1 = lax.rsqrt(jnp.mean(token_own * token_own, -1, keepdims=True) + EPSILON)
    normed1 = token_own * inverse1
    half_dim = HEAD_DIM // 2
    frequency = ROPE_BASE ** (-2.0 * jnp.arange(half_dim, dtype=jnp.float32) / HEAD_DIM)
    angles = own_of(positions[0]).astype(jnp.float32)[:, None] * frequency[None, :]
    turns = jnp.concatenate([jnp.cos(angles), jnp.sin(angles)], 1)
    turns_high = turns.astype(bf16)
    turns_low = (turns - turns_high.astype(jnp.float32)).astype(bf16)
    send1 = jnp.concatenate([(normed1 * gain1).astype(bf16), turns_high, turns_low], 1)
    qkv_in = jnp.transpose(
        qkv_weight.reshape(block, 3, parts, HEAD_DIM), (2, 0, 1, 3)
    ).reshape(parts * block, 3 * HEAD_DIM)
    bias_here = lax.dynamic_slice_in_dim(
        qkv_bias.reshape(3, parts, HEAD_DIM), place, 1, 1
    ).reshape(1, 3 * HEAD_DIM)
    shared1, qkv_w, out_w, down_w, query, key, value, attended, lse, head_sum = attention_first(
        send1, qkv_in, out_weight, bias_here.astype(jnp.float32), shared_w_down, expert_down, 1
    )
    hidden = token_own + head_sum
    inverse2 = lax.rsqrt(jnp.mean(hidden * hidden, -1, keepdims=True) + EPSILON)
    normed2 = hidden * inverse2
    xn2_own = (normed2 * gain2).astype(bf16)
    router_here = own_half_first(router_weight.T).T
    gate_here = own_half_first(shared_gate)
    heads_w = jnp.concatenate([router_here, gate_here[:, None]], 1)
    logits = dot_nn(xn2_own, heads_w)
    prob = jax.nn.softmax(logits[:, :expert_count], -1)
    sig_own = jax.nn.sigmoid(logits[:, expert_count])
    named = jnp.sum(
        (
            own_of(routes[0])[:, :, None] == jnp.arange(expert_count, dtype=jnp.int32)[None, None, :]
        ).astype(jnp.float32),
        1,
    )
    gates = jnp.pad(
        jnp.concatenate([prob * named, sig_own[:, None]], 1), ((0, 0), (0, 63 - expert_count))
    )
    gates_high = gates.astype(bf16)
    gates_low = (gates - gates_high.astype(jnp.float32)).astype(bf16)
    send3 = jnp.concatenate([xn2_own, grad_own_b, gates_high, gates_low], 1)

    both, send4, branch_part, dup, act_c, up_g, down_g = share_move_compute(
        send3, shared_w_gate, shared_w_up, expert_gate, expert_up, down_w, 3
    )
    up_grads, down_grads = [None] * (2 * stacks), [None] * stacks
    side = 128 - expert_count - 1
    chances = jnp.pad(jnp.concatenate([prob, sig_own[:, None]], 1), ((0, 0), (0, side)))
    named_wide = jnp.pad(named, ((0, 0), (0, 128 - expert_count)))
    router_wide = jnp.pad(heads_w.T.astype(jnp.float32), ((0, side), (0, 0)))
    (
        _,
        up_grads[0],
        up_grads[1],
        down_grads[0],
        up_grads[2],
        up_grads[3],
        dots_own,
        dxn2,
        dhidden,
        out_g,
        qkv_g,
        bias_part,
        dxn1,
    ) = attention_last(
        send4,
        up_g,
        down_g,
        hidden,
        grad_own_b,
        gain2[None, :],
        chances,
        named_wide,
        router_wide,
        out_w,
        qkv_w,
        (query, key, value, attended),
        lse,
        shared1,
        4,
    )

    dprob = dots_own[:, :expert_count] * named
    dlogit = prob * (dprob - jnp.sum(prob * dprob, -1, keepdims=True))
    coef = sig_own * (1.0 - sig_own) * dots_own[:, expert_count]
    xn2_float = xn2_own.astype(jnp.float32)
    router_grad = jnp.dot(xn2_float.T, dlogit, precision=PRECISE)
    shared_gate_grad = jnp.dot(coef, xn2_float, precision=PRECISE)
    norm2_grad = jnp.sum(dxn2 * normed2, 0)
    norm1_grad = jnp.sum(dxn1 * normed1, 0)
    dscaled1 = dxn1 * gain1
    tokens_grad_own = dhidden + inverse1 * (
        dscaled1 - normed1 * jnp.mean(dscaled1 * normed1, -1, keepdims=True)
    )

    bias_wide = jnp.zeros((group_size, parts, 3 * HEAD_DIM), jnp.float32)
    bias_wide = lax.dynamic_update_slice(bias_wide, bias_part[None], (group, place, 0))
    small = jnp.concatenate(
        [
            own_half_first(norm1_grad),
            own_half_first(norm2_grad),
            own_half_first(shared_gate_grad),
            own_half_first(router_grad.T).T.reshape(-1),
            bias_wide.reshape(-1),
        ]
    )
    (
        out_w_grad,
        qkv_grad,
        down_grads[1],
        up_grads[4],
        up_grads[5],
        down_grads[2],
        _,
        _,
        block_out,
        tokens_grad,
        small,
    ) = last_exchange(
        down_g,
        out_g,
        qkv_g,
        both,
        dup,
        act_c,
        branch_part,
        hidden,
        own_half_first(tokens_grad_own),
        small.reshape(-1, 128),
        7,
    )
    small = small.reshape(-1)
    router_size = width * expert_count
    bias_sum = small[3 * width + router_size :].reshape(group_size, parts, 3, HEAD_DIM)
    bias_grad = jnp.transpose(
        lax.dynamic_slice_in_dim(bias_sum, group, 1, 0)[0], (1, 0, 2)
    ).reshape(3, parts * HEAD_DIM)

    qkv_grad = jnp.transpose(
        qkv_grad.reshape(parts, block, 3, HEAD_DIM), (1, 2, 0, 3)
    ).reshape(block, 3, parts * HEAD_DIM).astype(jnp.float32)
    singles = [(block_out, True), (tokens_grad, False), (out_w_grad, False)]
    singles += [(up_grads[0], False), (up_grads[1], False), (down_grads[0], False)]
    pairs = [up_grads[2::2], up_grads[3::2], down_grads[1:]]
    block_out, tokens_grad, out_w_grad, *shared_grads, gate_grads, up_grads, down_grads = widen(singles, pairs)

    return (
        block_out[None],
        tokens_grad[None],
        small[:width],
        qkv_grad,
        bias_grad,
        out_w_grad,
        small[width : 2 * width],
        small[3 * width : 3 * width + router_size].reshape(width, expert_count),
        gate_grads,
        up_grads,
        down_grads,
        small[2 * width : 3 * width],
        *shared_grads,
    )


def plan_of(mesh):
    sizes = mesh.shape
    return split_body if (sizes["dp"], sizes["context"], sizes["experts"]) == (2, 4, 4) else general_body


def solution(mesh):
    return jax.shard_map(
        plan_of(mesh),
        mesh=mesh,
        in_specs=(
            P("dp", "context", None),
            P("dp", "context"),
            P("dp", "context", None),
            P("dp", "context", None),
            P(),
            P(("dp", "context"), None, "experts"),
            P(None, "experts"),
            P("experts", ("dp", "context")),
            P(),
            P(),
            P("experts", ("dp", "context"), None),
            P("experts", ("dp", "context"), None),
            P("experts", None, ("dp", "context")),
            P(),
            P(("dp", "context"), "experts"),
            P(("dp", "context"), "experts"),
            P("experts", ("dp", "context")),
        ),
        out_specs=(
            P("dp", "context", None),
            P("dp", "context", None),
            P(),
            P(("dp", "context"), None, "experts"),
            P(None, "experts"),
            P("experts", ("dp", "context")),
            P(),
            P(),
            P("experts", ("dp", "context"), None),
            P("experts", ("dp", "context"), None),
            P("experts", None, ("dp", "context")),
            P(),
            P(("dp", "context"), "experts"),
            P(("dp", "context"), "experts"),
            P("experts", ("dp", "context")),
        ),
        check_vma=False,
    )
```

```python
import functools

import jax
import jax.numpy as jnp
from jax import lax
from jax.experimental import pallas as pl
from jax.experimental.pallas import tpu as pltpu
from jax.sharding import PartitionSpec as P

HEAD_DIM = 128


EPSILON = 1e-06
ROPE_BASE = 1000000.0
MASKED = -1e30
PRECISE = lax.Precision.HIGHEST


def rope_tables(position_ids):
    half_dim = HEAD_DIM // 2
    inverse = ROPE_BASE ** (-2.0 * jnp.arange(half_dim, dtype=jnp.float32) / HEAD_DIM)
    angles = position_ids.astype(jnp.float32)[:, None] * inverse[None, :]
    cosine = jnp.cos(angles)
    sine_part = jnp.sin(angles)
    return (
        jnp.concatenate([cosine, cosine], -1)[:, None, :],
        jnp.concatenate([sine_part, sine_part], -1)[:, None, :],
    )


def rotate(value):
    half_dim = value.shape[-1] // 2
    return jnp.concatenate([-value[..., half_dim:], value[..., :half_dim]], -1)


def rotate_back(value):
    half_dim = value.shape[-1] // 2
    return jnp.concatenate([value[..., half_dim:], -value[..., :half_dim]], -1)


def silu_grad(gate_vals):
    sigmoid_vals = jax.nn.sigmoid(gate_vals)
    return sigmoid_vals * (1.0 + gate_vals * (1.0 - sigmoid_vals))


def block_rank(route_rows, expert_count):
    hits = (
        route_rows[:, :, None] == jnp.arange(expert_count, dtype=jnp.int32)[None, None, :]
    ).astype(jnp.int32)
    flat_hits = hits.reshape(-1, expert_count)
    earlier = jnp.cumsum(flat_hits, axis=0) - flat_hits
    return jnp.sum(earlier * flat_hits, -1).reshape(route_rows.shape)


def block_width_of():
    return 512


def gather_weights(shard_set):
    return (
        lax.all_gather(shard_set[0], ("dp", "context"), axis=0, tiled=True),
        lax.all_gather(shard_set[1], ("dp", "context"), axis=1, tiled=True),
        lax.all_gather(shard_set[2], ("dp", "context"), axis=1, tiled=True),
        lax.all_gather(shard_set[3], ("dp", "context"), axis=1, tiled=True),
        lax.all_gather(shard_set[4], ("dp", "context"), axis=2, tiled=True),
        lax.all_gather(shard_set[5], ("dp", "context"), axis=0, tiled=True),
        lax.all_gather(shard_set[6], ("dp", "context"), axis=0, tiled=True),
        lax.all_gather(shard_set[7], ("dp", "context"), axis=1, tiled=True),
    )


def forward_fold(query, query_first, scale, carry, piece):
    row_count, head_count, head_size = query.shape
    query_index = query_first + jnp.arange(row_count, dtype=jnp.int32)
    query_last = query_first + row_count - 1
    key_part, value_part = piece
    piece_rows = key_part.shape[0]
    block_width = block_width_of()
    block_count = piece_rows // block_width
    key_blocks = key_part.reshape(block_count, block_width, head_count, head_size)
    value_blocks = value_part.reshape(block_count, block_width, head_count, head_size)
    offsets = block_width * jnp.arange(block_count, dtype=jnp.int32)

    def forward_visit(state, item):
        key_block, value_block, first_key = item

        def forward_compute(current):
            run_max, run_sum, accum = current
            scores = (
                jnp.einsum("qhd,khd->hqk", query, key_block, preferred_element_type=jnp.float32)
                * scale
            )
            key_index = first_key + jnp.arange(block_width, dtype=jnp.int32)
            allowed = key_index[None, None, :] <= query_index[None, :, None]
            new_max = jnp.maximum(run_max, jnp.max(jnp.where(allowed, scores, MASKED), -1))
            weights = jnp.where(allowed, jnp.exp(scores - new_max[..., None]), 0.0)
            factor = jnp.exp(run_max - new_max)
            new_sum = run_sum * factor + jnp.sum(weights, -1)
            new_accum = accum * factor[..., None] + jnp.einsum(
                "hqk,khd->hqd",
                weights.astype(jnp.bfloat16),
                value_block,
                preferred_element_type=jnp.float32,
            )
            return (new_max, new_sum, new_accum)

        return (
            lax.cond(first_key > query_last, lambda current: current, forward_compute, state),
            None,
        )

    carry, _ = lax.scan(forward_visit, carry, (key_blocks, value_blocks, offsets))
    return carry


def key_grad_fold(key_rows, value_rows, key_first, scale, carry, piece):
    row_count, head_count, head_size = key_rows.shape
    key_index = key_first + jnp.arange(row_count, dtype=jnp.int32)
    query_part, dout_part, lse_part, delta_part = piece
    piece_rows = query_part.shape[0]
    block_width = block_width_of()
    block_count = piece_rows // block_width
    query_blocks = query_part.reshape(block_count, block_width, head_count, head_size)
    dout_blocks = dout_part.reshape(block_count, block_width, head_count, head_size)
    lse_blocks = lse_part.reshape(block_count, block_width, head_count)
    delta_blocks = delta_part.reshape(block_count, block_width, head_count)
    offsets = block_width * jnp.arange(block_count, dtype=jnp.int32)

    def key_visit(state, item):
        query_block, dout_block, lse_block, delta_block, first_query = item

        def key_compute(current):
            dkey_sum, dvalue_sum = current
            query_b = query_block.astype(jnp.bfloat16)
            dout_b = dout_block.astype(jnp.bfloat16)
            scores = (
                jnp.einsum("qhd,khd->hqk", query_b, key_rows, preferred_element_type=jnp.float32)
                * scale
            )
            query_index = first_query + jnp.arange(block_width, dtype=jnp.int32)
            allowed = key_index[None, None, :] <= query_index[None, :, None]
            prob_att = jnp.where(
                allowed, jnp.exp(scores - jnp.transpose(lse_block)[:, :, None]), 0.0
            )
            dvalue_sum = dvalue_sum + jnp.einsum(
                "hqk,qhd->hkd",
                prob_att.astype(jnp.bfloat16),
                dout_b,
                preferred_element_type=jnp.float32,
            )
            dprob = jnp.einsum(
                "qhd,khd->hqk", dout_b, value_rows, preferred_element_type=jnp.float32
            )
            dscore = (prob_att * (dprob - jnp.transpose(delta_block)[:, :, None])).astype(
                jnp.bfloat16
            )
            dkey_sum = (
                dkey_sum
                + jnp.einsum("hqk,qhd->hkd", dscore, query_b, preferred_element_type=jnp.float32)
                * scale
            )
            return (dkey_sum, dvalue_sum)

        return (
            lax.cond(
                first_query + block_width - 1 < key_first,
                lambda current: current,
                key_compute,
                state,
            ),
            None,
        )

    carry, _ = lax.scan(
        key_visit, carry, (query_blocks, dout_blocks, lse_blocks, delta_blocks, offsets)
    )
    return carry


def query_grad_fold(query, dattended, lse_heads, delta_heads, query_first, scale, carry, piece):
    row_count, head_count, head_size = query.shape
    query_index = query_first + jnp.arange(row_count, dtype=jnp.int32)
    query_last = query_first + row_count - 1
    key_part, value_part = piece
    piece_rows = key_part.shape[0]
    block_width = block_width_of()
    block_count = piece_rows // block_width
    key_blocks = key_part.reshape(block_count, block_width, head_count, head_size)
    value_blocks = value_part.reshape(block_count, block_width, head_count, head_size)
    offsets = block_width * jnp.arange(block_count, dtype=jnp.int32)

    def query_visit(state, item):
        key_block, value_block, first_key = item

        def query_compute(current):
            scores = (
                jnp.einsum("qhd,khd->hqk", query, key_block, preferred_element_type=jnp.float32)
                * scale
            )
            key_index = first_key + jnp.arange(block_width, dtype=jnp.int32)
            allowed = key_index[None, None, :] <= query_index[None, :, None]
            prob_att = jnp.where(allowed, jnp.exp(scores - lse_heads[:, :, None]), 0.0)
            dprob = jnp.einsum(
                "qhd,khd->hqk", dattended, value_block, preferred_element_type=jnp.float32
            )
            dscore = (prob_att * (dprob - delta_heads[:, :, None])).astype(jnp.bfloat16)
            return (
                current
                + jnp.einsum("hqk,khd->hqd", dscore, key_block, preferred_element_type=jnp.float32)
                * scale
            )

        return (
            lax.cond(first_key > query_last, lambda current: current, query_compute, state),
            None,
        )

    carry, _ = lax.scan(query_visit, carry, (key_blocks, value_blocks, offsets))
    return carry


def general_body(
    tokens,
    positions,
    routes,
    out_grad,
    norm1_gain,
    qkv_weight,
    qkv_bias,
    out_weight,
    norm2_gain,
    router_weight,
    expert_gate,
    expert_up,
    expert_down,
    shared_gate,
    shared_w_gate,
    shared_w_up,
    shared_w_down,
):
    row_count = tokens.shape[1]
    model_width = tokens.shape[2]
    head_span = qkv_bias.shape[1]
    heads_here = head_span // HEAD_DIM
    local_experts = expert_gate.shape[0]
    group_size = lax.axis_size("experts")
    quarter = row_count // group_size
    capacity = 3 * quarter // 4
    expert_count = local_experts * group_size
    group_index = lax.axis_index("experts")
    scale = HEAD_DIM ** (-0.5)
    shard_set = (
        qkv_weight,
        out_weight,
        expert_gate,
        expert_up,
        expert_down,
        shared_w_gate,
        shared_w_up,
        shared_w_down,
    )
    qkv_full, out_full, gate_full, up_full, down_full, sgate_full, sup_full, sdown_full = (
        gather_weights(shard_set)
    )
    token_float = tokens[0].astype(jnp.float32)
    inverse1 = lax.rsqrt(jnp.mean(token_float * token_float, -1, keepdims=True) + EPSILON)
    normed1 = token_float * inverse1
    gain1 = norm1_gain.astype(jnp.float32)
    normed1_b = (normed1 * gain1).astype(jnp.bfloat16)
    qkv_flat = qkv_full.reshape(model_width, 3 * head_span)
    qkv = (
        jnp.dot(normed1_b, qkv_flat, preferred_element_type=jnp.float32).reshape(
            row_count, 3, head_span
        )
        + qkv_bias.astype(jnp.float32)[None]
    )
    cosine, sine_part = rope_tables(positions[0])
    query_raw = qkv[:, 0].reshape(row_count, heads_here, HEAD_DIM)
    key_raw = qkv[:, 1].reshape(row_count, heads_here, HEAD_DIM)
    query = (query_raw * cosine + rotate(query_raw) * sine_part).astype(jnp.bfloat16)
    key_rows = (key_raw * cosine + rotate(key_raw) * sine_part).astype(jnp.bfloat16)
    value_flat = qkv[:, 2].astype(jnp.bfloat16)
    key_flat = key_rows.reshape(row_count, head_span)
    value_rows = value_flat.reshape(row_count, heads_here, HEAD_DIM)
    query_first = lax.axis_index("context") * row_count
    start_state = (
        jnp.full((heads_here, row_count), MASKED, jnp.float32),
        jnp.zeros((heads_here, row_count), jnp.float32),
        jnp.zeros((heads_here, row_count, HEAD_DIM), jnp.float32),
    )
    run_max, run_sum, accum = forward_fold(
        query,
        query_first,
        scale,
        start_state,
        (
            lax.all_gather(key_flat, "context", axis=0, tiled=True),
            lax.all_gather(value_flat, "context", axis=0, tiled=True),
        ),
    )
    attended = jnp.transpose(accum / run_sum[..., None], (1, 0, 2)).astype(jnp.bfloat16)
    lse_heads = run_max + jnp.log(run_sum)
    attended_flat = attended.reshape(row_count, head_span)
    head_part = jnp.dot(attended_flat, out_full, preferred_element_type=jnp.float32)
    hidden = token_float + lax.psum(head_part, "experts")
    inverse2 = lax.rsqrt(jnp.mean(hidden * hidden, -1, keepdims=True) + EPSILON)
    normed2 = hidden * inverse2
    gain2 = norm2_gain.astype(jnp.float32)
    normed2_b = (normed2 * gain2).astype(jnp.bfloat16)
    first_row = group_index * quarter
    normed2_q = lax.dynamic_slice_in_dim(normed2_b, first_row, quarter, 0)
    route_q = lax.dynamic_slice_in_dim(routes[0], first_row, quarter, 0)
    logits = jnp.dot(normed2_q, router_weight, preferred_element_type=jnp.float32)
    prob = jax.nn.softmax(logits, -1)
    gate_k = jnp.take_along_axis(prob, route_q, 1)
    slot_ids = route_q * capacity + block_rank(route_q, expert_count)
    slot_hits = (
        slot_ids[:, :, None] == jnp.arange(expert_count * capacity, dtype=jnp.int32)[None, None, :]
    )
    placer = jnp.sum(slot_hits.astype(jnp.bfloat16), 1)
    send_rows = (
        jnp.dot(placer.T, normed2_q, preferred_element_type=jnp.float32)
        .astype(jnp.bfloat16)
        .reshape(group_size, local_experts, capacity, model_width)
    )
    arrived = lax.all_to_all(send_rows, "experts", split_axis=0, concat_axis=0, tiled=True)
    expert_gvals = jnp.einsum(
        "secd,edf->secf", arrived, gate_full, preferred_element_type=jnp.float32
    )
    expert_uvals = jnp.einsum(
        "secd,edf->secf", arrived, up_full, preferred_element_type=jnp.float32
    )
    expert_act = (jax.nn.silu(expert_gvals) * expert_uvals).astype(jnp.bfloat16)
    expert_out = jnp.einsum(
        "secf,efd->secd", expert_act, down_full, preferred_element_type=jnp.float32
    ).astype(jnp.bfloat16)
    returned = lax.all_to_all(
        expert_out, "experts", split_axis=0, concat_axis=0, tiled=True
    ).reshape(expert_count * capacity, model_width)
    picked = returned[slot_ids].astype(jnp.float32)
    routed = jnp.sum(gate_k[:, :, None] * picked, 1)
    shared_sig = jax.nn.sigmoid(
        jnp.dot(normed2_b, shared_gate[:, None], preferred_element_type=jnp.float32)[:, 0]
    )
    shared_gvals = jnp.dot(normed2_b, sgate_full, preferred_element_type=jnp.float32)
    shared_uvals = jnp.dot(normed2_b, sup_full, preferred_element_type=jnp.float32)
    shared_act = (jax.nn.silu(shared_gvals) * shared_uvals).astype(jnp.bfloat16)
    shared_part = jnp.dot(shared_act, sdown_full, preferred_element_type=jnp.float32)
    routed_pad = lax.dynamic_update_slice_in_dim(
        jnp.zeros((row_count, model_width), jnp.float32), routed, first_row, 0
    )
    branch_total = lax.psum(
        (shared_sig[:, None] * shared_part + routed_pad).astype(jnp.bfloat16), "experts"
    ).astype(jnp.float32)
    block_out = (hidden + branch_total).astype(jnp.bfloat16)
    held = lax.optimization_barrier((shard_set, block_out))
    qkv_full, out_full, gate_full, up_full, down_full, sgate_full, sup_full, sdown_full = (
        gather_weights(held[0])
    )
    qkv_flat = qkv_full.reshape(model_width, 3 * head_span)
    grad_float = out_grad[0].astype(jnp.float32)
    grad_q = lax.dynamic_slice_in_dim(grad_float, first_row, quarter, 0)
    dgate_k = jnp.sum(grad_q[:, None, :] * picked, -1)
    weighted = jnp.sum(slot_hits.astype(jnp.float32) * gate_k[:, :, None], 1)
    dsend = (
        jnp.dot(weighted.T, grad_q, precision=PRECISE)
        .astype(jnp.bfloat16)
        .reshape(group_size, local_experts, capacity, model_width)
    )
    darrived = lax.all_to_all(dsend, "experts", split_axis=0, concat_axis=0, tiled=True)
    expert_dact = jnp.einsum(
        "secd,efd->secf", darrived, down_full, preferred_element_type=jnp.float32
    )
    down_grad = jnp.einsum(
        "secf,secd->efd", expert_act, darrived, preferred_element_type=jnp.float32
    )
    expert_dgate = (expert_dact * expert_uvals * silu_grad(expert_gvals)).astype(jnp.bfloat16)
    expert_dup = (expert_dact * jax.nn.silu(expert_gvals)).astype(jnp.bfloat16)
    gate_grad = jnp.einsum(
        "secd,secf->edf", arrived, expert_dgate, preferred_element_type=jnp.float32
    )
    up_grad = jnp.einsum("secd,secf->edf", arrived, expert_dup, preferred_element_type=jnp.float32)
    expert_din = (
        jnp.einsum("secf,edf->secd", expert_dgate, gate_full, preferred_element_type=jnp.float32)
        + jnp.einsum("secf,edf->secd", expert_dup, up_full, preferred_element_type=jnp.float32)
    ).astype(jnp.bfloat16)
    dreturned = lax.all_to_all(
        expert_din, "experts", split_axis=0, concat_axis=0, tiled=True
    ).reshape(expert_count * capacity, model_width)
    dnormed2_q = jnp.dot(placer, dreturned, preferred_element_type=jnp.float32)
    route_hits = (
        route_q[:, :, None] == jnp.arange(expert_count, dtype=jnp.int32)[None, None, :]
    ).astype(jnp.float32)
    dprob = jnp.sum(route_hits * dgate_k[:, :, None], 1)
    dlogit = prob * (dprob - jnp.sum(prob * dprob, -1, keepdims=True))
    router_part = jnp.dot(normed2_q.astype(jnp.float32).T, dlogit, precision=PRECISE)
    dnormed2_q = dnormed2_q + jnp.dot(
        dlogit, router_weight.astype(jnp.float32).T, precision=PRECISE
    )
    shared_dout = (shared_sig[:, None] * grad_float).astype(jnp.bfloat16)
    shared_dact = jnp.dot(shared_dout, sdown_full.T, preferred_element_type=jnp.float32)
    sdown_grad = jnp.dot(shared_act.T, shared_dout, preferred_element_type=jnp.float32)
    shared_dgate = (shared_dact * shared_uvals * silu_grad(shared_gvals)).astype(jnp.bfloat16)
    shared_dup = (shared_dact * jax.nn.silu(shared_gvals)).astype(jnp.bfloat16)
    sgate_grad = jnp.dot(normed2_b.T, shared_dgate, preferred_element_type=jnp.float32)
    sup_grad = jnp.dot(normed2_b.T, shared_dup, preferred_element_type=jnp.float32)
    row_dots = jnp.sum(grad_float * shared_part, -1)
    dnormed2_part = jnp.dot(
        shared_dgate, sgate_full.T, preferred_element_type=jnp.float32
    ) + jnp.dot(shared_dup, sup_full.T, preferred_element_type=jnp.float32)
    dnormed2_part = dnormed2_part + lax.dynamic_update_slice_in_dim(
        jnp.zeros((row_count, model_width), jnp.float32), dnormed2_q, first_row, 0
    )
    dnormed2, row_dots, router_grad = lax.psum((dnormed2_part, row_dots, router_part), "experts")
    coef = shared_sig * (1.0 - shared_sig) * row_dots
    dnormed2 = dnormed2 + coef[:, None] * shared_gate.astype(jnp.float32)[None, :]
    shared_gate_grad = jnp.dot(coef, normed2_b.astype(jnp.float32), precision=PRECISE)
    norm2_grad = jnp.sum(dnormed2 * normed2, 0)
    dscaled2 = dnormed2 * gain2
    dhidden = grad_float + inverse2 * (
        dscaled2 - normed2 * jnp.mean(dscaled2 * normed2, -1, keepdims=True)
    )
    dhidden_b = dhidden.astype(jnp.bfloat16)
    out_grad_part = jnp.dot(attended_flat.T, dhidden_b, preferred_element_type=jnp.float32)
    dattended = jnp.dot(dhidden_b, out_full.T, preferred_element_type=jnp.float32).astype(
        jnp.bfloat16
    )
    dattended3 = dattended.reshape(row_count, heads_here, HEAD_DIM)
    delta = jnp.sum(dattended3.astype(jnp.float32) * attended.astype(jnp.float32), -1)
    zero_state = jnp.zeros((heads_here, row_count, HEAD_DIM), jnp.float32)
    dkey_sum, dvalue_sum = key_grad_fold(
        key_rows,
        value_rows,
        query_first,
        scale,
        (zero_state, zero_state),
        (
            lax.all_gather(
                query.reshape(row_count, head_span).astype(jnp.float32),
                "context",
                axis=0,
                tiled=True,
            ),
            lax.all_gather(dattended.astype(jnp.float32), "context", axis=0, tiled=True),
            lax.all_gather(jnp.transpose(lse_heads), "context", axis=0, tiled=True),
            lax.all_gather(delta, "context", axis=0, tiled=True),
        ),
    )
    dquery_sum = query_grad_fold(
        query,
        dattended3,
        lse_heads,
        jnp.transpose(delta),
        query_first,
        scale,
        zero_state,
        (
            lax.all_gather(key_flat, "context", axis=0, tiled=True),
            lax.all_gather(value_flat, "context", axis=0, tiled=True),
        ),
    )
    dquery = jnp.transpose(dquery_sum, (1, 0, 2))
    dkey = jnp.transpose(dkey_sum, (1, 0, 2))
    dvalue = jnp.transpose(dvalue_sum, (1, 0, 2))
    dquery_raw = dquery * cosine + rotate_back(dquery * sine_part)
    dkey_raw = dkey * cosine + rotate_back(dkey * sine_part)
    dqkv = jnp.stack(
        [
            dquery_raw.reshape(row_count, head_span),
            dkey_raw.reshape(row_count, head_span),
            dvalue.reshape(row_count, head_span),
        ],
        1,
    )
    bias_grad = jnp.sum(dqkv, 0)
    dqkv_b = dqkv.astype(jnp.bfloat16).reshape(row_count, 3 * head_span)
    qkv_grad = jnp.dot(normed1_b.T, dqkv_b, preferred_element_type=jnp.float32).reshape(
        model_width, 3, head_span
    )
    dnormed1 = lax.psum(
        jnp.dot(dqkv_b, qkv_flat.T, preferred_element_type=jnp.float32).astype(jnp.bfloat16),
        "experts",
    ).astype(jnp.float32)
    norm1_grad = jnp.sum(dnormed1 * normed1, 0)
    dscaled1 = dnormed1 * gain1
    tokens_grad = dhidden + inverse1 * (
        dscaled1 - normed1 * jnp.mean(dscaled1 * normed1, -1, keepdims=True)
    )
    small_sums = (
        lax.psum(norm1_grad.astype(jnp.bfloat16), ("dp", "context")).astype(jnp.float32),
        lax.psum(norm2_grad.astype(jnp.bfloat16), ("dp", "context")).astype(jnp.float32),
        lax.psum(router_grad.astype(jnp.bfloat16), ("dp", "context")).astype(jnp.float32),
        lax.psum(shared_gate_grad.astype(jnp.bfloat16), ("dp", "context")).astype(jnp.float32),
        lax.psum(bias_grad.astype(jnp.bfloat16), ("dp", "context")).astype(jnp.float32),
    )
    large_sums = (
        lax.psum_scatter(
            qkv_grad.astype(jnp.bfloat16), ("dp", "context"), scatter_dimension=0, tiled=True
        ).astype(jnp.float32),
        lax.psum_scatter(
            out_grad_part.astype(jnp.bfloat16), ("dp", "context"), scatter_dimension=1, tiled=True
        ).astype(jnp.float32),
        lax.psum_scatter(
            gate_grad.astype(jnp.bfloat16), ("dp", "context"), scatter_dimension=1, tiled=True
        ).astype(jnp.float32),
        lax.psum_scatter(
            up_grad.astype(jnp.bfloat16), ("dp", "context"), scatter_dimension=1, tiled=True
        ).astype(jnp.float32),
        lax.psum_scatter(
            down_grad.astype(jnp.bfloat16), ("dp", "context"), scatter_dimension=2, tiled=True
        ).astype(jnp.float32),
        lax.psum_scatter(
            sgate_grad.astype(jnp.bfloat16), ("dp", "context"), scatter_dimension=0, tiled=True
        ).astype(jnp.float32),
        lax.psum_scatter(
            sup_grad.astype(jnp.bfloat16), ("dp", "context"), scatter_dimension=0, tiled=True
        ).astype(jnp.float32),
        lax.psum_scatter(
            sdown_grad.astype(jnp.bfloat16), ("dp", "context"), scatter_dimension=1, tiled=True
        ).astype(jnp.float32),
    )
    return (
        block_out[None],
        tokens_grad[None],
        small_sums[0],
        large_sums[0],
        small_sums[4],
        large_sums[1],
        small_sums[1],
        small_sums[2],
        large_sums[2],
        large_sums[3],
        large_sums[4],
        small_sums[3],
        large_sums[5],
        large_sums[6],
        large_sums[7],
    )


def own_half_first(value):
    half = value.shape[-1] // 2
    turned = jnp.concatenate([value[..., half:], value[..., :half]], -1)
    return jnp.where(lax.axis_index("dp") == 0, value, turned)


def dot_nn(left, right):
    return jnp.dot(left, right, preferred_element_type=jnp.float32)


def dot_nt(left, right):
    return lax.dot_general(
        left, right, (((1,), (1,)), ((), ())), preferred_element_type=jnp.float32
    )


def dot_tn(left, right):
    return lax.dot_general(
        left, right, (((0,), (0,)), ((), ())), preferred_element_type=jnp.float32
    )


MESH = pl.DeviceIdType.MESH
DMA = pltpu.SemaphoreType.DMA


def remote(source, target, send_sem, recv_sem, device):
    return pltpu.make_async_remote_copy(
        src_ref=source,
        dst_ref=target,
        send_sem=send_sem,
        recv_sem=recv_sem,
        device_id=device,
        device_id_type=MESH,
    )


def rows_at(ref, start, size):
    return ref.at[pl.ds(pl.multiple_of(start, 16), size), :]


def lanes_at(ref, start, size):
    return ref.at[:, pl.ds(pl.multiple_of(start, 128), size)]


def by_width(device, narrow, body):
    if narrow is None:
        body(False)
    elif isinstance(device, int):
        body(device == narrow)
    else:

        @pl.when(device == narrow)
        def _():
            body(True)

        @pl.when(device != narrow)
        def _():
            body(False)


class Spot:
    def __init__(self):
        self.parts = lax.axis_size("context")
        self.place, self.group = lax.axis_index("context"), lax.axis_index("experts")
        self.twin = {"dp": 1 - lax.axis_index("dp")}
        self.across = lax.rem(self.group + 2, 4)
        self.beside = self.group + 1 - 2 * lax.rem(self.group, 2)
        self.corner = lax.rem(self.beside + 2, 4)
        self.has_left, self.has_right = self.place > 0, self.place < self.parts - 1

    def greet(self, whole_line, twins):
        barrier = pltpu.get_barrier_semaphore()
        devices = [{"experts": self.across}, {"experts": self.beside}]
        if twins:
            devices.append(self.twin)
        for device in devices:
            pl.semaphore_signal(barrier, inc=1, device_id=device, device_id_type=MESH)
        count = len(devices)
        if whole_line:
            for gap in range(1, self.parts):
                device = {"context": lax.rem(self.place + gap, self.parts)}
                pl.semaphore_signal(barrier, inc=1, device_id=device, device_id_type=MESH)
            pl.semaphore_wait(barrier, count + self.parts - 1)
        else:
            for step, there in ((-1, self.has_left), (1, self.has_right)):

                @pl.when(there)
                def _():
                    device = {"context": self.place + step}
                    pl.semaphore_signal(barrier, inc=1, device_id=device, device_id_type=MESH)

            ends = jnp.where(self.has_left & self.has_right, 0, 1)
            pl.semaphore_wait(barrier, count + 2 - ends)

    def far_first(self):
        upper = self.place // (self.parts // 2)
        return [3 * (1 - upper), 2 - upper, 1 + 4 * upper - self.place, self.place]

    def others(self, gap, body):
        @pl.when(self.place >= gap)
        def _():
            body(self.place - gap)

        @pl.when(self.place + gap < self.parts)
        def _():
            body(self.place + gap)


class Share:
    def __init__(self, spot, own, out, sems):
        self.spot, self.own, self.out = spot, own, out
        self.local_sem, self.right_s, self.left_s, self.line_r, self.across_s, self.across_r, self.beside_s, self.beside_r = sems

    @staticmethod
    def sems(parts):
        return [DMA, DMA((parts,)), DMA((parts,)), DMA((parts,)), DMA((parts,)), DMA((parts,)), DMA((2 * parts,)), DMA((2 * parts,))]

    def block(self, part, column):
        rows = self.own.shape[0]
        return rows_at(self.out, (part * 4 + column) * rows, rows)

    def to_right(self, part, source):
        s = self.spot
        return remote(source, self.block(part, s.group), self.right_s.at[part], self.line_r.at[part], {"context": s.place + 1})

    def to_left(self, part, source):
        s = self.spot
        return remote(source, self.block(part, s.group), self.left_s.at[part], self.line_r.at[part], {"context": s.place - 1})

    def to_across(self, part, source):
        s = self.spot
        return remote(source, self.block(part, s.group), self.across_s.at[part], self.across_r.at[part], {"experts": s.across})

    def to_beside(self, part, column, slot, source):
        s = self.spot
        return remote(source, self.block(part, column), self.beside_s.at[slot], self.beside_r.at[slot], {"experts": s.beside})

    def begin(self):
        s = self.spot

        @pl.when(s.has_right)
        def _():
            self.to_right(s.place, self.own).start()

        @pl.when(s.has_left)
        def _():
            self.to_left(s.place, self.own).start()

        self.to_across(s.place, self.own).start()
        self.to_beside(s.place, s.group, s.place, self.own).start()
        self.local().start()

    def local(self):
        return pltpu.make_async_copy(self.own, self.block(self.spot.place, self.spot.group), self.local_sem)

    def pass_on(self, part):
        s = self.spot
        self.to_across(part, self.block(part, s.group)).wait_recv()
        self.to_beside(part, s.across, s.parts + part, self.block(part, s.across)).start()

    def arrival(self, part, onward, there):
        s = self.spot
        mine = self.block(part, s.group)
        self.to_right(part, mine).wait_recv()

        @pl.when(there)
        def _():
            onward(part, mine).start()

        self.to_across(part, mine).start()
        self.to_beside(part, s.group, part, mine).start()

    def step(self, gap):
        s = self.spot

        @pl.when(s.place >= gap)
        def _():
            self.arrival(s.place - gap, self.to_right, s.has_right)

        @pl.when(s.place + gap < s.parts)
        def _():
            self.arrival(s.place + gap, self.to_left, s.has_left)

        if gap == 1:
            self.pass_on(s.place)
        else:
            s.others(gap - 1, self.pass_on)

    def end(self):
        s = self.spot
        s.others(s.parts - 1, self.pass_on)
        self.local().wait()
        for part in range(s.parts):
            self.to_beside(part, s.beside, part, self.own).wait_recv()
            self.to_beside(part, s.beside, s.parts + part, self.own).wait_recv()
            self.to_across(part, self.own).wait_send()
            self.to_beside(part, s.group, part, self.own).wait_send()
            self.to_beside(part, s.group, s.parts + part, self.own).wait_send()

            @pl.when(s.has_right & (part <= s.place))
            def _():
                self.to_right(part, self.own).wait_send()

            @pl.when(s.has_left & (part >= s.place))
            def _():
                self.to_left(part, self.own).wait_send()


class Sum:
    def __init__(self, spot, part_ref, out, scratch):
        self.spot, self.part_ref, self.out = spot, part_ref, out
        (self.beside_buf, self.across_out, self.across_buf, self.line_out, self.left_buf, self.right_buf,
         self.beside_s, self.beside_r, self.across_s, self.across_r, self.right_s, self.left_s, self.from_left, self.from_right) = scratch
        self.order = spot.far_first()

    @staticmethod
    def scratch(parts, rows, width):
        one = pltpu.VMEM((parts, rows, width), jnp.bfloat16)
        two = pltpu.VMEM((2 * parts, rows, width), jnp.bfloat16)
        return [two, one, one, one, one, one, DMA((2 * parts,)), DMA((2 * parts,))] + [DMA((parts,))] * 6

    def base(self, part, column):
        rows = self.out.shape[0]
        return pl.multiple_of((part * 4 + column) * rows, rows)

    def to_beside(self, part, column, slot):
        source = self.part_ref.at[pl.ds(self.base(part, column), self.out.shape[0]), :]
        return remote(source, self.beside_buf.at[slot], self.beside_s.at[slot], self.beside_r.at[slot], {"experts": self.spot.beside})

    def to_across(self, part):
        return remote(self.across_out.at[part], self.across_buf.at[part], self.across_s.at[part], self.across_r.at[part], {"experts": self.spot.across})

    def to_right(self, part):
        return remote(self.line_out.at[part], self.left_buf.at[part], self.right_s.at[part], self.from_left.at[part], {"context": self.spot.place + 1})

    def to_left(self, part):
        return remote(self.line_out.at[part], self.right_buf.at[part], self.left_s.at[part], self.from_right.at[part], {"context": self.spot.place - 1})

    def chunks(self, body):
        step = 16

        def one(index, carry):
            start = pl.multiple_of(index * step, step)
            body(pl.ds(start, step), start, step)
            return carry

        lax.fori_loop(0, self.out.shape[0] // step, one, 0)

    def mine(self, base, start, step):
        return self.part_ref[pl.ds(pl.multiple_of(base + start, step), step), :].astype(jnp.float32)

    def begin(self):
        s = self.spot
        for part in self.order:
            self.to_beside(part, s.corner, s.parts + part).start()
        for part in self.order:
            self.to_beside(part, s.beside, part).start()

    def cross(self, index):
        s, part = self.spot, self.order[index]
        self.to_beside(part, s.corner, s.parts + part).wait_recv()
        base = self.base(part, s.across)

        def add(at, start, step):
            total = self.mine(base, start, step) + self.beside_buf[s.parts + part, at, :].astype(jnp.float32)
            self.across_out[part, at, :] = total.astype(jnp.bfloat16)

        self.chunks(add)
        self.to_across(part).start()

    def line(self, index):
        s, part = self.spot, self.order[index]
        self.to_beside(part, s.beside, part).wait_recv()
        self.to_across(part).wait_recv()
        base = self.base(part, s.group)
        f32 = jnp.float32

        def total(at, start, step):
            return self.mine(base, start, step) + self.beside_buf[part, at, :].astype(f32) + self.across_buf[part, at, :].astype(f32)

        def send(buf):
            def add(at, start, step):
                value = total(at, start, step)
                if buf is not None:
                    value = value + buf[part, at, :].astype(f32)
                self.line_out[part, at, :] = value.astype(jnp.bfloat16)

            self.chunks(add)

        if index < s.parts - 1:
            goes_right = part > s.place
            goes_left = jnp.logical_not(goes_right)

            @pl.when(goes_right & s.has_left)
            def _():
                self.to_right(part).wait_recv()
                send(self.left_buf)

            @pl.when(goes_left & s.has_right)
            def _():
                self.to_left(part).wait_recv()
                send(self.right_buf)

            @pl.when((goes_right & jnp.logical_not(s.has_left)) | (goes_left & jnp.logical_not(s.has_right)))
            def _():
                send(None)

            @pl.when(goes_right)
            def _():
                self.to_right(part).start()

            @pl.when(goes_left)
            def _():
                self.to_left(part).start()
        else:

            def keep(at, start, step):
                self.out[at, :] = total(at, start, step)

            self.chunks(keep)
            for there, copy, buf in ((s.has_left, self.to_right, self.left_buf), (s.has_right, self.to_left, self.right_buf)):

                @pl.when(there)
                def _():
                    copy(part).wait_recv()

                    def add(at, start, step):
                        self.out[at, :] = self.out[at, :] + buf[part, at, :].astype(f32)

                    self.chunks(add)

    def end(self):
        s = self.spot
        for part in range(s.parts):
            self.to_beside(part, s.corner, s.parts + part).wait_send()
            self.to_beside(part, s.beside, part).wait_send()
            self.to_across(part).wait_send()

            @pl.when(part > s.place)
            def _():
                self.to_right(part).wait_send()

            @pl.when(part < s.place)
            def _():
                self.to_left(part).wait_send()


class Move:
    def __init__(self, spot, items, sems):
        self.spot, self.items = spot, items
        self.line_s, self.line_r, self.twin_s, self.twin_r, self.local_sem = sems

    @staticmethod
    def sems(count, parts):
        return [DMA((count * parts,))] * 4 + [DMA((count,))]

    def fit(self, number, device, body):
        by_width(device, self.items[number]["short"], body)

    def to(self, number, target, source, short):
        s, item = self.spot, self.items[number]
        sems = self.line_s.at[number * s.parts + target], self.line_r.at[number * s.parts + source]
        return remote(item["src"](target, short), item["dst"](0, source, short), *sems, {"context": target})

    def on(self, number, source, short, view=None):
        s, item = self.spot, self.items[number]
        slot = number * s.parts + source
        view = item["dst"](0, source, short) if view is None else view
        return remote(view, item["dst"](1, source, short), self.twin_s.at[slot], self.twin_r.at[slot], s.twin)

    def local(self, number, short):
        s, item = self.spot, self.items[number]
        return pltpu.make_async_copy(item["src"](s.place, short), item["dst"](0, s.place, short), self.local_sem.at[number])

    def own(self, number):
        s, item = self.spot, self.items[number]

        def one(short):
            self.on(number, s.place, short, item["src"](s.place, short)).start()
            self.local(number, short).start()

        self.fit(number, s.place, one)

    def send_gap(self, number, gap):
        s = self.spot

        def one(target):
            self.fit(number, target, lambda short: self.to(number, target, s.place, short).start())

        s.others(gap, one)

    def send(self, number):
        for gap in range(self.spot.parts - 1, 0, -1):
            self.send_gap(number, gap)

    def forward(self, number, gap):
        s = self.spot

        def one(source):
            def step(short):
                self.to(number, s.place, source, short).wait_recv()
                self.on(number, source, short).start()

            self.fit(number, s.place, step)

        s.others(gap, one)

    def ready(self, number):
        s = self.spot

        def one(short):
            self.local(number, short).wait()
            for part in range(s.parts):
                self.on(number, part, short).wait_recv()

        self.fit(number, s.place, one)

    def sent(self):
        s = self.spot
        for number in range(len(self.items)):

            def one(short):
                for part in range(s.parts):
                    self.on(number, part, short).wait_send()

            self.fit(number, s.place, one)
            for part in range(s.parts):

                @pl.when(part != s.place)
                def _():
                    self.fit(number, part, lambda short: self.to(number, part, s.place, short).wait_send())

    def end(self):
        for number in range(len(self.items)):
            self.ready(number)
        self.sent()


class Return:
    def __init__(self, spot, items, got, mine, sems):
        self.spot, self.items, self.got, self.mine_buf = spot, items, got, mine
        self.twin_s, self.twin_r, self.load, self.line_s, self.line_r, self.local_sem = sems
        self.order = spot.far_first()
        self.bases = []
        for item in items:
            self.bases.append(self.bases[-1][1] if self.bases else 0)
            self.bases[-1] = (self.bases[-1], self.bases[-1] + len(item["pieces"]) * spot.parts)

    @staticmethod
    def scratch(shapes, pieces, parts):
        count = len(shapes)
        buf = [pltpu.VMEM((parts,) + shape, jnp.bfloat16) for shape in shapes]
        sems = [DMA((count * parts,))] * 3 + [DMA((sum(pieces) * parts,))] * 2 + [DMA((sum(pieces),))]
        return buf + buf + sems

    def swap(self, number, part):
        item, slot = self.items[number], number * self.spot.parts + part
        return remote(item["block"](1, part), self.got[number].at[part], self.twin_s.at[slot], self.twin_r.at[slot], self.spot.twin)

    def fetch(self, number, part):
        item, slot = self.items[number], number * self.spot.parts + part
        return pltpu.make_async_copy(item["block"](0, part), self.mine_buf[number].at[part], self.load.at[slot])

    def start_one(self, number, index):
        self.swap(number, self.order[index]).start()
        self.fetch(number, self.order[index]).start()

    def start(self, number):
        for index in range(self.spot.parts):
            self.start_one(number, index)

    def piece(self, number, which, target, source, short):
        s = self.spot
        cut, out = self.items[number]["pieces"][which]
        slot = self.bases[number][0] + which * s.parts
        return remote(cut(self.mine_buf[number].at[target], short), out(source, short), self.line_s.at[slot + target], self.line_r.at[slot + source], {"context": target})

    def keep(self, number, which, short):
        s = self.spot
        cut, out = self.items[number]["pieces"][which]
        slot = self.bases[number][0] // s.parts + which
        return pltpu.make_async_copy(cut(self.mine_buf[number].at[s.place], short), out(s.place, short), self.local_sem.at[slot])

    def fit(self, number, source, body):
        by_width(source, self.items[number].get("short"), body)

    def reduce(self, number, index):
        s, part = self.spot, self.order[index]
        item = self.items[number]
        self.swap(number, part).wait_recv()
        self.fetch(number, part).wait()
        mine, got = self.mine_buf[number], self.got[number]
        rows, step = mine.shape[1], 32

        def one(at, carry):
            span = pl.ds(pl.multiple_of(at * step, step), step)
            total = mine[part, span, :].astype(jnp.float32) + got[part, span, :].astype(jnp.float32)
            mine[part, span, :] = total.astype(jnp.bfloat16)
            return carry

        lax.fori_loop(0, rows // step, one, 0)
        for which in range(len(item["pieces"])):
            if index < s.parts - 1:
                self.fit(number, s.place, lambda short: self.piece(number, which, part, s.place, short).start())
            else:
                self.fit(number, s.place, lambda short: self.keep(number, which, short).start())

    def end(self):
        s = self.spot
        for number, item in enumerate(self.items):
            for part in range(s.parts):
                self.swap(number, part).wait_send()
                for which in range(len(item["pieces"])):

                    @pl.when(part != s.place)
                    def _():
                        self.fit(number, s.place, lambda short: self.piece(number, which, part, s.place, short).wait_send())
                        self.fit(number, part, lambda short: self.piece(number, which, s.place, part, short).wait_recv())

            for which in range(len(item["pieces"])):
                self.fit(number, s.place, lambda short: self.keep(number, which, short).wait())


class Grads:
    def __init__(self, rows, cotangents, dup, act, up_out, down_out, up_buf, down_buf, up_s, down_s):
        self.rows, self.cotangents, self.dup, self.act = rows, cotangents, dup, act
        self.up_out, self.down_out, self.up_buf, self.down_buf = up_out, down_out, up_buf, down_buf
        self.up_s, self.down_s = up_s, down_s
        self.step = 256

    @staticmethod
    def scratch():
        up, down = pltpu.VMEM((2, 256, 2 * WINDOW), jnp.bfloat16), pltpu.VMEM((2, WINDOW, 256), jnp.bfloat16)
        return [up, down, DMA((2,)), DMA((2,))]

    def copies(self, index):
        at = pl.ds(pl.multiple_of(index * self.step, self.step), self.step)
        slot = lax.rem(index, 2)
        return (
            lambda: pltpu.make_async_copy(self.up_buf.at[slot], self.up_out.at[at, :], self.up_s.at[slot]),
            lambda: pltpu.make_async_copy(self.down_buf.at[slot], self.down_out.at[:, at], self.down_s.at[slot]),
        )

    def run(self):
        count = self.cotangents.shape[1] // self.step

        def one(index, carry):
            up_copy, down_copy = self.copies(index)

            @pl.when(index >= 2)
            def _():
                up_copy().wait()
                down_copy().wait()

            slot = lax.rem(index, 2)
            at = pl.multiple_of(index * self.step, self.step)
            up = dot_tn(self.rows[:, pl.ds(at, self.step)], self.dup[...])
            self.up_buf[slot] = up.astype(jnp.bfloat16)
            down = dot_tn(self.act[...], self.cotangents[:, pl.ds(at, self.step)])
            self.down_buf[slot] = down.astype(jnp.bfloat16)
            up_copy().start()
            down_copy().start()
            return carry

        lax.fori_loop(0, count, one, 0)
        for index in (count - 2, count - 1):
            for copy in self.copies(index):
                copy().wait()


def comm_call(kernel, number, name, out_shape, out_specs, in_specs, scratch, bytes_moved):
    return pl.pallas_call(
        kernel,
        out_shape=out_shape,
        in_specs=in_specs,
        out_specs=out_specs,
        scratch_shapes=scratch,
        compiler_params=pltpu.CompilerParams(collective_id=number, has_side_effects=True),
        cost_estimate=pl.CostEstimate(flops=0, bytes_accessed=bytes_moved, transcendentals=0),
        name=name,
    )


IN_VMEM = pl.BlockSpec(memory_space=pltpu.VMEM)
IN_PLACE = pl.BlockSpec(memory_space=pl.ANY)
WINDOW = 384


SPARE = 128


def narrow_of(k):
    return 0 if k % 2 else 3


def window_of(k, index, narrow):
    if narrow_of(k) == 0:
        return (0, WINDOW - SPARE, 0) if narrow else (index * WINDOW - SPARE, WINDOW, 0)
    return (index * WINDOW, WINDOW - SPARE, SPARE) if narrow else (index * WINDOW, WINDOW, 0)


def first_unit(value):
    return value if isinstance(value, int) else pl.multiple_of(value, SPARE)


def units_at(ref, k, index, narrow, axis, base=0):
    start, size, inside = window_of(k, index, narrow)
    start = first_unit(start) if base is None else base + inside
    return ref.at[pl.ds(start, size), :] if axis == 0 else ref.at[:, pl.ds(start, size)]


def turn(value, cosine, sine_part):
    return value * cosine + pltpu.roll(value, HEAD_DIM // 2, 1) * sine_part


def turn_tables(facts):
    both = facts[:, :HEAD_DIM].astype(jnp.float32) + facts[:, HEAD_DIM:].astype(jnp.float32)
    swapped = pltpu.roll(both, HEAD_DIM // 2, 1)
    low = lax.broadcasted_iota(jnp.int32, (1, HEAD_DIM), 1) < HEAD_DIM // 2
    return jnp.where(low, both, swapped), jnp.where(low, -swapped, both)


def attention_first(value, grad, qkv_in, out_weight, bias, shared_down, expert_down, number):
    parts = lax.axis_size("context")
    rows, wide = value.shape
    block, span = qkv_in.shape[0] // parts, qkv_in.shape[1]
    head, lanes = out_weight.shape[0] // parts, out_weight.shape[1]
    width, length = 2 * parts * lanes, rows * parts * 4
    count = 1 + expert_down.shape[0]
    step = 256
    scale = HEAD_DIM ** (-0.5)
    f32, bf16 = jnp.float32, jnp.bfloat16
    sets = [
        [
            pltpu.VMEM((length, wide), bf16),
            pltpu.VMEM((2 * parts * block, span), bf16),
            pltpu.VMEM((head, width), bf16),
            pltpu.VMEM((length, width), bf16),
            DMA((3,)),
        ],
        Share.sems(parts),
        Move.sems(2 + count, parts),
        Sum.scratch(parts, rows, width),
        Share.sems(parts),
    ]

    def kernel(own_ref, grad_ref, qkv_ref, outw_ref, bias_ref, shared_ref, expert_ref,
               all_hbm, grad_all, wqkv_hbm, wout_hbm, wd_ref, q_ref, k_ref, v_ref, att_ref, lse_ref, sum_ref, *scratch):
        scratch, split = list(scratch), []
        for one in sets:
            split.append(scratch[: len(one)])
            scratch = scratch[len(one) :]
        all_ref, wqkv_ref, wout_ref, part_ref, keep = split[0]
        spot = Spot()
        share = Share(spot, own_ref, all_ref, split[1])
        grads = Share(spot, grad_ref, grad_all, split[4])
        items = [
            {
                "src": lambda target, short: rows_at(qkv_ref, target * block, block),
                "dst": lambda side, source, short: rows_at(wqkv_ref, (side * parts + source) * block, block),
                "short": None,
            },
            {
                "src": lambda target, short: rows_at(outw_ref, target * head, head),
                "dst": lambda side, source, short: lanes_at(wout_ref, (side * parts + source) * lanes, lanes),
                "short": None,
            },
        ]

        def down(k):
            ref = shared_ref if k == 0 else expert_ref.at[k - 1]
            return {
                "src": lambda target, short: units_at(ref, k, target, short, 0, None),
                "dst": lambda side, source, short: lanes_at(
                    units_at(wd_ref, k, 0, short, 0, k * WINDOW), (side * parts + source) * lanes, lanes
                ),
                "short": narrow_of(k),
            }

        move = Move(spot, items + [down(k) for k in range(count)], split[2])
        summed = Sum(spot, part_ref, sum_ref, split[3])
        copies = [
            pltpu.make_async_copy(source, target, keep.at[index])
            for index, (source, target) in enumerate(((all_ref, all_hbm), (wqkv_ref, wqkv_hbm), (wout_ref, wout_hbm)))
        ]

        def project(index, carry):
            at = pl.ds(pl.multiple_of(index * step, step), step)
            qkv = jnp.dot(all_ref[at, :width], wqkv_ref[...], preferred_element_type=f32) + bias_ref[...]
            cosine, sine_part = turn_tables(all_ref[at, width:])
            q_ref[at, :] = turn(qkv[:, :HEAD_DIM], cosine, sine_part).astype(bf16)
            k_ref[at, :] = turn(qkv[:, HEAD_DIM : 2 * HEAD_DIM], cosine, sine_part).astype(bf16)
            v_ref[at, :] = qkv[:, 2 * HEAD_DIM :].astype(bf16)
            return carry

        def attend(index, carry):
            start = pl.multiple_of(index * step, step)
            at = pl.ds(start, step)
            scores = dot_nt(q_ref[at, :], k_ref[...]) * scale
            query_index = start + lax.broadcasted_iota(jnp.int32, scores.shape, 0)
            allowed = lax.broadcasted_iota(jnp.int32, scores.shape, 1) <= query_index
            row_max = jnp.max(jnp.where(allowed, scores, MASKED), -1, keepdims=True)
            weights = jnp.where(allowed, jnp.exp(scores - row_max), 0.0)
            row_sum = jnp.sum(weights, -1, keepdims=True)
            attended = (jnp.dot(weights.astype(bf16), v_ref[...], preferred_element_type=f32) / row_sum).astype(bf16)
            att_ref[at, :] = attended
            lse_ref[at, :] = jnp.broadcast_to(row_max + jnp.log(row_sum), (step, HEAD_DIM))
            part_ref[at, :] = jnp.dot(attended, wout_ref[...], preferred_element_type=f32).astype(bf16)
            return carry

        spot.greet(True, True)
        share.begin()
        for number in range(len(move.items)):
            move.own(number)
        move.send_gap(0, 3)
        share.step(1)
        move.send_gap(0, 2)
        share.step(2)
        move.send_gap(0, 1)
        share.step(3)
        move.send(1)
        move.send(2)
        for gap in (1, 2, 3):
            move.forward(0, gap)
        for gap in (1, 2, 3):
            move.forward(1, gap)
        share.end()
        grads.begin()
        copies[0].start()
        move.ready(0)
        copies[1].start()
        lax.fori_loop(0, length // step, project, 0)
        move.ready(1)
        copies[2].start()
        grads.step(1)
        for number in range(3, len(move.items)):
            move.send(number)
        lax.fori_loop(0, length // step, attend, 0)
        summed.begin()
        for gap in (1, 2, 3):
            move.forward(2, gap)
        grads.step(2)
        for index in range(parts):
            summed.cross(index)
        for number in range(3, len(move.items)):
            for gap in (1, 2, 3):
                move.forward(number, gap)
        grads.step(3)
        for index in range(parts):
            summed.line(index)
        grads.end()
        summed.end()
        for number in range(2, len(move.items)):
            move.ready(number)
        move.sent()
        for copy in copies:
            copy.wait()

    heads = jax.ShapeDtypeStruct((length, HEAD_DIM), bf16)
    return comm_call(
        kernel,
        number,
        "attention_first",
        [
            jax.ShapeDtypeStruct((length, wide), bf16),
            jax.ShapeDtypeStruct((length, width), bf16),
            jax.ShapeDtypeStruct((2 * parts * block, span), bf16),
            jax.ShapeDtypeStruct((head, width), bf16),
            jax.ShapeDtypeStruct((count * WINDOW, width), bf16),
            heads,
            heads,
            heads,
            heads,
            jax.ShapeDtypeStruct((length, HEAD_DIM), f32),
            jax.ShapeDtypeStruct((rows, width), f32),
        ],
        [IN_PLACE] * 5 + [IN_VMEM] * 6,
        [IN_VMEM, IN_VMEM, IN_PLACE, IN_PLACE, IN_VMEM, IN_PLACE, IN_PLACE],
        [one for group in sets for one in group],
        250_000_000,
    )(value, grad, qkv_in, out_weight, bias, shared_down, expert_down)


def share_move_compute(value, grad_all, shared_gate, shared_up, expert_gate, expert_up, wd, number):
    parts = lax.axis_size("context")
    rows, wide = value.shape
    width = wd.shape[1]
    block = shared_gate.shape[0]
    stacks = 1 + expert_gate.shape[0]
    count = 2 * stacks
    length = rows * parts * 4
    experts = (stacks - 1) * 4
    step = 256
    f32, bf16 = jnp.float32, jnp.bfloat16
    share_sems, move_sems, grad_scratch = Share.sems(parts), Move.sems(count, parts), Grads.scratch()
    back_scratch = Return.scratch([(block, 2 * WINDOW)], [2], parts)
    scratch = [
        pltpu.VMEM((length, wide), bf16),
        pltpu.VMEM((length, width), bf16),
        pltpu.VMEM((2 * parts * block, count * WINDOW), bf16),
        pltpu.VMEM(wd.shape, bf16),
        pltpu.VMEM((length, width), f32),
        pltpu.VMEM((length, width), f32),
        pltpu.VMEM((length, 128), f32),
        pltpu.VMEM((length, 2 * WINDOW), bf16),
        pltpu.VMEM((length, 4 * WINDOW), bf16),
        pltpu.VMEM((2, step, width + 128), bf16),
        pltpu.VMEM((2, step, width), bf16),
        DMA((3,)),
        DMA((stacks,)),
        DMA((stacks,)),
        DMA((length // step,)),
        DMA((length // step,)),
    ]

    def kernel(own_ref, grad_hbm, sg_ref, su_ref, eg_ref, eu_ref, wd_hbm, both_hbm, send_hbm, branch_hbm, dup_hbm, act_hbm, upg_hbm, downg_hbm, gate_out, up_out, *rest):
        both, grads_ref, wgu, wd_ref, dx_acc, out_acc, dot_acc, act_ref, dup_ref, send_buf, branch_buf, load, act_s, dup_s, send_s, branch_s = rest[: len(scratch)]
        grad_refs, sems = rest[len(scratch) : len(scratch) + 4], rest[len(scratch) + 4 :]
        back_refs, sems = sems[: len(back_scratch)], sems[len(back_scratch) :]
        spot = Spot()
        share = Share(spot, own_ref, both, sems[: len(share_sems)])

        def item(number):
            k = number // 2
            shared, expert = (sg_ref, eg_ref) if number % 2 == 0 else (su_ref, eu_ref)
            ref = shared if k == 0 else expert.at[k - 1]
            return {
                "src": lambda target, short: units_at(ref, k, target, short, 1, None),
                "dst": lambda side, source, short: rows_at(
                    units_at(wgu, k, 0, short, 1, number * WINDOW), (side * parts + source) * block, block
                ),
                "short": narrow_of(k),
            }

        move = Move(spot, [item(number) for number in range(count)], sems[len(share_sems) :])
        weights = pltpu.make_async_copy(wd_hbm, wd_ref, load.at[0])
        keep = pltpu.make_async_copy(both, both_hbm, load.at[1])
        cotangents = pltpu.make_async_copy(grad_hbm, grads_ref, load.at[2])
        column = lax.broadcasted_iota(jnp.int32, (1, 128), 1)
        pieces = length // step

        def send_out(index):
            at = pl.ds(pl.multiple_of(index * step, step), step)
            return pltpu.make_async_copy(send_buf.at[lax.rem(index, 2)], send_hbm.at[at, :], send_s.at[index])

        def branch_out(index):
            at = pl.ds(pl.multiple_of(index * step, step), step)
            return pltpu.make_async_copy(branch_buf.at[lax.rem(index, 2)], branch_hbm.at[at, :], branch_s.at[index])

        back = Return(
            spot, [up_item(upg_hbm, 0, 0, gate_out, up_out, block, parts)], back_refs[:1], back_refs[1:2], back_refs[2:]
        )

        def slots(k):
            return pl.ds(2 * (k % 2) * WINDOW, 2 * WINDOW), pl.ds((k % 2) * WINDOW, WINDOW)

        def act_out():
            return pltpu.make_async_copy(act_ref.at[:, slots(stacks - 1)[1]], act_hbm, act_s.at[0])

        def dup_out():
            return pltpu.make_async_copy(dup_ref.at[:, slots(stacks - 1)[0]], dup_hbm, dup_s.at[0])

        def gradients(k):
            up, down = pl.ds(2 * k * WINDOW, 2 * WINDOW), pl.ds(k * WINDOW, WINDOW)
            dup_slot, act_slot = slots(k)
            Grads(both, grads_ref, dup_ref.at[:, dup_slot], act_ref.at[:, act_slot], upg_hbm.at[:, up], downg_hbm.at[down, :], *grad_refs).run()

        def compute(k, halfway):
            up, down = pl.ds(2 * k * WINDOW, 2 * WINDOW), pl.ds(k * WINDOW, WINDOW)
            dup_slot, act_slot = slots(k)
            at = experts if k == 0 else spot.group * (stacks - 1) + k - 1
            here = jnp.where(column == at, 1.0, 0.0)
            both_parts = jnp.where((column == at) | (column == at + 64), 1.0, 0.0)

            def one(index, carry):
                pl.when(index == pieces // 2)(halfway)
                rows_here = pl.ds(pl.multiple_of(index * step, step), step)
                vals = jnp.dot(both[rows_here, :width], wgu[:, up], preferred_element_type=f32)
                raw = dot_nt(grads_ref[rows_here, :], wd_ref[down, :])
                coef = jnp.sum(both[rows_here, width:].astype(f32) * both_parts, -1, keepdims=True)
                g_vals, u_vals = vals[:, :WINDOW], vals[:, WINDOW:]
                sig_g = jax.nn.sigmoid(g_vals)
                silu_g = g_vals * sig_g
                act = silu_g * u_vals
                dots = jnp.sum(raw * act, -1, keepdims=True) * here
                act_ref[rows_here, act_slot] = (act * coef).astype(bf16)
                dact = raw * coef
                dup_ref[rows_here, pl.ds(2 * (k % 2) * WINDOW, WINDOW)] = (
                    dact * u_vals * (sig_g * (1.0 + g_vals * (1.0 - sig_g)))
                ).astype(bf16)
                dup_ref[rows_here, pl.ds((2 * (k % 2) + 1) * WINDOW, WINDOW)] = (dact * silu_g).astype(bf16)
                out_part = jnp.dot(act_ref[rows_here, act_slot], wd_ref[down, :], preferred_element_type=f32)
                dx_part = dot_nt(dup_ref[rows_here, dup_slot], wgu[:, up])
                if k == 0:
                    out_acc[rows_here, :] = out_part
                    dx_acc[rows_here, :] = dx_part
                    dot_acc[rows_here, :] = dots
                elif k < stacks - 1:
                    out_acc[rows_here, :] += out_part
                    dx_acc[rows_here, :] += dx_part
                    dot_acc[rows_here, :] += dots
                else:

                    @pl.when(index >= 2)
                    def _():
                        send_out(index - 2).wait()
                        branch_out(index - 2).wait()

                    slot = lax.rem(index, 2)
                    branch_buf[slot] = (out_acc[rows_here, :] + out_part).astype(bf16)
                    send_buf[slot, :, :width] = (dx_acc[rows_here, :] + dx_part).astype(bf16)
                    send_buf[slot, :, width:] = (dot_acc[rows_here, :] + dots).astype(bf16)
                    send_out(index).start()
                    branch_out(index).start()
                return carry

            lax.fori_loop(0, pieces, one, 0)

        def forward(number):
            for gap in (1, 2, 3):
                move.forward(number, gap)

        spot.greet(True, True)
        share.begin()
        weights.start()
        cotangents.start()
        for number in range(count):
            move.own(number)
        move.send(0)
        share.step(1)
        move.send(1)
        share.step(2)
        forward(0)
        share.step(3)
        for number in range(2, count):
            move.send(number)
        share.end()
        keep.start()
        forward(1)
        weights.wait()
        cotangents.wait()
        for k in range(stacks):

            @pl.when(spot.place == narrow_of(k))
            def _():
                spare = 0 if narrow_of(k) else WINDOW - SPARE
                wd_ref[pl.ds(k * WINDOW + spare, SPARE), :] = jnp.zeros((SPARE, width), bf16)
                for which in (2 * k, 2 * k + 1):
                    wgu[:, pl.ds(which * WINDOW + spare, SPARE)] = jnp.zeros((2 * parts * block, SPARE), bf16)

        for k in range(stacks):
            last = k == stacks - 1
            if not last:
                forward(2 * k + 2)
                if k == stacks - 2:
                    back.start_one(0, 1)
            else:
                back.reduce(0, 0)
                back.reduce(0, 1)
            move.ready(2 * k)
            move.ready(2 * k + 1)

            def halfway():
                if last:
                    back.reduce(0, 2)
                else:
                    forward(2 * k + 3)
                if k == stacks - 2:
                    back.start_one(0, 2)
                    back.start_one(0, 3)

            compute(k, halfway)
            if not last:
                gradients(k)
            if k == 0:
                back.start_one(0, 0)
        back.reduce(0, 3)
        act_out().start()
        dup_out().start()
        for index in (pieces - 2, pieces - 1):
            send_out(index).wait()
            branch_out(index).wait()
        act_out().wait()
        dup_out().wait()
        keep.wait()
        move.sent()
        back.end()

    return comm_call(
        kernel,
        number,
        "share_move_compute",
        [
            jax.ShapeDtypeStruct((length, wide), bf16),
            jax.ShapeDtypeStruct((length, width + 128), bf16),
            jax.ShapeDtypeStruct((length, width), bf16),
            jax.ShapeDtypeStruct((length, 2 * WINDOW), bf16),
            jax.ShapeDtypeStruct((length, WINDOW), bf16),
            jax.ShapeDtypeStruct((width, 2 * (stacks - 1) * WINDOW), bf16),
            jax.ShapeDtypeStruct(((stacks - 1) * WINDOW, width), bf16),
            jax.ShapeDtypeStruct(shared_gate.shape, bf16),
            jax.ShapeDtypeStruct(shared_gate.shape, bf16),
        ],
        [IN_PLACE] * 9,
        [IN_VMEM] + [IN_PLACE] * 6,
        scratch + grad_scratch + back_scratch + share_sems + move_sems,
        300_000_000,
    )(value, grad_all, shared_gate, shared_up, expert_gate, expert_up, wd)


def up_item(grads_ref, at, k, gate_ref, up_ref, block, parts):
    def piece(offset, ref):
        return (
            lambda buf, short: units_at(buf, k, 0, short, 1, offset),
            lambda source, short: units_at(ref, k, source, short, 1, None),
        )

    return {
        "block": lambda side, part: grads_ref.at[
            pl.ds(pl.multiple_of((side * parts + part) * block, block), block), pl.ds(2 * at * WINDOW, 2 * WINDOW)
        ],
        "pieces": [piece(0, gate_ref), piece(WINDOW, up_ref)],
        "short": narrow_of(k),
    }


def down_item(grads_ref, at, k, down_ref, parts):
    lanes = down_ref.shape[1]
    return {
        "block": lambda side, part: grads_ref.at[
            pl.ds(at * WINDOW, WINDOW), pl.ds(pl.multiple_of((side * parts + part) * lanes, lanes), lanes)
        ],
        "pieces": [
            (
                lambda buf, short: units_at(buf, k, 0, short, 0),
                lambda source, short: units_at(down_ref, k, source, short, 0, None),
            )
        ],
        "short": narrow_of(k),
    }


def attention_last(send4, up_grads, down_grads, hidden, grad, gain, chances, named, router, out_w, qkv_w, heads, lse, shared, number):
    parts = lax.axis_size("context")
    length, width = send4.shape[0], hidden.shape[1]
    rows, wide = hidden.shape[0], send4.shape[1]
    block = up_grads.shape[0] // (2 * parts)
    lanes = down_grads.shape[1] // (2 * parts)
    units = WINDOW * parts - 128
    step = 256
    experts = 8
    scale = HEAD_DIM ** (-0.5)
    f32, bf16 = jnp.float32, jnp.bfloat16
    shapes, pieces = [(WINDOW, lanes), (block, 2 * WINDOW)], [1, 2]
    sets = [
        [
            pltpu.VMEM((rows, wide), f32),
            pltpu.VMEM((rows, width), bf16),
            pltpu.VMEM((length, width), bf16),
            pltpu.VMEM((length, width), bf16),
            pltpu.VMEM((length, 3 * HEAD_DIM), bf16),
            pltpu.VMEM((length, HEAD_DIM), f32),
            pltpu.VMEM((length, HEAD_DIM), f32),
            pltpu.VMEM((length, HEAD_DIM), f32),
            pltpu.VMEM(shared.shape, bf16),
            DMA((2,)),
        ],
        Sum.scratch(parts, rows, wide),
        Share.sems(parts),
        Sum.scratch(parts, rows, width),
        Return.scratch(shapes, pieces, parts),
    ]

    def kernel(send_ref, upg_ref, downg_ref, hidden_ref, grad_ref, gain_ref, chance_ref, named_ref, router_ref, wout_ref, wqkv_ref,
               q_ref, k_ref, v_ref, att_ref, lse_ref, shared_hbm,
               dh_hbm, down_out, gate_out1, up_out1, dots_ref, dxn2_ref, dhidden_ref, outg_ref, qkvg_ref, bias_ref, dxn1_ref, *scratch):
        scratch, split = list(scratch), []
        for one in sets:
            split.append(scratch[: len(one)])
            scratch = scratch[len(one) :]
        sums, dh_own, dh_all, part_ref, dqkv_ref, dq_acc, dk_acc, dv_acc, shared_ref, keep_sem = split[0]
        spot = Spot()
        first = Sum(spot, send_ref, sums, split[1])
        share = Share(spot, dh_own, dh_all, split[2])
        second = Sum(spot, part_ref, dxn1_ref, split[3])
        items = [
            down_item(downg_ref, 0, 0, down_out, parts),
            up_item(upg_ref, 1, 1, gate_out1, up_out1, block, parts),
        ]
        back = Return(spot, items, split[4][:2], split[4][2:4], split[4][4:])
        keep = pltpu.make_async_copy(dh_all, dh_hbm, keep_sem.at[0])
        fetch = pltpu.make_async_copy(shared_hbm, shared_ref, keep_sem.at[1])

        def owner():
            lane = lax.broadcasted_iota(jnp.int32, (rows, 128), 1)
            dots = sums[:, width:]
            dots_ref[...] = dots
            chance = chance_ref[...]
            dprob = dots * named_ref[...]
            prob = jnp.where(lane < experts, chance, 0.0)
            dlogit = prob * (dprob - jnp.sum(prob * dprob, -1, keepdims=True))
            mix = jnp.where(lane < experts, dlogit, jnp.where(lane == experts, chance * (1.0 - chance) * dots, 0.0))
            dxn2_ref[...] = jnp.dot(mix, router_ref[...], precision=PRECISE, preferred_element_type=f32)

            def one(index, carry):
                at = pl.ds(pl.multiple_of(index * 16, 16), 16)
                dxn2 = dxn2_ref[at, :] + sums[at, :width]
                dxn2_ref[at, :] = dxn2
                value = hidden_ref[at, :]
                inverse = lax.rsqrt(jnp.mean(value * value, -1, keepdims=True) + EPSILON)
                normed = value * inverse
                scaled = dxn2 * gain_ref[...]
                dhidden = grad_ref[at, :].astype(f32) + inverse * (scaled - normed * jnp.mean(scaled * normed, -1, keepdims=True))
                dhidden_ref[at, :] = dhidden
                dh_own[at, :] = dhidden.astype(bf16)
                return carry

            lax.fori_loop(0, rows // 16, one, 0)

        def attend(index, carry):
            start = pl.multiple_of(index * step, step)
            at = pl.ds(start, step)
            datt = dot_nt(dh_all[at, :], wout_ref[...]).astype(bf16)
            delta = jnp.sum(datt.astype(f32) * att_ref[at, :].astype(f32), -1, keepdims=True)
            scores = dot_nt(q_ref[at, :], k_ref[...]) * scale
            query_index = start + lax.broadcasted_iota(jnp.int32, scores.shape, 0)
            allowed = lax.broadcasted_iota(jnp.int32, scores.shape, 1) <= query_index
            prob = jnp.where(allowed, jnp.exp(scores - lse_ref[at, :1]), 0.0)
            dscore = (prob * (dot_nt(datt, v_ref[...]) - delta)).astype(bf16)
            dq_acc[at, :] = jnp.dot(dscore, k_ref[...], preferred_element_type=f32) * scale
            dk_acc[...] += dot_tn(dscore, q_ref[at, :])
            dv_acc[...] += dot_tn(prob.astype(bf16), datt)
            return carry

        def project(index, carry):
            at = pl.ds(pl.multiple_of(index * step, step), step)
            cosine, sine_part = turn_tables(shared_ref[at, width:])
            dq, dk, dv = dq_acc[at, :], dk_acc[at, :] * scale, dv_acc[at, :]
            dq = dq * cosine - pltpu.roll(dq, HEAD_DIM // 2, 1) * sine_part
            dk = dk * cosine - pltpu.roll(dk, HEAD_DIM // 2, 1) * sine_part
            for which, value in enumerate((dq, dk, dv)):
                bias_ref[:, pl.ds(which * HEAD_DIM, HEAD_DIM)] += jnp.sum(value, 0, keepdims=True)
                dqkv_ref[at, pl.ds(which * HEAD_DIM, HEAD_DIM)] = value.astype(bf16)
            part_ref[at, :] = dot_nt(dqkv_ref[at, :], wqkv_ref[...]).astype(bf16)
            return carry

        def features(index, carry):
            at = pl.ds(pl.multiple_of(index * step, step), step)
            qkvg_ref[at, :] = dot_tn(shared_ref[:, at], dqkv_ref[...]).astype(bf16)
            outg_ref[:, at] = dot_tn(att_ref[...], dh_all[:, at]).astype(bf16)
            return carry

        spot.greet(True, True)
        first.begin()
        for number in range(2):
            back.start(number)
        fetch.start()
        dk_acc[...] = jnp.zeros_like(dk_acc)
        dv_acc[...] = jnp.zeros_like(dv_acc)
        bias_ref[...] = jnp.zeros_like(bias_ref)
        for index in range(parts):
            first.cross(index)
        back.reduce(0, 0)
        back.reduce(0, 1)
        for index in range(parts):
            first.line(index)
        owner()
        share.begin()
        share.step(1)
        share.step(2)
        back.reduce(0, 2)
        share.step(3)
        back.reduce(0, 3)
        back.reduce(1, 0)
        share.end()
        keep.start()
        back.reduce(1, 1)
        back.reduce(1, 2)
        lax.fori_loop(0, length // step, attend, 0)
        fetch.wait()
        lax.fori_loop(0, length // step, project, 0)
        second.begin()
        back.reduce(1, 3)
        for index in range(parts):
            second.cross(index)
        lax.fori_loop(0, width // step, features, 0)
        for index in range(parts):
            second.line(index)
        first.end()
        second.end()
        back.end()
        keep.wait()

    piece = jax.ShapeDtypeStruct((block, units), bf16)
    return comm_call(
        kernel,
        number,
        "attention_last",
        [
            jax.ShapeDtypeStruct((length, width), bf16),
            jax.ShapeDtypeStruct((units, lanes), bf16),
            piece,
            piece,
            jax.ShapeDtypeStruct((rows, 128), f32),
            jax.ShapeDtypeStruct((rows, width), f32),
            jax.ShapeDtypeStruct((rows, width), f32),
            jax.ShapeDtypeStruct((HEAD_DIM, width), bf16),
            jax.ShapeDtypeStruct((width, 3 * HEAD_DIM), bf16),
            jax.ShapeDtypeStruct((1, 3 * HEAD_DIM), f32),
            jax.ShapeDtypeStruct((rows, width), f32),
        ],
        [IN_PLACE] * 4 + [IN_VMEM] * 7,
        [IN_VMEM, IN_PLACE, IN_PLACE] + [IN_VMEM] * 13 + [IN_PLACE],
        [one for group in sets for one in group],
        250_000_000,
    )(send4, up_grads, down_grads, hidden, grad, gain, chances, named, router, out_w, qkv_w, *heads, lse, shared)


class Group:
    def __init__(self, spot, own, out, sems):
        self.spot, self.own, self.out = spot, own, out
        self.local_sem, self.across_s, self.across_r, self.beside_s, self.beside_r = sems

    @staticmethod
    def sems():
        return [DMA, DMA, DMA, DMA((2,)), DMA((2,))]

    def block(self, column):
        rows = self.own.shape[0]
        return rows_at(self.out, column * rows, rows)

    def to_across(self):
        s = self.spot
        return remote(self.own, self.block(s.group), self.across_s, self.across_r, {"experts": s.across})

    def to_beside(self, slot):
        s = self.spot
        column = s.across if slot else s.group
        source = self.block(column) if slot else self.own
        return remote(source, self.block(column), self.beside_s.at[slot], self.beside_r.at[slot], {"experts": s.beside})

    def local(self):
        return pltpu.make_async_copy(self.own, self.block(self.spot.group), self.local_sem)

    def begin(self):
        self.to_across().start()
        self.to_beside(0).start()
        self.local().start()

    def end(self):
        self.to_across().wait_recv()
        self.to_beside(1).start()
        self.local().wait()
        self.to_across().wait_send()
        for slot in range(2):
            self.to_beside(slot).wait()


class Total:
    def __init__(self, spot, value, out, scratch):
        self.out = out
        self.sent, self.got, self.send_s, self.recv_s = scratch
        place = spot.place
        self.turns = [
            spot.twin,
            {"context": place + 1 - 2 * lax.rem(place, 2)},
            {"context": lax.rem(place + 2, spot.parts)},
            {"experts": spot.beside},
            {"experts": spot.across},
        ]
        self.value = value

    @staticmethod
    def scratch(shape):
        buf = pltpu.VMEM((5,) + shape, jnp.float32)
        return [buf, buf, DMA((5,)), DMA((5,))]

    def copy(self, index):
        return remote(self.sent.at[index], self.got.at[index], self.send_s.at[index], self.recv_s.at[index], self.turns[index])

    def begin(self):
        self.out[...] = self.value[...]
        self.send(0)

    def send(self, index):
        self.sent[index] = self.out[...]
        self.copy(index).start()

    def take(self, index):
        self.copy(index).wait()
        self.out[...] = self.out[...] + self.got[index]


def last_exchange(down_grads, out_grads, qkv_grads, both, cotangents, dup, act, branch, hidden, tokens_grad, small, number):
    parts = lax.axis_size("context")
    rows, width = hidden.shape
    block = lanes = width // (2 * parts)
    units = WINDOW * parts - 128
    head, span = out_grads.shape[0], qkv_grads.shape[1]
    shapes = [(head, lanes), (block, span), (WINDOW, lanes), (block, 2 * WINDOW), (WINDOW, lanes)]
    pieces = [1, 1, 1, 2, 1]
    count, bf16 = len(shapes), jnp.bfloat16
    groups = [
        Return.scratch(shapes, pieces, parts),
        Sum.scratch(parts, rows, width) + [pltpu.VMEM((rows, width), jnp.float32), pltpu.VMEM((rows, width), bf16)],
        Total.scratch(small.shape),
        Group.sems(),
        Group.sems(),
        Grads.scratch() + [pltpu.VMEM(one.shape, bf16) for one in (both, cotangents, dup, act)] + [DMA((4,))],
    ]
    piece, column = jax.ShapeDtypeStruct((block, units), bf16), jax.ShapeDtypeStruct((units, lanes), bf16)
    out_shape = [jax.ShapeDtypeStruct((parts * head, lanes), bf16), jax.ShapeDtypeStruct((parts * block, span), bf16)]
    out_shape += [column, piece, piece, column]
    out_shape += [
        jax.ShapeDtypeStruct((width, 2 * WINDOW), bf16),
        jax.ShapeDtypeStruct((WINDOW, width), bf16),
        jax.ShapeDtypeStruct((4 * rows, width), bf16),
        jax.ShapeDtypeStruct((4 * rows, width), jnp.float32),
        jax.ShapeDtypeStruct(small.shape, jnp.float32),
    ]

    def kernel(downg_ref, outg_ref, qkvg_ref, both_hbm, cots_hbm, dup_hbm, act_hbm, branch_ref, hidden_ref, tokens_ref, small_ref, *rest):
        outs, scratch = rest[: len(out_shape)], list(rest[len(out_shape) :])
        sets = []
        for one in groups:
            sets.append(scratch[: len(one)])
            scratch = scratch[len(one) :]
        grads, (upg2_hbm, downg2_hbm, block_all, tokens_all, small_out) = outs[:-5], outs[-5:]
        *grad_refs, both_ref, cots_ref, dup_ref, act_ref, load = sets[5]
        loads = [
            pltpu.make_async_copy(source, target, load.at[index])
            for index, (source, target) in enumerate(
                ((both_hbm, both_ref), (cots_hbm, cots_ref), (dup_hbm, dup_ref), (act_hbm, act_ref))
            )
        ]
        items = [
            {
                "block": lambda side, part: lanes_at(outg_ref, (side * parts + part) * lanes, lanes),
                "pieces": [(lambda buf, short: buf, lambda source, short: rows_at(grads[0], source * head, head))],
            },
            {
                "block": lambda side, part: rows_at(qkvg_ref, (side * parts + part) * block, block),
                "pieces": [(lambda buf, short: buf, lambda source, short: rows_at(grads[1], source * block, block))],
            },
        ]
        items += [
            down_item(downg_ref, 1, 1, grads[2], parts),
            up_item(upg2_hbm, 0, 2, grads[3], grads[4], block, parts),
            down_item(downg2_hbm, 0, 2, grads[5], parts),
        ]
        spot = Spot()
        back = Return(spot, items, sets[0][:count], sets[0][count : 2 * count], sets[0][2 * count :])
        total_branch, own_block = sets[1][-2:]
        summed = Sum(spot, branch_ref, total_branch, sets[1][:-2])
        total = Total(spot, small_ref, small_out, sets[2])
        tokens_group = Group(spot, tokens_ref, tokens_all, sets[3])
        block_group = Group(spot, own_block, block_all, sets[4])
        spot.greet(True, True)
        total.begin()
        summed.begin()
        for item in range(3):
            back.start(item)
        for copy in loads:
            copy.start()
        total.take(0)
        total.send(1)
        for index in range(parts):
            summed.cross(index)
        total.take(1)
        total.send(2)
        for index in range(parts):
            back.reduce(0, index)
        total.take(2)
        total.send(3)
        for index in range(parts):
            back.reduce(1, index)
        total.take(3)
        total.send(4)
        for copy in loads:
            copy.wait()
        Grads(both_ref, cots_ref, dup_ref, act_ref, upg2_hbm, downg2_hbm, *grad_refs).run()
        back.start(3)
        back.start(4)
        for index in range(parts):
            back.reduce(2, index)
        total.take(4)
        tokens_group.begin()
        for index in range(parts):
            summed.line(index)
        half = width // 2

        def finish(at, start, step):
            value = (hidden_ref[at, :] + total_branch[at, :]).astype(bf16)
            turned = lax.axis_index("dp") == 0

            @pl.when(turned)
            def _():
                own_block[at, :] = value

            @pl.when(jnp.logical_not(turned))
            def _():
                own_block[at, :half] = value[:, half:]
                own_block[at, half:] = value[:, :half]

        summed.chunks(finish)
        block_group.begin()
        for item in range(3, count):
            for index in range(parts):
                back.reduce(item, index)
        summed.end()
        tokens_group.end()
        block_group.end()
        back.end()

    return comm_call(
        kernel,
        number,
        "last_exchange",
        out_shape,
        [IN_PLACE] * (len(out_shape) - 1) + [IN_VMEM],
        [IN_PLACE] * 7 + [IN_VMEM] * 4,
        [one for group in groups for one in group],
        300_000_000,
    )(down_grads, out_grads, qkv_grads, both, cotangents, dup, act, branch, hidden, tokens_grad, small)


def widen(singles, pairs):
    steps = 8

    def spec(shape):
        if len(shape) == 3:
            return pl.BlockSpec((shape[0], shape[1] // steps, shape[2]), lambda i: (0, i, 0))
        return pl.BlockSpec((shape[0] // steps, shape[1]), lambda i: (i, 0))

    kinds = [jnp.bfloat16 if keep else jnp.float32 for _, keep in singles]
    arrays = [array for array, _ in singles] + [one for pair in pairs for one in pair]
    out_shape = [jax.ShapeDtypeStruct(array.shape, kind) for (array, _), kind in zip(singles, kinds)]
    out_shape += [jax.ShapeDtypeStruct((2,) + pair[0].shape, jnp.float32) for pair in pairs]
    count = len(singles)

    def kernel(*refs):
        sources, targets = refs[: len(arrays)], refs[len(arrays) :]
        for source, target in zip(sources[:count], targets[:count]):
            target[...] = source[...].astype(target.dtype)
        for index, target in enumerate(targets[count:]):
            for which in range(2):
                target[which] = sources[count + 2 * index + which][...].astype(jnp.float32)

    return pl.pallas_call(
        kernel,
        grid=(steps,),
        in_specs=[spec(array.shape) for array in arrays],
        out_specs=[spec(one.shape) for one in out_shape],
        out_shape=out_shape,
        name="widen",
    )(*arrays)


def split_body(
    tokens,
    positions,
    routes,
    out_grad,
    norm1_gain,
    qkv_weight,
    qkv_bias,
    out_weight,
    norm2_gain,
    router_weight,
    expert_gate,
    expert_up,
    expert_down,
    shared_gate,
    shared_w_gate,
    shared_w_up,
    shared_w_down,
):
    rows, width = tokens.shape[1], tokens.shape[2]
    parts = lax.axis_size("context")
    group_size = lax.axis_size("experts")
    place, group = lax.axis_index("context"), lax.axis_index("experts")
    local_experts = expert_gate.shape[0]
    expert_count = local_experts * group_size
    own_rows = rows // group_size
    length = rows * parts
    half = width // 2
    block = width // (2 * parts)
    hidden_here = shared_w_gate.shape[1] // parts
    stacks = local_experts + 1
    scale = HEAD_DIM ** (-0.5)
    bf16 = jnp.bfloat16

    first = group * own_rows

    def own_of(array):
        return lax.dynamic_slice_in_dim(array, first, own_rows, 0)

    grad_own_b = own_half_first(own_of(out_grad[0]))
    grad_own = grad_own_b.astype(jnp.float32)
    gain1 = own_half_first(norm1_gain).astype(jnp.float32)
    gain2 = own_half_first(norm2_gain).astype(jnp.float32)
    token_own = own_half_first(own_of(tokens[0])).astype(jnp.float32)
    inverse1 = lax.rsqrt(jnp.mean(token_own * token_own, -1, keepdims=True) + EPSILON)
    normed1 = token_own * inverse1
    half_dim = HEAD_DIM // 2
    frequency = ROPE_BASE ** (-2.0 * jnp.arange(half_dim, dtype=jnp.float32) / HEAD_DIM)
    angles = own_of(positions[0]).astype(jnp.float32)[:, None] * frequency[None, :]
    turns = jnp.concatenate([jnp.cos(angles), jnp.sin(angles)], 1)
    turns_high = turns.astype(bf16)
    turns_low = (turns - turns_high.astype(jnp.float32)).astype(bf16)
    send1 = jnp.concatenate([(normed1 * gain1).astype(bf16), turns_high, turns_low], 1)
    qkv_in = jnp.transpose(
        qkv_weight.reshape(block, 3, parts, HEAD_DIM), (2, 0, 1, 3)
    ).reshape(parts * block, 3 * HEAD_DIM)
    bias_here = lax.dynamic_slice_in_dim(
        qkv_bias.reshape(3, parts, HEAD_DIM), place, 1, 1
    ).reshape(1, 3 * HEAD_DIM)
    shared1, grad_all, qkv_w, out_w, down_w, query, key, value, attended, lse, head_sum = attention_first(
        send1, grad_own_b, qkv_in, out_weight, bias_here.astype(jnp.float32), shared_w_down, expert_down, 1
    )
    hidden = token_own + head_sum
    inverse2 = lax.rsqrt(jnp.mean(hidden * hidden, -1, keepdims=True) + EPSILON)
    normed2 = hidden * inverse2
    xn2_own = (normed2 * gain2).astype(bf16)
    router_here = own_half_first(router_weight.T).T
    gate_here = own_half_first(shared_gate)
    heads_w = jnp.concatenate([router_here, gate_here[:, None]], 1)
    logits = dot_nn(xn2_own, heads_w)
    prob = jax.nn.softmax(logits[:, :expert_count], -1)
    sig_own = jax.nn.sigmoid(logits[:, expert_count])
    named = jnp.sum(
        (
            own_of(routes[0])[:, :, None] == jnp.arange(expert_count, dtype=jnp.int32)[None, None, :]
        ).astype(jnp.float32),
        1,
    )
    gates = jnp.pad(
        jnp.concatenate([prob * named, sig_own[:, None]], 1), ((0, 0), (0, 63 - expert_count))
    )
    gates_high = gates.astype(bf16)
    gates_low = (gates - gates_high.astype(jnp.float32)).astype(bf16)
    send3 = jnp.concatenate([xn2_own, gates_high, gates_low], 1)

    both, send4, branch_part, dup, act_c, up_g, down_g, *first_grads = share_move_compute(
        send3, grad_all, shared_w_gate, shared_w_up, expert_gate, expert_up, down_w, 3
    )
    up_grads, down_grads = [None] * (2 * stacks), [None] * stacks
    up_grads[:2] = first_grads
    side = 128 - expert_count - 1
    chances = jnp.pad(jnp.concatenate([prob, sig_own[:, None]], 1), ((0, 0), (0, side)))
    named_wide = jnp.pad(named, ((0, 0), (0, 128 - expert_count)))
    router_wide = jnp.pad(heads_w.T.astype(jnp.float32), ((0, side), (0, 0)))
    (
        _,
        down_grads[0],
        up_grads[2],
        up_grads[3],
        dots_own,
        dxn2,
        dhidden,
        out_g,
        qkv_g,
        bias_part,
        dxn1,
    ) = attention_last(
        send4,
        up_g,
        down_g,
        hidden,
        grad_own_b,
        gain2[None, :],
        chances,
        named_wide,
        router_wide,
        out_w,
        qkv_w,
        (query, key, value, attended),
        lse,
        shared1,
        4,
    )

    dprob = dots_own[:, :expert_count] * named
    dlogit = prob * (dprob - jnp.sum(prob * dprob, -1, keepdims=True))
    coef = sig_own * (1.0 - sig_own) * dots_own[:, expert_count]
    xn2_float = xn2_own.astype(jnp.float32)
    router_grad = jnp.dot(xn2_float.T, dlogit, precision=PRECISE)
    shared_gate_grad = jnp.dot(coef, xn2_float, precision=PRECISE)
    norm2_grad = jnp.sum(dxn2 * normed2, 0)
    norm1_grad = jnp.sum(dxn1 * normed1, 0)
    dscaled1 = dxn1 * gain1
    tokens_grad_own = dhidden + inverse1 * (
        dscaled1 - normed1 * jnp.mean(dscaled1 * normed1, -1, keepdims=True)
    )

    bias_wide = jnp.zeros((group_size, parts, 3 * HEAD_DIM), jnp.float32)
    bias_wide = lax.dynamic_update_slice(bias_wide, bias_part[None], (group, place, 0))
    small = jnp.concatenate(
        [
            own_half_first(norm1_grad),
            own_half_first(norm2_grad),
            own_half_first(shared_gate_grad),
            own_half_first(router_grad.T).T.reshape(-1),
            bias_wide.reshape(-1),
        ]
    )
    (
        out_w_grad,
        qkv_grad,
        down_grads[1],
        up_grads[4],
        up_grads[5],
        down_grads[2],
        _,
        _,
        block_out,
        tokens_grad,
        small,
    ) = last_exchange(
        down_g,
        out_g,
        qkv_g,
        both,
        grad_all,
        dup,
        act_c,
        branch_part,
        hidden,
        own_half_first(tokens_grad_own),
        small.reshape(-1, 128),
        7,
    )
    small = small.reshape(-1)
    router_size = width * expert_count
    bias_sum = small[3 * width + router_size :].reshape(group_size, parts, 3, HEAD_DIM)
    bias_grad = jnp.transpose(
        lax.dynamic_slice_in_dim(bias_sum, group, 1, 0)[0], (1, 0, 2)
    ).reshape(3, parts * HEAD_DIM)

    qkv_grad = jnp.transpose(
        qkv_grad.reshape(parts, block, 3, HEAD_DIM), (1, 2, 0, 3)
    ).reshape(block, 3, parts * HEAD_DIM).astype(jnp.float32)
    singles = [(block_out, True), (tokens_grad, False), (out_w_grad, False)]
    singles += [(up_grads[0], False), (up_grads[1], False), (down_grads[0], False)]
    pairs = [up_grads[2::2], up_grads[3::2], down_grads[1:]]
    block_out, tokens_grad, out_w_grad, *shared_grads, gate_grads, up_grads, down_grads = widen(singles, pairs)

    return (
        block_out[None],
        tokens_grad[None],
        small[:width],
        qkv_grad,
        bias_grad,
        out_w_grad,
        small[width : 2 * width],
        small[3 * width : 3 * width + router_size].reshape(width, expert_count),
        gate_grads,
        up_grads,
        down_grads,
        small[2 * width : 3 * width],
        *shared_grads,
    )


def plan_of(mesh):
    sizes = mesh.shape
    return split_body if (sizes["dp"], sizes["context"], sizes["experts"]) == (2, 4, 4) else general_body


def solution(mesh):
    return jax.shard_map(
        plan_of(mesh),
        mesh=mesh,
        in_specs=(
            P("dp", "context", None),
            P("dp", "context"),
            P("dp", "context", None),
            P("dp", "context", None),
            P(),
            P(("dp", "context"), None, "experts"),
            P(None, "experts"),
            P("experts", ("dp", "context")),
            P(),
            P(),
            P("experts", ("dp", "context"), None),
            P("experts", ("dp", "context"), None),
            P("experts", None, ("dp", "context")),
            P(),
            P(("dp", "context"), "experts"),
            P(("dp", "context"), "experts"),
            P("experts", ("dp", "context")),
        ),
        out_specs=(
            P("dp", "context", None),
            P("dp", "context", None),
            P(),
            P(("dp", "context"), None, "experts"),
            P(None, "experts"),
            P("experts", ("dp", "context")),
            P(),
            P(),
            P("experts", ("dp", "context"), None),
            P("experts", ("dp", "context"), None),
            P("experts", None, ("dp", "context")),
            P(),
            P(("dp", "context"), "experts"),
            P(("dp", "context"), "experts"),
            P("experts", ("dp", "context")),
        ),
        check_vma=False,
    )
```

```python
import functools

import jax
import jax.numpy as jnp
from jax import lax
from jax.experimental import pallas as pl
from jax.experimental.pallas import tpu as pltpu
from jax.sharding import PartitionSpec as P

HEAD_DIM = 128


EPSILON = 1e-06
ROPE_BASE = 1000000.0
MASKED = -1e30
PRECISE = lax.Precision.HIGHEST


def rope_tables(position_ids):
    half_dim = HEAD_DIM // 2
    inverse = ROPE_BASE ** (-2.0 * jnp.arange(half_dim, dtype=jnp.float32) / HEAD_DIM)
    angles = position_ids.astype(jnp.float32)[:, None] * inverse[None, :]
    cosine = jnp.cos(angles)
    sine_part = jnp.sin(angles)
    return (
        jnp.concatenate([cosine, cosine], -1)[:, None, :],
        jnp.concatenate([sine_part, sine_part], -1)[:, None, :],
    )


def rotate(value):
    half_dim = value.shape[-1] // 2
    return jnp.concatenate([-value[..., half_dim:], value[..., :half_dim]], -1)


def rotate_back(value):
    half_dim = value.shape[-1] // 2
    return jnp.concatenate([value[..., half_dim:], -value[..., :half_dim]], -1)


def silu_grad(gate_vals):
    sigmoid_vals = jax.nn.sigmoid(gate_vals)
    return sigmoid_vals * (1.0 + gate_vals * (1.0 - sigmoid_vals))


def block_rank(route_rows, expert_count):
    hits = (
        route_rows[:, :, None] == jnp.arange(expert_count, dtype=jnp.int32)[None, None, :]
    ).astype(jnp.int32)
    flat_hits = hits.reshape(-1, expert_count)
    earlier = jnp.cumsum(flat_hits, axis=0) - flat_hits
    return jnp.sum(earlier * flat_hits, -1).reshape(route_rows.shape)


def block_width_of():
    return 512


def gather_weights(shard_set):
    return (
        lax.all_gather(shard_set[0], ("dp", "context"), axis=0, tiled=True),
        lax.all_gather(shard_set[1], ("dp", "context"), axis=1, tiled=True),
        lax.all_gather(shard_set[2], ("dp", "context"), axis=1, tiled=True),
        lax.all_gather(shard_set[3], ("dp", "context"), axis=1, tiled=True),
        lax.all_gather(shard_set[4], ("dp", "context"), axis=2, tiled=True),
        lax.all_gather(shard_set[5], ("dp", "context"), axis=0, tiled=True),
        lax.all_gather(shard_set[6], ("dp", "context"), axis=0, tiled=True),
        lax.all_gather(shard_set[7], ("dp", "context"), axis=1, tiled=True),
    )


def forward_fold(query, query_first, scale, carry, piece):
    row_count, head_count, head_size = query.shape
    query_index = query_first + jnp.arange(row_count, dtype=jnp.int32)
    query_last = query_first + row_count - 1
    key_part, value_part = piece
    piece_rows = key_part.shape[0]
    block_width = block_width_of()
    block_count = piece_rows // block_width
    key_blocks = key_part.reshape(block_count, block_width, head_count, head_size)
    value_blocks = value_part.reshape(block_count, block_width, head_count, head_size)
    offsets = block_width * jnp.arange(block_count, dtype=jnp.int32)

    def forward_visit(state, item):
        key_block, value_block, first_key = item

        def forward_compute(current):
            run_max, run_sum, accum = current
            scores = (
                jnp.einsum("qhd,khd->hqk", query, key_block, preferred_element_type=jnp.float32)
                * scale
            )
            key_index = first_key + jnp.arange(block_width, dtype=jnp.int32)
            allowed = key_index[None, None, :] <= query_index[None, :, None]
            new_max = jnp.maximum(run_max, jnp.max(jnp.where(allowed, scores, MASKED), -1))
            weights = jnp.where(allowed, jnp.exp(scores - new_max[..., None]), 0.0)
            factor = jnp.exp(run_max - new_max)
            new_sum = run_sum * factor + jnp.sum(weights, -1)
            new_accum = accum * factor[..., None] + jnp.einsum(
                "hqk,khd->hqd",
                weights.astype(jnp.bfloat16),
                value_block,
                preferred_element_type=jnp.float32,
            )
            return (new_max, new_sum, new_accum)

        return (
            lax.cond(first_key > query_last, lambda current: current, forward_compute, state),
            None,
        )

    carry, _ = lax.scan(forward_visit, carry, (key_blocks, value_blocks, offsets))
    return carry


def key_grad_fold(key_rows, value_rows, key_first, scale, carry, piece):
    row_count, head_count, head_size = key_rows.shape
    key_index = key_first + jnp.arange(row_count, dtype=jnp.int32)
    query_part, dout_part, lse_part, delta_part = piece
    piece_rows = query_part.shape[0]
    block_width = block_width_of()
    block_count = piece_rows // block_width
    query_blocks = query_part.reshape(block_count, block_width, head_count, head_size)
    dout_blocks = dout_part.reshape(block_count, block_width, head_count, head_size)
    lse_blocks = lse_part.reshape(block_count, block_width, head_count)
    delta_blocks = delta_part.reshape(block_count, block_width, head_count)
    offsets = block_width * jnp.arange(block_count, dtype=jnp.int32)

    def key_visit(state, item):
        query_block, dout_block, lse_block, delta_block, first_query = item

        def key_compute(current):
            dkey_sum, dvalue_sum = current
            query_b = query_block.astype(jnp.bfloat16)
            dout_b = dout_block.astype(jnp.bfloat16)
            scores = (
                jnp.einsum("qhd,khd->hqk", query_b, key_rows, preferred_element_type=jnp.float32)
                * scale
            )
            query_index = first_query + jnp.arange(block_width, dtype=jnp.int32)
            allowed = key_index[None, None, :] <= query_index[None, :, None]
            prob_att = jnp.where(
                allowed, jnp.exp(scores - jnp.transpose(lse_block)[:, :, None]), 0.0
            )
            dvalue_sum = dvalue_sum + jnp.einsum(
                "hqk,qhd->hkd",
                prob_att.astype(jnp.bfloat16),
                dout_b,
                preferred_element_type=jnp.float32,
            )
            dprob = jnp.einsum(
                "qhd,khd->hqk", dout_b, value_rows, preferred_element_type=jnp.float32
            )
            dscore = (prob_att * (dprob - jnp.transpose(delta_block)[:, :, None])).astype(
                jnp.bfloat16
            )
            dkey_sum = (
                dkey_sum
                + jnp.einsum("hqk,qhd->hkd", dscore, query_b, preferred_element_type=jnp.float32)
                * scale
            )
            return (dkey_sum, dvalue_sum)

        return (
            lax.cond(
                first_query + block_width - 1 < key_first,
                lambda current: current,
                key_compute,
                state,
            ),
            None,
        )

    carry, _ = lax.scan(
        key_visit, carry, (query_blocks, dout_blocks, lse_blocks, delta_blocks, offsets)
    )
    return carry


def query_grad_fold(query, dattended, lse_heads, delta_heads, query_first, scale, carry, piece):
    row_count, head_count, head_size = query.shape
    query_index = query_first + jnp.arange(row_count, dtype=jnp.int32)
    query_last = query_first + row_count - 1
    key_part, value_part = piece
    piece_rows = key_part.shape[0]
    block_width = block_width_of()
    block_count = piece_rows // block_width
    key_blocks = key_part.reshape(block_count, block_width, head_count, head_size)
    value_blocks = value_part.reshape(block_count, block_width, head_count, head_size)
    offsets = block_width * jnp.arange(block_count, dtype=jnp.int32)

    def query_visit(state, item):
        key_block, value_block, first_key = item

        def query_compute(current):
            scores = (
                jnp.einsum("qhd,khd->hqk", query, key_block, preferred_element_type=jnp.float32)
                * scale
            )
            key_index = first_key + jnp.arange(block_width, dtype=jnp.int32)
            allowed = key_index[None, None, :] <= query_index[None, :, None]
            prob_att = jnp.where(allowed, jnp.exp(scores - lse_heads[:, :, None]), 0.0)
            dprob = jnp.einsum(
                "qhd,khd->hqk", dattended, value_block, preferred_element_type=jnp.float32
            )
            dscore = (prob_att * (dprob - delta_heads[:, :, None])).astype(jnp.bfloat16)
            return (
                current
                + jnp.einsum("hqk,khd->hqd", dscore, key_block, preferred_element_type=jnp.float32)
                * scale
            )

        return (
            lax.cond(first_key > query_last, lambda current: current, query_compute, state),
            None,
        )

    carry, _ = lax.scan(query_visit, carry, (key_blocks, value_blocks, offsets))
    return carry


def general_body(
    tokens,
    positions,
    routes,
    out_grad,
    norm1_gain,
    qkv_weight,
    qkv_bias,
    out_weight,
    norm2_gain,
    router_weight,
    expert_gate,
    expert_up,
    expert_down,
    shared_gate,
    shared_w_gate,
    shared_w_up,
    shared_w_down,
):
    row_count = tokens.shape[1]
    model_width = tokens.shape[2]
    head_span = qkv_bias.shape[1]
    heads_here = head_span // HEAD_DIM
    local_experts = expert_gate.shape[0]
    group_size = lax.axis_size("experts")
    quarter = row_count // group_size
    capacity = 3 * quarter // 4
    expert_count = local_experts * group_size
    group_index = lax.axis_index("experts")
    scale = HEAD_DIM ** (-0.5)
    shard_set = (
        qkv_weight,
        out_weight,
        expert_gate,
        expert_up,
        expert_down,
        shared_w_gate,
        shared_w_up,
        shared_w_down,
    )
    qkv_full, out_full, gate_full, up_full, down_full, sgate_full, sup_full, sdown_full = (
        gather_weights(shard_set)
    )
    token_float = tokens[0].astype(jnp.float32)
    inverse1 = lax.rsqrt(jnp.mean(token_float * token_float, -1, keepdims=True) + EPSILON)
    normed1 = token_float * inverse1
    gain1 = norm1_gain.astype(jnp.float32)
    normed1_b = (normed1 * gain1).astype(jnp.bfloat16)
    qkv_flat = qkv_full.reshape(model_width, 3 * head_span)
    qkv = (
        jnp.dot(normed1_b, qkv_flat, preferred_element_type=jnp.float32).reshape(
            row_count, 3, head_span
        )
        + qkv_bias.astype(jnp.float32)[None]
    )
    cosine, sine_part = rope_tables(positions[0])
    query_raw = qkv[:, 0].reshape(row_count, heads_here, HEAD_DIM)
    key_raw = qkv[:, 1].reshape(row_count, heads_here, HEAD_DIM)
    query = (query_raw * cosine + rotate(query_raw) * sine_part).astype(jnp.bfloat16)
    key_rows = (key_raw * cosine + rotate(key_raw) * sine_part).astype(jnp.bfloat16)
    value_flat = qkv[:, 2].astype(jnp.bfloat16)
    key_flat = key_rows.reshape(row_count, head_span)
    value_rows = value_flat.reshape(row_count, heads_here, HEAD_DIM)
    query_first = lax.axis_index("context") * row_count
    start_state = (
        jnp.full((heads_here, row_count), MASKED, jnp.float32),
        jnp.zeros((heads_here, row_count), jnp.float32),
        jnp.zeros((heads_here, row_count, HEAD_DIM), jnp.float32),
    )
    run_max, run_sum, accum = forward_fold(
        query,
        query_first,
        scale,
        start_state,
        (
            lax.all_gather(key_flat, "context", axis=0, tiled=True),
            lax.all_gather(value_flat, "context", axis=0, tiled=True),
        ),
    )
    attended = jnp.transpose(accum / run_sum[..., None], (1, 0, 2)).astype(jnp.bfloat16)
    lse_heads = run_max + jnp.log(run_sum)
    attended_flat = attended.reshape(row_count, head_span)
    head_part = jnp.dot(attended_flat, out_full, preferred_element_type=jnp.float32)
    hidden = token_float + lax.psum(head_part, "experts")
    inverse2 = lax.rsqrt(jnp.mean(hidden * hidden, -1, keepdims=True) + EPSILON)
    normed2 = hidden * inverse2
    gain2 = norm2_gain.astype(jnp.float32)
    normed2_b = (normed2 * gain2).astype(jnp.bfloat16)
    first_row = group_index * quarter
    normed2_q = lax.dynamic_slice_in_dim(normed2_b, first_row, quarter, 0)
    route_q = lax.dynamic_slice_in_dim(routes[0], first_row, quarter, 0)
    logits = jnp.dot(normed2_q, router_weight, preferred_element_type=jnp.float32)
    prob = jax.nn.softmax(logits, -1)
    gate_k = jnp.take_along_axis(prob, route_q, 1)
    slot_ids = route_q * capacity + block_rank(route_q, expert_count)
    slot_hits = (
        slot_ids[:, :, None] == jnp.arange(expert_count * capacity, dtype=jnp.int32)[None, None, :]
    )
    placer = jnp.sum(slot_hits.astype(jnp.bfloat16), 1)
    send_rows = (
        jnp.dot(placer.T, normed2_q, preferred_element_type=jnp.float32)
        .astype(jnp.bfloat16)
        .reshape(group_size, local_experts, capacity, model_width)
    )
    arrived = lax.all_to_all(send_rows, "experts", split_axis=0, concat_axis=0, tiled=True)
    expert_gvals = jnp.einsum(
        "secd,edf->secf", arrived, gate_full, preferred_element_type=jnp.float32
    )
    expert_uvals = jnp.einsum(
        "secd,edf->secf", arrived, up_full, preferred_element_type=jnp.float32
    )
    expert_act = (jax.nn.silu(expert_gvals) * expert_uvals).astype(jnp.bfloat16)
    expert_out = jnp.einsum(
        "secf,efd->secd", expert_act, down_full, preferred_element_type=jnp.float32
    ).astype(jnp.bfloat16)
    returned = lax.all_to_all(
        expert_out, "experts", split_axis=0, concat_axis=0, tiled=True
    ).reshape(expert_count * capacity, model_width)
    picked = returned[slot_ids].astype(jnp.float32)
    routed = jnp.sum(gate_k[:, :, None] * picked, 1)
    shared_sig = jax.nn.sigmoid(
        jnp.dot(normed2_b, shared_gate[:, None], preferred_element_type=jnp.float32)[:, 0]
    )
    shared_gvals = jnp.dot(normed2_b, sgate_full, preferred_element_type=jnp.float32)
    shared_uvals = jnp.dot(normed2_b, sup_full, preferred_element_type=jnp.float32)
    shared_act = (jax.nn.silu(shared_gvals) * shared_uvals).astype(jnp.bfloat16)
    shared_part = jnp.dot(shared_act, sdown_full, preferred_element_type=jnp.float32)
    routed_pad = lax.dynamic_update_slice_in_dim(
        jnp.zeros((row_count, model_width), jnp.float32), routed, first_row, 0
    )
    branch_total = lax.psum(
        (shared_sig[:, None] * shared_part + routed_pad).astype(jnp.bfloat16), "experts"
    ).astype(jnp.float32)
    block_out = (hidden + branch_total).astype(jnp.bfloat16)
    held = lax.optimization_barrier((shard_set, block_out))
    qkv_full, out_full, gate_full, up_full, down_full, sgate_full, sup_full, sdown_full = (
        gather_weights(held[0])
    )
    qkv_flat = qkv_full.reshape(model_width, 3 * head_span)
    grad_float = out_grad[0].astype(jnp.float32)
    grad_q = lax.dynamic_slice_in_dim(grad_float, first_row, quarter, 0)
    dgate_k = jnp.sum(grad_q[:, None, :] * picked, -1)
    weighted = jnp.sum(slot_hits.astype(jnp.float32) * gate_k[:, :, None], 1)
    dsend = (
        jnp.dot(weighted.T, grad_q, precision=PRECISE)
        .astype(jnp.bfloat16)
        .reshape(group_size, local_experts, capacity, model_width)
    )
    darrived = lax.all_to_all(dsend, "experts", split_axis=0, concat_axis=0, tiled=True)
    expert_dact = jnp.einsum(
        "secd,efd->secf", darrived, down_full, preferred_element_type=jnp.float32
    )
    down_grad = jnp.einsum(
        "secf,secd->efd", expert_act, darrived, preferred_element_type=jnp.float32
    )
    expert_dgate = (expert_dact * expert_uvals * silu_grad(expert_gvals)).astype(jnp.bfloat16)
    expert_dup = (expert_dact * jax.nn.silu(expert_gvals)).astype(jnp.bfloat16)
    gate_grad = jnp.einsum(
        "secd,secf->edf", arrived, expert_dgate, preferred_element_type=jnp.float32
    )
    up_grad = jnp.einsum("secd,secf->edf", arrived, expert_dup, preferred_element_type=jnp.float32)
    expert_din = (
        jnp.einsum("secf,edf->secd", expert_dgate, gate_full, preferred_element_type=jnp.float32)
        + jnp.einsum("secf,edf->secd", expert_dup, up_full, preferred_element_type=jnp.float32)
    ).astype(jnp.bfloat16)
    dreturned = lax.all_to_all(
        expert_din, "experts", split_axis=0, concat_axis=0, tiled=True
    ).reshape(expert_count * capacity, model_width)
    dnormed2_q = jnp.dot(placer, dreturned, preferred_element_type=jnp.float32)
    route_hits = (
        route_q[:, :, None] == jnp.arange(expert_count, dtype=jnp.int32)[None, None, :]
    ).astype(jnp.float32)
    dprob = jnp.sum(route_hits * dgate_k[:, :, None], 1)
    dlogit = prob * (dprob - jnp.sum(prob * dprob, -1, keepdims=True))
    router_part = jnp.dot(normed2_q.astype(jnp.float32).T, dlogit, precision=PRECISE)
    dnormed2_q = dnormed2_q + jnp.dot(
        dlogit, router_weight.astype(jnp.float32).T, precision=PRECISE
    )
    shared_dout = (shared_sig[:, None] * grad_float).astype(jnp.bfloat16)
    shared_dact = jnp.dot(shared_dout, sdown_full.T, preferred_element_type=jnp.float32)
    sdown_grad = jnp.dot(shared_act.T, shared_dout, preferred_element_type=jnp.float32)
    shared_dgate = (shared_dact * shared_uvals * silu_grad(shared_gvals)).astype(jnp.bfloat16)
    shared_dup = (shared_dact * jax.nn.silu(shared_gvals)).astype(jnp.bfloat16)
    sgate_grad = jnp.dot(normed2_b.T, shared_dgate, preferred_element_type=jnp.float32)
    sup_grad = jnp.dot(normed2_b.T, shared_dup, preferred_element_type=jnp.float32)
    row_dots = jnp.sum(grad_float * shared_part, -1)
    dnormed2_part = jnp.dot(
        shared_dgate, sgate_full.T, preferred_element_type=jnp.float32
    ) + jnp.dot(shared_dup, sup_full.T, preferred_element_type=jnp.float32)
    dnormed2_part = dnormed2_part + lax.dynamic_update_slice_in_dim(
        jnp.zeros((row_count, model_width), jnp.float32), dnormed2_q, first_row, 0
    )
    dnormed2, row_dots, router_grad = lax.psum((dnormed2_part, row_dots, router_part), "experts")
    coef = shared_sig * (1.0 - shared_sig) * row_dots
    dnormed2 = dnormed2 + coef[:, None] * shared_gate.astype(jnp.float32)[None, :]
    shared_gate_grad = jnp.dot(coef, normed2_b.astype(jnp.float32), precision=PRECISE)
    norm2_grad = jnp.sum(dnormed2 * normed2, 0)
    dscaled2 = dnormed2 * gain2
    dhidden = grad_float + inverse2 * (
        dscaled2 - normed2 * jnp.mean(dscaled2 * normed2, -1, keepdims=True)
    )
    dhidden_b = dhidden.astype(jnp.bfloat16)
    out_grad_part = jnp.dot(attended_flat.T, dhidden_b, preferred_element_type=jnp.float32)
    dattended = jnp.dot(dhidden_b, out_full.T, preferred_element_type=jnp.float32).astype(
        jnp.bfloat16
    )
    dattended3 = dattended.reshape(row_count, heads_here, HEAD_DIM)
    delta = jnp.sum(dattended3.astype(jnp.float32) * attended.astype(jnp.float32), -1)
    zero_state = jnp.zeros((heads_here, row_count, HEAD_DIM), jnp.float32)
    dkey_sum, dvalue_sum = key_grad_fold(
        key_rows,
        value_rows,
        query_first,
        scale,
        (zero_state, zero_state),
        (
            lax.all_gather(
                query.reshape(row_count, head_span).astype(jnp.float32),
                "context",
                axis=0,
                tiled=True,
            ),
            lax.all_gather(dattended.astype(jnp.float32), "context", axis=0, tiled=True),
            lax.all_gather(jnp.transpose(lse_heads), "context", axis=0, tiled=True),
            lax.all_gather(delta, "context", axis=0, tiled=True),
        ),
    )
    dquery_sum = query_grad_fold(
        query,
        dattended3,
        lse_heads,
        jnp.transpose(delta),
        query_first,
        scale,
        zero_state,
        (
            lax.all_gather(key_flat, "context", axis=0, tiled=True),
            lax.all_gather(value_flat, "context", axis=0, tiled=True),
        ),
    )
    dquery = jnp.transpose(dquery_sum, (1, 0, 2))
    dkey = jnp.transpose(dkey_sum, (1, 0, 2))
    dvalue = jnp.transpose(dvalue_sum, (1, 0, 2))
    dquery_raw = dquery * cosine + rotate_back(dquery * sine_part)
    dkey_raw = dkey * cosine + rotate_back(dkey * sine_part)
    dqkv = jnp.stack(
        [
            dquery_raw.reshape(row_count, head_span),
            dkey_raw.reshape(row_count, head_span),
            dvalue.reshape(row_count, head_span),
        ],
        1,
    )
    bias_grad = jnp.sum(dqkv, 0)
    dqkv_b = dqkv.astype(jnp.bfloat16).reshape(row_count, 3 * head_span)
    qkv_grad = jnp.dot(normed1_b.T, dqkv_b, preferred_element_type=jnp.float32).reshape(
        model_width, 3, head_span
    )
    dnormed1 = lax.psum(
        jnp.dot(dqkv_b, qkv_flat.T, preferred_element_type=jnp.float32).astype(jnp.bfloat16),
        "experts",
    ).astype(jnp.float32)
    norm1_grad = jnp.sum(dnormed1 * normed1, 0)
    dscaled1 = dnormed1 * gain1
    tokens_grad = dhidden + inverse1 * (
        dscaled1 - normed1 * jnp.mean(dscaled1 * normed1, -1, keepdims=True)
    )
    small_sums = (
        lax.psum(norm1_grad.astype(jnp.bfloat16), ("dp", "context")).astype(jnp.float32),
        lax.psum(norm2_grad.astype(jnp.bfloat16), ("dp", "context")).astype(jnp.float32),
        lax.psum(router_grad.astype(jnp.bfloat16), ("dp", "context")).astype(jnp.float32),
        lax.psum(shared_gate_grad.astype(jnp.bfloat16), ("dp", "context")).astype(jnp.float32),
        lax.psum(bias_grad.astype(jnp.bfloat16), ("dp", "context")).astype(jnp.float32),
    )
    large_sums = (
        lax.psum_scatter(
            qkv_grad.astype(jnp.bfloat16), ("dp", "context"), scatter_dimension=0, tiled=True
        ).astype(jnp.float32),
        lax.psum_scatter(
            out_grad_part.astype(jnp.bfloat16), ("dp", "context"), scatter_dimension=1, tiled=True
        ).astype(jnp.float32),
        lax.psum_scatter(
            gate_grad.astype(jnp.bfloat16), ("dp", "context"), scatter_dimension=1, tiled=True
        ).astype(jnp.float32),
        lax.psum_scatter(
            up_grad.astype(jnp.bfloat16), ("dp", "context"), scatter_dimension=1, tiled=True
        ).astype(jnp.float32),
        lax.psum_scatter(
            down_grad.astype(jnp.bfloat16), ("dp", "context"), scatter_dimension=2, tiled=True
        ).astype(jnp.float32),
        lax.psum_scatter(
            sgate_grad.astype(jnp.bfloat16), ("dp", "context"), scatter_dimension=0, tiled=True
        ).astype(jnp.float32),
        lax.psum_scatter(
            sup_grad.astype(jnp.bfloat16), ("dp", "context"), scatter_dimension=0, tiled=True
        ).astype(jnp.float32),
        lax.psum_scatter(
            sdown_grad.astype(jnp.bfloat16), ("dp", "context"), scatter_dimension=1, tiled=True
        ).astype(jnp.float32),
    )
    return (
        block_out[None],
        tokens_grad[None],
        small_sums[0],
        large_sums[0],
        small_sums[4],
        large_sums[1],
        small_sums[1],
        small_sums[2],
        large_sums[2],
        large_sums[3],
        large_sums[4],
        small_sums[3],
        large_sums[5],
        large_sums[6],
        large_sums[7],
    )


def own_half_first(value):
    half = value.shape[-1] // 2
    turned = jnp.concatenate([value[..., half:], value[..., :half]], -1)
    return jnp.where(lax.axis_index("dp") == 0, value, turned)


def dot_nn(left, right):
    return jnp.dot(left, right, preferred_element_type=jnp.float32)


def dot_nt(left, right):
    return lax.dot_general(
        left, right, (((1,), (1,)), ((), ())), preferred_element_type=jnp.float32
    )


def dot_tn(left, right):
    return lax.dot_general(
        left, right, (((0,), (0,)), ((), ())), preferred_element_type=jnp.float32
    )


MESH = pl.DeviceIdType.MESH
DMA = pltpu.SemaphoreType.DMA


def remote(source, target, send_sem, recv_sem, device):
    return pltpu.make_async_remote_copy(
        src_ref=source,
        dst_ref=target,
        send_sem=send_sem,
        recv_sem=recv_sem,
        device_id=device,
        device_id_type=MESH,
    )


def rows_at(ref, start, size):
    return ref.at[pl.ds(pl.multiple_of(start, 16), size), :]


def lanes_at(ref, start, size):
    return ref.at[:, pl.ds(pl.multiple_of(start, 128), size)]


def by_width(device, narrow, body):
    if narrow is None:
        body(False)
    elif isinstance(device, int):
        body(device == narrow)
    else:

        @pl.when(device == narrow)
        def _():
            body(True)

        @pl.when(device != narrow)
        def _():
            body(False)


class Spot:
    def __init__(self):
        self.parts = lax.axis_size("context")
        self.place, self.group = lax.axis_index("context"), lax.axis_index("experts")
        self.twin = {"dp": 1 - lax.axis_index("dp")}
        self.across = lax.rem(self.group + 2, 4)
        self.beside = self.group + 1 - 2 * lax.rem(self.group, 2)
        self.corner = lax.rem(self.beside + 2, 4)
        self.has_left, self.has_right = self.place > 0, self.place < self.parts - 1

    def greet(self, whole_line, twins):
        barrier = pltpu.get_barrier_semaphore()
        devices = [{"experts": self.across}, {"experts": self.beside}]
        if twins:
            devices.append(self.twin)
        for device in devices:
            pl.semaphore_signal(barrier, inc=1, device_id=device, device_id_type=MESH)
        count = len(devices)
        if whole_line:
            for gap in range(1, self.parts):
                device = {"context": lax.rem(self.place + gap, self.parts)}
                pl.semaphore_signal(barrier, inc=1, device_id=device, device_id_type=MESH)
            pl.semaphore_wait(barrier, count + self.parts - 1)
        else:
            for step, there in ((-1, self.has_left), (1, self.has_right)):

                @pl.when(there)
                def _():
                    device = {"context": self.place + step}
                    pl.semaphore_signal(barrier, inc=1, device_id=device, device_id_type=MESH)

            ends = jnp.where(self.has_left & self.has_right, 0, 1)
            pl.semaphore_wait(barrier, count + 2 - ends)

    def far_first(self):
        upper = self.place // (self.parts // 2)
        return [3 * (1 - upper), 2 - upper, 1 + 4 * upper - self.place, self.place]

    def others(self, gap, body):
        @pl.when(self.place >= gap)
        def _():
            body(self.place - gap)

        @pl.when(self.place + gap < self.parts)
        def _():
            body(self.place + gap)


class Share:
    def __init__(self, spot, own, out, sems):
        self.spot, self.own, self.out = spot, own, out
        self.local_sem, self.right_s, self.left_s, self.line_r, self.across_s, self.across_r, self.beside_s, self.beside_r = sems

    @staticmethod
    def sems(parts):
        return [DMA, DMA((parts,)), DMA((parts,)), DMA((parts,)), DMA((parts,)), DMA((parts,)), DMA((2 * parts,)), DMA((2 * parts,))]

    def block(self, part, column):
        rows = self.own.shape[0]
        return rows_at(self.out, (part * 4 + column) * rows, rows)

    def to_right(self, part, source):
        s = self.spot
        return remote(source, self.block(part, s.group), self.right_s.at[part], self.line_r.at[part], {"context": s.place + 1})

    def to_left(self, part, source):
        s = self.spot
        return remote(source, self.block(part, s.group), self.left_s.at[part], self.line_r.at[part], {"context": s.place - 1})

    def to_across(self, part, source):
        s = self.spot
        return remote(source, self.block(part, s.group), self.across_s.at[part], self.across_r.at[part], {"experts": s.across})

    def to_beside(self, part, column, slot, source):
        s = self.spot
        return remote(source, self.block(part, column), self.beside_s.at[slot], self.beside_r.at[slot], {"experts": s.beside})

    def begin(self):
        s = self.spot

        @pl.when(s.has_right)
        def _():
            self.to_right(s.place, self.own).start()

        @pl.when(s.has_left)
        def _():
            self.to_left(s.place, self.own).start()

        self.to_across(s.place, self.own).start()
        self.to_beside(s.place, s.group, s.place, self.own).start()
        self.local().start()

    def local(self):
        return pltpu.make_async_copy(self.own, self.block(self.spot.place, self.spot.group), self.local_sem)

    def pass_on(self, part):
        s = self.spot
        self.to_across(part, self.block(part, s.group)).wait_recv()
        self.to_beside(part, s.across, s.parts + part, self.block(part, s.across)).start()

    def arrival(self, part, onward, there):
        s = self.spot
        mine = self.block(part, s.group)
        self.to_right(part, mine).wait_recv()

        @pl.when(there)
        def _():
            onward(part, mine).start()

        self.to_across(part, mine).start()
        self.to_beside(part, s.group, part, mine).start()

    def step(self, gap):
        s = self.spot

        @pl.when(s.place >= gap)
        def _():
            self.arrival(s.place - gap, self.to_right, s.has_right)

        @pl.when(s.place + gap < s.parts)
        def _():
            self.arrival(s.place + gap, self.to_left, s.has_left)

        if gap == 1:
            self.pass_on(s.place)
        else:
            s.others(gap - 1, self.pass_on)

    def end(self):
        s = self.spot
        s.others(s.parts - 1, self.pass_on)
        self.local().wait()
        for part in range(s.parts):
            self.to_beside(part, s.beside, part, self.own).wait_recv()
            self.to_beside(part, s.beside, s.parts + part, self.own).wait_recv()
            self.to_across(part, self.own).wait_send()
            self.to_beside(part, s.group, part, self.own).wait_send()
            self.to_beside(part, s.group, s.parts + part, self.own).wait_send()

            @pl.when(s.has_right & (part <= s.place))
            def _():
                self.to_right(part, self.own).wait_send()

            @pl.when(s.has_left & (part >= s.place))
            def _():
                self.to_left(part, self.own).wait_send()


class Sum:
    def __init__(self, spot, part_ref, out, scratch):
        self.spot, self.part_ref, self.out = spot, part_ref, out
        (self.beside_buf, self.across_out, self.across_buf, self.line_out, self.left_buf, self.right_buf,
         self.beside_s, self.beside_r, self.across_s, self.across_r, self.right_s, self.left_s, self.from_left, self.from_right) = scratch
        self.order = spot.far_first()

    @staticmethod
    def scratch(parts, rows, width):
        one = pltpu.VMEM((parts, rows, width), jnp.bfloat16)
        two = pltpu.VMEM((2 * parts, rows, width), jnp.bfloat16)
        return [two, one, one, one, one, one, DMA((2 * parts,)), DMA((2 * parts,))] + [DMA((parts,))] * 6

    def base(self, part, column):
        rows = self.out.shape[0]
        return pl.multiple_of((part * 4 + column) * rows, rows)

    def to_beside(self, part, column, slot):
        source = self.part_ref.at[pl.ds(self.base(part, column), self.out.shape[0]), :]
        return remote(source, self.beside_buf.at[slot], self.beside_s.at[slot], self.beside_r.at[slot], {"experts": self.spot.beside})

    def to_across(self, part):
        return remote(self.across_out.at[part], self.across_buf.at[part], self.across_s.at[part], self.across_r.at[part], {"experts": self.spot.across})

    def to_right(self, part):
        return remote(self.line_out.at[part], self.left_buf.at[part], self.right_s.at[part], self.from_left.at[part], {"context": self.spot.place + 1})

    def to_left(self, part):
        return remote(self.line_out.at[part], self.right_buf.at[part], self.left_s.at[part], self.from_right.at[part], {"context": self.spot.place - 1})

    def chunks(self, body):
        step = 16

        def one(index, carry):
            start = pl.multiple_of(index * step, step)
            body(pl.ds(start, step), start, step)
            return carry

        lax.fori_loop(0, self.out.shape[0] // step, one, 0)

    def mine(self, base, start, step):
        return self.part_ref[pl.ds(pl.multiple_of(base + start, step), step), :].astype(jnp.float32)

    def begin(self):
        s = self.spot
        for part in self.order:
            self.to_beside(part, s.corner, s.parts + part).start()
        for part in self.order:
            self.to_beside(part, s.beside, part).start()

    def cross(self, index):
        s, part = self.spot, self.order[index]
        self.to_beside(part, s.corner, s.parts + part).wait_recv()
        base = self.base(part, s.across)

        def add(at, start, step):
            total = self.mine(base, start, step) + self.beside_buf[s.parts + part, at, :].astype(jnp.float32)
            self.across_out[part, at, :] = total.astype(jnp.bfloat16)

        self.chunks(add)
        self.to_across(part).start()

    def line(self, index):
        s, part = self.spot, self.order[index]
        self.to_beside(part, s.beside, part).wait_recv()
        self.to_across(part).wait_recv()
        base = self.base(part, s.group)
        f32 = jnp.float32

        def total(at, start, step):
            return self.mine(base, start, step) + self.beside_buf[part, at, :].astype(f32) + self.across_buf[part, at, :].astype(f32)

        def send(buf):
            def add(at, start, step):
                value = total(at, start, step)
                if buf is not None:
                    value = value + buf[part, at, :].astype(f32)
                self.line_out[part, at, :] = value.astype(jnp.bfloat16)

            self.chunks(add)

        if index < s.parts - 1:
            goes_right = part > s.place
            goes_left = jnp.logical_not(goes_right)

            @pl.when(goes_right & s.has_left)
            def _():
                self.to_right(part).wait_recv()
                send(self.left_buf)

            @pl.when(goes_left & s.has_right)
            def _():
                self.to_left(part).wait_recv()
                send(self.right_buf)

            @pl.when((goes_right & jnp.logical_not(s.has_left)) | (goes_left & jnp.logical_not(s.has_right)))
            def _():
                send(None)

            @pl.when(goes_right)
            def _():
                self.to_right(part).start()

            @pl.when(goes_left)
            def _():
                self.to_left(part).start()
        else:

            def keep(at, start, step):
                self.out[at, :] = total(at, start, step)

            self.chunks(keep)
            for there, copy, buf in ((s.has_left, self.to_right, self.left_buf), (s.has_right, self.to_left, self.right_buf)):

                @pl.when(there)
                def _():
                    copy(part).wait_recv()

                    def add(at, start, step):
                        self.out[at, :] = self.out[at, :] + buf[part, at, :].astype(f32)

                    self.chunks(add)

    def end(self):
        s = self.spot
        for part in range(s.parts):
            self.to_beside(part, s.corner, s.parts + part).wait_send()
            self.to_beside(part, s.beside, part).wait_send()
            self.to_across(part).wait_send()

            @pl.when(part > s.place)
            def _():
                self.to_right(part).wait_send()

            @pl.when(part < s.place)
            def _():
                self.to_left(part).wait_send()


class Move:
    def __init__(self, spot, items, sems):
        self.spot, self.items = spot, items
        self.line_s, self.line_r, self.twin_s, self.twin_r, self.local_sem = sems

    @staticmethod
    def sems(count, parts):
        return [DMA((count * parts,))] * 4 + [DMA((count,))]

    def fit(self, number, device, body):
        by_width(device, self.items[number]["short"], body)

    def to(self, number, target, source, short):
        s, item = self.spot, self.items[number]
        sems = self.line_s.at[number * s.parts + target], self.line_r.at[number * s.parts + source]
        return remote(item["src"](target, short), item["dst"](0, source, short), *sems, {"context": target})

    def on(self, number, source, short, view=None):
        s, item = self.spot, self.items[number]
        slot = number * s.parts + source
        view = item["dst"](0, source, short) if view is None else view
        return remote(view, item["dst"](1, source, short), self.twin_s.at[slot], self.twin_r.at[slot], s.twin)

    def local(self, number, short):
        s, item = self.spot, self.items[number]
        return pltpu.make_async_copy(item["src"](s.place, short), item["dst"](0, s.place, short), self.local_sem.at[number])

    def own(self, number):
        s, item = self.spot, self.items[number]

        def one(short):
            self.on(number, s.place, short, item["src"](s.place, short)).start()
            self.local(number, short).start()

        self.fit(number, s.place, one)

    def send_gap(self, number, gap):
        s = self.spot

        def one(target):
            self.fit(number, target, lambda short: self.to(number, target, s.place, short).start())

        s.others(gap, one)

    def send(self, number):
        for gap in range(self.spot.parts - 1, 0, -1):
            self.send_gap(number, gap)

    def forward(self, number, gap):
        s = self.spot

        def one(source):
            def step(short):
                self.to(number, s.place, source, short).wait_recv()
                self.on(number, source, short).start()

            self.fit(number, s.place, step)

        s.others(gap, one)

    def ready(self, number):
        s = self.spot

        def one(short):
            self.local(number, short).wait()
            for part in range(s.parts):
                self.on(number, part, short).wait_recv()

        self.fit(number, s.place, one)

    def sent(self):
        s = self.spot
        for number in range(len(self.items)):

            def one(short):
                for part in range(s.parts):
                    self.on(number, part, short).wait_send()

            self.fit(number, s.place, one)
            for part in range(s.parts):

                @pl.when(part != s.place)
                def _():
                    self.fit(number, part, lambda short: self.to(number, part, s.place, short).wait_send())

    def end(self):
        for number in range(len(self.items)):
            self.ready(number)
        self.sent()


class Return:
    def __init__(self, spot, items, got, mine, sems):
        self.spot, self.items, self.got, self.mine_buf = spot, items, got, mine
        self.twin_s, self.twin_r, self.load, self.line_s, self.line_r, self.local_sem = sems
        self.order = spot.far_first()
        self.bases = []
        for item in items:
            self.bases.append(self.bases[-1][1] if self.bases else 0)
            self.bases[-1] = (self.bases[-1], self.bases[-1] + len(item["pieces"]) * spot.parts)

    @staticmethod
    def scratch(shapes, pieces, parts):
        count = len(shapes)
        buf = [pltpu.VMEM((parts,) + shape, jnp.bfloat16) for shape in shapes]
        sems = [DMA((count * parts,))] * 3 + [DMA((sum(pieces) * parts,))] * 2 + [DMA((sum(pieces),))]
        return buf + buf + sems

    def swap(self, number, part):
        item, slot = self.items[number], number * self.spot.parts + part
        return remote(item["block"](1, part), self.got[number].at[part], self.twin_s.at[slot], self.twin_r.at[slot], self.spot.twin)

    def fetch(self, number, part):
        item, slot = self.items[number], number * self.spot.parts + part
        return pltpu.make_async_copy(item["block"](0, part), self.mine_buf[number].at[part], self.load.at[slot])

    def start_one(self, number, index):
        self.swap(number, self.order[index]).start()
        self.fetch(number, self.order[index]).start()

    def start(self, number):
        for index in range(self.spot.parts):
            self.start_one(number, index)

    def piece(self, number, which, target, source, short):
        s = self.spot
        cut, out = self.items[number]["pieces"][which]
        slot = self.bases[number][0] + which * s.parts
        return remote(cut(self.mine_buf[number].at[target], short), out(source, short), self.line_s.at[slot + target], self.line_r.at[slot + source], {"context": target})

    def keep(self, number, which, short):
        s = self.spot
        cut, out = self.items[number]["pieces"][which]
        slot = self.bases[number][0] // s.parts + which
        return pltpu.make_async_copy(cut(self.mine_buf[number].at[s.place], short), out(s.place, short), self.local_sem.at[slot])

    def fit(self, number, source, body):
        by_width(source, self.items[number].get("short"), body)

    def reduce(self, number, index):
        s, part = self.spot, self.order[index]
        item = self.items[number]
        self.swap(number, part).wait_recv()
        self.fetch(number, part).wait()
        mine, got = self.mine_buf[number], self.got[number]
        rows, step = mine.shape[1], 32

        def one(at, carry):
            span = pl.ds(pl.multiple_of(at * step, step), step)
            total = mine[part, span, :].astype(jnp.float32) + got[part, span, :].astype(jnp.float32)
            mine[part, span, :] = total.astype(jnp.bfloat16)
            return carry

        lax.fori_loop(0, rows // step, one, 0)
        for which in range(len(item["pieces"])):
            if index < s.parts - 1:
                self.fit(number, s.place, lambda short: self.piece(number, which, part, s.place, short).start())
            else:
                self.fit(number, s.place, lambda short: self.keep(number, which, short).start())

    def end(self):
        s = self.spot
        for number, item in enumerate(self.items):
            for part in range(s.parts):
                self.swap(number, part).wait_send()
                for which in range(len(item["pieces"])):

                    @pl.when(part != s.place)
                    def _():
                        self.fit(number, s.place, lambda short: self.piece(number, which, part, s.place, short).wait_send())
                        self.fit(number, part, lambda short: self.piece(number, which, s.place, part, short).wait_recv())

            for which in range(len(item["pieces"])):
                self.fit(number, s.place, lambda short: self.keep(number, which, short).wait())


class Grads:
    def __init__(self, rows, cotangents, dup, act, up_out, down_out, up_buf, down_buf, up_s, down_s):
        self.rows, self.cotangents, self.dup, self.act = rows, cotangents, dup, act
        self.up_out, self.down_out, self.up_buf, self.down_buf = up_out, down_out, up_buf, down_buf
        self.up_s, self.down_s = up_s, down_s
        self.step = 256

    @staticmethod
    def scratch():
        up, down = pltpu.VMEM((2, 256, 2 * WINDOW), jnp.bfloat16), pltpu.VMEM((2, WINDOW, 256), jnp.bfloat16)
        return [up, down, DMA((2,)), DMA((2,))]

    def copies(self, index):
        at = pl.ds(pl.multiple_of(index * self.step, self.step), self.step)
        slot = lax.rem(index, 2)
        return (
            lambda: pltpu.make_async_copy(self.up_buf.at[slot], self.up_out.at[at, :], self.up_s.at[slot]),
            lambda: pltpu.make_async_copy(self.down_buf.at[slot], self.down_out.at[:, at], self.down_s.at[slot]),
        )

    def run(self):
        count = self.cotangents.shape[1] // self.step

        def one(index, carry):
            up_copy, down_copy = self.copies(index)

            @pl.when(index >= 2)
            def _():
                up_copy().wait()
                down_copy().wait()

            slot = lax.rem(index, 2)
            at = pl.multiple_of(index * self.step, self.step)
            up = dot_tn(self.rows[:, pl.ds(at, self.step)], self.dup[...])
            self.up_buf[slot] = up.astype(jnp.bfloat16)
            down = dot_tn(self.act[...], self.cotangents[:, pl.ds(at, self.step)])
            self.down_buf[slot] = down.astype(jnp.bfloat16)
            up_copy().start()
            down_copy().start()
            return carry

        lax.fori_loop(0, count, one, 0)
        for index in (count - 2, count - 1):
            for copy in self.copies(index):
                copy().wait()


def comm_call(kernel, number, name, out_shape, out_specs, in_specs, scratch, bytes_moved):
    return pl.pallas_call(
        kernel,
        out_shape=out_shape,
        in_specs=in_specs,
        out_specs=out_specs,
        scratch_shapes=scratch,
        compiler_params=pltpu.CompilerParams(collective_id=number, has_side_effects=True),
        cost_estimate=pl.CostEstimate(flops=0, bytes_accessed=bytes_moved, transcendentals=0),
        name=name,
    )


IN_VMEM = pl.BlockSpec(memory_space=pltpu.VMEM)
IN_PLACE = pl.BlockSpec(memory_space=pl.ANY)
WINDOW = 384


SPARE = 128


def narrow_of(k):
    return 0 if k % 2 else 3


def window_of(k, index, narrow):
    if narrow_of(k) == 0:
        return (0, WINDOW - SPARE, 0) if narrow else (index * WINDOW - SPARE, WINDOW, 0)
    return (index * WINDOW, WINDOW - SPARE, SPARE) if narrow else (index * WINDOW, WINDOW, 0)


def first_unit(value):
    return value if isinstance(value, int) else pl.multiple_of(value, SPARE)


def units_at(ref, k, index, narrow, axis, base=0):
    start, size, inside = window_of(k, index, narrow)
    start = first_unit(start) if base is None else base + inside
    return ref.at[pl.ds(start, size), :] if axis == 0 else ref.at[:, pl.ds(start, size)]


def turn(value, cosine, sine_part):
    return value * cosine + pltpu.roll(value, HEAD_DIM // 2, 1) * sine_part


def turn_tables(facts):
    both = facts[:, :HEAD_DIM].astype(jnp.float32) + facts[:, HEAD_DIM:].astype(jnp.float32)
    swapped = pltpu.roll(both, HEAD_DIM // 2, 1)
    low = lax.broadcasted_iota(jnp.int32, (1, HEAD_DIM), 1) < HEAD_DIM // 2
    return jnp.where(low, both, swapped), jnp.where(low, -swapped, both)


def attention_first(value, grad, qkv_in, out_weight, bias, shared_down, expert_down, number):
    parts = lax.axis_size("context")
    rows, wide = value.shape
    block, span = qkv_in.shape[1], 3 * HEAD_DIM
    head, lanes = out_weight.shape[0] // parts, out_weight.shape[1]
    width, length = 2 * parts * lanes, rows * parts * 4
    count = 1 + expert_down.shape[0]
    step = 256
    scale = HEAD_DIM ** (-0.5)
    f32, bf16 = jnp.float32, jnp.bfloat16
    sets = [
        [
            pltpu.VMEM((length, wide), bf16),
            pltpu.VMEM((2 * parts * block, span), bf16),
            pltpu.VMEM((head, width), bf16),
            pltpu.VMEM((length, width), bf16),
            DMA((3,)),
        ],
        Share.sems(parts),
        Move.sems(4 + count, parts),
        Sum.scratch(parts, rows, width),
        Share.sems(parts),
    ]

    def kernel(own_ref, grad_ref, qkv_ref, outw_ref, bias_ref, shared_ref, expert_ref,
               all_hbm, grad_all, wqkv_hbm, wout_hbm, wd_ref, q_ref, k_ref, v_ref, att_ref, lse_ref, sum_ref, *scratch):
        scratch, split = list(scratch), []
        for one in sets:
            split.append(scratch[: len(one)])
            scratch = scratch[len(one) :]
        all_ref, wqkv_ref, wout_ref, part_ref, keep = split[0]
        spot = Spot()
        share = Share(spot, own_ref, all_ref, split[1])
        grads = Share(spot, grad_ref, grad_all, split[4])
        items = [
            {
                "src": lambda target, short, which=which: lanes_at(qkv_ref.at[which], target * HEAD_DIM, HEAD_DIM),
                "dst": lambda side, source, short, which=which: rows_at(
                    wqkv_ref.at[:, pl.ds(which * HEAD_DIM, HEAD_DIM)], (side * parts + source) * block, block
                ),
                "short": None,
            }
            for which in range(3)
        ]
        items += [
            {
                "src": lambda target, short: rows_at(outw_ref, target * head, head),
                "dst": lambda side, source, short: lanes_at(wout_ref, (side * parts + source) * lanes, lanes),
                "short": None,
            },
        ]

        def down(k):
            ref = shared_ref if k == 0 else expert_ref.at[k - 1]
            return {
                "src": lambda target, short: units_at(ref, k, target, short, 0, None),
                "dst": lambda side, source, short: lanes_at(
                    units_at(wd_ref, k, 0, short, 0, k * WINDOW), (side * parts + source) * lanes, lanes
                ),
                "short": narrow_of(k),
            }

        move = Move(spot, items + [down(k) for k in range(count)], split[2])
        summed = Sum(spot, part_ref, sum_ref, split[3])
        copies = [
            pltpu.make_async_copy(source, target, keep.at[index])
            for index, (source, target) in enumerate(((all_ref, all_hbm), (wqkv_ref, wqkv_hbm), (wout_ref, wout_hbm)))
        ]

        def project(index, carry):
            at = pl.ds(pl.multiple_of(index * step, step), step)
            qkv = jnp.dot(all_ref[at, :width], wqkv_ref[...], preferred_element_type=f32) + bias_ref[...]
            cosine, sine_part = turn_tables(all_ref[at, width:])
            q_ref[at, :] = turn(qkv[:, :HEAD_DIM], cosine, sine_part).astype(bf16)
            k_ref[at, :] = turn(qkv[:, HEAD_DIM : 2 * HEAD_DIM], cosine, sine_part).astype(bf16)
            v_ref[at, :] = qkv[:, 2 * HEAD_DIM :].astype(bf16)
            return carry

        def attend(index, carry):
            start = pl.multiple_of(index * step, step)
            at = pl.ds(start, step)
            scores = dot_nt(q_ref[at, :], k_ref[...]) * scale
            query_index = start + lax.broadcasted_iota(jnp.int32, scores.shape, 0)
            allowed = lax.broadcasted_iota(jnp.int32, scores.shape, 1) <= query_index
            row_max = jnp.max(jnp.where(allowed, scores, MASKED), -1, keepdims=True)
            weights = jnp.where(allowed, jnp.exp(scores - row_max), 0.0)
            row_sum = jnp.sum(weights, -1, keepdims=True)
            attended = (jnp.dot(weights.astype(bf16), v_ref[...], preferred_element_type=f32) / row_sum).astype(bf16)
            att_ref[at, :] = attended
            lse_ref[at, :] = jnp.broadcast_to(row_max + jnp.log(row_sum), (step, HEAD_DIM))
            part_ref[at, :] = jnp.dot(attended, wout_ref[...], preferred_element_type=f32).astype(bf16)
            return carry

        spot.greet(True, True)
        share.begin()
        for number in range(len(move.items)):
            move.own(number)
        move.send(0)
        share.step(1)
        move.send(1)
        share.step(2)
        move.send(2)
        share.step(3)
        move.send(3)
        move.send(4)
        for number in range(4):
            for gap in (1, 2, 3):
                move.forward(number, gap)
        share.end()
        grads.begin()
        copies[0].start()
        for number in range(3):
            move.ready(number)
        copies[1].start()
        lax.fori_loop(0, length // step, project, 0)
        move.ready(3)
        copies[2].start()
        grads.step(1)
        for number in range(5, len(move.items)):
            move.send(number)
        lax.fori_loop(0, length // step, attend, 0)
        summed.begin()
        for gap in (1, 2, 3):
            move.forward(4, gap)
        grads.step(2)
        for index in range(parts):
            summed.cross(index)
        for number in range(5, len(move.items)):
            for gap in (1, 2, 3):
                move.forward(number, gap)
        grads.step(3)
        for index in range(parts):
            summed.line(index)
        grads.end()
        summed.end()
        for number in range(4, len(move.items)):
            move.ready(number)
        move.sent()
        for copy in copies:
            copy.wait()

    heads = jax.ShapeDtypeStruct((length, HEAD_DIM), bf16)
    return comm_call(
        kernel,
        number,
        "attention_first",
        [
            jax.ShapeDtypeStruct((length, wide), bf16),
            jax.ShapeDtypeStruct((length, width), bf16),
            jax.ShapeDtypeStruct((2 * parts * block, span), bf16),
            jax.ShapeDtypeStruct((head, width), bf16),
            jax.ShapeDtypeStruct((count * WINDOW, width), bf16),
            heads,
            heads,
            heads,
            heads,
            jax.ShapeDtypeStruct((length, HEAD_DIM), f32),
            jax.ShapeDtypeStruct((rows, width), f32),
        ],
        [IN_PLACE] * 5 + [IN_VMEM] * 6,
        [IN_VMEM, IN_VMEM, IN_PLACE, IN_PLACE, IN_VMEM, IN_PLACE, IN_PLACE],
        [one for group in sets for one in group],
        250_000_000,
    )(value, grad, qkv_in, out_weight, bias, shared_down, expert_down)


def share_move_compute(value, grad_all, shared_gate, shared_up, expert_gate, expert_up, wd, number):
    parts = lax.axis_size("context")
    rows, wide = value.shape
    width = wd.shape[1]
    block = shared_gate.shape[0]
    stacks = 1 + expert_gate.shape[0]
    count = 2 * stacks
    length = rows * parts * 4
    experts = (stacks - 1) * 4
    step = 256
    f32, bf16 = jnp.float32, jnp.bfloat16
    share_sems, move_sems, grad_scratch = Share.sems(parts), Move.sems(count, parts), Grads.scratch()
    back_scratch = Return.scratch([(block, 2 * WINDOW)], [2], parts)
    scratch = [
        pltpu.VMEM((length, wide), bf16),
        pltpu.VMEM((length, width), bf16),
        pltpu.VMEM((2 * parts * block, count * WINDOW), bf16),
        pltpu.VMEM(wd.shape, bf16),
        pltpu.VMEM((length, width), f32),
        pltpu.VMEM((length, width), f32),
        pltpu.VMEM((length, 128), f32),
        pltpu.VMEM((length, 2 * WINDOW), bf16),
        pltpu.VMEM((length, 4 * WINDOW), bf16),
        pltpu.VMEM((length, WINDOW), f32),
        pltpu.VMEM((length, WINDOW), f32),
        pltpu.VMEM((2, step, width + 128), bf16),
        pltpu.VMEM((2, step, width), bf16),
        DMA((3,)),
        DMA((stacks,)),
        DMA((stacks,)),
        DMA((length // step,)),
        DMA((length // step,)),
    ]

    def kernel(own_ref, grad_hbm, sg_ref, su_ref, eg_ref, eu_ref, wd_hbm, both_hbm, send_hbm, branch_hbm, dup_hbm, act_hbm, upg_hbm, downg_hbm, gate_out, up_out, *rest):
        both, grads_ref, wgu, wd_ref, dx_acc, out_acc, dot_acc, act_ref, dup_ref, raw_ref, gate_ref, send_buf, branch_buf, load, act_s, dup_s, send_s, branch_s = rest[: len(scratch)]
        grad_refs, sems = rest[len(scratch) : len(scratch) + 4], rest[len(scratch) + 4 :]
        back_refs, sems = sems[: len(back_scratch)], sems[len(back_scratch) :]
        spot = Spot()
        share = Share(spot, own_ref, both, sems[: len(share_sems)])

        def item(number):
            k = number // 2
            shared, expert = (sg_ref, eg_ref) if number % 2 == 0 else (su_ref, eu_ref)
            ref = shared if k == 0 else expert.at[k - 1]
            return {
                "src": lambda target, short: units_at(ref, k, target, short, 1, None),
                "dst": lambda side, source, short: rows_at(
                    units_at(wgu, k, 0, short, 1, number * WINDOW), (side * parts + source) * block, block
                ),
                "short": narrow_of(k),
            }

        move = Move(spot, [item(number) for number in range(count)], sems[len(share_sems) :])
        weights = pltpu.make_async_copy(wd_hbm, wd_ref, load.at[0])
        keep = pltpu.make_async_copy(both, both_hbm, load.at[1])
        cotangents = pltpu.make_async_copy(grad_hbm, grads_ref, load.at[2])
        column = lax.broadcasted_iota(jnp.int32, (1, 128), 1)
        pieces = length // step

        def send_out(index):
            at = pl.ds(pl.multiple_of(index * step, step), step)
            return pltpu.make_async_copy(send_buf.at[lax.rem(index, 2)], send_hbm.at[at, :], send_s.at[index])

        def branch_out(index):
            at = pl.ds(pl.multiple_of(index * step, step), step)
            return pltpu.make_async_copy(branch_buf.at[lax.rem(index, 2)], branch_hbm.at[at, :], branch_s.at[index])

        back = Return(
            spot, [up_item(upg_hbm, 0, 0, gate_out, up_out, block, parts)], back_refs[:1], back_refs[1:2], back_refs[2:]
        )

        def slots(k):
            return pl.ds(2 * (k % 2) * WINDOW, 2 * WINDOW), pl.ds((k % 2) * WINDOW, WINDOW)

        def act_out():
            return pltpu.make_async_copy(act_ref.at[:, slots(stacks - 1)[1]], act_hbm, act_s.at[0])

        def dup_out():
            return pltpu.make_async_copy(dup_ref.at[:, slots(stacks - 1)[0]], dup_hbm, dup_s.at[0])

        def gradients(k):
            up, down = pl.ds(2 * k * WINDOW, 2 * WINDOW), pl.ds(k * WINDOW, WINDOW)
            dup_slot, act_slot = slots(k)
            Grads(both, grads_ref, dup_ref.at[:, dup_slot], act_ref.at[:, act_slot], upg_hbm.at[:, up], downg_hbm.at[down, :], *grad_refs).run()

        def compute(k, halfway):
            up, down = pl.ds(2 * k * WINDOW, 2 * WINDOW), pl.ds(k * WINDOW, WINDOW)
            dup_slot, act_slot = slots(k)
            at = experts if k == 0 else spot.group * (stacks - 1) + k - 1
            here = jnp.where(column == at, 1.0, 0.0)
            both_parts = jnp.where((column == at) | (column == at + 64), 1.0, 0.0)

            def one(index, carry):
                pl.when(index == pieces // 2)(halfway)
                rows_here = pl.ds(pl.multiple_of(index * step, step), step)
                if k == stacks - 1:
                    raw, g_vals = raw_ref[rows_here, :], gate_ref[rows_here, :]
                    u_vals = jnp.dot(
                        both[rows_here, :width], wgu[:, pl.ds((2 * k + 1) * WINDOW, WINDOW)], preferred_element_type=f32
                    )
                else:
                    vals = jnp.dot(both[rows_here, :width], wgu[:, up], preferred_element_type=f32)
                    raw = dot_nt(grads_ref[rows_here, :], wd_ref[down, :])
                    g_vals, u_vals = vals[:, :WINDOW], vals[:, WINDOW:]
                coef = jnp.sum(both[rows_here, width:].astype(f32) * both_parts, -1, keepdims=True)
                sig_g = jax.nn.sigmoid(g_vals)
                silu_g = g_vals * sig_g
                act = silu_g * u_vals
                dots = jnp.sum(raw * act, -1, keepdims=True) * here
                act_ref[rows_here, act_slot] = (act * coef).astype(bf16)
                dact = raw * coef
                dup_ref[rows_here, pl.ds(2 * (k % 2) * WINDOW, WINDOW)] = (
                    dact * u_vals * (sig_g * (1.0 + g_vals * (1.0 - sig_g)))
                ).astype(bf16)
                dup_ref[rows_here, pl.ds((2 * (k % 2) + 1) * WINDOW, WINDOW)] = (dact * silu_g).astype(bf16)
                out_part = jnp.dot(act_ref[rows_here, act_slot], wd_ref[down, :], preferred_element_type=f32)
                dx_part = dot_nt(dup_ref[rows_here, dup_slot], wgu[:, up])
                if k == 0:
                    out_acc[rows_here, :] = out_part
                    dx_acc[rows_here, :] = dx_part
                    dot_acc[rows_here, :] = dots
                elif k < stacks - 1:
                    out_acc[rows_here, :] += out_part
                    dx_acc[rows_here, :] += dx_part
                    dot_acc[rows_here, :] += dots
                else:

                    @pl.when(index >= 2)
                    def _():
                        send_out(index - 2).wait()
                        branch_out(index - 2).wait()

                    slot = lax.rem(index, 2)
                    branch_buf[slot] = (out_acc[rows_here, :] + out_part).astype(bf16)
                    send_buf[slot, :, :width] = (dx_acc[rows_here, :] + dx_part).astype(bf16)
                    send_buf[slot, :, width:] = (dot_acc[rows_here, :] + dots).astype(bf16)
                    send_out(index).start()
                    branch_out(index).start()
                return carry

            lax.fori_loop(0, pieces, one, 0)

        def prepare(index, carry):
            rows_here = pl.ds(pl.multiple_of(index * step, step), step)
            last = stacks - 1
            raw_ref[rows_here, :] = dot_nt(grads_ref[rows_here, :], wd_ref[pl.ds(last * WINDOW, WINDOW), :])
            gate_ref[rows_here, :] = jnp.dot(
                both[rows_here, :width], wgu[:, pl.ds(2 * last * WINDOW, WINDOW)], preferred_element_type=f32
            )
            return carry

        def forward(number):
            for gap in (1, 2, 3):
                move.forward(number, gap)

        spot.greet(True, True)
        share.begin()
        weights.start()
        cotangents.start()
        for number in range(count):
            move.own(number)
        move.send(0)
        share.step(1)
        move.send(1)
        share.step(2)
        forward(0)
        share.step(3)
        for number in range(2, count):
            move.send(number)
        share.end()
        keep.start()
        forward(1)
        weights.wait()
        cotangents.wait()
        for k in range(stacks):

            @pl.when(spot.place == narrow_of(k))
            def _():
                spare = 0 if narrow_of(k) else WINDOW - SPARE
                wd_ref[pl.ds(k * WINDOW + spare, SPARE), :] = jnp.zeros((SPARE, width), bf16)
                for which in (2 * k, 2 * k + 1):
                    wgu[:, pl.ds(which * WINDOW + spare, SPARE)] = jnp.zeros((2 * parts * block, SPARE), bf16)

        for k in range(stacks):
            last = k == stacks - 1
            if not last:
                forward(2 * k + 2)
                if k == stacks - 2:
                    back.start_one(0, 1)
            else:
                back.reduce(0, 0)
                back.reduce(0, 1)
            move.ready(2 * k)
            if last:
                lax.fori_loop(0, pieces, prepare, 0)
            move.ready(2 * k + 1)

            def halfway():
                if last:
                    back.reduce(0, 2)
                else:
                    forward(2 * k + 3)
                if k == stacks - 2:
                    back.start_one(0, 2)
                    back.start_one(0, 3)

            compute(k, halfway)
            if not last:
                gradients(k)
            if k == 0:
                back.start_one(0, 0)
        back.reduce(0, 3)
        act_out().start()
        dup_out().start()
        for index in (pieces - 2, pieces - 1):
            send_out(index).wait()
            branch_out(index).wait()
        act_out().wait()
        dup_out().wait()
        keep.wait()
        move.sent()
        back.end()

    return comm_call(
        kernel,
        number,
        "share_move_compute",
        [
            jax.ShapeDtypeStruct((length, wide), bf16),
            jax.ShapeDtypeStruct((length, width + 128), bf16),
            jax.ShapeDtypeStruct((length, width), bf16),
            jax.ShapeDtypeStruct((length, 2 * WINDOW), bf16),
            jax.ShapeDtypeStruct((length, WINDOW), bf16),
            jax.ShapeDtypeStruct((width, 2 * (stacks - 1) * WINDOW), bf16),
            jax.ShapeDtypeStruct(((stacks - 1) * WINDOW, width), bf16),
            jax.ShapeDtypeStruct(shared_gate.shape, bf16),
            jax.ShapeDtypeStruct(shared_gate.shape, bf16),
        ],
        [IN_PLACE] * 9,
        [IN_VMEM] + [IN_PLACE] * 6,
        scratch + grad_scratch + back_scratch + share_sems + move_sems,
        300_000_000,
    )(value, grad_all, shared_gate, shared_up, expert_gate, expert_up, wd)


def up_item(grads_ref, at, k, gate_ref, up_ref, block, parts):
    def piece(offset, ref):
        return (
            lambda buf, short: units_at(buf, k, 0, short, 1, offset),
            lambda source, short: units_at(ref, k, source, short, 1, None),
        )

    return {
        "block": lambda side, part: grads_ref.at[
            pl.ds(pl.multiple_of((side * parts + part) * block, block), block), pl.ds(2 * at * WINDOW, 2 * WINDOW)
        ],
        "pieces": [piece(0, gate_ref), piece(WINDOW, up_ref)],
        "short": narrow_of(k),
    }


def down_item(grads_ref, at, k, down_ref, parts):
    lanes = down_ref.shape[1]
    return {
        "block": lambda side, part: grads_ref.at[
            pl.ds(at * WINDOW, WINDOW), pl.ds(pl.multiple_of((side * parts + part) * lanes, lanes), lanes)
        ],
        "pieces": [
            (
                lambda buf, short: units_at(buf, k, 0, short, 0),
                lambda source, short: units_at(down_ref, k, source, short, 0, None),
            )
        ],
        "short": narrow_of(k),
    }


def attention_last(send4, up_grads, down_grads, hidden, grad, gain, chances, named, router, out_w, qkv_w, heads, lse, shared, number):
    lazy = [send4, router, out_w, qkv_w, *heads, lse, shared]
    parts = lax.axis_size("context")
    length, width = send4.shape[0], hidden.shape[1]
    rows, wide = hidden.shape[0], send4.shape[1]
    block = up_grads.shape[0] // (2 * parts)
    lanes = down_grads.shape[1] // (2 * parts)
    units = WINDOW * parts - 128
    step = 256
    experts = 8
    scale = HEAD_DIM ** (-0.5)
    f32, bf16 = jnp.float32, jnp.bfloat16
    shapes, pieces = [(WINDOW, lanes), (block, 2 * WINDOW), (WINDOW, lanes)], [1, 2, 1]
    sets = [
        [
            pltpu.VMEM((rows, wide), f32),
            pltpu.VMEM((rows, width), bf16),
            pltpu.VMEM((length, width), bf16),
            pltpu.VMEM((length, width), bf16),
            pltpu.VMEM((length, 3 * HEAD_DIM), bf16),
            pltpu.VMEM((length, HEAD_DIM), f32),
            pltpu.VMEM((length, HEAD_DIM), f32),
            pltpu.VMEM((length, HEAD_DIM), f32),
            DMA,
        ],
        [pltpu.VMEM(one.shape, one.dtype) for one in lazy] + [DMA((len(lazy),))],
        Sum.scratch(parts, rows, wide),
        Share.sems(parts),
        Sum.scratch(parts, rows, width),
        Return.scratch(shapes, pieces, parts),
    ]

    def kernel(upg_ref, downg_ref, hidden_ref, grad_ref, gain_ref, chance_ref, named_ref, *rest):
        sources, rest = rest[: len(lazy)], rest[len(lazy) :]
        (dh_hbm, down_out, gate_out1, up_out1, down_out1, dots_ref, dxn2_ref, dhidden_ref, outg_ref, qkvg_ref, bias_ref, dxn1_ref), scratch = rest[:12], rest[12:]
        scratch, split = list(scratch), []
        for one in sets:
            split.append(scratch[: len(one)])
            scratch = scratch[len(one) :]
        sums, dh_own, dh_all, part_ref, dqkv_ref, dq_acc, dk_acc, dv_acc, keep_sem = split[0]
        *targets, load = split[1]
        send_ref, router_ref, wout_ref, wqkv_ref, q_ref, k_ref, v_ref, att_ref, lse_ref, shared_ref = targets
        loads = [
            pltpu.make_async_copy(source, target, load.at[index])
            for index, (source, target) in enumerate(zip(sources, targets))
        ]
        spot = Spot()
        first = Sum(spot, send_ref, sums, split[2])
        share = Share(spot, dh_own, dh_all, split[3])
        second = Sum(spot, part_ref, dxn1_ref, split[4])
        items = [
            down_item(downg_ref, 0, 0, down_out, parts),
            up_item(upg_ref, 1, 1, gate_out1, up_out1, block, parts),
            down_item(downg_ref, 1, 1, down_out1, parts),
        ]
        back = Return(spot, items, split[5][:3], split[5][3:6], split[5][6:])
        keep = pltpu.make_async_copy(dh_all, dh_hbm, keep_sem)

        def owner():
            lane = lax.broadcasted_iota(jnp.int32, (rows, 128), 1)
            dots = sums[:, width:]
            dots_ref[...] = dots
            chance = chance_ref[...]
            dprob = dots * named_ref[...]
            prob = jnp.where(lane < experts, chance, 0.0)
            dlogit = prob * (dprob - jnp.sum(prob * dprob, -1, keepdims=True))
            mix = jnp.where(lane < experts, dlogit, jnp.where(lane == experts, chance * (1.0 - chance) * dots, 0.0))
            dxn2_ref[...] = jnp.dot(mix, router_ref[...], precision=PRECISE, preferred_element_type=f32)

            def one(index, carry):
                at = pl.ds(pl.multiple_of(index * 16, 16), 16)
                dxn2 = dxn2_ref[at, :] + sums[at, :width]
                dxn2_ref[at, :] = dxn2
                value = hidden_ref[at, :]
                inverse = lax.rsqrt(jnp.mean(value * value, -1, keepdims=True) + EPSILON)
                normed = value * inverse
                scaled = dxn2 * gain_ref[...]
                dhidden = grad_ref[at, :].astype(f32) + inverse * (scaled - normed * jnp.mean(scaled * normed, -1, keepdims=True))
                dhidden_ref[at, :] = dhidden
                dh_own[at, :] = dhidden.astype(bf16)
                return carry

            lax.fori_loop(0, rows // 16, one, 0)

        def attend(index, carry):
            start = pl.multiple_of(index * step, step)
            at = pl.ds(start, step)
            datt = dot_nt(dh_all[at, :], wout_ref[...]).astype(bf16)
            delta = jnp.sum(datt.astype(f32) * att_ref[at, :].astype(f32), -1, keepdims=True)
            scores = dot_nt(q_ref[at, :], k_ref[...]) * scale
            query_index = start + lax.broadcasted_iota(jnp.int32, scores.shape, 0)
            allowed = lax.broadcasted_iota(jnp.int32, scores.shape, 1) <= query_index
            prob = jnp.where(allowed, jnp.exp(scores - lse_ref[at, :1]), 0.0)
            dscore = (prob * (dot_nt(datt, v_ref[...]) - delta)).astype(bf16)
            dq_acc[at, :] = jnp.dot(dscore, k_ref[...], preferred_element_type=f32) * scale
            dk_acc[...] += dot_tn(dscore, q_ref[at, :])
            dv_acc[...] += dot_tn(prob.astype(bf16), datt)
            return carry

        def project(index, carry):
            at = pl.ds(pl.multiple_of(index * step, step), step)
            cosine, sine_part = turn_tables(shared_ref[at, width:])
            dq, dk, dv = dq_acc[at, :], dk_acc[at, :] * scale, dv_acc[at, :]
            dq = dq * cosine - pltpu.roll(dq, HEAD_DIM // 2, 1) * sine_part
            dk = dk * cosine - pltpu.roll(dk, HEAD_DIM // 2, 1) * sine_part
            for which, value in enumerate((dq, dk, dv)):
                bias_ref[:, pl.ds(which * HEAD_DIM, HEAD_DIM)] += jnp.sum(value, 0, keepdims=True)
                dqkv_ref[at, pl.ds(which * HEAD_DIM, HEAD_DIM)] = value.astype(bf16)
            part_ref[at, :] = dot_nt(dqkv_ref[at, :], wqkv_ref[...]).astype(bf16)
            return carry

        def features(index, carry):
            at = pl.ds(pl.multiple_of(index * step, step), step)
            qkvg_ref[at, :] = dot_tn(shared_ref[:, at], dqkv_ref[...]).astype(bf16)
            outg_ref[:, at] = dot_tn(att_ref[...], dh_all[:, at]).astype(bf16)
            return carry

        for copy in loads:
            copy.start()
        spot.greet(True, True)
        loads[0].wait()
        first.begin()
        for number in range(3):
            back.start(number)
        dk_acc[...] = jnp.zeros_like(dk_acc)
        dv_acc[...] = jnp.zeros_like(dv_acc)
        bias_ref[...] = jnp.zeros_like(bias_ref)
        for index in range(parts):
            first.cross(index)
        back.reduce(0, 0)
        back.reduce(0, 1)
        for index in range(parts):
            first.line(index)
        for copy in loads[1:]:
            copy.wait()
        owner()
        share.begin()
        share.step(1)
        share.step(2)
        back.reduce(0, 2)
        share.step(3)
        back.reduce(0, 3)
        back.reduce(1, 0)
        share.end()
        keep.start()
        back.reduce(1, 1)
        back.reduce(1, 2)
        back.reduce(2, 0)
        back.reduce(2, 1)
        back.reduce(2, 2)
        lax.fori_loop(0, length // step, attend, 0)
        lax.fori_loop(0, length // step, project, 0)
        second.begin()
        back.reduce(1, 3)
        for index in range(parts):
            second.cross(index)
        lax.fori_loop(0, width // step, features, 0)
        for index in range(parts):
            second.line(index)
        back.reduce(2, 3)
        first.end()
        second.end()
        back.end()
        keep.wait()

    piece = jax.ShapeDtypeStruct((block, units), bf16)
    return comm_call(
        kernel,
        number,
        "attention_last",
        [
            jax.ShapeDtypeStruct((length, width), bf16),
            jax.ShapeDtypeStruct((units, lanes), bf16),
            piece,
            piece,
            jax.ShapeDtypeStruct((units, lanes), bf16),
            jax.ShapeDtypeStruct((rows, 128), f32),
            jax.ShapeDtypeStruct((rows, width), f32),
            jax.ShapeDtypeStruct((rows, width), f32),
            jax.ShapeDtypeStruct((HEAD_DIM, width), bf16),
            jax.ShapeDtypeStruct((width, 3 * HEAD_DIM), bf16),
            jax.ShapeDtypeStruct((1, 3 * HEAD_DIM), f32),
            jax.ShapeDtypeStruct((rows, width), f32),
        ],
        [IN_PLACE] * 5 + [IN_VMEM] * 7,
        [IN_PLACE] * 2 + [IN_VMEM] * 5 + [IN_PLACE] * len(lazy),
        [one for group in sets for one in group],
        250_000_000,
    )(up_grads, down_grads, hidden, grad, gain, chances, named, *lazy)


class Group:
    def __init__(self, spot, own, out, sems):
        self.spot, self.own, self.out = spot, own, out
        self.local_sem, self.across_s, self.across_r, self.beside_s, self.beside_r = sems

    @staticmethod
    def sems():
        return [DMA, DMA, DMA, DMA((2,)), DMA((2,))]

    def block(self, column):
        rows = self.own.shape[0]
        return rows_at(self.out, column * rows, rows)

    def to_across(self):
        s = self.spot
        return remote(self.own, self.block(s.group), self.across_s, self.across_r, {"experts": s.across})

    def to_beside(self, slot):
        s = self.spot
        column = s.across if slot else s.group
        source = self.block(column) if slot else self.own
        return remote(source, self.block(column), self.beside_s.at[slot], self.beside_r.at[slot], {"experts": s.beside})

    def local(self):
        return pltpu.make_async_copy(self.own, self.block(self.spot.group), self.local_sem)

    def begin(self):
        self.to_across().start()
        self.to_beside(0).start()
        self.local().start()

    def end(self):
        self.to_across().wait_recv()
        self.to_beside(1).start()
        self.local().wait()
        self.to_across().wait_send()
        for slot in range(2):
            self.to_beside(slot).wait()


class Total:
    def __init__(self, spot, value, out, scratch):
        self.out = out
        self.sent, self.got, self.send_s, self.recv_s = scratch
        place = spot.place
        self.turns = [
            spot.twin,
            {"context": place + 1 - 2 * lax.rem(place, 2)},
            {"context": lax.rem(place + 2, spot.parts)},
            {"experts": spot.beside},
            {"experts": spot.across},
        ]
        self.value = value

    @staticmethod
    def scratch(shape):
        buf = pltpu.VMEM((5,) + shape, jnp.float32)
        return [buf, buf, DMA((5,)), DMA((5,))]

    def copy(self, index):
        return remote(self.sent.at[index], self.got.at[index], self.send_s.at[index], self.recv_s.at[index], self.turns[index])

    def begin(self):
        self.out[...] = self.value[...]
        self.send(0)

    def send(self, index):
        self.sent[index] = self.out[...]
        self.copy(index).start()

    def take(self, index):
        self.copy(index).wait()
        self.out[...] = self.out[...] + self.got[index]


def last_exchange(out_grads, qkv_grads, both, cotangents, dup, act, branch, hidden, tokens_grad, small, number):
    parts = lax.axis_size("context")
    rows, width = hidden.shape
    block = lanes = width // (2 * parts)
    units = WINDOW * parts - 128
    head, span = out_grads.shape[0], qkv_grads.shape[1]
    shapes = [(head, lanes), (block, span), (block, 2 * WINDOW), (WINDOW, lanes)]
    pieces = [1, 3, 2, 1]
    count, bf16 = len(shapes), jnp.bfloat16
    groups = [
        Return.scratch(shapes, pieces, parts),
        Sum.scratch(parts, rows, width) + [pltpu.VMEM((rows, width), jnp.float32), pltpu.VMEM((rows, width), bf16)],
        Total.scratch(small.shape),
        Group.sems(),
        Group.sems(),
        Grads.scratch() + [pltpu.VMEM(one.shape, bf16) for one in (both, cotangents, dup, act)] + [DMA((4,))],
    ]
    piece, column = jax.ShapeDtypeStruct((block, units), bf16), jax.ShapeDtypeStruct((units, lanes), bf16)
    out_shape = [jax.ShapeDtypeStruct((parts * head, lanes), bf16), jax.ShapeDtypeStruct((3, block, parts * HEAD_DIM), bf16)]
    out_shape += [piece, piece, column]
    out_shape += [
        jax.ShapeDtypeStruct((width, 2 * WINDOW), bf16),
        jax.ShapeDtypeStruct((WINDOW, width), bf16),
        jax.ShapeDtypeStruct((4 * rows, width), bf16),
        jax.ShapeDtypeStruct((4 * rows, width), jnp.float32),
        jax.ShapeDtypeStruct(small.shape, jnp.float32),
    ]

    def kernel(outg_ref, qkvg_ref, both_hbm, cots_hbm, dup_hbm, act_hbm, branch_ref, hidden_ref, tokens_ref, small_ref, *rest):
        outs, scratch = rest[: len(out_shape)], list(rest[len(out_shape) :])
        sets = []
        for one in groups:
            sets.append(scratch[: len(one)])
            scratch = scratch[len(one) :]
        grads, (upg2_hbm, downg2_hbm, block_all, tokens_all, small_out) = outs[:-5], outs[-5:]
        *grad_refs, both_ref, cots_ref, dup_ref, act_ref, load = sets[5]
        loads = [
            pltpu.make_async_copy(source, target, load.at[index])
            for index, (source, target) in enumerate(
                ((both_hbm, both_ref), (cots_hbm, cots_ref), (dup_hbm, dup_ref), (act_hbm, act_ref))
            )
        ]
        items = [
            {
                "block": lambda side, part: lanes_at(outg_ref, (side * parts + part) * lanes, lanes),
                "pieces": [(lambda buf, short: buf, lambda source, short: rows_at(grads[0], source * head, head))],
            },
            {
                "block": lambda side, part: rows_at(qkvg_ref, (side * parts + part) * block, block),
                "pieces": [
                    (
                        lambda buf, short, which=which: buf.at[:, pl.ds(which * HEAD_DIM, HEAD_DIM)],
                        lambda source, short, which=which: lanes_at(grads[1].at[which], source * HEAD_DIM, HEAD_DIM),
                    )
                    for which in range(3)
                ],
            },
        ]
        items += [
            up_item(upg2_hbm, 0, 2, grads[2], grads[3], block, parts),
            down_item(downg2_hbm, 0, 2, grads[4], parts),
        ]
        spot = Spot()
        back = Return(spot, items, sets[0][:count], sets[0][count : 2 * count], sets[0][2 * count :])
        total_branch, own_block = sets[1][-2:]
        summed = Sum(spot, branch_ref, total_branch, sets[1][:-2])
        total = Total(spot, small_ref, small_out, sets[2])
        tokens_group = Group(spot, tokens_ref, tokens_all, sets[3])
        block_group = Group(spot, own_block, block_all, sets[4])
        spot.greet(True, True)
        total.begin()
        summed.begin()
        for item in range(2):
            back.start(item)
        for copy in loads:
            copy.start()
        total.take(0)
        total.send(1)
        for index in range(parts):
            summed.cross(index)
        total.take(1)
        total.send(2)
        for index in range(parts):
            back.reduce(0, index)
        total.take(2)
        total.send(3)
        for index in range(parts):
            back.reduce(1, index)
        total.take(3)
        total.send(4)
        for copy in loads:
            copy.wait()
        Grads(both_ref, cots_ref, dup_ref, act_ref, upg2_hbm, downg2_hbm, *grad_refs).run()
        back.start(2)
        back.start(3)
        total.take(4)
        tokens_group.begin()
        for index in range(parts):
            summed.line(index)
        half = width // 2

        def finish(at, start, step):
            value = (hidden_ref[at, :] + total_branch[at, :]).astype(bf16)
            turned = lax.axis_index("dp") == 0

            @pl.when(turned)
            def _():
                own_block[at, :] = value

            @pl.when(jnp.logical_not(turned))
            def _():
                own_block[at, :half] = value[:, half:]
                own_block[at, half:] = value[:, :half]

        summed.chunks(finish)
        block_group.begin()
        for item in range(2, count):
            for index in range(parts):
                back.reduce(item, index)
        summed.end()
        tokens_group.end()
        block_group.end()
        back.end()

    return comm_call(
        kernel,
        number,
        "last_exchange",
        out_shape,
        [IN_PLACE] * (len(out_shape) - 1) + [IN_VMEM],
        [IN_PLACE] * 6 + [IN_VMEM] * 4,
        [one for group in groups for one in group],
        300_000_000,
    )(out_grads, qkv_grads, both, cotangents, dup, act, branch, hidden, tokens_grad, small)


def widen(singles, pairs):
    steps = 8

    def spec(shape):
        if len(shape) == 3:
            return pl.BlockSpec((shape[0], shape[1] // steps, shape[2]), lambda i: (0, i, 0))
        return pl.BlockSpec((shape[0] // steps, shape[1]), lambda i: (i, 0))

    kinds = [jnp.bfloat16 if keep else jnp.float32 for _, keep in singles]
    arrays = [array for array, _ in singles] + [one for pair in pairs for one in pair]
    out_shape = [jax.ShapeDtypeStruct(array.shape, kind) for (array, _), kind in zip(singles, kinds)]
    out_shape += [jax.ShapeDtypeStruct((2,) + pair[0].shape, jnp.float32) for pair in pairs]
    count = len(singles)

    def kernel(*refs):
        sources, targets = refs[: len(arrays)], refs[len(arrays) :]
        for source, target in zip(sources[:count], targets[:count]):
            target[...] = source[...].astype(target.dtype)
        for index, target in enumerate(targets[count:]):
            for which in range(2):
                target[which] = sources[count + 2 * index + which][...].astype(jnp.float32)

    return pl.pallas_call(
        kernel,
        grid=(steps,),
        in_specs=[spec(array.shape) for array in arrays],
        out_specs=[spec(one.shape) for one in out_shape],
        out_shape=out_shape,
        name="widen",
    )(*arrays)


def split_body(
    tokens,
    positions,
    routes,
    out_grad,
    norm1_gain,
    qkv_weight,
    qkv_bias,
    out_weight,
    norm2_gain,
    router_weight,
    expert_gate,
    expert_up,
    expert_down,
    shared_gate,
    shared_w_gate,
    shared_w_up,
    shared_w_down,
):
    rows, width = tokens.shape[1], tokens.shape[2]
    parts = lax.axis_size("context")
    group_size = lax.axis_size("experts")
    place, group = lax.axis_index("context"), lax.axis_index("experts")
    local_experts = expert_gate.shape[0]
    expert_count = local_experts * group_size
    own_rows = rows // group_size
    length = rows * parts
    half = width // 2
    block = width // (2 * parts)
    hidden_here = shared_w_gate.shape[1] // parts
    stacks = local_experts + 1
    scale = HEAD_DIM ** (-0.5)
    bf16 = jnp.bfloat16

    first = group * own_rows

    def own_of(array):
        return lax.dynamic_slice_in_dim(array, first, own_rows, 0)

    grad_own_b = own_half_first(own_of(out_grad[0]))
    grad_own = grad_own_b.astype(jnp.float32)
    gain1 = own_half_first(norm1_gain).astype(jnp.float32)
    gain2 = own_half_first(norm2_gain).astype(jnp.float32)
    token_own = own_half_first(own_of(tokens[0])).astype(jnp.float32)
    inverse1 = lax.rsqrt(jnp.mean(token_own * token_own, -1, keepdims=True) + EPSILON)
    normed1 = token_own * inverse1
    half_dim = HEAD_DIM // 2
    frequency = ROPE_BASE ** (-2.0 * jnp.arange(half_dim, dtype=jnp.float32) / HEAD_DIM)
    angles = own_of(positions[0]).astype(jnp.float32)[:, None] * frequency[None, :]
    turns = jnp.concatenate([jnp.cos(angles), jnp.sin(angles)], 1)
    turns_high = turns.astype(bf16)
    turns_low = (turns - turns_high.astype(jnp.float32)).astype(bf16)
    send1 = jnp.concatenate([(normed1 * gain1).astype(bf16), turns_high, turns_low], 1)
    qkv_in = jnp.transpose(qkv_weight, (1, 0, 2))
    bias_here = lax.dynamic_slice_in_dim(
        qkv_bias.reshape(3, parts, HEAD_DIM), place, 1, 1
    ).reshape(1, 3 * HEAD_DIM)
    shared1, grad_all, qkv_w, out_w, down_w, query, key, value, attended, lse, head_sum = attention_first(
        send1, grad_own_b, qkv_in, out_weight, bias_here.astype(jnp.float32), shared_w_down, expert_down, 1
    )
    hidden = token_own + head_sum
    inverse2 = lax.rsqrt(jnp.mean(hidden * hidden, -1, keepdims=True) + EPSILON)
    normed2 = hidden * inverse2
    xn2_own = (normed2 * gain2).astype(bf16)
    router_here = own_half_first(router_weight.T).T
    gate_here = own_half_first(shared_gate)
    heads_w = jnp.concatenate([router_here, gate_here[:, None]], 1)
    logits = dot_nn(xn2_own, heads_w)
    prob = jax.nn.softmax(logits[:, :expert_count], -1)
    sig_own = jax.nn.sigmoid(logits[:, expert_count])
    named = jnp.sum(
        (
            own_of(routes[0])[:, :, None] == jnp.arange(expert_count, dtype=jnp.int32)[None, None, :]
        ).astype(jnp.float32),
        1,
    )
    gates = jnp.pad(
        jnp.concatenate([prob * named, sig_own[:, None]], 1), ((0, 0), (0, 63 - expert_count))
    )
    gates_high = gates.astype(bf16)
    gates_low = (gates - gates_high.astype(jnp.float32)).astype(bf16)
    send3 = jnp.concatenate([xn2_own, gates_high, gates_low], 1)

    both, send4, branch_part, dup, act_c, up_g, down_g, *first_grads = share_move_compute(
        send3, grad_all, shared_w_gate, shared_w_up, expert_gate, expert_up, down_w, 3
    )
    up_grads, down_grads = [None] * (2 * stacks), [None] * stacks
    up_grads[:2] = first_grads
    side = 128 - expert_count - 1
    chances = jnp.pad(jnp.concatenate([prob, sig_own[:, None]], 1), ((0, 0), (0, side)))
    named_wide = jnp.pad(named, ((0, 0), (0, 128 - expert_count)))
    router_wide = jnp.pad(heads_w.T.astype(jnp.float32), ((0, side), (0, 0)))
    (
        _,
        down_grads[0],
        up_grads[2],
        up_grads[3],
        down_grads[1],
        dots_own,
        dxn2,
        dhidden,
        out_g,
        qkv_g,
        bias_part,
        dxn1,
    ) = attention_last(
        send4,
        up_g,
        down_g,
        hidden,
        grad_own_b,
        gain2[None, :],
        chances,
        named_wide,
        router_wide,
        out_w,
        qkv_w,
        (query, key, value, attended),
        lse,
        shared1,
        4,
    )

    dprob = dots_own[:, :expert_count] * named
    dlogit = prob * (dprob - jnp.sum(prob * dprob, -1, keepdims=True))
    coef = sig_own * (1.0 - sig_own) * dots_own[:, expert_count]
    xn2_float = xn2_own.astype(jnp.float32)
    router_grad = jnp.dot(xn2_float.T, dlogit, precision=PRECISE)
    shared_gate_grad = jnp.dot(coef, xn2_float, precision=PRECISE)
    norm2_grad = jnp.sum(dxn2 * normed2, 0)
    norm1_grad = jnp.sum(dxn1 * normed1, 0)
    dscaled1 = dxn1 * gain1
    tokens_grad_own = dhidden + inverse1 * (
        dscaled1 - normed1 * jnp.mean(dscaled1 * normed1, -1, keepdims=True)
    )

    bias_wide = jnp.zeros((group_size, parts, 3 * HEAD_DIM), jnp.float32)
    bias_wide = lax.dynamic_update_slice(bias_wide, bias_part[None], (group, place, 0))
    small = jnp.concatenate(
        [
            own_half_first(norm1_grad),
            own_half_first(norm2_grad),
            own_half_first(shared_gate_grad),
            own_half_first(router_grad.T).T.reshape(-1),
            bias_wide.reshape(-1),
        ]
    )
    (
        out_w_grad,
        qkv_grad,
        up_grads[4],
        up_grads[5],
        down_grads[2],
        _,
        _,
        block_out,
        tokens_grad,
        small,
    ) = last_exchange(
        out_g,
        qkv_g,
        both,
        grad_all,
        dup,
        act_c,
        branch_part,
        hidden,
        own_half_first(tokens_grad_own),
        small.reshape(-1, 128),
        7,
    )
    small = small.reshape(-1)
    router_size = width * expert_count
    bias_sum = small[3 * width + router_size :].reshape(group_size, parts, 3, HEAD_DIM)
    bias_grad = jnp.transpose(
        lax.dynamic_slice_in_dim(bias_sum, group, 1, 0)[0], (1, 0, 2)
    ).reshape(3, parts * HEAD_DIM)

    singles = [(block_out, True), (tokens_grad, False), (out_w_grad, False), (qkv_grad, False)]
    singles += [(up_grads[0], False), (up_grads[1], False), (down_grads[0], False)]
    pairs = [up_grads[2::2], up_grads[3::2], down_grads[1:]]
    block_out, tokens_grad, out_w_grad, qkv_grad, *shared_grads, gate_grads, up_grads, down_grads = widen(singles, pairs)

    return (
        block_out[None],
        tokens_grad[None],
        small[:width],
        jnp.transpose(qkv_grad, (1, 0, 2)),
        bias_grad,
        out_w_grad,
        small[width : 2 * width],
        small[3 * width : 3 * width + router_size].reshape(width, expert_count),
        gate_grads,
        up_grads,
        down_grads,
        small[2 * width : 3 * width],
        *shared_grads,
    )


def plan_of(mesh):
    sizes = mesh.shape
    return split_body if (sizes["dp"], sizes["context"], sizes["experts"]) == (2, 4, 4) else general_body


def solution(mesh):
    return jax.shard_map(
        plan_of(mesh),
        mesh=mesh,
        in_specs=(
            P("dp", "context", None),
            P("dp", "context"),
            P("dp", "context", None),
            P("dp", "context", None),
            P(),
            P(("dp", "context"), None, "experts"),
            P(None, "experts"),
            P("experts", ("dp", "context")),
            P(),
            P(),
            P("experts", ("dp", "context"), None),
            P("experts", ("dp", "context"), None),
            P("experts", None, ("dp", "context")),
            P(),
            P(("dp", "context"), "experts"),
            P(("dp", "context"), "experts"),
            P("experts", ("dp", "context")),
        ),
        out_specs=(
            P("dp", "context", None),
            P("dp", "context", None),
            P(),
            P(("dp", "context"), None, "experts"),
            P(None, "experts"),
            P("experts", ("dp", "context")),
            P(),
            P(),
            P("experts", ("dp", "context"), None),
            P("experts", ("dp", "context"), None),
            P("experts", None, ("dp", "context")),
            P(),
            P(("dp", "context"), "experts"),
            P(("dp", "context"), "experts"),
            P("experts", ("dp", "context")),
        ),
        check_vma=False,
    )
```

```python
import functools

import jax
import jax.numpy as jnp
from jax import lax
from jax.experimental import pallas as pl
from jax.experimental.pallas import tpu as pltpu
from jax.sharding import PartitionSpec as P

HEAD_DIM = 128


EPSILON = 1e-06
ROPE_BASE = 1000000.0
MASKED = -1e30
PRECISE = lax.Precision.HIGHEST


def rope_tables(position_ids):
    half_dim = HEAD_DIM // 2
    inverse = ROPE_BASE ** (-2.0 * jnp.arange(half_dim, dtype=jnp.float32) / HEAD_DIM)
    angles = position_ids.astype(jnp.float32)[:, None] * inverse[None, :]
    cosine = jnp.cos(angles)
    sine_part = jnp.sin(angles)
    return (
        jnp.concatenate([cosine, cosine], -1)[:, None, :],
        jnp.concatenate([sine_part, sine_part], -1)[:, None, :],
    )


def rotate(value):
    half_dim = value.shape[-1] // 2
    return jnp.concatenate([-value[..., half_dim:], value[..., :half_dim]], -1)


def rotate_back(value):
    half_dim = value.shape[-1] // 2
    return jnp.concatenate([value[..., half_dim:], -value[..., :half_dim]], -1)


def silu_grad(gate_vals):
    sigmoid_vals = jax.nn.sigmoid(gate_vals)
    return sigmoid_vals * (1.0 + gate_vals * (1.0 - sigmoid_vals))


def block_rank(route_rows, expert_count):
    hits = (
        route_rows[:, :, None] == jnp.arange(expert_count, dtype=jnp.int32)[None, None, :]
    ).astype(jnp.int32)
    flat_hits = hits.reshape(-1, expert_count)
    earlier = jnp.cumsum(flat_hits, axis=0) - flat_hits
    return jnp.sum(earlier * flat_hits, -1).reshape(route_rows.shape)


def block_width_of():
    return 512


def gather_weights(shard_set):
    return (
        lax.all_gather(shard_set[0], ("dp", "context"), axis=0, tiled=True),
        lax.all_gather(shard_set[1], ("dp", "context"), axis=1, tiled=True),
        lax.all_gather(shard_set[2], ("dp", "context"), axis=1, tiled=True),
        lax.all_gather(shard_set[3], ("dp", "context"), axis=1, tiled=True),
        lax.all_gather(shard_set[4], ("dp", "context"), axis=2, tiled=True),
        lax.all_gather(shard_set[5], ("dp", "context"), axis=0, tiled=True),
        lax.all_gather(shard_set[6], ("dp", "context"), axis=0, tiled=True),
        lax.all_gather(shard_set[7], ("dp", "context"), axis=1, tiled=True),
    )


def forward_fold(query, query_first, scale, carry, piece):
    row_count, head_count, head_size = query.shape
    query_index = query_first + jnp.arange(row_count, dtype=jnp.int32)
    query_last = query_first + row_count - 1
    key_part, value_part = piece
    piece_rows = key_part.shape[0]
    block_width = block_width_of()
    block_count = piece_rows // block_width
    key_blocks = key_part.reshape(block_count, block_width, head_count, head_size)
    value_blocks = value_part.reshape(block_count, block_width, head_count, head_size)
    offsets = block_width * jnp.arange(block_count, dtype=jnp.int32)

    def forward_visit(state, item):
        key_block, value_block, first_key = item

        def forward_compute(current):
            run_max, run_sum, accum = current
            scores = (
                jnp.einsum("qhd,khd->hqk", query, key_block, preferred_element_type=jnp.float32)
                * scale
            )
            key_index = first_key + jnp.arange(block_width, dtype=jnp.int32)
            allowed = key_index[None, None, :] <= query_index[None, :, None]
            new_max = jnp.maximum(run_max, jnp.max(jnp.where(allowed, scores, MASKED), -1))
            weights = jnp.where(allowed, jnp.exp(scores - new_max[..., None]), 0.0)
            factor = jnp.exp(run_max - new_max)
            new_sum = run_sum * factor + jnp.sum(weights, -1)
            new_accum = accum * factor[..., None] + jnp.einsum(
                "hqk,khd->hqd",
                weights.astype(jnp.bfloat16),
                value_block,
                preferred_element_type=jnp.float32,
            )
            return (new_max, new_sum, new_accum)

        return (
            lax.cond(first_key > query_last, lambda current: current, forward_compute, state),
            None,
        )

    carry, _ = lax.scan(forward_visit, carry, (key_blocks, value_blocks, offsets))
    return carry


def key_grad_fold(key_rows, value_rows, key_first, scale, carry, piece):
    row_count, head_count, head_size = key_rows.shape
    key_index = key_first + jnp.arange(row_count, dtype=jnp.int32)
    query_part, dout_part, lse_part, delta_part = piece
    piece_rows = query_part.shape[0]
    block_width = block_width_of()
    block_count = piece_rows // block_width
    query_blocks = query_part.reshape(block_count, block_width, head_count, head_size)
    dout_blocks = dout_part.reshape(block_count, block_width, head_count, head_size)
    lse_blocks = lse_part.reshape(block_count, block_width, head_count)
    delta_blocks = delta_part.reshape(block_count, block_width, head_count)
    offsets = block_width * jnp.arange(block_count, dtype=jnp.int32)

    def key_visit(state, item):
        query_block, dout_block, lse_block, delta_block, first_query = item

        def key_compute(current):
            dkey_sum, dvalue_sum = current
            query_b = query_block.astype(jnp.bfloat16)
            dout_b = dout_block.astype(jnp.bfloat16)
            scores = (
                jnp.einsum("qhd,khd->hqk", query_b, key_rows, preferred_element_type=jnp.float32)
                * scale
            )
            query_index = first_query + jnp.arange(block_width, dtype=jnp.int32)
            allowed = key_index[None, None, :] <= query_index[None, :, None]
            prob_att = jnp.where(
                allowed, jnp.exp(scores - jnp.transpose(lse_block)[:, :, None]), 0.0
            )
            dvalue_sum = dvalue_sum + jnp.einsum(
                "hqk,qhd->hkd",
                prob_att.astype(jnp.bfloat16),
                dout_b,
                preferred_element_type=jnp.float32,
            )
            dprob = jnp.einsum(
                "qhd,khd->hqk", dout_b, value_rows, preferred_element_type=jnp.float32
            )
            dscore = (prob_att * (dprob - jnp.transpose(delta_block)[:, :, None])).astype(
                jnp.bfloat16
            )
            dkey_sum = (
                dkey_sum
                + jnp.einsum("hqk,qhd->hkd", dscore, query_b, preferred_element_type=jnp.float32)
                * scale
            )
            return (dkey_sum, dvalue_sum)

        return (
            lax.cond(
                first_query + block_width - 1 < key_first,
                lambda current: current,
                key_compute,
                state,
            ),
            None,
        )

    carry, _ = lax.scan(
        key_visit, carry, (query_blocks, dout_blocks, lse_blocks, delta_blocks, offsets)
    )
    return carry


def query_grad_fold(query, dattended, lse_heads, delta_heads, query_first, scale, carry, piece):
    row_count, head_count, head_size = query.shape
    query_index = query_first + jnp.arange(row_count, dtype=jnp.int32)
    query_last = query_first + row_count - 1
    key_part, value_part = piece
    piece_rows = key_part.shape[0]
    block_width = block_width_of()
    block_count = piece_rows // block_width
    key_blocks = key_part.reshape(block_count, block_width, head_count, head_size)
    value_blocks = value_part.reshape(block_count, block_width, head_count, head_size)
    offsets = block_width * jnp.arange(block_count, dtype=jnp.int32)

    def query_visit(state, item):
        key_block, value_block, first_key = item

        def query_compute(current):
            scores = (
                jnp.einsum("qhd,khd->hqk", query, key_block, preferred_element_type=jnp.float32)
                * scale
            )
            key_index = first_key + jnp.arange(block_width, dtype=jnp.int32)
            allowed = key_index[None, None, :] <= query_index[None, :, None]
            prob_att = jnp.where(allowed, jnp.exp(scores - lse_heads[:, :, None]), 0.0)
            dprob = jnp.einsum(
                "qhd,khd->hqk", dattended, value_block, preferred_element_type=jnp.float32
            )
            dscore = (prob_att * (dprob - delta_heads[:, :, None])).astype(jnp.bfloat16)
            return (
                current
                + jnp.einsum("hqk,khd->hqd", dscore, key_block, preferred_element_type=jnp.float32)
                * scale
            )

        return (
            lax.cond(first_key > query_last, lambda current: current, query_compute, state),
            None,
        )

    carry, _ = lax.scan(query_visit, carry, (key_blocks, value_blocks, offsets))
    return carry


def general_body(
    tokens,
    positions,
    routes,
    out_grad,
    norm1_gain,
    qkv_weight,
    qkv_bias,
    out_weight,
    norm2_gain,
    router_weight,
    expert_gate,
    expert_up,
    expert_down,
    shared_gate,
    shared_w_gate,
    shared_w_up,
    shared_w_down,
):
    row_count = tokens.shape[1]
    model_width = tokens.shape[2]
    head_span = qkv_bias.shape[1]
    heads_here = head_span // HEAD_DIM
    local_experts = expert_gate.shape[0]
    group_size = lax.axis_size("experts")
    quarter = row_count // group_size
    capacity = 3 * quarter // 4
    expert_count = local_experts * group_size
    group_index = lax.axis_index("experts")
    scale = HEAD_DIM ** (-0.5)
    shard_set = (
        qkv_weight,
        out_weight,
        expert_gate,
        expert_up,
        expert_down,
        shared_w_gate,
        shared_w_up,
        shared_w_down,
    )
    qkv_full, out_full, gate_full, up_full, down_full, sgate_full, sup_full, sdown_full = (
        gather_weights(shard_set)
    )
    token_float = tokens[0].astype(jnp.float32)
    inverse1 = lax.rsqrt(jnp.mean(token_float * token_float, -1, keepdims=True) + EPSILON)
    normed1 = token_float * inverse1
    gain1 = norm1_gain.astype(jnp.float32)
    normed1_b = (normed1 * gain1).astype(jnp.bfloat16)
    qkv_flat = qkv_full.reshape(model_width, 3 * head_span)
    qkv = (
        jnp.dot(normed1_b, qkv_flat, preferred_element_type=jnp.float32).reshape(
            row_count, 3, head_span
        )
        + qkv_bias.astype(jnp.float32)[None]
    )
    cosine, sine_part = rope_tables(positions[0])
    query_raw = qkv[:, 0].reshape(row_count, heads_here, HEAD_DIM)
    key_raw = qkv[:, 1].reshape(row_count, heads_here, HEAD_DIM)
    query = (query_raw * cosine + rotate(query_raw) * sine_part).astype(jnp.bfloat16)
    key_rows = (key_raw * cosine + rotate(key_raw) * sine_part).astype(jnp.bfloat16)
    value_flat = qkv[:, 2].astype(jnp.bfloat16)
    key_flat = key_rows.reshape(row_count, head_span)
    value_rows = value_flat.reshape(row_count, heads_here, HEAD_DIM)
    query_first = lax.axis_index("context") * row_count
    start_state = (
        jnp.full((heads_here, row_count), MASKED, jnp.float32),
        jnp.zeros((heads_here, row_count), jnp.float32),
        jnp.zeros((heads_here, row_count, HEAD_DIM), jnp.float32),
    )
    run_max, run_sum, accum = forward_fold(
        query,
        query_first,
        scale,
        start_state,
        (
            lax.all_gather(key_flat, "context", axis=0, tiled=True),
            lax.all_gather(value_flat, "context", axis=0, tiled=True),
        ),
    )
    attended = jnp.transpose(accum / run_sum[..., None], (1, 0, 2)).astype(jnp.bfloat16)
    lse_heads = run_max + jnp.log(run_sum)
    attended_flat = attended.reshape(row_count, head_span)
    head_part = jnp.dot(attended_flat, out_full, preferred_element_type=jnp.float32)
    hidden = token_float + lax.psum(head_part, "experts")
    inverse2 = lax.rsqrt(jnp.mean(hidden * hidden, -1, keepdims=True) + EPSILON)
    normed2 = hidden * inverse2
    gain2 = norm2_gain.astype(jnp.float32)
    normed2_b = (normed2 * gain2).astype(jnp.bfloat16)
    first_row = group_index * quarter
    normed2_q = lax.dynamic_slice_in_dim(normed2_b, first_row, quarter, 0)
    route_q = lax.dynamic_slice_in_dim(routes[0], first_row, quarter, 0)
    logits = jnp.dot(normed2_q, router_weight, preferred_element_type=jnp.float32)
    prob = jax.nn.softmax(logits, -1)
    gate_k = jnp.take_along_axis(prob, route_q, 1)
    slot_ids = route_q * capacity + block_rank(route_q, expert_count)
    slot_hits = (
        slot_ids[:, :, None] == jnp.arange(expert_count * capacity, dtype=jnp.int32)[None, None, :]
    )
    placer = jnp.sum(slot_hits.astype(jnp.bfloat16), 1)
    send_rows = (
        jnp.dot(placer.T, normed2_q, preferred_element_type=jnp.float32)
        .astype(jnp.bfloat16)
        .reshape(group_size, local_experts, capacity, model_width)
    )
    arrived = lax.all_to_all(send_rows, "experts", split_axis=0, concat_axis=0, tiled=True)
    expert_gvals = jnp.einsum(
        "secd,edf->secf", arrived, gate_full, preferred_element_type=jnp.float32
    )
    expert_uvals = jnp.einsum(
        "secd,edf->secf", arrived, up_full, preferred_element_type=jnp.float32
    )
    expert_act = (jax.nn.silu(expert_gvals) * expert_uvals).astype(jnp.bfloat16)
    expert_out = jnp.einsum(
        "secf,efd->secd", expert_act, down_full, preferred_element_type=jnp.float32
    ).astype(jnp.bfloat16)
    returned = lax.all_to_all(
        expert_out, "experts", split_axis=0, concat_axis=0, tiled=True
    ).reshape(expert_count * capacity, model_width)
    picked = returned[slot_ids].astype(jnp.float32)
    routed = jnp.sum(gate_k[:, :, None] * picked, 1)
    shared_sig = jax.nn.sigmoid(
        jnp.dot(normed2_b, shared_gate[:, None], preferred_element_type=jnp.float32)[:, 0]
    )
    shared_gvals = jnp.dot(normed2_b, sgate_full, preferred_element_type=jnp.float32)
    shared_uvals = jnp.dot(normed2_b, sup_full, preferred_element_type=jnp.float32)
    shared_act = (jax.nn.silu(shared_gvals) * shared_uvals).astype(jnp.bfloat16)
    shared_part = jnp.dot(shared_act, sdown_full, preferred_element_type=jnp.float32)
    routed_pad = lax.dynamic_update_slice_in_dim(
        jnp.zeros((row_count, model_width), jnp.float32), routed, first_row, 0
    )
    branch_total = lax.psum(
        (shared_sig[:, None] * shared_part + routed_pad).astype(jnp.bfloat16), "experts"
    ).astype(jnp.float32)
    block_out = (hidden + branch_total).astype(jnp.bfloat16)
    held = lax.optimization_barrier((shard_set, block_out))
    qkv_full, out_full, gate_full, up_full, down_full, sgate_full, sup_full, sdown_full = (
        gather_weights(held[0])
    )
    qkv_flat = qkv_full.reshape(model_width, 3 * head_span)
    grad_float = out_grad[0].astype(jnp.float32)
    grad_q = lax.dynamic_slice_in_dim(grad_float, first_row, quarter, 0)
    dgate_k = jnp.sum(grad_q[:, None, :] * picked, -1)
    weighted = jnp.sum(slot_hits.astype(jnp.float32) * gate_k[:, :, None], 1)
    dsend = (
        jnp.dot(weighted.T, grad_q, precision=PRECISE)
        .astype(jnp.bfloat16)
        .reshape(group_size, local_experts, capacity, model_width)
    )
    darrived = lax.all_to_all(dsend, "experts", split_axis=0, concat_axis=0, tiled=True)
    expert_dact = jnp.einsum(
        "secd,efd->secf", darrived, down_full, preferred_element_type=jnp.float32
    )
    down_grad = jnp.einsum(
        "secf,secd->efd", expert_act, darrived, preferred_element_type=jnp.float32
    )
    expert_dgate = (expert_dact * expert_uvals * silu_grad(expert_gvals)).astype(jnp.bfloat16)
    expert_dup = (expert_dact * jax.nn.silu(expert_gvals)).astype(jnp.bfloat16)
    gate_grad = jnp.einsum(
        "secd,secf->edf", arrived, expert_dgate, preferred_element_type=jnp.float32
    )
    up_grad = jnp.einsum("secd,secf->edf", arrived, expert_dup, preferred_element_type=jnp.float32)
    expert_din = (
        jnp.einsum("secf,edf->secd", expert_dgate, gate_full, preferred_element_type=jnp.float32)
        + jnp.einsum("secf,edf->secd", expert_dup, up_full, preferred_element_type=jnp.float32)
    ).astype(jnp.bfloat16)
    dreturned = lax.all_to_all(
        expert_din, "experts", split_axis=0, concat_axis=0, tiled=True
    ).reshape(expert_count * capacity, model_width)
    dnormed2_q = jnp.dot(placer, dreturned, preferred_element_type=jnp.float32)
    route_hits = (
        route_q[:, :, None] == jnp.arange(expert_count, dtype=jnp.int32)[None, None, :]
    ).astype(jnp.float32)
    dprob = jnp.sum(route_hits * dgate_k[:, :, None], 1)
    dlogit = prob * (dprob - jnp.sum(prob * dprob, -1, keepdims=True))
    router_part = jnp.dot(normed2_q.astype(jnp.float32).T, dlogit, precision=PRECISE)
    dnormed2_q = dnormed2_q + jnp.dot(
        dlogit, router_weight.astype(jnp.float32).T, precision=PRECISE
    )
    shared_dout = (shared_sig[:, None] * grad_float).astype(jnp.bfloat16)
    shared_dact = jnp.dot(shared_dout, sdown_full.T, preferred_element_type=jnp.float32)
    sdown_grad = jnp.dot(shared_act.T, shared_dout, preferred_element_type=jnp.float32)
    shared_dgate = (shared_dact * shared_uvals * silu_grad(shared_gvals)).astype(jnp.bfloat16)
    shared_dup = (shared_dact * jax.nn.silu(shared_gvals)).astype(jnp.bfloat16)
    sgate_grad = jnp.dot(normed2_b.T, shared_dgate, preferred_element_type=jnp.float32)
    sup_grad = jnp.dot(normed2_b.T, shared_dup, preferred_element_type=jnp.float32)
    row_dots = jnp.sum(grad_float * shared_part, -1)
    dnormed2_part = jnp.dot(
        shared_dgate, sgate_full.T, preferred_element_type=jnp.float32
    ) + jnp.dot(shared_dup, sup_full.T, preferred_element_type=jnp.float32)
    dnormed2_part = dnormed2_part + lax.dynamic_update_slice_in_dim(
        jnp.zeros((row_count, model_width), jnp.float32), dnormed2_q, first_row, 0
    )
    dnormed2, row_dots, router_grad = lax.psum((dnormed2_part, row_dots, router_part), "experts")
    coef = shared_sig * (1.0 - shared_sig) * row_dots
    dnormed2 = dnormed2 + coef[:, None] * shared_gate.astype(jnp.float32)[None, :]
    shared_gate_grad = jnp.dot(coef, normed2_b.astype(jnp.float32), precision=PRECISE)
    norm2_grad = jnp.sum(dnormed2 * normed2, 0)
    dscaled2 = dnormed2 * gain2
    dhidden = grad_float + inverse2 * (
        dscaled2 - normed2 * jnp.mean(dscaled2 * normed2, -1, keepdims=True)
    )
    dhidden_b = dhidden.astype(jnp.bfloat16)
    out_grad_part = jnp.dot(attended_flat.T, dhidden_b, preferred_element_type=jnp.float32)
    dattended = jnp.dot(dhidden_b, out_full.T, preferred_element_type=jnp.float32).astype(
        jnp.bfloat16
    )
    dattended3 = dattended.reshape(row_count, heads_here, HEAD_DIM)
    delta = jnp.sum(dattended3.astype(jnp.float32) * attended.astype(jnp.float32), -1)
    zero_state = jnp.zeros((heads_here, row_count, HEAD_DIM), jnp.float32)
    dkey_sum, dvalue_sum = key_grad_fold(
        key_rows,
        value_rows,
        query_first,
        scale,
        (zero_state, zero_state),
        (
            lax.all_gather(
                query.reshape(row_count, head_span).astype(jnp.float32),
                "context",
                axis=0,
                tiled=True,
            ),
            lax.all_gather(dattended.astype(jnp.float32), "context", axis=0, tiled=True),
            lax.all_gather(jnp.transpose(lse_heads), "context", axis=0, tiled=True),
            lax.all_gather(delta, "context", axis=0, tiled=True),
        ),
    )
    dquery_sum = query_grad_fold(
        query,
        dattended3,
        lse_heads,
        jnp.transpose(delta),
        query_first,
        scale,
        zero_state,
        (
            lax.all_gather(key_flat, "context", axis=0, tiled=True),
            lax.all_gather(value_flat, "context", axis=0, tiled=True),
        ),
    )
    dquery = jnp.transpose(dquery_sum, (1, 0, 2))
    dkey = jnp.transpose(dkey_sum, (1, 0, 2))
    dvalue = jnp.transpose(dvalue_sum, (1, 0, 2))
    dquery_raw = dquery * cosine + rotate_back(dquery * sine_part)
    dkey_raw = dkey * cosine + rotate_back(dkey * sine_part)
    dqkv = jnp.stack(
        [
            dquery_raw.reshape(row_count, head_span),
            dkey_raw.reshape(row_count, head_span),
            dvalue.reshape(row_count, head_span),
        ],
        1,
    )
    bias_grad = jnp.sum(dqkv, 0)
    dqkv_b = dqkv.astype(jnp.bfloat16).reshape(row_count, 3 * head_span)
    qkv_grad = jnp.dot(normed1_b.T, dqkv_b, preferred_element_type=jnp.float32).reshape(
        model_width, 3, head_span
    )
    dnormed1 = lax.psum(
        jnp.dot(dqkv_b, qkv_flat.T, preferred_element_type=jnp.float32).astype(jnp.bfloat16),
        "experts",
    ).astype(jnp.float32)
    norm1_grad = jnp.sum(dnormed1 * normed1, 0)
    dscaled1 = dnormed1 * gain1
    tokens_grad = dhidden + inverse1 * (
        dscaled1 - normed1 * jnp.mean(dscaled1 * normed1, -1, keepdims=True)
    )
    small_sums = (
        lax.psum(norm1_grad.astype(jnp.bfloat16), ("dp", "context")).astype(jnp.float32),
        lax.psum(norm2_grad.astype(jnp.bfloat16), ("dp", "context")).astype(jnp.float32),
        lax.psum(router_grad.astype(jnp.bfloat16), ("dp", "context")).astype(jnp.float32),
        lax.psum(shared_gate_grad.astype(jnp.bfloat16), ("dp", "context")).astype(jnp.float32),
        lax.psum(bias_grad.astype(jnp.bfloat16), ("dp", "context")).astype(jnp.float32),
    )
    large_sums = (
        lax.psum_scatter(
            qkv_grad.astype(jnp.bfloat16), ("dp", "context"), scatter_dimension=0, tiled=True
        ).astype(jnp.float32),
        lax.psum_scatter(
            out_grad_part.astype(jnp.bfloat16), ("dp", "context"), scatter_dimension=1, tiled=True
        ).astype(jnp.float32),
        lax.psum_scatter(
            gate_grad.astype(jnp.bfloat16), ("dp", "context"), scatter_dimension=1, tiled=True
        ).astype(jnp.float32),
        lax.psum_scatter(
            up_grad.astype(jnp.bfloat16), ("dp", "context"), scatter_dimension=1, tiled=True
        ).astype(jnp.float32),
        lax.psum_scatter(
            down_grad.astype(jnp.bfloat16), ("dp", "context"), scatter_dimension=2, tiled=True
        ).astype(jnp.float32),
        lax.psum_scatter(
            sgate_grad.astype(jnp.bfloat16), ("dp", "context"), scatter_dimension=0, tiled=True
        ).astype(jnp.float32),
        lax.psum_scatter(
            sup_grad.astype(jnp.bfloat16), ("dp", "context"), scatter_dimension=0, tiled=True
        ).astype(jnp.float32),
        lax.psum_scatter(
            sdown_grad.astype(jnp.bfloat16), ("dp", "context"), scatter_dimension=1, tiled=True
        ).astype(jnp.float32),
    )
    return (
        block_out[None],
        tokens_grad[None],
        small_sums[0],
        large_sums[0],
        small_sums[4],
        large_sums[1],
        small_sums[1],
        small_sums[2],
        large_sums[2],
        large_sums[3],
        large_sums[4],
        small_sums[3],
        large_sums[5],
        large_sums[6],
        large_sums[7],
    )


def own_half_first(value):
    half = value.shape[-1] // 2
    turned = jnp.concatenate([value[..., half:], value[..., :half]], -1)
    return jnp.where(lax.axis_index("dp") == 0, value, turned)


def dot_nn(left, right):
    return jnp.dot(left, right, preferred_element_type=jnp.float32)


def dot_nt(left, right):
    return lax.dot_general(
        left, right, (((1,), (1,)), ((), ())), preferred_element_type=jnp.float32
    )


def dot_tn(left, right):
    return lax.dot_general(
        left, right, (((0,), (0,)), ((), ())), preferred_element_type=jnp.float32
    )


MESH = pl.DeviceIdType.MESH
DMA = pltpu.SemaphoreType.DMA


def remote(source, target, send_sem, recv_sem, device):
    return pltpu.make_async_remote_copy(
        src_ref=source,
        dst_ref=target,
        send_sem=send_sem,
        recv_sem=recv_sem,
        device_id=device,
        device_id_type=MESH,
    )


def rows_at(ref, start, size):
    return ref.at[pl.ds(pl.multiple_of(start, 16), size), :]


def lanes_at(ref, start, size):
    return ref.at[:, pl.ds(pl.multiple_of(start, 128), size)]


def by_width(device, narrow, body):
    if narrow is None:
        body(False)
    elif isinstance(device, int):
        body(device == narrow)
    else:

        @pl.when(device == narrow)
        def _():
            body(True)

        @pl.when(device != narrow)
        def _():
            body(False)


class Spot:
    def __init__(self):
        self.parts = lax.axis_size("context")
        self.place, self.group = lax.axis_index("context"), lax.axis_index("experts")
        self.twin = {"dp": 1 - lax.axis_index("dp")}
        self.across = lax.rem(self.group + 2, 4)
        self.beside = self.group + 1 - 2 * lax.rem(self.group, 2)
        self.corner = lax.rem(self.beside + 2, 4)
        self.has_left, self.has_right = self.place > 0, self.place < self.parts - 1

    def greet(self, whole_line, twins):
        barrier = pltpu.get_barrier_semaphore()
        devices = [{"experts": self.across}, {"experts": self.beside}]
        if twins:
            devices.append(self.twin)
        for device in devices:
            pl.semaphore_signal(barrier, inc=1, device_id=device, device_id_type=MESH)
        count = len(devices)
        if whole_line:
            for gap in range(1, self.parts):
                device = {"context": lax.rem(self.place + gap, self.parts)}
                pl.semaphore_signal(barrier, inc=1, device_id=device, device_id_type=MESH)
            pl.semaphore_wait(barrier, count + self.parts - 1)
        else:
            for step, there in ((-1, self.has_left), (1, self.has_right)):

                @pl.when(there)
                def _():
                    device = {"context": self.place + step}
                    pl.semaphore_signal(barrier, inc=1, device_id=device, device_id_type=MESH)

            ends = jnp.where(self.has_left & self.has_right, 0, 1)
            pl.semaphore_wait(barrier, count + 2 - ends)

    def far_first(self):
        upper = self.place // (self.parts // 2)
        return [3 * (1 - upper), 2 - upper, 1 + 4 * upper - self.place, self.place]

    def others(self, gap, body):
        @pl.when(self.place >= gap)
        def _():
            body(self.place - gap)

        @pl.when(self.place + gap < self.parts)
        def _():
            body(self.place + gap)


class Share:
    def __init__(self, spot, own, out, sems):
        self.spot, self.own, self.out = spot, own, out
        self.local_sem, self.right_s, self.left_s, self.line_r, self.across_s, self.across_r, self.beside_s, self.beside_r = sems

    @staticmethod
    def sems(parts):
        return [DMA, DMA((parts,)), DMA((parts,)), DMA((parts,)), DMA((parts,)), DMA((parts,)), DMA((2 * parts,)), DMA((2 * parts,))]

    def block(self, part, column):
        rows = self.own.shape[0]
        return rows_at(self.out, (part * 4 + column) * rows, rows)

    def to_right(self, part, source):
        s = self.spot
        return remote(source, self.block(part, s.group), self.right_s.at[part], self.line_r.at[part], {"context": s.place + 1})

    def to_left(self, part, source):
        s = self.spot
        return remote(source, self.block(part, s.group), self.left_s.at[part], self.line_r.at[part], {"context": s.place - 1})

    def to_across(self, part, source):
        s = self.spot
        return remote(source, self.block(part, s.group), self.across_s.at[part], self.across_r.at[part], {"experts": s.across})

    def to_beside(self, part, column, slot, source):
        s = self.spot
        return remote(source, self.block(part, column), self.beside_s.at[slot], self.beside_r.at[slot], {"experts": s.beside})

    def begin(self):
        s = self.spot

        @pl.when(s.has_right)
        def _():
            self.to_right(s.place, self.own).start()

        @pl.when(s.has_left)
        def _():
            self.to_left(s.place, self.own).start()

        self.to_across(s.place, self.own).start()
        self.to_beside(s.place, s.group, s.place, self.own).start()
        self.local().start()

    def local(self):
        return pltpu.make_async_copy(self.own, self.block(self.spot.place, self.spot.group), self.local_sem)

    def pass_on(self, part):
        s = self.spot
        self.to_across(part, self.block(part, s.group)).wait_recv()
        self.to_beside(part, s.across, s.parts + part, self.block(part, s.across)).start()

    def arrival(self, part, onward, there):
        s = self.spot
        mine = self.block(part, s.group)
        self.to_right(part, mine).wait_recv()

        @pl.when(there)
        def _():
            onward(part, mine).start()

        self.to_across(part, mine).start()
        self.to_beside(part, s.group, part, mine).start()

    def step(self, gap):
        s = self.spot

        @pl.when(s.place >= gap)
        def _():
            self.arrival(s.place - gap, self.to_right, s.has_right)

        @pl.when(s.place + gap < s.parts)
        def _():
            self.arrival(s.place + gap, self.to_left, s.has_left)

        if gap == 1:
            self.pass_on(s.place)
        else:
            s.others(gap - 1, self.pass_on)

    def end(self):
        s = self.spot
        s.others(s.parts - 1, self.pass_on)
        self.local().wait()
        for part in range(s.parts):
            self.to_beside(part, s.beside, part, self.own).wait_recv()
            self.to_beside(part, s.beside, s.parts + part, self.own).wait_recv()
            self.to_across(part, self.own).wait_send()
            self.to_beside(part, s.group, part, self.own).wait_send()
            self.to_beside(part, s.group, s.parts + part, self.own).wait_send()

            @pl.when(s.has_right & (part <= s.place))
            def _():
                self.to_right(part, self.own).wait_send()

            @pl.when(s.has_left & (part >= s.place))
            def _():
                self.to_left(part, self.own).wait_send()


class Sum:
    def __init__(self, spot, part_ref, out, scratch):
        self.spot, self.part_ref, self.out = spot, part_ref, out
        (self.beside_buf, self.across_out, self.across_buf, self.line_out, self.left_buf, self.right_buf,
         self.beside_s, self.beside_r, self.across_s, self.across_r, self.right_s, self.left_s, self.from_left, self.from_right) = scratch
        self.order = spot.far_first()

    @staticmethod
    def scratch(parts, rows, width):
        one = pltpu.VMEM((parts, rows, width), jnp.bfloat16)
        two = pltpu.VMEM((2 * parts, rows, width), jnp.bfloat16)
        return [two, one, one, one, one, one, DMA((2 * parts,)), DMA((2 * parts,))] + [DMA((parts,))] * 6

    def base(self, part, column):
        rows = self.out.shape[0]
        return pl.multiple_of((part * 4 + column) * rows, rows)

    def to_beside(self, part, column, slot):
        source = self.part_ref.at[pl.ds(self.base(part, column), self.out.shape[0]), :]
        return remote(source, self.beside_buf.at[slot], self.beside_s.at[slot], self.beside_r.at[slot], {"experts": self.spot.beside})

    def to_across(self, part):
        return remote(self.across_out.at[part], self.across_buf.at[part], self.across_s.at[part], self.across_r.at[part], {"experts": self.spot.across})

    def to_right(self, part):
        return remote(self.line_out.at[part], self.left_buf.at[part], self.right_s.at[part], self.from_left.at[part], {"context": self.spot.place + 1})

    def to_left(self, part):
        return remote(self.line_out.at[part], self.right_buf.at[part], self.left_s.at[part], self.from_right.at[part], {"context": self.spot.place - 1})

    def chunks(self, body):
        step = 16

        def one(index, carry):
            start = pl.multiple_of(index * step, step)
            body(pl.ds(start, step), start, step)
            return carry

        lax.fori_loop(0, self.out.shape[0] // step, one, 0)

    def mine(self, base, start, step):
        return self.part_ref[pl.ds(pl.multiple_of(base + start, step), step), :].astype(jnp.float32)

    def begin(self):
        s = self.spot
        for part in self.order:
            self.to_beside(part, s.corner, s.parts + part).start()
        for part in self.order:
            self.to_beside(part, s.beside, part).start()

    def cross(self, index):
        s, part = self.spot, self.order[index]
        self.to_beside(part, s.corner, s.parts + part).wait_recv()
        base = self.base(part, s.across)

        def add(at, start, step):
            total = self.mine(base, start, step) + self.beside_buf[s.parts + part, at, :].astype(jnp.float32)
            self.across_out[part, at, :] = total.astype(jnp.bfloat16)

        self.chunks(add)
        self.to_across(part).start()

    def line(self, index):
        s, part = self.spot, self.order[index]
        self.to_beside(part, s.beside, part).wait_recv()
        self.to_across(part).wait_recv()
        base = self.base(part, s.group)
        f32 = jnp.float32

        def total(at, start, step):
            return self.mine(base, start, step) + self.beside_buf[part, at, :].astype(f32) + self.across_buf[part, at, :].astype(f32)

        def send(buf):
            def add(at, start, step):
                value = total(at, start, step)
                if buf is not None:
                    value = value + buf[part, at, :].astype(f32)
                self.line_out[part, at, :] = value.astype(jnp.bfloat16)

            self.chunks(add)

        if index < s.parts - 1:
            goes_right = part > s.place
            goes_left = jnp.logical_not(goes_right)

            @pl.when(goes_right & s.has_left)
            def _():
                self.to_right(part).wait_recv()
                send(self.left_buf)

            @pl.when(goes_left & s.has_right)
            def _():
                self.to_left(part).wait_recv()
                send(self.right_buf)

            @pl.when((goes_right & jnp.logical_not(s.has_left)) | (goes_left & jnp.logical_not(s.has_right)))
            def _():
                send(None)

            @pl.when(goes_right)
            def _():
                self.to_right(part).start()

            @pl.when(goes_left)
            def _():
                self.to_left(part).start()
        else:

            def keep(at, start, step):
                self.out[at, :] = total(at, start, step)

            self.chunks(keep)
            for there, copy, buf in ((s.has_left, self.to_right, self.left_buf), (s.has_right, self.to_left, self.right_buf)):

                @pl.when(there)
                def _():
                    copy(part).wait_recv()

                    def add(at, start, step):
                        self.out[at, :] = self.out[at, :] + buf[part, at, :].astype(f32)

                    self.chunks(add)

    def end(self):
        s = self.spot
        for part in range(s.parts):
            self.to_beside(part, s.corner, s.parts + part).wait_send()
            self.to_beside(part, s.beside, part).wait_send()
            self.to_across(part).wait_send()

            @pl.when(part > s.place)
            def _():
                self.to_right(part).wait_send()

            @pl.when(part < s.place)
            def _():
                self.to_left(part).wait_send()


class Move:
    def __init__(self, spot, items, sems):
        self.spot, self.items = spot, items
        self.line_s, self.line_r, self.twin_s, self.twin_r, self.local_sem = sems

    @staticmethod
    def sems(count, parts):
        return [DMA((count * parts,))] * 4 + [DMA((count,))]

    def fit(self, number, device, body):
        by_width(device, self.items[number]["short"], body)

    def to(self, number, target, source, short):
        s, item = self.spot, self.items[number]
        sems = self.line_s.at[number * s.parts + target], self.line_r.at[number * s.parts + source]
        return remote(item["src"](target, short), item["dst"](0, source, short), *sems, {"context": target})

    def on(self, number, source, short, view=None):
        s, item = self.spot, self.items[number]
        slot = number * s.parts + source
        view = item["dst"](0, source, short) if view is None else view
        return remote(view, item["dst"](1, source, short), self.twin_s.at[slot], self.twin_r.at[slot], s.twin)

    def local(self, number, short):
        s, item = self.spot, self.items[number]
        return pltpu.make_async_copy(item["src"](s.place, short), item["dst"](0, s.place, short), self.local_sem.at[number])

    def own(self, number):
        s, item = self.spot, self.items[number]

        def one(short):
            self.on(number, s.place, short, item["src"](s.place, short)).start()
            self.local(number, short).start()

        self.fit(number, s.place, one)

    def send_gap(self, number, gap):
        s = self.spot

        def one(target):
            self.fit(number, target, lambda short: self.to(number, target, s.place, short).start())

        s.others(gap, one)

    def send(self, number):
        for gap in range(self.spot.parts - 1, 0, -1):
            self.send_gap(number, gap)

    def forward(self, number, gap):
        s = self.spot

        def one(source):
            def step(short):
                self.to(number, s.place, source, short).wait_recv()
                self.on(number, source, short).start()

            self.fit(number, s.place, step)

        s.others(gap, one)

    def ready(self, number):
        s = self.spot

        def one(short):
            self.local(number, short).wait()
            for part in range(s.parts):
                self.on(number, part, short).wait_recv()

        self.fit(number, s.place, one)

    def sent(self):
        s = self.spot
        for number in range(len(self.items)):

            def one(short):
                for part in range(s.parts):
                    self.on(number, part, short).wait_send()

            self.fit(number, s.place, one)
            for part in range(s.parts):

                @pl.when(part != s.place)
                def _():
                    self.fit(number, part, lambda short: self.to(number, part, s.place, short).wait_send())

    def end(self):
        for number in range(len(self.items)):
            self.ready(number)
        self.sent()


class Return:
    def __init__(self, spot, items, got, mine, sems):
        self.spot, self.items, self.got, self.mine_buf = spot, items, got, mine
        self.twin_s, self.twin_r, self.load, self.line_s, self.line_r, self.local_sem = sems
        self.order = spot.far_first()
        self.bases = []
        for item in items:
            self.bases.append(self.bases[-1][1] if self.bases else 0)
            self.bases[-1] = (self.bases[-1], self.bases[-1] + len(item["pieces"]) * spot.parts)

    @staticmethod
    def scratch(shapes, pieces, parts):
        count = len(shapes)
        buf = [pltpu.VMEM((parts,) + shape, jnp.bfloat16) for shape in shapes]
        sems = [DMA((count * parts,))] * 3 + [DMA((sum(pieces) * parts,))] * 2 + [DMA((sum(pieces),))]
        return buf + buf + sems

    def swap(self, number, part):
        item, slot = self.items[number], number * self.spot.parts + part
        return remote(item["block"](1, part), self.got[number].at[part], self.twin_s.at[slot], self.twin_r.at[slot], self.spot.twin)

    def fetch(self, number, part):
        item, slot = self.items[number], number * self.spot.parts + part
        return pltpu.make_async_copy(item["block"](0, part), self.mine_buf[number].at[part], self.load.at[slot])

    def start_one(self, number, index):
        self.swap(number, self.order[index]).start()
        self.fetch(number, self.order[index]).start()

    def start(self, number):
        for index in range(self.spot.parts):
            self.start_one(number, index)

    def piece(self, number, which, target, source, short):
        s = self.spot
        cut, out = self.items[number]["pieces"][which]
        slot = self.bases[number][0] + which * s.parts
        return remote(cut(self.mine_buf[number].at[target], short), out(source, short), self.line_s.at[slot + target], self.line_r.at[slot + source], {"context": target})

    def keep(self, number, which, short):
        s = self.spot
        cut, out = self.items[number]["pieces"][which]
        slot = self.bases[number][0] // s.parts + which
        return pltpu.make_async_copy(cut(self.mine_buf[number].at[s.place], short), out(s.place, short), self.local_sem.at[slot])

    def fit(self, number, source, body):
        by_width(source, self.items[number].get("short"), body)

    def reduce(self, number, index):
        s, part = self.spot, self.order[index]
        item = self.items[number]
        self.swap(number, part).wait_recv()
        self.fetch(number, part).wait()
        mine, got = self.mine_buf[number], self.got[number]
        rows, step = mine.shape[1], 32

        def one(at, carry):
            span = pl.ds(pl.multiple_of(at * step, step), step)
            total = mine[part, span, :].astype(jnp.float32) + got[part, span, :].astype(jnp.float32)
            mine[part, span, :] = total.astype(jnp.bfloat16)
            return carry

        lax.fori_loop(0, rows // step, one, 0)
        for which in range(len(item["pieces"])):
            if index < s.parts - 1:
                self.fit(number, s.place, lambda short: self.piece(number, which, part, s.place, short).start())
            else:
                self.fit(number, s.place, lambda short: self.keep(number, which, short).start())

    def end(self):
        s = self.spot
        for number, item in enumerate(self.items):
            for part in range(s.parts):
                self.swap(number, part).wait_send()
                for which in range(len(item["pieces"])):

                    @pl.when(part != s.place)
                    def _():
                        self.fit(number, s.place, lambda short: self.piece(number, which, part, s.place, short).wait_send())
                        self.fit(number, part, lambda short: self.piece(number, which, s.place, part, short).wait_recv())

            for which in range(len(item["pieces"])):
                self.fit(number, s.place, lambda short: self.keep(number, which, short).wait())


class Grads:
    def __init__(self, rows, cotangents, dup, act, up_out, down_out, up_buf, down_buf, up_s, down_s):
        self.rows, self.cotangents, self.dup, self.act = rows, cotangents, dup, act
        self.up_out, self.down_out, self.up_buf, self.down_buf = up_out, down_out, up_buf, down_buf
        self.up_s, self.down_s = up_s, down_s
        self.step = 256

    @staticmethod
    def scratch():
        up, down = pltpu.VMEM((2, 256, 2 * WINDOW), jnp.bfloat16), pltpu.VMEM((2, WINDOW, 256), jnp.bfloat16)
        return [up, down, DMA((2,)), DMA((2,))]

    def copies(self, index):
        at = pl.ds(pl.multiple_of(index * self.step, self.step), self.step)
        slot = lax.rem(index, 2)
        return (
            lambda: pltpu.make_async_copy(self.up_buf.at[slot], self.up_out.at[at, :], self.up_s.at[slot]),
            lambda: pltpu.make_async_copy(self.down_buf.at[slot], self.down_out.at[:, at], self.down_s.at[slot]),
        )

    def run(self):
        count = self.cotangents.shape[1] // self.step

        def one(index, carry):
            up_copy, down_copy = self.copies(index)

            @pl.when(index >= 2)
            def _():
                up_copy().wait()
                down_copy().wait()

            slot = lax.rem(index, 2)
            at = pl.multiple_of(index * self.step, self.step)
            up = dot_tn(self.rows[:, pl.ds(at, self.step)], self.dup[...])
            self.up_buf[slot] = up.astype(jnp.bfloat16)
            down = dot_tn(self.act[...], self.cotangents[:, pl.ds(at, self.step)])
            self.down_buf[slot] = down.astype(jnp.bfloat16)
            up_copy().start()
            down_copy().start()
            return carry

        lax.fori_loop(0, count, one, 0)
        for index in (count - 2, count - 1):
            for copy in self.copies(index):
                copy().wait()


def comm_call(kernel, number, name, out_shape, out_specs, in_specs, scratch, bytes_moved):
    return pl.pallas_call(
        kernel,
        out_shape=out_shape,
        in_specs=in_specs,
        out_specs=out_specs,
        scratch_shapes=scratch,
        compiler_params=pltpu.CompilerParams(collective_id=number, has_side_effects=True),
        cost_estimate=pl.CostEstimate(flops=0, bytes_accessed=bytes_moved, transcendentals=0),
        name=name,
    )


IN_VMEM = pl.BlockSpec(memory_space=pltpu.VMEM)
IN_PLACE = pl.BlockSpec(memory_space=pl.ANY)
WINDOW = 384


SPARE = 128


def narrow_of(k):
    return 0 if k % 2 else 3


def window_of(k, index, narrow):
    if narrow_of(k) == 0:
        return (0, WINDOW - SPARE, 0) if narrow else (index * WINDOW - SPARE, WINDOW, 0)
    return (index * WINDOW, WINDOW - SPARE, SPARE) if narrow else (index * WINDOW, WINDOW, 0)


def first_unit(value):
    return value if isinstance(value, int) else pl.multiple_of(value, SPARE)


def units_at(ref, k, index, narrow, axis, base=0):
    start, size, inside = window_of(k, index, narrow)
    start = first_unit(start) if base is None else base + inside
    return ref.at[pl.ds(start, size), :] if axis == 0 else ref.at[:, pl.ds(start, size)]


def turn(value, cosine, sine_part):
    return value * cosine + pltpu.roll(value, HEAD_DIM // 2, 1) * sine_part


def turn_tables(facts):
    both = facts[:, :HEAD_DIM].astype(jnp.float32) + facts[:, HEAD_DIM:].astype(jnp.float32)
    swapped = pltpu.roll(both, HEAD_DIM // 2, 1)
    low = lax.broadcasted_iota(jnp.int32, (1, HEAD_DIM), 1) < HEAD_DIM // 2
    return jnp.where(low, both, swapped), jnp.where(low, -swapped, both)


def attention_first(value, grad, qkv_in, out_weight, bias, shared_down, expert_down, number):
    parts = lax.axis_size("context")
    rows, wide = value.shape
    block, span = qkv_in.shape[1], 3 * HEAD_DIM
    head, lanes = out_weight.shape[0] // parts, out_weight.shape[1]
    width, length = 2 * parts * lanes, rows * parts * 4
    count = 1 + expert_down.shape[0]
    step = 256
    scale = HEAD_DIM ** (-0.5)
    f32, bf16 = jnp.float32, jnp.bfloat16
    sets = [
        [
            pltpu.VMEM((length, wide), bf16),
            pltpu.VMEM((2 * parts * block, span), bf16),
            pltpu.VMEM((head, width), bf16),
            pltpu.VMEM((length, width), bf16),
            DMA((3,)),
        ],
        Share.sems(parts),
        Move.sems(4 + count, parts),
        Sum.scratch(parts, rows, width),
        Share.sems(parts),
    ]

    def kernel(own_ref, grad_ref, qkv_ref, outw_ref, bias_ref, shared_ref, expert_ref,
               all_hbm, grad_all, wqkv_hbm, wout_hbm, wd_ref, q_ref, k_ref, v_ref, att_ref, lse_ref, sum_ref, *scratch):
        scratch, split = list(scratch), []
        for one in sets:
            split.append(scratch[: len(one)])
            scratch = scratch[len(one) :]
        all_ref, wqkv_ref, wout_ref, part_ref, keep = split[0]
        spot = Spot()
        share = Share(spot, own_ref, all_ref, split[1])
        grads = Share(spot, grad_ref, grad_all, split[4])
        items = [
            {
                "src": lambda target, short, which=which: lanes_at(qkv_ref.at[which], target * HEAD_DIM, HEAD_DIM),
                "dst": lambda side, source, short, which=which: rows_at(
                    wqkv_ref.at[:, pl.ds(which * HEAD_DIM, HEAD_DIM)], (side * parts + source) * block, block
                ),
                "short": None,
            }
            for which in range(3)
        ]
        items += [
            {
                "src": lambda target, short: rows_at(outw_ref, target * head, head),
                "dst": lambda side, source, short: lanes_at(wout_ref, (side * parts + source) * lanes, lanes),
                "short": None,
            },
        ]

        def down(k):
            ref = shared_ref if k == 0 else expert_ref.at[k - 1]
            return {
                "src": lambda target, short: units_at(ref, k, target, short, 0, None),
                "dst": lambda side, source, short: lanes_at(
                    units_at(wd_ref, k, 0, short, 0, k * WINDOW), (side * parts + source) * lanes, lanes
                ),
                "short": narrow_of(k),
            }

        move = Move(spot, items + [down(k) for k in range(count)], split[2])
        summed = Sum(spot, part_ref, sum_ref, split[3])
        copies = [
            pltpu.make_async_copy(source, target, keep.at[index])
            for index, (source, target) in enumerate(((all_ref, all_hbm), (wqkv_ref, wqkv_hbm), (wout_ref, wout_hbm)))
        ]

        def project(index, carry):
            at = pl.ds(pl.multiple_of(index * step, step), step)
            qkv = jnp.dot(all_ref[at, :width], wqkv_ref[...], preferred_element_type=f32) + bias_ref[...]
            cosine, sine_part = turn_tables(all_ref[at, width:])
            q_ref[at, :] = turn(qkv[:, :HEAD_DIM], cosine, sine_part).astype(bf16)
            k_ref[at, :] = turn(qkv[:, HEAD_DIM : 2 * HEAD_DIM], cosine, sine_part).astype(bf16)
            v_ref[at, :] = qkv[:, 2 * HEAD_DIM :].astype(bf16)
            return carry

        def attend(index, carry):
            start = pl.multiple_of(index * step, step)
            at = pl.ds(start, step)
            scores = dot_nt(q_ref[at, :], k_ref[...]) * scale
            query_index = start + lax.broadcasted_iota(jnp.int32, scores.shape, 0)
            allowed = lax.broadcasted_iota(jnp.int32, scores.shape, 1) <= query_index
            row_max = jnp.max(jnp.where(allowed, scores, MASKED), -1, keepdims=True)
            weights = jnp.where(allowed, jnp.exp(scores - row_max), 0.0)
            row_sum = jnp.sum(weights, -1, keepdims=True)
            attended = (jnp.dot(weights.astype(bf16), v_ref[...], preferred_element_type=f32) / row_sum).astype(bf16)
            att_ref[at, :] = attended
            lse_ref[at, :] = jnp.broadcast_to(row_max + jnp.log(row_sum), (step, HEAD_DIM))
            part_ref[at, :] = jnp.dot(attended, wout_ref[...], preferred_element_type=f32).astype(bf16)
            return carry

        spot.greet(True, True)
        share.begin()
        for number in range(len(move.items)):
            move.own(number)
        move.send(0)
        share.step(1)
        move.send(1)
        share.step(2)
        move.send(2)
        share.step(3)
        move.send(3)
        move.send(4)
        for number in range(4):
            for gap in (1, 2, 3):
                move.forward(number, gap)
        share.end()
        grads.begin()
        copies[0].start()
        for number in range(3):
            move.ready(number)
        copies[1].start()
        lax.fori_loop(0, length // step, project, 0)
        move.ready(3)
        copies[2].start()
        grads.step(1)
        for number in range(5, len(move.items)):
            move.send(number)
        lax.fori_loop(0, length // step, attend, 0)
        summed.begin()
        for gap in (1, 2, 3):
            move.forward(4, gap)
        grads.step(2)
        for index in range(parts):
            summed.cross(index)
        for number in range(5, len(move.items)):
            for gap in (1, 2, 3):
                move.forward(number, gap)
        grads.step(3)
        for index in range(parts):
            summed.line(index)
        grads.end()
        summed.end()
        for number in range(4, len(move.items)):
            move.ready(number)
        move.sent()
        for copy in copies:
            copy.wait()

    heads = jax.ShapeDtypeStruct((length, HEAD_DIM), bf16)
    return comm_call(
        kernel,
        number,
        "attention_first",
        [
            jax.ShapeDtypeStruct((length, wide), bf16),
            jax.ShapeDtypeStruct((length, width), bf16),
            jax.ShapeDtypeStruct((2 * parts * block, span), bf16),
            jax.ShapeDtypeStruct((head, width), bf16),
            jax.ShapeDtypeStruct((count * WINDOW, width), bf16),
            heads,
            heads,
            heads,
            heads,
            jax.ShapeDtypeStruct((length, HEAD_DIM), f32),
            jax.ShapeDtypeStruct((rows, width), f32),
        ],
        [IN_PLACE] * 5 + [IN_VMEM] * 6,
        [IN_VMEM, IN_VMEM, IN_PLACE, IN_PLACE, IN_VMEM, IN_PLACE, IN_PLACE],
        [one for group in sets for one in group],
        250_000_000,
    )(value, grad, qkv_in, out_weight, bias, shared_down, expert_down)


def share_move_compute(value, grad_all, shared_gate, shared_up, expert_gate, expert_up, wd, number):
    parts = lax.axis_size("context")
    rows, wide = value.shape
    width = wd.shape[1]
    block = shared_gate.shape[0]
    stacks = 1 + expert_gate.shape[0]
    count = 2 * stacks
    length = rows * parts * 4
    experts = (stacks - 1) * 4
    step = 256
    f32, bf16 = jnp.float32, jnp.bfloat16
    share_sems, move_sems, grad_scratch = Share.sems(parts), Move.sems(count, parts), Grads.scratch()
    back_scratch = Return.scratch([(block, 2 * WINDOW)], [2], parts)
    scratch = [
        pltpu.VMEM((length, wide), bf16),
        pltpu.VMEM((length, width), bf16),
        pltpu.VMEM((2 * parts * block, count * WINDOW), bf16),
        pltpu.VMEM(wd.shape, bf16),
        pltpu.VMEM((length, width), f32),
        pltpu.VMEM((length, width), f32),
        pltpu.VMEM((length, 128), f32),
        pltpu.VMEM((length, 2 * WINDOW), bf16),
        pltpu.VMEM((length, 4 * WINDOW), bf16),
        pltpu.VMEM((length, WINDOW), f32),
        pltpu.VMEM((length, WINDOW), f32),
        pltpu.VMEM((2, step, width + 128), bf16),
        pltpu.VMEM((2, step, width), bf16),
        DMA((3,)),
        DMA((stacks,)),
        DMA((stacks,)),
        DMA((length // step,)),
        DMA((length // step,)),
    ]

    def kernel(own_ref, grad_hbm, sg_ref, su_ref, eg_ref, eu_ref, wd_hbm, both_hbm, send_hbm, branch_hbm, dup_hbm, act_hbm, upg_hbm, downg_hbm, gate_out, up_out, *rest):
        both, grads_ref, wgu, wd_ref, dx_acc, out_acc, dot_acc, act_ref, dup_ref, raw_ref, gate_ref, send_buf, branch_buf, load, act_s, dup_s, send_s, branch_s = rest[: len(scratch)]
        grad_refs, sems = rest[len(scratch) : len(scratch) + 4], rest[len(scratch) + 4 :]
        back_refs, sems = sems[: len(back_scratch)], sems[len(back_scratch) :]
        spot = Spot()
        share = Share(spot, own_ref, both, sems[: len(share_sems)])

        def item(number):
            k = number // 2
            shared, expert = (sg_ref, eg_ref) if number % 2 == 0 else (su_ref, eu_ref)
            ref = shared if k == 0 else expert.at[k - 1]
            return {
                "src": lambda target, short: units_at(ref, k, target, short, 1, None),
                "dst": lambda side, source, short: rows_at(
                    units_at(wgu, k, 0, short, 1, number * WINDOW), (side * parts + source) * block, block
                ),
                "short": narrow_of(k),
            }

        move = Move(spot, [item(number) for number in range(count)], sems[len(share_sems) :])
        weights = pltpu.make_async_copy(wd_hbm, wd_ref, load.at[0])
        keep = pltpu.make_async_copy(both, both_hbm, load.at[1])
        cotangents = pltpu.make_async_copy(grad_hbm, grads_ref, load.at[2])
        column = lax.broadcasted_iota(jnp.int32, (1, 128), 1)
        pieces = length // step

        def send_out(index):
            at = pl.ds(pl.multiple_of(index * step, step), step)
            return pltpu.make_async_copy(send_buf.at[lax.rem(index, 2)], send_hbm.at[at, :], send_s.at[index])

        def branch_out(index):
            at = pl.ds(pl.multiple_of(index * step, step), step)
            return pltpu.make_async_copy(branch_buf.at[lax.rem(index, 2)], branch_hbm.at[at, :], branch_s.at[index])

        back = Return(
            spot, [up_item(upg_hbm, 0, 0, gate_out, up_out, block, parts)], back_refs[:1], back_refs[1:2], back_refs[2:]
        )

        def slots(k):
            return pl.ds(2 * (k % 2) * WINDOW, 2 * WINDOW), pl.ds((k % 2) * WINDOW, WINDOW)

        def act_out():
            return pltpu.make_async_copy(act_ref.at[:, slots(stacks - 1)[1]], act_hbm, act_s.at[0])

        def dup_out():
            return pltpu.make_async_copy(dup_ref.at[:, slots(stacks - 1)[0]], dup_hbm, dup_s.at[0])

        def gradients(k):
            up, down = pl.ds(2 * k * WINDOW, 2 * WINDOW), pl.ds(k * WINDOW, WINDOW)
            dup_slot, act_slot = slots(k)
            Grads(both, grads_ref, dup_ref.at[:, dup_slot], act_ref.at[:, act_slot], upg_hbm.at[:, up], downg_hbm.at[down, :], *grad_refs).run()

        def compute(k, halfway):
            up, down = pl.ds(2 * k * WINDOW, 2 * WINDOW), pl.ds(k * WINDOW, WINDOW)
            dup_slot, act_slot = slots(k)
            at = experts if k == 0 else spot.group * (stacks - 1) + k - 1
            here = jnp.where(column == at, 1.0, 0.0)
            both_parts = jnp.where((column == at) | (column == at + 64), 1.0, 0.0)

            def one(index, carry):
                pl.when(index == pieces // 2)(halfway)
                rows_here = pl.ds(pl.multiple_of(index * step, step), step)
                if k == stacks - 1:
                    raw, g_vals = raw_ref[rows_here, :], gate_ref[rows_here, :]
                    u_vals = jnp.dot(
                        both[rows_here, :width], wgu[:, pl.ds((2 * k + 1) * WINDOW, WINDOW)], preferred_element_type=f32
                    )
                else:
                    vals = jnp.dot(both[rows_here, :width], wgu[:, up], preferred_element_type=f32)
                    raw = dot_nt(grads_ref[rows_here, :], wd_ref[down, :])
                    g_vals, u_vals = vals[:, :WINDOW], vals[:, WINDOW:]
                coef = jnp.sum(both[rows_here, width:].astype(f32) * both_parts, -1, keepdims=True)
                sig_g = jax.nn.sigmoid(g_vals)
                silu_g = g_vals * sig_g
                act = silu_g * u_vals
                dots = jnp.sum(raw * act, -1, keepdims=True) * here
                act_ref[rows_here, act_slot] = (act * coef).astype(bf16)
                dact = raw * coef
                dup_ref[rows_here, pl.ds(2 * (k % 2) * WINDOW, WINDOW)] = (
                    dact * u_vals * (sig_g * (1.0 + g_vals * (1.0 - sig_g)))
                ).astype(bf16)
                dup_ref[rows_here, pl.ds((2 * (k % 2) + 1) * WINDOW, WINDOW)] = (dact * silu_g).astype(bf16)
                out_part = jnp.dot(act_ref[rows_here, act_slot], wd_ref[down, :], preferred_element_type=f32)
                dx_part = dot_nt(dup_ref[rows_here, dup_slot], wgu[:, up])
                if k == 0:
                    out_acc[rows_here, :] = out_part
                    dx_acc[rows_here, :] = dx_part
                    dot_acc[rows_here, :] = dots
                elif k < stacks - 1:
                    out_acc[rows_here, :] += out_part
                    dx_acc[rows_here, :] += dx_part
                    dot_acc[rows_here, :] += dots
                else:

                    @pl.when(index >= 2)
                    def _():
                        send_out(index - 2).wait()
                        branch_out(index - 2).wait()

                    slot = lax.rem(index, 2)
                    branch_buf[slot] = (out_acc[rows_here, :] + out_part).astype(bf16)
                    send_buf[slot, :, :width] = (dx_acc[rows_here, :] + dx_part).astype(bf16)
                    send_buf[slot, :, width:] = (dot_acc[rows_here, :] + dots).astype(bf16)
                    send_out(index).start()
                    branch_out(index).start()
                return carry

            lax.fori_loop(0, pieces, one, 0)

        def prepare(index, carry):
            rows_here = pl.ds(pl.multiple_of(index * step, step), step)
            last = stacks - 1
            raw_ref[rows_here, :] = dot_nt(grads_ref[rows_here, :], wd_ref[pl.ds(last * WINDOW, WINDOW), :])
            gate_ref[rows_here, :] = jnp.dot(
                both[rows_here, :width], wgu[:, pl.ds(2 * last * WINDOW, WINDOW)], preferred_element_type=f32
            )
            return carry

        def forward(number):
            for gap in (1, 2, 3):
                move.forward(number, gap)

        spot.greet(True, True)
        share.begin()
        weights.start()
        cotangents.start()
        for number in range(count):
            move.own(number)
        move.send(0)
        share.step(1)
        move.send(1)
        share.step(2)
        forward(0)
        share.step(3)
        for number in range(2, count):
            move.send(number)
        share.end()
        keep.start()
        forward(1)
        weights.wait()
        cotangents.wait()
        for k in range(stacks):

            @pl.when(spot.place == narrow_of(k))
            def _():
                spare = 0 if narrow_of(k) else WINDOW - SPARE
                wd_ref[pl.ds(k * WINDOW + spare, SPARE), :] = jnp.zeros((SPARE, width), bf16)
                for which in (2 * k, 2 * k + 1):
                    wgu[:, pl.ds(which * WINDOW + spare, SPARE)] = jnp.zeros((2 * parts * block, SPARE), bf16)

        for k in range(stacks):
            last = k == stacks - 1
            if not last:
                forward(2 * k + 2)
                if k == stacks - 2:
                    back.start_one(0, 1)
            else:
                back.reduce(0, 0)
                back.reduce(0, 1)
            move.ready(2 * k)
            if last:
                lax.fori_loop(0, pieces, prepare, 0)
            move.ready(2 * k + 1)

            def halfway():
                if last:
                    back.reduce(0, 2)
                else:
                    forward(2 * k + 3)
                if k == stacks - 2:
                    back.start_one(0, 2)
                    back.start_one(0, 3)

            compute(k, halfway)
            if not last:
                gradients(k)
            if k == 0:
                back.start_one(0, 0)
        back.reduce(0, 3)
        act_out().start()
        dup_out().start()
        for index in (pieces - 2, pieces - 1):
            send_out(index).wait()
            branch_out(index).wait()
        act_out().wait()
        dup_out().wait()
        keep.wait()
        move.sent()
        back.end()

    return comm_call(
        kernel,
        number,
        "share_move_compute",
        [
            jax.ShapeDtypeStruct((length, wide), bf16),
            jax.ShapeDtypeStruct((length, width + 128), bf16),
            jax.ShapeDtypeStruct((length, width), bf16),
            jax.ShapeDtypeStruct((length, 2 * WINDOW), bf16),
            jax.ShapeDtypeStruct((length, WINDOW), bf16),
            jax.ShapeDtypeStruct((width, 2 * (stacks - 1) * WINDOW), bf16),
            jax.ShapeDtypeStruct(((stacks - 1) * WINDOW, width), bf16),
            jax.ShapeDtypeStruct(shared_gate.shape, bf16),
            jax.ShapeDtypeStruct(shared_gate.shape, bf16),
        ],
        [IN_PLACE] * 9,
        [IN_VMEM] + [IN_PLACE] * 6,
        scratch + grad_scratch + back_scratch + share_sems + move_sems,
        300_000_000,
    )(value, grad_all, shared_gate, shared_up, expert_gate, expert_up, wd)


def up_item(grads_ref, at, k, gate_ref, up_ref, block, parts):
    def piece(offset, ref):
        return (
            lambda buf, short: units_at(buf, k, 0, short, 1, offset),
            lambda source, short: units_at(ref, k, source, short, 1, None),
        )

    return {
        "block": lambda side, part: grads_ref.at[
            pl.ds(pl.multiple_of((side * parts + part) * block, block), block), pl.ds(2 * at * WINDOW, 2 * WINDOW)
        ],
        "pieces": [piece(0, gate_ref), piece(WINDOW, up_ref)],
        "short": narrow_of(k),
    }


def down_item(grads_ref, at, k, down_ref, parts):
    lanes = down_ref.shape[1]
    return {
        "block": lambda side, part: grads_ref.at[
            pl.ds(at * WINDOW, WINDOW), pl.ds(pl.multiple_of((side * parts + part) * lanes, lanes), lanes)
        ],
        "pieces": [
            (
                lambda buf, short: units_at(buf, k, 0, short, 0),
                lambda source, short: units_at(down_ref, k, source, short, 0, None),
            )
        ],
        "short": narrow_of(k),
    }


def attention_last(send4, up_grads, down_grads, hidden, grad, gain, chances, router, out_w, qkv_w, heads, lse, shared, number):
    lazy = [send4, router, out_w, qkv_w, *heads, lse, shared]
    parts = lax.axis_size("context")
    length, width = send4.shape[0], hidden.shape[1]
    rows, wide = hidden.shape[0], send4.shape[1]
    block = up_grads.shape[0] // (2 * parts)
    lanes = down_grads.shape[1] // (2 * parts)
    units = WINDOW * parts - 128
    step = 256
    experts = 8
    scale = HEAD_DIM ** (-0.5)
    f32, bf16 = jnp.float32, jnp.bfloat16
    shapes, pieces = [(WINDOW, lanes), (block, 2 * WINDOW), (WINDOW, lanes)], [1, 2, 1]
    sets = [
        [
            pltpu.VMEM((rows, wide), f32),
            pltpu.VMEM((rows, width), bf16),
            pltpu.VMEM((length, width), bf16),
            pltpu.VMEM((length, width), bf16),
            pltpu.VMEM((length, 3 * HEAD_DIM), bf16),
            pltpu.VMEM((length, HEAD_DIM), f32),
            pltpu.VMEM((length, HEAD_DIM), f32),
            pltpu.VMEM((length, HEAD_DIM), f32),
            DMA,
        ],
        [pltpu.VMEM(one.shape, one.dtype) for one in lazy] + [DMA((len(lazy),))],
        Sum.scratch(parts, rows, wide),
        Share.sems(parts),
        Sum.scratch(parts, rows, width),
        Return.scratch(shapes, pieces, parts),
    ]

    def kernel(upg_ref, downg_ref, hidden_ref, grad_ref, gain_ref, chance_ref, *rest):
        sources, rest = rest[: len(lazy)], rest[len(lazy) :]
        (dh_hbm, down_out, gate_out1, up_out1, down_out1, dots_ref, dxn2_ref, dhidden_ref, outg_ref, qkvg_ref, bias_ref, dxn1_ref), scratch = rest[:12], rest[12:]
        scratch, split = list(scratch), []
        for one in sets:
            split.append(scratch[: len(one)])
            scratch = scratch[len(one) :]
        sums, dh_own, dh_all, part_ref, dqkv_ref, dq_acc, dk_acc, dv_acc, keep_sem = split[0]
        *targets, load = split[1]
        send_ref, router_ref, wout_ref, wqkv_ref, q_ref, k_ref, v_ref, att_ref, lse_ref, shared_ref = targets
        loads = [
            pltpu.make_async_copy(source, target, load.at[index])
            for index, (source, target) in enumerate(zip(sources, targets))
        ]
        spot = Spot()
        first = Sum(spot, send_ref, sums, split[2])
        share = Share(spot, dh_own, dh_all, split[3])
        second = Sum(spot, part_ref, dxn1_ref, split[4])
        items = [
            down_item(downg_ref, 0, 0, down_out, parts),
            up_item(upg_ref, 1, 1, gate_out1, up_out1, block, parts),
            down_item(downg_ref, 1, 1, down_out1, parts),
        ]
        back = Return(spot, items, split[5][:3], split[5][3:6], split[5][6:])
        keep = pltpu.make_async_copy(dh_all, dh_hbm, keep_sem)

        def owner():
            lane = lax.broadcasted_iota(jnp.int32, (rows, 128), 1)
            dots = sums[:, width:]
            dots_ref[...] = dots
            chance = chance_ref[:, :128]
            dprob = dots * chance_ref[:, 128:]
            prob = jnp.where(lane < experts, chance, 0.0)
            dlogit = prob * (dprob - jnp.sum(prob * dprob, -1, keepdims=True))
            mix = jnp.where(lane < experts, dlogit, jnp.where(lane == experts, chance * (1.0 - chance) * dots, 0.0))
            dxn2_ref[...] = jnp.dot(mix, router_ref[...], precision=PRECISE, preferred_element_type=f32)

            def one(index, carry):
                at = pl.ds(pl.multiple_of(index * 16, 16), 16)
                dxn2 = dxn2_ref[at, :] + sums[at, :width]
                dxn2_ref[at, :] = dxn2
                value = hidden_ref[at, :]
                inverse = lax.rsqrt(jnp.mean(value * value, -1, keepdims=True) + EPSILON)
                normed = value * inverse
                scaled = dxn2 * gain_ref[...]
                dhidden = grad_ref[at, :].astype(f32) + inverse * (scaled - normed * jnp.mean(scaled * normed, -1, keepdims=True))
                dhidden_ref[at, :] = dhidden
                dh_own[at, :] = dhidden.astype(bf16)
                return carry

            lax.fori_loop(0, rows // 16, one, 0)

        def attend(index, carry):
            start = pl.multiple_of(index * step, step)
            at = pl.ds(start, step)
            datt = dot_nt(dh_all[at, :], wout_ref[...]).astype(bf16)
            delta = jnp.sum(datt.astype(f32) * att_ref[at, :].astype(f32), -1, keepdims=True)
            scores = dot_nt(q_ref[at, :], k_ref[...]) * scale
            query_index = start + lax.broadcasted_iota(jnp.int32, scores.shape, 0)
            allowed = lax.broadcasted_iota(jnp.int32, scores.shape, 1) <= query_index
            prob = jnp.where(allowed, jnp.exp(scores - lse_ref[at, :1]), 0.0)
            dscore = (prob * (dot_nt(datt, v_ref[...]) - delta)).astype(bf16)
            dq_acc[at, :] = jnp.dot(dscore, k_ref[...], preferred_element_type=f32) * scale
            dk_acc[...] += dot_tn(dscore, q_ref[at, :])
            dv_acc[...] += dot_tn(prob.astype(bf16), datt)
            return carry

        def project(index, carry):
            at = pl.ds(pl.multiple_of(index * step, step), step)
            cosine, sine_part = turn_tables(shared_ref[at, width:])
            dq, dk, dv = dq_acc[at, :], dk_acc[at, :] * scale, dv_acc[at, :]
            dq = dq * cosine - pltpu.roll(dq, HEAD_DIM // 2, 1) * sine_part
            dk = dk * cosine - pltpu.roll(dk, HEAD_DIM // 2, 1) * sine_part
            for which, value in enumerate((dq, dk, dv)):
                bias_ref[:, pl.ds(which * HEAD_DIM, HEAD_DIM)] += jnp.sum(value, 0, keepdims=True)
                dqkv_ref[at, pl.ds(which * HEAD_DIM, HEAD_DIM)] = value.astype(bf16)
            part_ref[at, :] = dot_nt(dqkv_ref[at, :], wqkv_ref[...]).astype(bf16)
            return carry

        def features(index, carry):
            at = pl.ds(pl.multiple_of(index * step, step), step)
            qkvg_ref[at, :] = dot_tn(shared_ref[:, at], dqkv_ref[...]).astype(bf16)
            outg_ref[:, at] = dot_tn(att_ref[...], dh_all[:, at]).astype(bf16)
            return carry

        for copy in loads:
            copy.start()
        spot.greet(True, True)
        loads[0].wait()
        first.begin()
        for number in range(3):
            back.start(number)
        dk_acc[...] = jnp.zeros_like(dk_acc)
        dv_acc[...] = jnp.zeros_like(dv_acc)
        bias_ref[...] = jnp.zeros_like(bias_ref)
        for index in range(parts):
            first.cross(index)
        back.reduce(0, 0)
        back.reduce(0, 1)
        for index in range(parts):
            first.line(index)
        for copy in loads[1:]:
            copy.wait()
        owner()
        share.begin()
        share.step(1)
        share.step(2)
        back.reduce(0, 2)
        share.step(3)
        back.reduce(0, 3)
        back.reduce(1, 0)
        share.end()
        keep.start()
        back.reduce(1, 1)
        back.reduce(1, 2)
        back.reduce(2, 0)
        back.reduce(2, 1)
        back.reduce(2, 2)
        lax.fori_loop(0, length // step, attend, 0)
        lax.fori_loop(0, length // step, project, 0)
        second.begin()
        back.reduce(1, 3)
        for index in range(parts):
            second.cross(index)
        lax.fori_loop(0, width // step, features, 0)
        for index in range(parts):
            second.line(index)
        back.reduce(2, 3)
        first.end()
        second.end()
        back.end()
        keep.wait()

    piece = jax.ShapeDtypeStruct((block, units), bf16)
    return comm_call(
        kernel,
        number,
        "attention_last",
        [
            jax.ShapeDtypeStruct((length, width), bf16),
            jax.ShapeDtypeStruct((units, lanes), bf16),
            piece,
            piece,
            jax.ShapeDtypeStruct((units, lanes), bf16),
            jax.ShapeDtypeStruct((rows, 128), f32),
            jax.ShapeDtypeStruct((rows, width), f32),
            jax.ShapeDtypeStruct((rows, width), f32),
            jax.ShapeDtypeStruct((HEAD_DIM, width), bf16),
            jax.ShapeDtypeStruct((width, 3 * HEAD_DIM), bf16),
            jax.ShapeDtypeStruct((1, 3 * HEAD_DIM), f32),
            jax.ShapeDtypeStruct((rows, width), f32),
        ],
        [IN_PLACE] * 5 + [IN_VMEM] * 7,
        [IN_PLACE] * 2 + [IN_VMEM] * 4 + [IN_PLACE] * len(lazy),
        [one for group in sets for one in group],
        250_000_000,
    )(up_grads, down_grads, hidden, grad, gain, chances, *lazy)


class Group:
    def __init__(self, spot, own, out, sems):
        self.spot, self.own, self.out = spot, own, out
        self.local_sem, self.across_s, self.across_r, self.beside_s, self.beside_r = sems

    @staticmethod
    def sems():
        return [DMA, DMA, DMA, DMA((2,)), DMA((2,))]

    def block(self, column):
        rows = self.own.shape[0]
        return rows_at(self.out, column * rows, rows)

    def to_across(self):
        s = self.spot
        return remote(self.own, self.block(s.group), self.across_s, self.across_r, {"experts": s.across})

    def to_beside(self, slot):
        s = self.spot
        column = s.across if slot else s.group
        source = self.block(column) if slot else self.own
        return remote(source, self.block(column), self.beside_s.at[slot], self.beside_r.at[slot], {"experts": s.beside})

    def local(self):
        return pltpu.make_async_copy(self.own, self.block(self.spot.group), self.local_sem)

    def begin(self):
        self.to_across().start()
        self.to_beside(0).start()
        self.local().start()

    def end(self):
        self.to_across().wait_recv()
        self.to_beside(1).start()
        self.local().wait()
        self.to_across().wait_send()
        for slot in range(2):
            self.to_beside(slot).wait()


class Total:
    def __init__(self, spot, value, out, scratch):
        self.out = out
        self.sent, self.got, self.send_s, self.recv_s = scratch
        place = spot.place
        self.turns = [
            spot.twin,
            {"context": place + 1 - 2 * lax.rem(place, 2)},
            {"context": lax.rem(place + 2, spot.parts)},
            {"experts": spot.beside},
            {"experts": spot.across},
        ]
        self.value = value

    @staticmethod
    def scratch(shape):
        buf = pltpu.VMEM((5,) + shape, jnp.float32)
        return [buf, buf, DMA((5,)), DMA((5,))]

    def copy(self, index):
        return remote(self.sent.at[index], self.got.at[index], self.send_s.at[index], self.recv_s.at[index], self.turns[index])

    def begin(self):
        self.out[...] = self.value[...]
        self.send(0)

    def send(self, index):
        self.sent[index] = self.out[...]
        self.copy(index).start()

    def take(self, index):
        self.copy(index).wait()
        self.out[...] = self.out[...] + self.got[index]


def last_exchange(out_grads, qkv_grads, both, cotangents, dup, act, branch, hidden, tokens_grad, small, number):
    parts = lax.axis_size("context")
    rows, width = hidden.shape
    block = lanes = width // (2 * parts)
    units = WINDOW * parts - 128
    head, span = out_grads.shape[0], qkv_grads.shape[1]
    shapes = [(head, lanes), (block, span), (block, 2 * WINDOW), (WINDOW, lanes)]
    pieces = [1, 3, 2, 1]
    count, bf16 = len(shapes), jnp.bfloat16
    groups = [
        Return.scratch(shapes, pieces, parts),
        Sum.scratch(parts, rows, width) + [pltpu.VMEM((rows, width), jnp.float32), pltpu.VMEM((rows, width), bf16)],
        Total.scratch(small.shape),
        Group.sems(),
        Group.sems(),
        Grads.scratch() + [pltpu.VMEM(one.shape, bf16) for one in (both, cotangents, dup, act, branch)] + [DMA((5,))],
    ]
    piece, column = jax.ShapeDtypeStruct((block, units), bf16), jax.ShapeDtypeStruct((units, lanes), bf16)
    out_shape = [jax.ShapeDtypeStruct((parts * head, lanes), bf16), jax.ShapeDtypeStruct((3, block, parts * HEAD_DIM), bf16)]
    out_shape += [piece, piece, column]
    out_shape += [
        jax.ShapeDtypeStruct((width, 2 * WINDOW), bf16),
        jax.ShapeDtypeStruct((WINDOW, width), bf16),
        jax.ShapeDtypeStruct((4 * rows, width), bf16),
        jax.ShapeDtypeStruct((4 * rows, width), jnp.float32),
        jax.ShapeDtypeStruct(small.shape, jnp.float32),
    ]

    def kernel(outg_ref, qkvg_ref, both_hbm, cots_hbm, dup_hbm, act_hbm, branch_hbm, hidden_ref, tokens_ref, small_ref, *rest):
        outs, scratch = rest[: len(out_shape)], list(rest[len(out_shape) :])
        sets = []
        for one in groups:
            sets.append(scratch[: len(one)])
            scratch = scratch[len(one) :]
        grads, (upg2_hbm, downg2_hbm, block_all, tokens_all, small_out) = outs[:-5], outs[-5:]
        *grad_refs, both_ref, cots_ref, dup_ref, act_ref, branch_ref, load = sets[5]
        loads = [
            pltpu.make_async_copy(source, target, load.at[index])
            for index, (source, target) in enumerate(
                ((both_hbm, both_ref), (cots_hbm, cots_ref), (dup_hbm, dup_ref), (act_hbm, act_ref), (branch_hbm, branch_ref))
            )
        ]
        items = [
            {
                "block": lambda side, part: lanes_at(outg_ref, (side * parts + part) * lanes, lanes),
                "pieces": [(lambda buf, short: buf, lambda source, short: rows_at(grads[0], source * head, head))],
            },
            {
                "block": lambda side, part: rows_at(qkvg_ref, (side * parts + part) * block, block),
                "pieces": [
                    (
                        lambda buf, short, which=which: buf.at[:, pl.ds(which * HEAD_DIM, HEAD_DIM)],
                        lambda source, short, which=which: lanes_at(grads[1].at[which], source * HEAD_DIM, HEAD_DIM),
                    )
                    for which in range(3)
                ],
            },
        ]
        items += [
            up_item(upg2_hbm, 0, 2, grads[2], grads[3], block, parts),
            down_item(downg2_hbm, 0, 2, grads[4], parts),
        ]
        spot = Spot()
        back = Return(spot, items, sets[0][:count], sets[0][count : 2 * count], sets[0][2 * count :])
        total_branch, own_block = sets[1][-2:]
        summed = Sum(spot, branch_ref, total_branch, sets[1][:-2])
        total = Total(spot, small_ref, small_out, sets[2])
        tokens_group = Group(spot, tokens_ref, tokens_all, sets[3])
        block_group = Group(spot, own_block, block_all, sets[4])
        loads[4].start()
        spot.greet(True, True)
        total.begin()
        for item in range(2):
            back.start(item)
        loads[4].wait()
        summed.begin()
        for copy in loads[:4]:
            copy.start()
        total.take(0)
        total.send(1)
        for index in range(parts):
            summed.cross(index)
        total.take(1)
        total.send(2)
        for index in range(parts):
            back.reduce(0, index)
        total.take(2)
        total.send(3)
        for index in range(parts):
            back.reduce(1, index)
        total.take(3)
        total.send(4)
        for copy in loads[:4]:
            copy.wait()
        Grads(both_ref, cots_ref, dup_ref, act_ref, upg2_hbm, downg2_hbm, *grad_refs).run()
        back.start(2)
        back.start(3)
        total.take(4)
        tokens_group.begin()
        for index in range(parts):
            summed.line(index)
        half = width // 2

        def finish(at, start, step):
            value = (hidden_ref[at, :] + total_branch[at, :]).astype(bf16)
            turned = lax.axis_index("dp") == 0

            @pl.when(turned)
            def _():
                own_block[at, :] = value

            @pl.when(jnp.logical_not(turned))
            def _():
                own_block[at, :half] = value[:, half:]
                own_block[at, half:] = value[:, :half]

        summed.chunks(finish)
        block_group.begin()
        for item in range(2, count):
            for index in range(parts):
                back.reduce(item, index)
        summed.end()
        tokens_group.end()
        block_group.end()
        back.end()

    return comm_call(
        kernel,
        number,
        "last_exchange",
        out_shape,
        [IN_PLACE] * (len(out_shape) - 1) + [IN_VMEM],
        [IN_PLACE] * 7 + [IN_VMEM] * 3,
        [one for group in groups for one in group],
        300_000_000,
    )(out_grads, qkv_grads, both, cotangents, dup, act, branch, hidden, tokens_grad, small)


def widen(singles, pairs):
    steps = 8

    def spec(shape):
        if len(shape) == 3:
            return pl.BlockSpec((shape[0], shape[1] // steps, shape[2]), lambda i: (0, i, 0))
        return pl.BlockSpec((shape[0] // steps, shape[1]), lambda i: (i, 0))

    kinds = [jnp.bfloat16 if keep else jnp.float32 for _, keep in singles]
    arrays = [array for array, _ in singles] + [one for pair in pairs for one in pair]
    out_shape = [jax.ShapeDtypeStruct(array.shape, kind) for (array, _), kind in zip(singles, kinds)]
    out_shape += [jax.ShapeDtypeStruct((2,) + pair[0].shape, jnp.float32) for pair in pairs]
    count = len(singles)

    def kernel(*refs):
        sources, targets = refs[: len(arrays)], refs[len(arrays) :]
        for source, target in zip(sources[:count], targets[:count]):
            target[...] = source[...].astype(target.dtype)
        for index, target in enumerate(targets[count:]):
            for which in range(2):
                target[which] = sources[count + 2 * index + which][...].astype(jnp.float32)

    return pl.pallas_call(
        kernel,
        grid=(steps,),
        in_specs=[spec(array.shape) for array in arrays],
        out_specs=[spec(one.shape) for one in out_shape],
        out_shape=out_shape,
        name="widen",
    )(*arrays)


def split_body(
    tokens,
    positions,
    routes,
    out_grad,
    norm1_gain,
    qkv_weight,
    qkv_bias,
    out_weight,
    norm2_gain,
    router_weight,
    expert_gate,
    expert_up,
    expert_down,
    shared_gate,
    shared_w_gate,
    shared_w_up,
    shared_w_down,
):
    rows, width = tokens.shape[1], tokens.shape[2]
    parts = lax.axis_size("context")
    group_size = lax.axis_size("experts")
    place, group = lax.axis_index("context"), lax.axis_index("experts")
    local_experts = expert_gate.shape[0]
    expert_count = local_experts * group_size
    own_rows = rows // group_size
    length = rows * parts
    half = width // 2
    block = width // (2 * parts)
    hidden_here = shared_w_gate.shape[1] // parts
    stacks = local_experts + 1
    scale = HEAD_DIM ** (-0.5)
    bf16 = jnp.bfloat16

    first = group * own_rows

    def own_of(array):
        return lax.dynamic_slice_in_dim(array, first, own_rows, 0)

    grad_own_b = own_half_first(own_of(out_grad[0]))
    grad_own = grad_own_b.astype(jnp.float32)
    gain1 = own_half_first(norm1_gain).astype(jnp.float32)
    gain2 = own_half_first(norm2_gain).astype(jnp.float32)
    token_own = own_half_first(own_of(tokens[0])).astype(jnp.float32)
    inverse1 = lax.rsqrt(jnp.mean(token_own * token_own, -1, keepdims=True) + EPSILON)
    normed1 = token_own * inverse1
    half_dim = HEAD_DIM // 2
    frequency = ROPE_BASE ** (-2.0 * jnp.arange(half_dim, dtype=jnp.float32) / HEAD_DIM)
    angles = own_of(positions[0]).astype(jnp.float32)[:, None] * frequency[None, :]
    turns = jnp.concatenate([jnp.cos(angles), jnp.sin(angles)], 1)
    turns_high = turns.astype(bf16)
    turns_low = (turns - turns_high.astype(jnp.float32)).astype(bf16)
    send1 = jnp.concatenate([(normed1 * gain1).astype(bf16), turns_high, turns_low], 1)
    qkv_in = jnp.transpose(qkv_weight, (1, 0, 2))
    bias_here = lax.dynamic_slice_in_dim(
        qkv_bias.reshape(3, parts, HEAD_DIM), place, 1, 1
    ).reshape(1, 3 * HEAD_DIM)
    shared1, grad_all, qkv_w, out_w, down_w, query, key, value, attended, lse, head_sum = attention_first(
        send1, grad_own_b, qkv_in, out_weight, bias_here.astype(jnp.float32), shared_w_down, expert_down, 1
    )
    hidden = token_own + head_sum
    inverse2 = lax.rsqrt(jnp.mean(hidden * hidden, -1, keepdims=True) + EPSILON)
    normed2 = hidden * inverse2
    xn2_own = (normed2 * gain2).astype(bf16)
    router_here = own_half_first(router_weight.T).T
    gate_here = own_half_first(shared_gate)
    heads_w = jnp.concatenate([router_here, gate_here[:, None]], 1)
    logits = dot_nn(xn2_own, heads_w)
    prob = jax.nn.softmax(logits[:, :expert_count], -1)
    sig_own = jax.nn.sigmoid(logits[:, expert_count])
    named = jnp.sum(
        (
            own_of(routes[0])[:, :, None] == jnp.arange(expert_count, dtype=jnp.int32)[None, None, :]
        ).astype(jnp.float32),
        1,
    )
    gates = jnp.pad(
        jnp.concatenate([prob * named, sig_own[:, None]], 1), ((0, 0), (0, 63 - expert_count))
    )
    gates_high = gates.astype(bf16)
    gates_low = (gates - gates_high.astype(jnp.float32)).astype(bf16)
    send3 = jnp.concatenate([xn2_own, gates_high, gates_low], 1)

    both, send4, branch_part, dup, act_c, up_g, down_g, *first_grads = share_move_compute(
        send3, grad_all, shared_w_gate, shared_w_up, expert_gate, expert_up, down_w, 3
    )
    up_grads, down_grads = [None] * (2 * stacks), [None] * stacks
    up_grads[:2] = first_grads
    side = 128 - expert_count - 1
    blank = jnp.zeros((own_rows, side), jnp.float32)
    chances = jnp.concatenate([prob, sig_own[:, None], blank, named, blank, blank[:, :1]], 1)
    router_wide = jnp.pad(heads_w.T.astype(jnp.float32), ((0, side), (0, 0)))
    (
        _,
        down_grads[0],
        up_grads[2],
        up_grads[3],
        down_grads[1],
        dots_own,
        dxn2,
        dhidden,
        out_g,
        qkv_g,
        bias_part,
        dxn1,
    ) = attention_last(
        send4,
        up_g,
        down_g,
        hidden,
        grad_own_b,
        gain2[None, :],
        chances,
        router_wide,
        out_w,
        qkv_w,
        (query, key, value, attended),
        lse,
        shared1,
        4,
    )

    dprob = dots_own[:, :expert_count] * named
    dlogit = prob * (dprob - jnp.sum(prob * dprob, -1, keepdims=True))
    coef = sig_own * (1.0 - sig_own) * dots_own[:, expert_count]
    xn2_float = xn2_own.astype(jnp.float32)
    router_grad = jnp.dot(xn2_float.T, dlogit, precision=PRECISE)
    shared_gate_grad = jnp.dot(coef, xn2_float, precision=PRECISE)
    norm2_grad = jnp.sum(dxn2 * normed2, 0)
    norm1_grad = jnp.sum(dxn1 * normed1, 0)
    dscaled1 = dxn1 * gain1
    tokens_grad_own = dhidden + inverse1 * (
        dscaled1 - normed1 * jnp.mean(dscaled1 * normed1, -1, keepdims=True)
    )

    bias_wide = jnp.zeros((group_size, parts, 3 * HEAD_DIM), jnp.float32)
    bias_wide = lax.dynamic_update_slice(bias_wide, bias_part[None], (group, place, 0))
    small = jnp.concatenate(
        [
            own_half_first(norm1_grad),
            own_half_first(norm2_grad),
            own_half_first(shared_gate_grad),
            own_half_first(router_grad.T).T.reshape(-1),
            bias_wide.reshape(-1),
        ]
    )
    (
        out_w_grad,
        qkv_grad,
        up_grads[4],
        up_grads[5],
        down_grads[2],
        _,
        _,
        block_out,
        tokens_grad,
        small,
    ) = last_exchange(
        out_g,
        qkv_g,
        both,
        grad_all,
        dup,
        act_c,
        branch_part,
        hidden,
        own_half_first(tokens_grad_own),
        small.reshape(-1, 128),
        7,
    )
    small = small.reshape(-1)
    router_size = width * expert_count
    bias_sum = small[3 * width + router_size :].reshape(group_size, parts, 3, HEAD_DIM)
    bias_grad = jnp.transpose(
        lax.dynamic_slice_in_dim(bias_sum, group, 1, 0)[0], (1, 0, 2)
    ).reshape(3, parts * HEAD_DIM)

    singles = [(block_out, True), (tokens_grad, False), (out_w_grad, False), (qkv_grad, False)]
    singles += [(up_grads[0], False), (up_grads[1], False), (down_grads[0], False)]
    pairs = [up_grads[2::2], up_grads[3::2], down_grads[1:]]
    block_out, tokens_grad, out_w_grad, qkv_grad, *shared_grads, gate_grads, up_grads, down_grads = widen(singles, pairs)

    return (
        block_out[None],
        tokens_grad[None],
        small[:width],
        jnp.transpose(qkv_grad, (1, 0, 2)),
        bias_grad,
        out_w_grad,
        small[width : 2 * width],
        small[3 * width : 3 * width + router_size].reshape(width, expert_count),
        gate_grads,
        up_grads,
        down_grads,
        small[2 * width : 3 * width],
        *shared_grads,
    )


def plan_of(mesh):
    sizes = mesh.shape
    return split_body if (sizes["dp"], sizes["context"], sizes["experts"]) == (2, 4, 4) else general_body


def solution(mesh):
    return jax.shard_map(
        plan_of(mesh),
        mesh=mesh,
        in_specs=(
            P("dp", "context", None),
            P("dp", "context"),
            P("dp", "context", None),
            P("dp", "context", None),
            P(),
            P(("dp", "context"), None, "experts"),
            P(None, "experts"),
            P("experts", ("dp", "context")),
            P(),
            P(),
            P("experts", ("dp", "context"), None),
            P("experts", ("dp", "context"), None),
            P("experts", None, ("dp", "context")),
            P(),
            P(("dp", "context"), "experts"),
            P(("dp", "context"), "experts"),
            P("experts", ("dp", "context")),
        ),
        out_specs=(
            P("dp", "context", None),
            P("dp", "context", None),
            P(),
            P(("dp", "context"), None, "experts"),
            P(None, "experts"),
            P("experts", ("dp", "context")),
            P(),
            P(),
            P("experts", ("dp", "context"), None),
            P("experts", ("dp", "context"), None),
            P("experts", None, ("dp", "context")),
            P(),
            P(("dp", "context"), "experts"),
            P(("dp", "context"), "experts"),
            P("experts", ("dp", "context")),
        ),
        check_vma=False,
    )
```
